256 devices in a mesh: fsdp: 32 (over z, y), model: 8 (over x, core).
Axes of the slice: x: 4, y: 4, z: 8, core: 2. Of those that a mesh axis runs over, the one named last changes fastest.
Arguments:
- x_in: bfloat16 [32, 512, 3072], P('fsdp', 'model')
- dy_in: bfloat16 [32, 512, 3072], P('fsdp', 'model')
- norm_gain: float32 [3072], replicated
- w_qkv: bfloat16 [3072, 5120], P('fsdp', 'model')
- w_out: bfloat16 [3072, 3072], P('model', 'fsdp')
- w_gate: bfloat16 [3072, 8192], P('fsdp', 'model')
- w_up: bfloat16 [3072, 8192], P('fsdp', 'model')
- w_down: bfloat16 [8192, 3072], P('model', 'fsdp')
- rope_cos: float32 [512, 64], replicated
- rope_sin: float32 [512, 64], replicated
Outputs:
- output 1: bfloat16 [32, 512, 3072], P('fsdp', 'model')
- output 2: bfloat16 [32, 512, 3072], P('fsdp', 'model')
- output 3: float32 [3072, 5120], P('fsdp', 'model')
- output 4: float32 [3072, 3072], P('model', 'fsdp')
- output 5: float32 [3072, 8192], P('fsdp', 'model')
- output 6: float32 [3072, 8192], P('fsdp', 'model')
- output 7: float32 [8192, 3072], P('model', 'fsdp')
All inputs are finite; a program needn't handle non-finite values.
Results may differ from the reference program's by a relative error of at most 0.00904269.
Values are sent between devices in bfloat16 or wider.
A program may use at most 768 MiB of HBM per device.

```python
import math
import jax
import jax.numpy as jnp
from jax import lax

D = 3072
FF = 8192
HEADS = 24
KV_HEADS = 8
HEAD = 128
BATCH = 32
SEQ = 512
ROPE_THETA = 500000

NORM_EPS = 1e-5
GROUP_SIZE = HEADS // KV_HEADS
QKV_COLS = (HEADS + 2 * KV_HEADS) * HEAD


def rope_tables(key):
    pos_gaps = jax.random.randint(key, (SEQ,), 1, 4)
    positions = (jnp.cumsum(pos_gaps) - pos_gaps[0]).astype(jnp.float32)
    inv_freq = jnp.exp(jnp.arange(HEAD // 2, dtype=jnp.float32) * (-2.0 * math.log(ROPE_THETA) / HEAD))
    angles = positions[:, None] * inv_freq[None, :]
    return jnp.cos(angles), jnp.sin(angles)


def setup_inputs(seed: int = 0) -> dict:
    key_list = jax.random.split(jax.random.key(seed), 9)
    x_in = jax.random.normal(key_list[0], (BATCH, SEQ, D), jnp.float32)
    dy_in = jax.random.normal(key_list[1], (BATCH, SEQ, D), jnp.float32)
    norm_gain = jax.random.uniform(key_list[2], (D,), jnp.float32, 0.5, 1.5)
    w_qkv = jax.random.normal(key_list[3], (D, QKV_COLS), jnp.float32) * D ** -0.5
    w_out = jax.random.normal(key_list[4], (HEADS * HEAD, D), jnp.float32) * (HEADS * HEAD) ** -0.5
    w_gate = jax.random.normal(key_list[5], (D, FF), jnp.float32) * D ** -0.5
    w_up = jax.random.normal(key_list[6], (D, FF), jnp.float32) * D ** -0.5
    w_down = jax.random.normal(key_list[7], (FF, D), jnp.float32) * FF ** -0.5
    rope_cos, rope_sin = rope_tables(key_list[8])
    return {
        "x_in": x_in.astype(jnp.bfloat16),
        "dy_in": dy_in.astype(jnp.bfloat16),
        "norm_gain": norm_gain,
        "w_qkv": w_qkv.astype(jnp.bfloat16),
        "w_out": w_out.astype(jnp.bfloat16),
        "w_gate": w_gate.astype(jnp.bfloat16),
        "w_up": w_up.astype(jnp.bfloat16),
        "w_down": w_down.astype(jnp.bfloat16),
        "rope_cos": rope_cos,
        "rope_sin": rope_sin,
    }


def rotate(tensor, cos_tab, sin_tab):
    half_dim = HEAD // 2
    wide = tensor.astype(jnp.float32)
    lower_half = wide[..., :half_dim]
    upper_half = wide[..., half_dim:]
    return jnp.concatenate([lower_half * cos_tab - upper_half * sin_tab, upper_half * cos_tab + lower_half * sin_tab], axis=-1).astype(jnp.bfloat16)


def swiglu(gate_val, up_val):
    return (jax.nn.silu(gate_val.astype(jnp.float32)) * up_val.astype(jnp.float32)).astype(jnp.bfloat16)


def attention(qkv_seq, rope_cos, rope_sin):
    queries = rotate(qkv_seq[:, :, :GROUP_SIZE, :], rope_cos[:, None, None, :], rope_sin[:, None, None, :])
    key_rot = rotate(qkv_seq[:, :, GROUP_SIZE, :], rope_cos[:, None, :], rope_sin[:, None, :])
    values = qkv_seq[:, :, GROUP_SIZE + 1, :]
    scores = jnp.einsum("qkgh,pkh->kgqp", queries.astype(jnp.float32), key_rot.astype(jnp.float32)) * HEAD ** -0.5
    causal = jnp.arange(SEQ)[:, None] >= jnp.arange(SEQ)[None, :]
    attn_probs = jax.nn.softmax(jnp.where(causal, scores, -1e30), axis=-1).astype(jnp.bfloat16)
    attn_out = jnp.einsum("kgqp,pkh->qkgh", attn_probs.astype(jnp.float32), values.astype(jnp.float32))
    return attn_out.astype(jnp.bfloat16).reshape(SEQ, HEADS * HEAD)


def reference(x_in, dy_in, norm_gain, w_qkv, w_out, w_gate, w_up, w_down, rope_cos, rope_sin):
    tokens = BATCH * SEQ
    x_rows = x_in.reshape(tokens, D).astype(jnp.float32)
    dy_rows = dy_in.reshape(tokens, D)
    normed, norm_pull = jax.vjp(lambda row_vals: row_vals * lax.rsqrt(jnp.mean(row_vals * row_vals, axis=-1, keepdims=True) + NORM_EPS) * norm_gain, x_rows)
    h_val = normed.astype(jnp.bfloat16)
    qkv_seqs = jnp.dot(h_val, w_qkv, preferred_element_type=jnp.float32).astype(jnp.bfloat16).reshape(BATCH, SEQ, KV_HEADS, GROUP_SIZE + 2, HEAD)
    attn_fn = lambda packed: attention(packed, rope_cos, rope_sin)
    attn_val = lax.map(attn_fn, qkv_seqs).reshape(tokens, HEADS * HEAD)
    gate_val = jnp.dot(h_val, w_gate, preferred_element_type=jnp.float32).astype(jnp.bfloat16)
    up_val = jnp.dot(h_val, w_up, preferred_element_type=jnp.float32).astype(jnp.bfloat16)
    act_val, act_pull = jax.vjp(swiglu, gate_val, up_val)
    mix_sum = jnp.dot(attn_val, w_out, preferred_element_type=jnp.float32) + jnp.dot(act_val, w_down, preferred_element_type=jnp.float32)
    y_out = (x_rows + mix_sum).astype(jnp.bfloat16)
    d_attn = jnp.dot(dy_rows, w_out.T, preferred_element_type=jnp.float32).astype(jnp.bfloat16)
    d_act = jnp.dot(dy_rows, w_down.T, preferred_element_type=jnp.float32).astype(jnp.bfloat16)
    d_gate, d_up = act_pull(d_act)

    def seq_grad(seq_pair):
        seq_pull = jax.vjp(attn_fn, seq_pair[0])[1]
        return seq_pull(seq_pair[1])[0]

    d_qkv = lax.map(seq_grad, (qkv_seqs, d_attn.reshape(BATCH, SEQ, HEADS * HEAD))).reshape(tokens, QKV_COLS)
    d_h = (jnp.dot(d_qkv, w_qkv.T, preferred_element_type=jnp.float32) + jnp.dot(d_gate, w_gate.T, preferred_element_type=jnp.float32) + jnp.dot(d_up, w_up.T, preferred_element_type=jnp.float32)).astype(jnp.bfloat16)
    dx_rows = (dy_rows.astype(jnp.float32) + norm_pull(d_h.astype(jnp.float32))[0]).astype(jnp.bfloat16)
    return (
        y_out.reshape(BATCH, SEQ, D),
        dx_rows.reshape(BATCH, SEQ, D),
        jnp.dot(h_val.T, d_qkv, preferred_element_type=jnp.float32),
        jnp.dot(attn_val.T, dy_rows, preferred_element_type=jnp.float32),
        jnp.dot(h_val.T, d_gate, preferred_element_type=jnp.float32),
        jnp.dot(h_val.T, d_up, preferred_element_type=jnp.float32),
        jnp.dot(act_val.T, dy_rows, preferred_element_type=jnp.float32),
    )
```

```python
import functools
import heapq

import jax
import jax.numpy as jnp
from jax import lax
from jax.experimental import pallas as pl
from jax.experimental.pallas import tpu as pltpu
from jax.sharding import PartitionSpec as P

NORM_EPS = 1e-5
NY, NX, NC = 4, 4, 2
MESH = pl.DeviceIdType.MESH
LINK = 46.6e3
PAIR = 330e3
HOP = 3.5
ADD = 0.4
VMEM_LIMIT = 62 * 1024 * 1024


class Place:
    def __init__(self, nz):
        i, j = lax.axis_index("fsdp"), lax.axis_index("model")
        self.size = {"z": nz, "y": NY, "x": NX, "c": NC}
        self.at = {"z": lax.div(i, NY), "y": lax.rem(i, NY), "x": lax.div(j, NC), "c": lax.rem(j, NC)}

    def get(self, axis, step=0):
        n = self.size[axis]
        return lax.rem(self.at[axis] + (step + 2 * n) % n, n)

    def device(self, axis, step):
        at = dict(self.at)
        at[axis] = self.get(axis, step)
        return {"fsdp": at["z"] * NY + at["y"], "model": at["x"] * NC + at["c"]}

    def meet(self, peers):
        barrier = pltpu.get_barrier_semaphore()
        for axis, step in peers:
            pl.semaphore_signal(barrier, inc=1, device_id=self.device(axis, step), device_id_type=MESH)
        pl.semaphore_wait(barrier, len(peers))


class Flow:
    def __init__(self, place, send_sem, recv_sem, emit=True):
        self.place, self.send_sem, self.recv_sem, self.emit = place, send_sem, recv_sem, emit
        self.now, self.free, self.events, self.copies = 0.0, {}, [], []

    def send(self, axis, step, src, dst, size, then=None, link=None):
        k = len(self.copies)
        link = link or (axis, step)
        begin = max(self.now, self.free.get(link, 0.0))
        rate, lag = (PAIR, 1.5) if axis == "c" else (LINK, HOP)
        self.free[link] = begin + size / rate
        copy = None
        if self.emit:
            copy = pltpu.make_async_remote_copy(
                src_ref=src(),
                dst_ref=dst(),
                send_sem=self.send_sem.at[k],
                recv_sem=self.recv_sem.at[k],
                device_id=self.place.device(axis, step),
                device_id_type=MESH,
            )
            copy.start()
        self.copies.append(copy)
        heapq.heappush(self.events, (self.free[link] + lag, k, then))

    def run(self):
        while self.events:
            when, k, then = heapq.heappop(self.events)
            self.now = max(self.now, when)
            if self.emit:
                self.copies[k].wait_recv()
            if then is not None:
                then()
        if self.emit:
            for copy in self.copies:
                copy.wait_send()


def after(count, then):
    left = [count]

    def one():
        left[0] -= 1
        if left[0] == 0:
            then()

    return one


def nbytes(ref, lead):
    n = 1
    for d in ref.shape[lead:]:
        n *= d
    return n * jnp.dtype(ref.dtype).itemsize


def gather_kernel(nz, h_ref, dy_ref, w_ref, h_all, dy_all, w_all, send_sem, recv_sem, own_sem):
    place = Place(nz)
    y, x, c, z = place.get("y"), place.get("x"), place.get("c"), place.get("z")
    place.meet([("x", 1), ("x", -1), ("y", 1), ("y", -1), ("y", 2), ("z", 1), ("z", -1), ("c", 1)])
    flow = Flow(place, send_sem, recv_sem)
    own = [
        pltpu.make_async_copy(h_ref, h_all.at[y, x, c], own_sem.at[0]),
        pltpu.make_async_copy(dy_ref, dy_all.at[y, x, c], own_sem.at[1]),
        pltpu.make_async_copy(w_ref.at[y], w_all.at[0, z, y], own_sem.at[2]),
    ]
    for copy in own:
        copy.start()
    piece = nbytes(h_ref, 1)

    def spot(ref, dy, dx, half):
        return lambda: ref.at[place.get("y", dy), place.get("x", dx), c, half]

    def spread(axis, half, offset, src, got):
        def come(step, onward):
            def then():
                if onward:
                    flow.send(axis, -step, got.spot(axis, step, offset, half), got.spot(axis, step, offset, half), piece, lambda: got(axis, 2, offset, half))
                got(axis, step, offset, half)

            return then

        flow.send(axis, 1, src, got.spot(axis, 0, offset, half), piece, come(-1, half == 0))
        flow.send(axis, -1, src, got.spot(axis, 0, offset, half), piece, come(1, half == 1))

    class Got:
        def __init__(self, ref, first):
            self.ref, self.first, self.second = ref, first, "y" if first == "x" else "x"

        def spot(self, axis, step, offset, half):
            d = {axis: step, ("y" if axis == "x" else "x"): offset}
            return spot(self.ref, d["y"], d["x"], half)

        def __call__(self, axis, step, offset, half):
            here = self.spot(axis, step, offset, half)
            if axis == self.first:
                spread(self.second, half, step, here, self)
            flow.send("c", 1, here, here, piece)

    arrays = [(h_ref, Got(h_all, "x")), (dy_ref, Got(dy_all, "y"))]
    for ref, got in arrays:
        for half in (0, 1):
            spread(got.first, half, 0, lambda ref=ref, half=half: ref.at[half], got)

    size = nbytes(w_ref, 1)

    def w_spot(who, dz, dy):
        return lambda: w_all.at[who, place.get("z", dz), place.get("y", dy)]

    def ring(step, dy):
        def pair(dz):
            flow.send("c", 1, w_spot(0, dz, dy), w_spot(1, dz, dy), size)

        def hop(n):
            def then():
                if n < nz - 1:
                    flow.send("z", step, w_spot(0, -step * n, dy), w_spot(0, -step * n, dy), size, hop(n + 1))
                pair(-step * n)

            return then

        return hop(0)

    flow.send("y", -1, lambda: w_ref.at[place.get("y", -1)], w_spot(0, 0, 0), size, ring(1, 1))
    flow.send("y", 1, lambda: w_ref.at[place.get("y", 1)], w_spot(0, 0, 0), size, ring(-1, -1))
    flow.send("y", 2, lambda: w_ref.at[place.get("y", 2)], w_spot(0, 0, 0), size, ring(-1, 2), link=("y", 1))
    for ref, got in arrays:
        for half in (0, 1):
            src = lambda ref=ref, half=half: ref.at[half]
            spread(got.second, half, 0, src, got)
            flow.send("c", 1, src, got.spot(got.second, 0, 0, half), piece)
    own[2].wait()
    ring(1, 0)()
    flow.run()
    own[0].wait()
    own[1].wait()


def any_specs(n):
    return [pl.BlockSpec(memory_space=pl.ANY)] * n


def gather(nz, h, dy, w):
    half, rows, width = h.shape
    everywhere = (NY, NX, NC) + h.shape
    count = 60 + 64 + 3 + 4 * (nz - 1) + 4 * nz
    vmem = pl.BlockSpec(memory_space=pltpu.VMEM)
    return pl.pallas_call(
        functools.partial(gather_kernel, nz),
        out_shape=(
            jax.ShapeDtypeStruct(everywhere, h.dtype),
            jax.ShapeDtypeStruct(everywhere, dy.dtype),
            jax.ShapeDtypeStruct((NC, nz) + w.shape, w.dtype),
        ),
        in_specs=[vmem] * 3,
        out_specs=tuple(any_specs(3)),
        scratch_shapes=[pltpu.SemaphoreType.DMA((count,)), pltpu.SemaphoreType.DMA((count,)), pltpu.SemaphoreType.DMA((3,))],
        compiler_params=pltpu.CompilerParams(collective_id=0, has_side_effects=True),
        name="gather",
    )(h, dy, w)


def exchange(flow, place, src, dst, far):
    size = nbytes(src, 1)

    def to(step):
        return lambda: src.at[place.get("y", step)]

    def spot(step):
        return lambda: dst.at[place.get("y", step)]

    def onward(step, half):
        def then():
            flow.send("y", step, lambda: far.at[half], lambda: dst.at[place.get("y", -step), half], size // 2)

        return then

    flow.send("y", 1, lambda: src.at[place.get("y", 2), 0], lambda: far.at[0], size // 2, onward(1, 0))
    flow.send("y", -1, lambda: src.at[place.get("y", 2), 1], lambda: far.at[1], size // 2, onward(-1, 1))
    flow.send("y", 1, to(1), spot(0), size)
    flow.send("y", -1, to(-1), spot(0), size)


def first_exchange_kernel(nz, src, dst, far, send_sem, recv_sem, own_sem):
    place = Place(nz)
    y = place.get("y")
    place.meet([("y", 1), ("y", -1)])
    flow = Flow(place, send_sem, recv_sem)
    own = pltpu.make_async_copy(src.at[y], dst.at[y], own_sem)
    own.start()
    exchange(flow, place, src, dst, far)
    flow.run()
    own.wait()


def first_exchange(nz, src):
    vmem = pl.BlockSpec(memory_space=pltpu.VMEM)
    return pl.pallas_call(
        functools.partial(first_exchange_kernel, nz),
        out_shape=jax.ShapeDtypeStruct(src.shape, src.dtype),
        in_specs=[vmem],
        out_specs=pl.BlockSpec(memory_space=pl.ANY),
        scratch_shapes=[pltpu.VMEM(src.shape[1:], src.dtype), pltpu.SemaphoreType.DMA((6,)), pltpu.SemaphoreType.DMA((6,)), pltpu.SemaphoreType.DMA],
        compiler_params=pltpu.CompilerParams(collective_id=1, has_side_effects=True),
        name="exchange_in",
    )(src)


def second_exchange_kernel(nz, src, acts, dst, pair_dst, pair_acts, far, send_sem, recv_sem, own_sem):
    place = Place(nz)
    y, c = place.get("y"), place.get("c")
    other = place.get("c", 1)
    place.meet([("y", 1), ("y", -1), ("c", 1)])
    flow = Flow(place, send_sem, recv_sem)
    own = pltpu.make_async_copy(src.at[y], dst.at[y], own_sem)
    own.start()
    exchange(flow, place, src, dst, far)
    for q in range(NY):
        flow.send("c", 1, lambda q=q: acts.at[q, :, other], lambda q=q: pair_acts.at[q], nbytes(pair_acts, 1))
    flow.run()
    own.wait()
    tail = Flow(place, send_sem, recv_sem)
    tail.copies = [None] * len(flow.copies)
    count = len(flow.copies)
    for q in range(NY):
        for p in range(2):
            tail.send("c", 1, lambda q=q, p=p: dst.at[q, p, :, other], lambda q=q, p=p: pair_dst.at[q, p], nbytes(pair_dst, 2))
    tail.copies = tail.copies
    while tail.events:
        _, k, _ = heapq.heappop(tail.events)
        tail.copies[k].wait_recv()
    for copy in tail.copies[count:]:
        copy.wait_send()


def second_exchange(nz, src, acts):
    vmem = pl.BlockSpec(memory_space=pltpu.VMEM)
    count = 6 + NY + 2 * NY
    return pl.pallas_call(
        functools.partial(second_exchange_kernel, nz),
        out_shape=(
            jax.ShapeDtypeStruct(src.shape, src.dtype),
            jax.ShapeDtypeStruct(src.shape[:3] + src.shape[4:], src.dtype),
            jax.ShapeDtypeStruct(acts.shape[:2] + acts.shape[3:], acts.dtype),
        ),
        in_specs=[vmem, vmem],
        out_specs=tuple(any_specs(3)),
        scratch_shapes=[pltpu.VMEM(src.shape[1:], src.dtype), pltpu.SemaphoreType.DMA((count,)), pltpu.SemaphoreType.DMA((count,)), pltpu.SemaphoreType.DMA],
        compiler_params=pltpu.CompilerParams(collective_id=2, has_side_effects=True),
        name="exchange_out",
    )(src, acts)


class Stage:
    def __init__(self, buffers, sem, depth, order=None):
        self.buffers, self.sem, self.depth, self.order = buffers, sem, depth, order
        self.used, self.copies = [], []

    def fetch(self):
        k = len(self.copies)
        if k < len(self.order):
            copy = pltpu.make_async_copy(self.order[k](), self.buffers.at[k % self.depth], self.sem.at[k % self.depth])
            copy.start()
            self.copies.append(copy)

    def begin(self):
        for _ in range(self.depth):
            self.fetch()

    def take(self, src, use):
        k = len(self.used)
        self.used.append(src)
        if self.order is not None:
            self.copies[k].wait()
            use(self.buffers.at[k % self.depth])
            self.fetch()


def scatter_plan(nz, place, flow, take, refs, add):
    y_part, d_part, g_part, y_sum, d_sum, g_all, land, z_land, far = refs
    piece = nbytes(y_part, 3)

    def reduce_ring(axis, raw, take_local, slot, done):
        def turn(s, goal, half, step):
            def then():
                take_local(goal, half, lambda ref: add(slot(s), ref))
                flow.send(axis, step, slot(s), slot(s + 4), piece, final[half])

            return then

        def finish(half):
            def then():
                mine, other = (slot(5), slot(2)) if half == 0 else (slot(4), slot(3))
                add(mine, other)
                take_local(0, half, lambda ref: add(mine, ref))
                done(half, mine)

            return then

        final = [after(2, finish(0)), after(2, finish(1))]

        def start(goal, half):
            if (goal, half) == (2, 1):
                flow.send(axis, 1, raw(2, 1), slot(0), piece, turn(0, 1, 1, 1))
            if (goal, half) == (2, 0):
                flow.send(axis, -1, raw(2, 0), slot(1), piece, turn(1, -1, 0, -1))
            if (goal, half) == (1, 0):
                flow.send(axis, 1, raw(1, 0), slot(2), piece, final[0])
            if (goal, half) == (-1, 1):
                flow.send(axis, -1, raw(-1, 1), slot(3), piece, final[1])

        return start

    sets = (2, 1, -1, 0)

    def plane(n, part, out, first):
        second = "y" if first == "x" else "x"
        sums = {}

        def slot_of(s):
            return lambda i: (lambda: land.at[n, s, i])

        def direct(step, half):
            return sums[step, half]

        def take_sum(step, half, use):
            use(sums[step, half])

        waits = {}

        def last(half, ref):
            if flow.emit:
                out[half] = ref()[...]

        def ready(step, half):
            return (step, half) in sums

        held = []

        def take_second(step, half, use):
            if ready(step, half):
                use(sums[step, half])
            else:
                raise AssertionError("order")

        second_start = reduce_ring(second, direct, take_second, slot_of(4), last)

        def first_done(step):
            def done(half, ref):
                sums[step, half] = ref
                second_start(step, half)

            return done

        starts = []
        for s, other in enumerate(sets):

            def raw(step, half, other=other):
                d = {first: step, second: other}
                return lambda: part.at[place.get("y", d["y"]), place.get("x", d["x"]), half]

            def take_local(step, half, use, raw=raw):
                take(raw(step, half), use)

            starts.append(reduce_ring(first, raw, take_local, slot_of(s), first_done(other)))
        return starts

    y_starts = plane(0, y_part, y_sum, "y")
    d_starts = plane(1, d_part, d_sum, "x")

    size = nbytes(g_part, 2)

    def g_raw(dz, dy):
        return lambda: g_part.at[place.get("z", dz), place.get("y", dy)]

    def home(dy, ref):
        mine = lambda: g_all.at[place.get("y")]
        if dy == 0:
            flow.keep(ref, mine)
        elif dy == 2:
            for half, step in ((0, 1), (1, -1)):

                def onward(half=half, step=step):
                    flow.send("y", step, lambda: far.at[half], lambda: g_all.at[place.get("y", -step), half], size // 2)

                flow.send("y", step, lambda half=half: ref().at[half], lambda half=half: far.at[half], size // 2, onward)
        else:
            flow.send("y", dy, ref, mine, size)

    def ring(step, lane, dy):
        n = 0 if step == 1 else 1

        def spot(s):
            return lambda: z_land.at[n, s, lane]

        def hop(s):
            def then():
                take_g(g_raw(-step * (s + 2), dy), spot(s))
                if s < nz - 2:
                    flow.send("z", step, spot(s), spot(s + 1), size, hop(s + 1))
                else:
                    home(dy, spot(s))

            return then

        flow.send("z", step, g_raw(-step, dy), spot(0), size, hop(0))

    def take_g(src, ref):
        take(src, lambda got: add(ref, got), True)

    ring(1, 0, 2)
    ring(-1, 0, 1)
    ring(1, 1, 0)
    ring(-1, 1, -1)
    for one, two in zip(y_starts, d_starts):
        for start in (one, two):
            start(2, 1)
            start(2, 0)
            start(1, 0)
            start(-1, 1)
    flow.run()


def add_into(mine, other, chunk=96):
    a, b = mine(), other
    if callable(b):
        b = b()
    flat = a.shape[:-2]
    index = tuple([slice(None)] * len(flat))
    a[...] = a[...] + b[...]


def scatter_kernel(nz, depth, y_part, d_part, g_part, y_sum, d_sum, g_all, land, z_land, far, stage, g_stage, send_sem, recv_sem, stage_sem, g_stage_sem, own_sem):
    place = Place(nz)
    refs = (y_part, d_part, g_part, y_sum, d_sum, g_all, land, z_land, far)

    def trial(flow, stages):
        def keep(ref, mine):
            if flow.emit:
                flow.own = pltpu.make_async_copy(ref(), mine(), own_sem)
                flow.own.start()

        flow.keep = keep

        def take(src, use, grad=False):
            flow.now += ADD
            stages[int(grad)].take(src, use)

        def add(mine, other):
            if flow.emit:
                add_into(mine, other)

        scatter_plan(nz, place, flow, take, refs, add)

    dry = [Stage(None, None, depth), Stage(None, None, depth)]
    trial(Flow(place, None, None, emit=False), dry)
    wet = [Stage(stage, stage_sem, depth, dry[0].used), Stage(g_stage, g_stage_sem, depth, dry[1].used)]
    for one in wet:
        one.begin()
    place.meet([("x", 1), ("x", -1), ("y", 1), ("y", -1), ("z", 1), ("z", -1)])
    flow = Flow(place, send_sem, recv_sem)
    trial(flow, wet)
    flow.own.wait()


def scatter(nz, y_part, d_part, g_part):
    depth = 6
    piece = y_part.shape[2:]
    block = g_part.shape[2:]
    count = 2 * 5 * 6 + 4 * (nz - 1) + 2 + 4
    vmem = pl.BlockSpec(memory_space=pltpu.VMEM)
    f32 = jnp.float32
    dma = pltpu.SemaphoreType.DMA
    return pl.pallas_call(
        functools.partial(scatter_kernel, nz, depth),
        out_shape=(
            jax.ShapeDtypeStruct(piece, f32),
            jax.ShapeDtypeStruct(piece, f32),
            jax.ShapeDtypeStruct((NY,) + block, f32),
        ),
        in_specs=any_specs(3),
        out_specs=(vmem, vmem, pl.BlockSpec(memory_space=pl.ANY)),
        scratch_shapes=[
            pltpu.VMEM((2, 5, 6) + piece[1:], f32),
            pltpu.VMEM((2, nz - 1, 2) + block, f32),
            pltpu.VMEM(block, f32),
            pltpu.VMEM((depth,) + piece[1:], f32),
            pltpu.VMEM((depth,) + block, f32),
            dma((count,)),
            dma((count,)),
            dma((depth,)),
            dma((depth,)),
            dma,
        ],
        compiler_params=pltpu.CompilerParams(collective_id=3, has_side_effects=True, vmem_limit_bytes=VMEM_LIMIT),
        name="scatter",
    )(y_part, d_part, g_part)


def norm_fwd(row_vals, norm_gain):
    return row_vals * lax.rsqrt(jnp.mean(row_vals * row_vals, axis=-1, keepdims=True) + NORM_EPS) * norm_gain


def swiglu(gate_val, up_val):
    return (jax.nn.silu(gate_val.astype(jnp.float32)) * up_val.astype(jnp.float32)).astype(jnp.bfloat16)


def rotate(tensor, cos_tab, sin_tab):
    half_dim = tensor.shape[-1] // 2
    wide = tensor.astype(jnp.float32)
    lower_half = wide[..., :half_dim]
    upper_half = wide[..., half_dim:]
    return jnp.concatenate([lower_half * cos_tab - upper_half * sin_tab, upper_half * cos_tab + lower_half * sin_tab], axis=-1).astype(jnp.bfloat16)


def attention(heads, rope_cos, rope_sin):
    seq_len, head_dim = heads.shape[1:]
    queries = rotate(heads[:-2], rope_cos[None], rope_sin[None])
    key_rot = rotate(heads[-2], rope_cos, rope_sin)
    values = heads[-1]
    scores = jnp.einsum("gqh,ph->gqp", queries, key_rot, preferred_element_type=jnp.float32) * head_dim ** -0.5
    causal = jnp.arange(seq_len)[:, None] >= jnp.arange(seq_len)[None, :]
    attn_probs = jax.nn.softmax(jnp.where(causal, scores, -1e30), axis=-1).astype(jnp.bfloat16)
    return jnp.einsum("gqp,ph->gqh", attn_probs, values, preferred_element_type=jnp.float32).astype(jnp.bfloat16)


def mm(a, b, ca, cb):
    return lax.dot_general(a, b, (((ca,), (cb,)), ((), ())), preferred_element_type=jnp.float32)


def solution(mesh):
    act_spec = P("fsdp", "model", None)
    col_spec = P("fsdp", "model")
    row_spec = P("model", "fsdp")
    nz = mesh.shape["fsdp"] // NY

    def layer_body(x_in, dy_in, norm_gain, w_qkv, w_out, w_gate, w_up, w_down, rope_cos, rope_sin):
        bf16 = jnp.bfloat16
        _, rows, width = x_in.shape
        slab = w_qkv.shape[0]
        head = 2 * rope_cos.shape[1]
        group = w_out.shape[0] // head
        seq = rows * NX * NC
        ff = w_gate.shape[1] // NY
        y = lax.rem(lax.axis_index("fsdp"), NY)
        c = lax.rem(lax.axis_index("model"), NC)
        last = y == NY - 1

        x_rows = x_in[0].astype(jnp.float32)
        normed, norm_pull = jax.vjp(lambda row_vals: norm_fwd(row_vals, norm_gain), x_rows)
        h_loc = normed.astype(bf16).reshape(2, rows // 2, width)
        dy_loc = dy_in.reshape(2, rows // 2, width)
        q, k, v = w_qkv[:, : group * head], w_qkv[:, group * head : -head], w_qkv[:, -head:]
        out_t, down_t = w_out.T, w_down.T
        parts = []
        for i in range(NY):
            at = slice(i * head, (i + 1) * head)
            ffs = slice(i * ff, (i + 1) * ff)
            heads = [q[:, at], out_t[:, at]] if i < NY - 1 else [k, v]
            parts.append(jnp.concatenate(heads + [w_gate[:, ffs], w_up[:, ffs], down_t[:, ffs]], axis=1))
        w_loc = jnp.stack(parts)

        h_all, dy_all, w_all = gather(nz, h_loc, dy_loc, w_loc)
        tokens = NY * seq
        h_all = h_all.reshape(tokens, width)
        dy_all = dy_all.reshape(tokens, width)
        w_all = w_all.reshape(NC, nz * NY * slab, w_loc.shape[2])
        w_own, w_pair = w_all[0], w_all[1]
        s0, s1, s2, s3, s4 = head, 2 * head, 2 * head + ff, 2 * head + 2 * ff, 2 * head + 3 * ff

        z_h = mm(h_all, w_own[:, :s1], 1, 0)
        z_d = mm(dy_all, w_own[:, s0:s1], 1, 0)
        heads_in = jnp.concatenate([z_h[:, :s0], jnp.where(last, z_h[:, s0:], z_d)], axis=1).astype(bf16)
        gate_val = mm(h_all, w_own[:, s1:s2], 1, 0).astype(bf16)
        up_val = mm(h_all, w_own[:, s2:s3], 1, 0).astype(bf16)
        d_act = mm(dy_all, w_own[:, s3:s4], 1, 0).astype(bf16)
        act_val, act_pull = jax.vjp(swiglu, gate_val, up_val)
        d_gate, d_up = act_pull(d_act)
        acts = jnp.concatenate([d_gate, d_up, act_val], axis=1)

        got = first_exchange(nz, heads_in.reshape(NY, 2, seq // 2, s1)).reshape(NY, seq, s1)
        heads = jnp.concatenate([got[:group, :, :s0], got[group:, :, :s0], got[group:, :, s0:]], axis=0)
        attn_val, attn_pull = jax.vjp(lambda packed: attention(packed, rope_cos, rope_sin), heads)
        d_heads = attn_pull(got[:group, :, s0:])[0]
        back = jnp.concatenate(
            [jnp.concatenate([d_heads[:group], d_heads[group : group + 1]], axis=0), jnp.concatenate([attn_val, d_heads[group + 1 :]], axis=0)], axis=2
        )
        heads_out, pair_heads, pair_acts = second_exchange(
            nz, back.reshape(NY, 2, NX // 2, NC, rows, s1), acts.reshape(NY, NX, NC, rows, 3 * ff)
        )
        heads_out = heads_out.reshape(NY * NX, NC, rows, s1)

        def mine(array):
            return lax.dynamic_index_in_dim(array, c, 1, keepdims=False).reshape(tokens // NC, -1)

        own_heads = mine(heads_out)
        own_acts = mine(acts.reshape(NY * NX, NC, rows, 3 * ff))
        pair_heads = pair_heads.reshape(tokens // NC, s1)
        pair_acts = pair_acts.reshape(tokens // NC, 3 * ff)
        zero = jnp.zeros((), bf16)

        def for_y(heads_val, acts_val):
            return [jnp.where(last, zero, heads_val[:, s0:]), acts_val[:, 2 * ff :]]

        def for_d(heads_val, acts_val):
            return [heads_val[:, :s0], jnp.where(last, heads_val[:, s0:], zero), acts_val[:, : 2 * ff]]

        y_part = mm(
            jnp.concatenate(for_y(own_heads, own_acts) + for_y(pair_heads, pair_acts), axis=1),
            jnp.concatenate([w_own[:, s0:s1], w_own[:, s3:], w_pair[:, s0:s1], w_pair[:, s3:]], axis=1),
            1,
            1,
        )
        d_part = mm(
            jnp.concatenate(for_d(own_heads, own_acts) + for_d(pair_heads, pair_acts), axis=1),
            jnp.concatenate([w_own[:, :s3], w_pair[:, :s3]], axis=1),
            1,
            1,
        )
        heads_out = heads_out.reshape(tokens, s1)
        g_h = mm(h_all, jnp.concatenate([heads_out, acts[:, : 2 * ff]], axis=1), 0, 0)
        g_d = mm(dy_all, jnp.concatenate([heads_out[:, s0:], acts[:, 2 * ff :]], axis=1), 0, 0)
        g_part = jnp.concatenate([g_h[:, :s0], jnp.where(last, g_h[:, s0:s1], g_d[:, :s0]), g_h[:, s1:], g_d[:, s0:]], axis=1)

        half = (NY, NX, 2, rows // 2, width)
        y_sum, d_sum, g_sum = scatter(nz, y_part.reshape(half), d_part.reshape(half), g_part.reshape(nz, NY, 2, slab // 2, s4))
        y_sum = y_sum.reshape(rows, width)
        d_sum = d_sum.reshape(rows, width)
        g_sum = g_sum.reshape(NY, slab, s4)

        y_out = (x_rows + y_sum).astype(bf16)
        d_h = d_sum.astype(bf16)
        dx_out = (dy_in[0].astype(jnp.float32) + norm_pull(d_h.astype(jnp.float32))[0]).astype(bf16)

        def cols(lo, hi, n=NY):
            return jnp.concatenate([g_sum[i, :, lo:hi] for i in range(n)], axis=1)

        return (
            y_out[None],
            dx_out[None],
            jnp.concatenate([cols(0, s0), g_sum[NY - 1, :, s0:s1]], axis=1),
            cols(s0, s1, group).T,
            cols(s1, s2),
            cols(s2, s3),
            cols(s3, s4).T,
        )

    return jax.shard_map(
        layer_body,
        mesh=mesh,
        in_specs=(act_spec, act_spec, P(), col_spec, row_spec, col_spec, col_spec, row_spec, P(), P()),
        out_specs=(act_spec, act_spec, col_spec, row_spec, col_spec, col_spec, row_spec),
        check_vma=False,
    )
```

```python
import functools
import heapq

import jax
import jax.numpy as jnp
from jax import lax
from jax.experimental import pallas as pl
from jax.experimental.pallas import tpu as pltpu
from jax.sharding import PartitionSpec as P

NORM_EPS = 1e-5
NY, NX, NC = 4, 4, 2
MESH = pl.DeviceIdType.MESH
LINK = 46.6e3
PAIR = 330e3
HOP = 3.5
ADD = 0.4
VMEM_LIMIT = 62 * 1024 * 1024


class Place:
    def __init__(self, nz):
        i, j = lax.axis_index("fsdp"), lax.axis_index("model")
        self.size = {"z": nz, "y": NY, "x": NX, "c": NC}
        self.at = {"z": lax.div(i, NY), "y": lax.rem(i, NY), "x": lax.div(j, NC), "c": lax.rem(j, NC)}

    def get(self, axis, step=0):
        n = self.size[axis]
        return lax.rem(self.at[axis] + (step + 2 * n) % n, n)

    def device(self, axis, step):
        at = dict(self.at)
        at[axis] = self.get(axis, step)
        return {"fsdp": at["z"] * NY + at["y"], "model": at["x"] * NC + at["c"]}

    def meet(self, peers):
        barrier = pltpu.get_barrier_semaphore()
        for axis, step in peers:
            pl.semaphore_signal(barrier, inc=1, device_id=self.device(axis, step), device_id_type=MESH)
        pl.semaphore_wait(barrier, len(peers))


class Flow:
    def __init__(self, place, send_sem, recv_sem, emit=True):
        self.place, self.send_sem, self.recv_sem, self.emit = place, send_sem, recv_sem, emit
        self.now, self.free, self.events, self.copies, self.tasks = 0.0, {}, [], [], []
        self.sent = set()

    def send(self, axis, step, src, dst, size, then=None, link=None):
        k = len(self.copies)
        link = link or (axis, step)
        begin = max(self.now, self.free.get(link, 0.0))
        rate, lag = (PAIR, 1.5) if axis == "c" else (LINK, HOP)
        self.free[link] = begin + size / rate
        copy = None
        if self.emit:
            copy = pltpu.make_async_remote_copy(
                src_ref=src(),
                dst_ref=dst(),
                send_sem=self.send_sem.at[k],
                recv_sem=self.recv_sem.at[k],
                device_id=self.place.device(axis, step),
                device_id_type=MESH,
            )
            copy.start()
        self.copies.append(copy)
        heapq.heappush(self.events, (self.free[link] + lag, k, then))
        return k

    def poll(self):
        while self.events and self.events[0][0] <= self.now:
            self.take()

    def take(self):
        when, k, then = heapq.heappop(self.events)
        self.now = max(self.now, when)
        if self.emit:
            self.copies[k].wait_recv()
        if then is not None:
            then()

    def task(self, cost, do):
        self.tasks.append((cost, do))

    def work(self, cost, do):
        if self.emit:
            do()
        self.now += cost

    def wait_sent(self, k):
        if self.emit and k not in self.sent:
            self.copies[k].wait_send()
        self.sent.add(k)

    def run(self):
        while self.events or self.tasks:
            if self.tasks and (not self.events or self.events[0][0] > self.now):
                cost, do = self.tasks.pop(0)
                do()
                self.now += cost
            else:
                self.take()
        for k in range(len(self.copies)):
            self.wait_sent(k)


def after(count, then):
    left = [count]

    def one():
        left[0] -= 1
        if left[0] == 0:
            then()

    return one


def nbytes(ref, lead):
    n = 1
    for d in ref.shape[lead:]:
        n *= d
    return n * jnp.dtype(ref.dtype).itemsize


def gather_kernel(nz, h_ref, dy_ref, w_ref, h_all, dy_all, w_all, send_sem, recv_sem, own_sem):
    place = Place(nz)
    y, x, c, z = place.get("y"), place.get("x"), place.get("c"), place.get("z")
    place.meet([("x", 1), ("x", -1), ("y", 1), ("y", -1), ("y", 2), ("z", 1), ("z", -1), ("c", 1)])
    flow = Flow(place, send_sem, recv_sem)
    own = [
        pltpu.make_async_copy(h_ref, h_all.at[y, x, c], own_sem.at[0]),
        pltpu.make_async_copy(dy_ref, dy_all.at[y, x, c], own_sem.at[1]),
        pltpu.make_async_copy(w_ref.at[y], w_all.at[0, z, y], own_sem.at[2]),
    ]
    for copy in own:
        copy.start()
    piece = nbytes(h_ref, 1)

    def spot(ref, dy, dx, half):
        return lambda: ref.at[place.get("y", dy), place.get("x", dx), c, half]

    def spread(axis, half, offset, src, got):
        def come(step, onward):
            def then():
                if onward:
                    flow.send(axis, -step, got.spot(axis, step, offset, half), got.spot(axis, step, offset, half), piece, lambda: got(axis, 2, offset, half))
                got(axis, step, offset, half)

            return then

        flow.send(axis, 1, src, got.spot(axis, 0, offset, half), piece, come(-1, half == 0))
        flow.send(axis, -1, src, got.spot(axis, 0, offset, half), piece, come(1, half == 1))

    class Got:
        def __init__(self, ref, first):
            self.ref, self.first, self.second = ref, first, "y" if first == "x" else "x"

        def spot(self, axis, step, offset, half):
            d = {axis: step, ("y" if axis == "x" else "x"): offset}
            return spot(self.ref, d["y"], d["x"], half)

        def __call__(self, axis, step, offset, half):
            here = self.spot(axis, step, offset, half)
            if axis == self.first:
                spread(self.second, half, step, here, self)
            flow.send("c", 1, here, here, piece)

    size = nbytes(w_ref, 1)

    def w_spot(who, dz, dy):
        return lambda: w_all.at[who, place.get("z", dz), place.get("y", dy)]

    def ring(step, dy, src=None):
        def hop(n):
            def then():
                here = src if src and n == 0 else w_spot(0, -step * n, dy)
                if n < nz - 1:
                    flow.send("z", step, here, w_spot(0, -step * n, dy), size, hop(n + 1))
                flow.send("c", 1, here, w_spot(1, -step * n, dy), size)

            return then

        return hop(0)

    def w_at(dy):
        return lambda: w_ref.at[place.get("y", dy)]

    flow.send("y", -1, w_at(-1), w_spot(0, 0, 0), size, ring(1, 1))
    flow.send("y", 1, w_at(1), w_spot(0, 0, 0), size, ring(-1, -1))
    flow.send("y", 2, w_at(2), w_spot(0, 0, 0), size, ring(-1, 2), link=("y", 1))
    ring(1, 0, w_at(0))()
    arrays = [(h_ref, Got(h_all, "x")), (dy_ref, Got(dy_all, "y"))]
    for ref, got in arrays:
        for half in (0, 1):
            spread(got.first, half, 0, lambda ref=ref, half=half: ref.at[half], got)
    for ref, got in arrays:
        for half in (0, 1):
            src = lambda ref=ref, half=half: ref.at[half]
            spread(got.second, half, 0, src, got)
            flow.send("c", 1, src, got.spot(got.second, 0, 0, half), piece)
    flow.run()
    for copy in own:
        copy.wait()


def any_specs(n):
    return [pl.BlockSpec(memory_space=pl.ANY)] * n


def gather(nz, h, dy, w):
    half, rows, width = h.shape
    everywhere = (NY, NX, NC) + h.shape
    count = 60 + 64 + 3 + 4 * (nz - 1) + 4 * nz
    vmem = pl.BlockSpec(memory_space=pltpu.VMEM)
    return pl.pallas_call(
        functools.partial(gather_kernel, nz),
        out_shape=(
            jax.ShapeDtypeStruct(everywhere, h.dtype),
            jax.ShapeDtypeStruct(everywhere, dy.dtype),
            jax.ShapeDtypeStruct((NC, nz) + w.shape, w.dtype),
        ),
        in_specs=[vmem] * 3,
        out_specs=tuple(any_specs(3)),
        scratch_shapes=[pltpu.SemaphoreType.DMA((count,)), pltpu.SemaphoreType.DMA((count,)), pltpu.SemaphoreType.DMA((3,))],
        compiler_params=pltpu.CompilerParams(collective_id=0, has_side_effects=True),
        name="gather",
    )(h, dy, w)


def mm(a, b, ca, cb):
    return lax.dot_general(a, b, (((ca,), (cb,)), ((), ())), preferred_element_type=jnp.float32)


def exchange_start(flow, place, src, dst, far, step):
    size = nbytes(src, 1)

    def onward(way, half):
        def then():
            flow.send("y", way, lambda: far.at[half], lambda: dst.at[place.get("y", -way), half], size // 2)

        return then

    if step == 2:
        flow.send("y", 1, lambda: src.at[place.get("y", 2), 0], lambda: far.at[0], size // 2, onward(1, 0))
        flow.send("y", -1, lambda: src.at[place.get("y", 2), 1], lambda: far.at[1], size // 2, onward(-1, 1))
    else:
        flow.send("y", step, lambda: src.at[place.get("y", step)], lambda: dst.at[place.get("y")], size)


def middle_kernel(
    nz,
    h_all,
    dy_all,
    w_all,
    cos_ref,
    sin_ref,
    x_all,
    g_all,
    h_v,
    dy_v,
    w_v,
    z_in,
    z_got,
    z_back,
    z_out,
    far,
    far_back,
    acts,
    keys,
    vals,
    dk,
    dv,
    tile,
    tile_heads,
    load_sem,
    own_sem,
    tile_sem,
    send_sem,
    recv_sem,
):
    bf16 = jnp.bfloat16
    place = Place(nz)
    y, c = place.get("y"), place.get("c")
    last = y == NY - 1
    other = place.get("c", 1)
    head = keys.shape[1]
    pair = 2 * head
    seq = keys.shape[0]
    ff = acts.shape[-1] // 3
    lo = 2 * ff
    rows = acts.shape[4]
    heads = 3
    part = seq // 2

    order = (2, 1, -1, 0)
    loads = [
        pltpu.make_async_copy(w_all.at[0, :, lo : lo + pair], w_v.at[:, lo : lo + pair], load_sem.at[0]),
        pltpu.make_async_copy(w_all.at[0, :, :lo], w_v.at[:, :lo], load_sem.at[1]),
        pltpu.make_async_copy(w_all.at[0, :, lo + pair :], w_v.at[:, lo + pair :], load_sem.at[2]),
    ]

    def span(q, n):
        return pl.ds(pl.multiple_of(q * n, n), n)

    row_loads = []
    for n, step in enumerate(order):
        at = span(place.get("y", step), seq)
        row_loads.append([pltpu.make_async_copy(a.at[at], b.at[at], load_sem.at[3 + 2 * n + m]) for m, (a, b) in enumerate(((h_all, h_v), (dy_all, dy_v)))])
    loads[0].start()
    for n in range(NY):
        for copy in row_loads[n]:
            copy.start()
    loads[1].start()
    loads[2].start()

    place.meet([("y", 1), ("y", -1), ("c", 1)])
    flow = Flow(place, send_sem, recv_sem)

    loads[0].wait()
    for n, step in enumerate(order):
        for copy in row_loads[n]:
            copy.wait()
        q = place.get("y", step)
        for p in range(2):
            at = pl.ds(pl.multiple_of(q * seq + p * part, part), part)
            from_h = mm(h_v[at, :], w_v[:, lo : lo + pair], 1, 0)
            from_dy = mm(dy_v[at, :], w_v[:, lo + head : lo + pair], 1, 0)
            z_in[q, p, :, :head] = from_h[:, :head].astype(bf16)
            z_in[q, p, :, head:] = jnp.where(last, from_h[:, head:], from_dy).astype(bf16)
        flow.now += 2.3
        flow.poll()
        if step:
            exchange_start(flow, place, z_in, z_got, far, step)
    z_got[y] = z_in[y]
    loads[1].wait()
    loads[2].wait()

    def gated(q):
        @pl.loop(0, 2)
        def _(p):
            at = pl.ds(pl.multiple_of(q * seq + p * part, part), part)
            h_rows = h_v[at, :]
            gate = mm(h_rows, w_v[:, :ff], 1, 0).astype(bf16).astype(jnp.float32)
            up = mm(h_rows, w_v[:, ff:lo], 1, 0).astype(bf16).astype(jnp.float32)
            d_act = mm(dy_v[at, :], w_v[:, lo + pair :], 1, 0).astype(bf16).astype(jnp.float32)
            sig = jax.nn.sigmoid(gate)
            silu = gate * sig
            shape = (NX // 2, NC, rows, ff)
            acts[q, p, :, :, :, :ff] = (d_act * up * (sig + silu * (1.0 - sig))).astype(bf16).reshape(shape)
            acts[q, p, :, :, :, ff:lo] = (d_act * silu).astype(bf16).reshape(shape)
            acts[q, p, :, :, :, lo:] = (silu * up).astype(bf16).reshape(shape)

    for n in range(NY):
        gated(n)
        flow.now += 3.0
        flow.poll()
    own = [pltpu.make_async_copy(acts.at[:, :, :, c, :, :lo], x_all.at[0, :, :, :, :, :lo], own_sem.at[0])]
    own.append(pltpu.make_async_copy(acts.at[:, :, :, c, :, lo:], x_all.at[0, :, :, :, :, lo + pair :], own_sem.at[1]))
    for copy in own:
        copy.start()
    size = nbytes(acts, 0) // NC
    flow.send("c", 1, lambda: acts.at[:, :, :, other, :, :lo], lambda: x_all.at[1, :, :, :, :, :lo], size * 2 // 3)
    flow.send("c", 1, lambda: acts.at[:, :, :, other, :, lo:], lambda: x_all.at[1, :, :, :, :, lo + pair :], size // 3)
    first_two = set(range(len(flow.copies) - 2, len(flow.copies)))
    later = [event for event in flow.events if event[1] in first_two]
    flow.events = [event for event in flow.events if event[1] not in first_two]
    heapq.heapify(flow.events)
    while flow.events:
        flow.take()

    def turn(values, at, sign):
        wide = values.astype(jnp.float32)
        swapped = pltpu.roll(wide, head // 2, 1)
        return (wide * cos_ref[at, :] + sign * (swapped * sin_ref[at, :])).astype(bf16)

    halves = [pl.ds(p * part, part) for p in range(2)]
    for p in range(2):
        keys[halves[p], :] = turn(z_got[heads, p, :, :head], halves[p], 1.0)
        vals[halves[p], :] = z_got[heads, p, :, head:]
    dk[...] = jnp.zeros_like(dk)
    dv[...] = jnp.zeros_like(dv)
    scale = head**-0.5
    spread = (NX // 2, NC, rows, head)

    @pl.loop(0, heads)
    def _(i):
        for p in range(2):
            n = (p + 1) * part
            query = turn(z_got[i, p, :, :head], halves[p], 1.0)
            d_out = z_got[i, p, :, head:]
            scores = mm(query, keys[:n, :], 1, 1) * scale
            causal = lax.broadcasted_iota(jnp.int32, scores.shape, 0) + p * part >= lax.broadcasted_iota(jnp.int32, scores.shape, 1)
            scores = jnp.where(causal, scores, -1e30)
            grown = jnp.exp(scores - jnp.max(scores, axis=1, keepdims=True))
            probs = grown / jnp.sum(grown, axis=1, keepdims=True)
            probs_low = probs.astype(bf16)
            z_back[i, p, :, :, :, head:] = mm(probs_low, vals[:n, :], 1, 0).astype(bf16).reshape(spread)
            d_probs = mm(d_out, vals[:n, :], 1, 1).astype(bf16).astype(jnp.float32)
            d_scores = (probs * (d_probs - jnp.sum(probs * d_probs, axis=1, keepdims=True)) * scale).astype(bf16)
            z_back[i, p, :, :, :, :head] = turn(mm(d_scores, keys[:n, :], 1, 0).astype(bf16), halves[p], -1.0).reshape(spread)
            dk[:n, :] += mm(d_scores, query, 0, 0)
            dv[:n, :] += mm(probs_low, d_out, 0, 0)

    for p in range(2):
        z_back[heads, p, :, :, :, :head] = turn(dk[halves[p], :].astype(bf16), halves[p], -1.0).reshape(spread)
        z_back[heads, p, :, :, :, head:] = dv[halves[p], :].astype(bf16).reshape(spread)
    flow.now += 8.0
    for step in order[:3]:
        exchange_start(flow, place, z_back, z_out, far_back, step)
    tokens = NY * seq

    z_out[y] = z_back[y]
    block = h_v.shape[1] // nz

    def weight_grads(first, count):
        @pl.loop(first, first + count)
        def _(b):
            slot = lax.rem(b, 2)
            at = pl.ds(pl.multiple_of(b * block, block), block)

            @pl.when(b >= 2)
            def _():
                grads_copy(b, slot).wait()

            act = acts[...].reshape(tokens, 3 * ff)
            tile[slot, :, :lo] = mm(h_v[:, at], act[:, :lo], 0, 0)
            tile[slot, :, lo:] = mm(dy_v[:, at], act[:, lo:], 0, 0)
            for copy in grads_copies(b, slot):
                copy.start()

    def grads_copies(b, slot):
        at = pl.ds(pl.multiple_of(b * block, block), block)
        return [
            pltpu.make_async_copy(tile.at[slot, :, :lo], g_all.at[at, :lo], tile_sem.at[slot, 0]),
            pltpu.make_async_copy(tile.at[slot, :, lo:], g_all.at[at, lo + pair :], tile_sem.at[slot, 1]),
        ]

    class grads_copy:
        def __init__(self, b, slot):
            self.copies = grads_copies(b, slot)

        def wait(self):
            for copy in self.copies:
                copy.wait()

    for n in range(nz // 2):
        weight_grads(2 * n, 2)
        flow.now += 3.0
        flow.poll()
    for event in later:
        heapq.heappush(flow.events, event)
    while flow.events:
        flow.take()
    for slot in range(2):
        grads_copy(slot, slot).wait()

    flow.send("c", 1, lambda: z_out.at[:, :, :, other], lambda: x_all.at[1, :, :, :, :, lo : lo + pair], 0)
    own.append(pltpu.make_async_copy(z_out.at[:, :, :, c], x_all.at[0, :, :, :, :, lo : lo + pair], own_sem.at[2]))
    own[-1].start()

    def heads_copy(b, slot):
        at = pl.ds(pl.multiple_of(b * block, block), block)
        return pltpu.make_async_copy(tile_heads.at[slot], g_all.at[at, lo : lo + pair], tile_sem.at[slot, 0])

    @pl.loop(0, nz)
    def _(b):
        slot = lax.rem(b, 2)
        at = pl.ds(pl.multiple_of(b * block, block), block)

        @pl.when(b >= 2)
        def _():
            heads_copy(b, slot).wait()

        out = z_out[...].reshape(tokens, pair)

        @pl.when(last)
        def _():
            tile_heads[slot] = mm(h_v[:, at], out, 0, 0)

        @pl.when(jnp.logical_not(last))
        def _():
            tile_heads[slot, :, :head] = mm(h_v[:, at], out[:, :head], 0, 0)
            tile_heads[slot, :, head:] = mm(dy_v[:, at], out[:, head:], 0, 0)

        heads_copy(b, slot).start()

    for slot in range(2):
        heads_copy(slot, slot).wait()
    flow.run()
    for copy in own:
        copy.wait()


def middle(nz, h_all, dy_all, w_all, cos, sin):
    tokens, width = h_all.shape
    seq, head = cos.shape
    pair = 2 * head
    cols = w_all.shape[2]
    ff = (cols - pair) // 3
    rows = seq // (NX * NC)
    bf16, f32 = h_all.dtype, jnp.float32
    vmem = pl.BlockSpec(memory_space=pltpu.VMEM)
    dma = pltpu.SemaphoreType.DMA
    blocks = pltpu.VMEM((NY, 2, NX // 2, NC, rows, pair), bf16)
    halves = pltpu.VMEM((NY, 2, seq // 2, pair), bf16)
    block = width // nz
    count = 2 * 6 + 2 + 1
    return pl.pallas_call(
        functools.partial(middle_kernel, nz),
        out_shape=(jax.ShapeDtypeStruct((NC, NY, 2, NX // 2, rows, cols), bf16), jax.ShapeDtypeStruct((width, cols), f32)),
        in_specs=any_specs(3) + [vmem, vmem],
        out_specs=tuple(any_specs(2)),
        scratch_shapes=[
            pltpu.VMEM((tokens, width), bf16),
            pltpu.VMEM((tokens, width), bf16),
            pltpu.VMEM((width, cols), bf16),
            halves,
            halves,
            blocks,
            blocks,
            pltpu.VMEM((2, seq // 2, pair), bf16),
            pltpu.VMEM((2, NX // 2, NC, rows, pair), bf16),
            pltpu.VMEM((NY, 2, NX // 2, NC, rows, 3 * ff), bf16),
            pltpu.VMEM((seq, head), bf16),
            pltpu.VMEM((seq, head), bf16),
            pltpu.VMEM((seq, head), f32),
            pltpu.VMEM((seq, head), f32),
            pltpu.VMEM((2, block, 3 * ff), f32),
            pltpu.VMEM((2, block, pair), f32),
            dma((3 + 2 * NY,)),
            dma((3,)),
            dma((2, 2)),
            dma((count,)),
            dma((count,)),
        ],
        compiler_params=pltpu.CompilerParams(collective_id=1, has_side_effects=True, vmem_limit_bytes=VMEM_LIMIT),
        name="middle",
    )(h_all, dy_all, w_all, cos, sin)


class Stage:
    def __init__(self, buffers, sem, depth, order=None):
        self.buffers, self.sem, self.depth, self.order = buffers, sem, depth, order
        self.used, self.copies = [], []

    def fetch(self):
        k = len(self.copies)
        if k < len(self.order):
            copy = pltpu.make_async_copy(self.order[k](), self.buffers.at[k % self.depth], self.sem.at[k % self.depth])
            copy.start()
            self.copies.append(copy)

    def begin(self):
        for _ in range(self.depth):
            self.fetch()

    def take(self, src, use):
        k = len(self.used)
        self.used.append(src)
        if self.order is not None:
            self.copies[k].wait()
            use(self.buffers.at[k % self.depth])
            self.fetch()


SETS = (2, 1, -1, 0)


def scatter_plan(nz, place, flow, compute, take, add, finish, refs):
    p_tile, q_tile, p_land, q_land, g_part, g_sum, z_land, far = refs

    def reduce_ring(axis, piece, raw, need, slot, done):
        sent = []

        def turn(s, goal, half, step):
            def then():
                add(slot(s), raw(goal, half))
                flow.send(axis, step, slot(s), slot(s + 4), piece, final[half])

            return lambda: need(goal, half, then)

        def ending(half):
            def then():
                mine, other = (slot(5), slot(2)) if half == 0 else (slot(4), slot(3))
                add(mine, other)
                add(mine, raw(0, half))
                done(half, mine)

            return lambda: need(0, half, then)

        final = [after(2, ending(0)), after(2, ending(1))]

        def start(goal, half):
            if (goal, half) == (2, 1):
                sent.append(flow.send(axis, 1, raw(2, 1), slot(0), piece, turn(0, 1, 1, 1)))
            if (goal, half) == (2, 0):
                sent.append(flow.send(axis, -1, raw(2, 0), slot(1), piece, turn(1, -1, 0, -1)))
            if (goal, half) == (1, 0):
                sent.append(flow.send(axis, 1, raw(1, 0), slot(2), piece, final[0]))
            if (goal, half) == (-1, 1):
                sent.append(flow.send(axis, -1, raw(-1, 1), slot(3), piece, final[1]))

        return start, sent

    finished = [0] * len(SETS)

    def plane(n, tiles, land, first):
        second = "y" if first == "x" else "x"
        sums = {}
        piece = nbytes(tiles, 3)

        def slot_of(s):
            return lambda i: (lambda: land.at[s, i])

        waiting = {}

        def need(step, half, then):
            if (step, half) in sums:
                then()
            else:
                waiting.setdefault((step, half), []).append(then)

        second_start, _ = reduce_ring(second, piece, lambda step, half: sums[step, half], need, slot_of(len(SETS)), lambda half, ref: finish(n, half, ref))

        def first_done(s, step):
            def done(half, ref):
                sums[step, half] = ref
                for then in waiting.pop((step, half), []):
                    then()
                finished[s] += 1
                if finished[s] == 4 and s + 2 < len(SETS):
                    set_up(s + 2)
                second_start(step, half)

            return done

        starts = []
        for s, other in enumerate(SETS):

            def raw(step, half, s=s):
                return lambda: tiles.at[s % 2, place.get(first, step), half]

            starts.append(reduce_ring(first, piece, raw, lambda step, half, then: then(), slot_of(s), first_done(s, other)))
        return starts

    starts = [plane(0, p_tile, p_land, "y"), plane(1, q_tile, q_land, "x")]

    def set_up(s):
        def go():
            for goal, half in ((2, 1), (2, 0), (1, 0), (-1, 1)):
                for one in starts:
                    one[s][0](goal, half)

        def clear():
            if s >= 2:
                for one in starts:
                    for k in one[s - 2][1]:
                        flow.wait_sent(k)

        compute(s, clear, go)

    size = nbytes(g_part, 2)

    def g_raw(dz, dy):
        return lambda: g_part.at[place.get("z", dz), place.get("y", dy)]

    def home(dy, ref):
        mine = lambda: g_sum.at[place.get("y")]
        if dy == 0:
            flow.keep(ref, mine)
        elif dy == 2:
            for half, step in ((0, 1), (1, -1)):

                def onward(half=half, step=step):
                    flow.send("y", step, lambda: far.at[half], lambda: g_sum.at[place.get("y", -step), half], size // 2)

                flow.send("y", step, lambda half=half: ref().at[half], lambda half=half: far.at[half], size // 2, onward)
        else:
            flow.send("y", dy, ref, mine, size)

    def ring(step, lane, dy):
        n = 0 if step == 1 else 1

        def spot(s):
            return lambda: z_land.at[n, s, lane]

        def hop(s):
            def then():
                take(g_raw(-step * (s + 2), dy), spot(s))
                if s < nz - 2:
                    flow.send("z", step, spot(s), spot(s + 1), size, hop(s + 1))
                else:
                    home(dy, spot(s))

            return then

        flow.send("z", step, g_raw(-step, dy), spot(0), size, hop(0))

    ring(1, 0, 2)
    ring(-1, 0, 1)
    ring(1, 1, 0)
    ring(-1, 1, -1)
    set_up(0)
    set_up(1)
    flow.run()


def scatter_kernel(
    nz,
    depth,
    ff,
    x_all,
    w_all,
    g_part,
    p_sum,
    q_sum,
    g_sum,
    xa,
    xb,
    xy,
    w_v,
    p_tile,
    q_tile,
    p_land,
    q_land,
    z_land,
    far,
    stage,
    x_sem,
    w_sem,
    send_sem,
    recv_sem,
    stage_sem,
    own_sem,
):
    place = Place(nz)
    last = place.get("y") == NY - 1
    rows, cols = xb.shape[3:]
    block = w_v.shape[2]
    width = block * nz
    pair = cols - 3 * ff
    head = pair // 2
    lo = 2 * ff
    bf16 = jnp.bfloat16
    refs = (p_tile, q_tile, p_land, q_land, g_part, g_sum, z_land, far)

    def x_copies(s):
        slot = s % 2
        return [
            pltpu.make_async_copy(x_all.at[:, :, place.get("x", SETS[s]), :, lo:], xa.at[slot], x_sem.at[slot, 0]),
            pltpu.make_async_copy(x_all.at[:, place.get("y", SETS[s])], xb.at[slot], x_sem.at[slot, 1]),
        ]

    def w_copy(d, slot):
        return pltpu.make_async_copy(w_all.at[:, pl.ds(pl.multiple_of(d * block, block), block), :], w_v.at[slot], w_sem.at[slot])

    def prepare(s):
        slot = s % 2
        for copy in x_copies(s):
            copy.wait()
        lane = lax.broadcasted_iota(jnp.int32, (rows, pair), 1)
        for_d = jnp.logical_or(lane < head, last)
        for k in range(NC):
            for i in range(NY):
                mixed = xa[slot, k, i, :, :pair]
                xa[slot, k, i, :, :pair] = jnp.where(for_d, jnp.zeros_like(mixed), mixed)
            for i in range(NX):
                mixed = xb[slot, k, i, :, lo : lo + pair]
                xy[k, i, :, :pair] = jnp.where(for_d, jnp.zeros_like(mixed), mixed)
                xy[k, i, :, pair:] = xb[slot, k, i, :, lo + pair :]
                xb[slot, k, i, :, lo : lo + pair] = jnp.where(for_d, mixed, jnp.zeros_like(mixed))

    def product(left, right, from_col, to_col):
        total = None
        for k in range(NC):
            one = mm(left[k].reshape(-1, to_col - from_col), right[k, :, from_col:to_col], 1, 1)
            total = one if total is None else total + one
        return total

    def blocks(s, first, count):
        slot = s % 2

        @pl.loop(first, first + count)
        def _(d):
            w_slot = lax.rem(d, 2)
            w_copy(d, w_slot).wait()
            w = w_v.at[w_slot]
            at = pl.ds(pl.multiple_of(d * block, block), block)
            shape = (NX, 2, rows // 2, block)
            q_tile[slot, :, :, :, at] = product([xb[slot, k, :, :, : lo + pair] for k in range(NC)], w, 0, lo + pair).reshape(shape)

            @pl.when(d < nz - 1)
            def _():
                p_tile[slot, :, :, :, at] = product([xa[slot, k] for k in range(NC)], w, lo, cols).reshape(shape)

            @pl.when(d == nz - 1)
            def _():
                q_tile[slot, :, :, :, width:] = product([xy[k] for k in range(NC)], w, lo, cols).reshape(shape)

            if s == len(SETS) - 1:

                @pl.when(d < nz - 2)
                def _():
                    w_copy(lax.rem(d + 2, nz), w_slot).start()

            else:
                w_copy(lax.rem(d + 2, nz), w_slot).start()

    def trial(flow, stage):
        def keep(ref, mine):
            if flow.emit:
                flow.own = pltpu.make_async_copy(ref(), mine(), own_sem)
                flow.own.start()

        flow.keep = keep

        def take(src, ref):
            flow.now += ADD
            stage.take(src, lambda got: add(ref, lambda: got))

        def add(mine, other):
            flow.now += ADD
            if flow.emit:
                a, b = mine(), other()
                a[...] = a[...] + b[...]

        def finish(n, half, ref):
            if flow.emit:
                (p_sum, q_sum)[n][half] = ref()[...]

        def compute(s, clear, go):
            chunk = max(nz // 4, 1)
            for first in range(0, nz, chunk):

                def do(first=first):
                    if first == 0:
                        clear()
                    if flow.emit:
                        if first == 0:
                            prepare(s)
                        blocks(s, first, min(chunk, nz - first))
                    if first + chunk >= nz:
                        if flow.emit and s + 1 < len(SETS):
                            for copy in x_copies(s + 1):
                                copy.start()
                        go()

                flow.task(1.8, do)

        scatter_plan(nz, place, flow, compute, take, add, finish, refs)

    for copy in x_copies(0):
        copy.start()
    for slot in range(2):
        w_copy(slot, slot).start()
    dry = Stage(None, None, depth)
    trial(Flow(place, None, None, emit=False), dry)
    wet = Stage(stage, stage_sem, depth, dry.used)
    wet.begin()
    place.meet([("x", 1), ("x", -1), ("y", 1), ("y", -1), ("z", 1), ("z", -1)])
    flow = Flow(place, send_sem, recv_sem)
    trial(flow, wet)
    flow.own.wait()


def scatter(nz, ff, x_all, w_all, g_part):
    depth = 6
    _, _, _, rows, cols = x_all.shape
    width = w_all.shape[1]
    block = width // nz
    p_piece = (rows // 2, width - block)
    q_piece = (rows // 2, width + block)
    g_piece = g_part.shape[2:]
    count = 2 * 5 * 6 + 4 * (nz - 1) + 2 + 4
    vmem = pl.BlockSpec(memory_space=pltpu.VMEM)
    f32, bf16 = jnp.float32, x_all.dtype
    dma = pltpu.SemaphoreType.DMA
    return pl.pallas_call(
        functools.partial(scatter_kernel, nz, depth, ff),
        out_shape=(
            jax.ShapeDtypeStruct((2,) + p_piece, f32),
            jax.ShapeDtypeStruct((2,) + q_piece, f32),
            jax.ShapeDtypeStruct((NY,) + g_piece, f32),
        ),
        in_specs=any_specs(3),
        out_specs=(vmem, vmem, pl.BlockSpec(memory_space=pl.ANY)),
        scratch_shapes=[
            pltpu.VMEM((2, NC, NY, rows, cols - 2 * ff), bf16),
            pltpu.VMEM((2, NC, NX, rows, cols), bf16),
            pltpu.VMEM((NC, NX, rows, cols - 2 * ff), bf16),
            pltpu.VMEM((2, NC, block, cols), bf16),
            pltpu.VMEM((2, NY, 2) + p_piece, f32),
            pltpu.VMEM((2, NX, 2) + q_piece, f32),
            pltpu.VMEM((5, 6) + p_piece, f32),
            pltpu.VMEM((5, 6) + q_piece, f32),
            pltpu.VMEM((2, nz - 1, 2) + g_piece, f32),
            pltpu.VMEM(g_piece, f32),
            pltpu.VMEM((depth,) + g_piece, f32),
            dma((2, 2)),
            dma((2,)),
            dma((count,)),
            dma((count,)),
            dma((depth,)),
            dma,
        ],
        compiler_params=pltpu.CompilerParams(collective_id=2, has_side_effects=True, vmem_limit_bytes=VMEM_LIMIT),
        name="scatter",
    )(x_all, w_all, g_part)


def norm_fwd(row_vals, norm_gain):
    return row_vals * lax.rsqrt(jnp.mean(row_vals * row_vals, axis=-1, keepdims=True) + NORM_EPS) * norm_gain


def solution(mesh):
    act_spec = P("fsdp", "model", None)
    col_spec = P("fsdp", "model")
    row_spec = P("model", "fsdp")
    nz = mesh.shape["fsdp"] // NY

    def layer_body(x_in, dy_in, norm_gain, w_qkv, w_out, w_gate, w_up, w_down, rope_cos, rope_sin):
        bf16 = jnp.bfloat16
        _, rows, width = x_in.shape
        slab = w_qkv.shape[0]
        head = 2 * rope_cos.shape[1]
        group = w_out.shape[0] // head
        seq = rows * NX * NC
        ff = w_gate.shape[1] // NY

        x_rows = x_in[0].astype(jnp.float32)
        normed, norm_pull = jax.vjp(lambda row_vals: norm_fwd(row_vals, norm_gain), x_rows)
        h_loc = normed.astype(bf16).reshape(2, rows // 2, width)
        dy_loc = dy_in.reshape(2, rows // 2, width)
        q, k, v = w_qkv[:, : group * head], w_qkv[:, group * head : -head], w_qkv[:, -head:]
        out_t, down_t = w_out.T, w_down.T
        parts = []
        for i in range(NY):
            at = slice(i * head, (i + 1) * head)
            ffs = slice(i * ff, (i + 1) * ff)
            heads = [q[:, at], out_t[:, at]] if i < NY - 1 else [k, v]
            parts.append(jnp.concatenate([w_gate[:, ffs], w_up[:, ffs]] + heads + [down_t[:, ffs]], axis=1))
        w_loc = jnp.stack(parts)
        cos = jnp.concatenate([rope_cos, rope_cos], axis=1)
        sin = jnp.concatenate([-rope_sin, rope_sin], axis=1)

        h_all, dy_all, w_all = gather(nz, h_loc, dy_loc, w_loc)
        tokens = NY * seq
        cols = w_loc.shape[2]
        h_all = h_all.reshape(tokens, width)
        dy_all = dy_all.reshape(tokens, width)
        w_all = w_all.reshape(NC, width, cols)
        x_all, g_part = middle(nz, h_all, dy_all, w_all, cos, sin)
        p_sum, q_sum, g_sum = scatter(nz, ff, x_all.reshape(NC, NY, NX, rows, cols), w_all, g_part.reshape(nz, NY, 2, slab // 2, cols))
        p_sum = p_sum.reshape(rows, -1)
        q_sum = q_sum.reshape(rows, -1)
        g_sum = g_sum.reshape(NY, slab, cols)

        y_sum = jnp.concatenate([p_sum, q_sum[:, width:]], axis=1)
        y_out = (x_rows + y_sum).astype(bf16)
        d_h = q_sum[:, :width].astype(bf16)
        dx_out = (dy_in[0].astype(jnp.float32) + norm_pull(d_h.astype(jnp.float32))[0]).astype(bf16)
        lo = 2 * ff
        mid = lo + head
        hi = mid + head

        def take(first, end, n=NY):
            return jnp.concatenate([g_sum[i, :, first:end] for i in range(n)], axis=1)

        return (
            y_out[None],
            dx_out[None],
            jnp.concatenate([take(lo, mid), g_sum[NY - 1, :, mid:hi]], axis=1),
            take(mid, hi, group).T,
            take(0, ff),
            take(ff, lo),
            take(hi, cols).T,
        )

    return jax.shard_map(
        layer_body,
        mesh=mesh,
        in_specs=(act_spec, act_spec, P(), col_spec, row_spec, col_spec, col_spec, row_spec, P(), P()),
        out_specs=(act_spec, act_spec, col_spec, row_spec, col_spec, col_spec, row_spec),
        check_vma=False,
    )
```

```python
import functools
import heapq

import jax
import jax.numpy as jnp
from jax import lax
from jax.experimental import pallas as pl
from jax.experimental.pallas import tpu as pltpu
from jax.sharding import PartitionSpec as P

NORM_EPS = 1e-5
NY, NX, NC = 4, 4, 2
MESH = pl.DeviceIdType.MESH
LINK = 46.6e3
PAIR = 330e3
LOCAL = 1500e3
HOP = 3.5
ADD = 0.4
VMEM_LIMIT = 67043328


class Place:
    def __init__(self, nz):
        i, j = lax.axis_index("fsdp"), lax.axis_index("model")
        self.size = {"z": nz, "y": NY, "x": NX, "c": NC}
        self.at = {"z": lax.div(i, NY), "y": lax.rem(i, NY), "x": lax.div(j, NC), "c": lax.rem(j, NC)}

    def get(self, axis, step=0):
        n = self.size[axis]
        return lax.rem(self.at[axis] + (step + 2 * n) % n, n)

    def device(self, axis, step):
        at = dict(self.at)
        at[axis] = self.get(axis, step)
        return {"fsdp": at["z"] * NY + at["y"], "model": at["x"] * NC + at["c"]}

    def meet(self, peers):
        barrier = pltpu.get_barrier_semaphore()
        for axis, step in peers:
            pl.semaphore_signal(barrier, inc=1, device_id=self.device(axis, step), device_id_type=MESH)
        pl.semaphore_wait(barrier, len(peers))


class Flow:
    def __init__(self, place, send_sem, recv_sem, base=0, now=0.0):
        self.place, self.send_sem, self.recv_sem, self.base = place, send_sem, recv_sem, base
        self.now, self.free, self.events, self.copies, self.tasks, self.order = now, {}, [], [], [], 0
        self.sent = set()

    def event(self, when, wait, then):
        heapq.heappush(self.events, (when, self.order, wait, then))
        self.order += 1

    def send(self, axis, step, src, dst, size, then=None, link=None):
        k = len(self.copies)
        link = link or (axis, step)
        begin = max(self.now, self.free.get(link, 0.0))
        rate, lag = (PAIR, 1.5) if axis == "c" else (LINK, HOP)
        self.free[link] = begin + size / rate
        copy = pltpu.make_async_remote_copy(
            src_ref=src(),
            dst_ref=dst(),
            send_sem=self.send_sem.at[self.base + k],
            recv_sem=self.recv_sem.at[self.base + k],
            device_id=self.place.device(axis, step),
            device_id_type=MESH,
        )
        copy.start()
        self.copies.append(copy)
        self.event(self.free[link] + lag, copy.wait_recv, then)
        return k

    def local(self, copy, size, then):
        copy.start()
        self.event(self.now + size / LOCAL + 1.0, copy.wait, then)

    def task(self, cost, do):
        self.tasks.append((cost, do))

    def take(self):
        when, _, wait, then = heapq.heappop(self.events)
        self.now = max(self.now, when)
        wait()
        if then is not None:
            then()

    def spend(self, cost):
        self.now += cost
        while self.events and self.events[0][0] <= self.now:
            self.take()

    def wait_sent(self, k):
        if k not in self.sent:
            self.copies[k].wait_send()
        self.sent.add(k)

    def run(self):
        while self.events or self.tasks:
            if self.tasks and (not self.events or self.events[0][0] > self.now):
                cost, do = self.tasks.pop(0)
                do()
                self.now += cost
            else:
                self.take()

    def close(self):
        for k in range(len(self.copies)):
            self.wait_sent(k)


def after(count, then):
    left = [count]

    def one():
        left[0] -= 1
        if left[0] == 0:
            then()

    return one


def nbytes(ref, lead):
    n = 1
    for d in ref.shape[lead:]:
        n *= d
    return n * jnp.dtype(ref.dtype).itemsize


def gather_kernel(nz, h_ref, dy_ref, w_ref, h_all, dy_all, w_all, send_sem, recv_sem, own_sem):
    place = Place(nz)
    y, x, c, z = place.get("y"), place.get("x"), place.get("c"), place.get("z")
    place.meet([("x", 1), ("x", -1), ("y", 1), ("y", -1), ("y", 2), ("z", 1), ("z", -1), ("c", 1)])
    flow = Flow(place, send_sem, recv_sem)
    own = [
        pltpu.make_async_copy(h_ref, h_all.at[y, x, c], own_sem.at[0]),
        pltpu.make_async_copy(dy_ref, dy_all.at[y, x, c], own_sem.at[1]),
        pltpu.make_async_copy(w_ref.at[y], w_all.at[0, z, y], own_sem.at[2]),
    ]
    for copy in own:
        copy.start()
    piece = nbytes(h_ref, 1)

    def spot(ref, dy, dx, half):
        return lambda: ref.at[place.get("y", dy), place.get("x", dx), c, half]

    def spread(axis, half, offset, src, got):
        def come(step, onward):
            def then():
                if onward:
                    flow.send(axis, -step, got.spot(axis, step, offset, half), got.spot(axis, step, offset, half), piece, lambda: got(axis, 2, offset, half))
                got(axis, step, offset, half)

            return then

        flow.send(axis, 1, src, got.spot(axis, 0, offset, half), piece, come(-1, half == 0))
        flow.send(axis, -1, src, got.spot(axis, 0, offset, half), piece, come(1, half == 1))

    class Got:
        def __init__(self, ref, first):
            self.ref, self.first, self.second = ref, first, "y" if first == "x" else "x"

        def spot(self, axis, step, offset, half):
            d = {axis: step, ("y" if axis == "x" else "x"): offset}
            return spot(self.ref, d["y"], d["x"], half)

        def __call__(self, axis, step, offset, half):
            here = self.spot(axis, step, offset, half)
            if axis == self.first:
                spread(self.second, half, step, here, self)
            flow.send("c", 1, here, here, piece)

    size = nbytes(w_ref, 1)

    def w_spot(who, dz, dy):
        return lambda: w_all.at[who, place.get("z", dz), place.get("y", dy)]

    def ring(step, dy, src=None):
        def hop(n):
            def then():
                here = src if src and n == 0 else w_spot(0, -step * n, dy)
                if n < nz - 1:
                    flow.send("z", step, here, w_spot(0, -step * n, dy), size, hop(n + 1))
                flow.send("c", 1, here, w_spot(1, -step * n, dy), size)

            return then

        return hop(0)

    def w_at(dy):
        return lambda: w_ref.at[place.get("y", dy)]

    flow.send("y", -1, w_at(-1), w_spot(0, 0, 0), size, ring(1, 1))
    flow.send("y", 1, w_at(1), w_spot(0, 0, 0), size, ring(-1, -1))
    flow.send("y", 2, w_at(2), w_spot(0, 0, 0), size, ring(-1, 2), link=("y", 1))
    ring(1, 0, w_at(0))()
    arrays = [(h_ref, Got(h_all, "x")), (dy_ref, Got(dy_all, "y"))]
    for ref, got in arrays:
        for half in (0, 1):
            spread(got.first, half, 0, lambda ref=ref, half=half: ref.at[half], got)
    for ref, got in arrays:
        for half in (0, 1):
            src = lambda ref=ref, half=half: ref.at[half]
            spread(got.second, half, 0, src, got)
            flow.send("c", 1, src, got.spot(got.second, 0, 0, half), piece)
    flow.run()
    flow.close()
    for copy in own:
        copy.wait()


def any_specs(n):
    return [pl.BlockSpec(memory_space=pl.ANY)] * n


def gather(nz, h, dy, w):
    half, rows, width = h.shape
    everywhere = (NY, NX, NC) + h.shape
    count = 60 + 64 + 3 + 4 * (nz - 1) + 4 * nz
    vmem = pl.BlockSpec(memory_space=pltpu.VMEM)
    return pl.pallas_call(
        functools.partial(gather_kernel, nz),
        out_shape=(
            jax.ShapeDtypeStruct(everywhere, h.dtype),
            jax.ShapeDtypeStruct(everywhere, dy.dtype),
            jax.ShapeDtypeStruct((NC, nz) + w.shape, w.dtype),
        ),
        in_specs=[vmem] * 3,
        out_specs=tuple(any_specs(3)),
        scratch_shapes=[pltpu.SemaphoreType.DMA((count,)), pltpu.SemaphoreType.DMA((count,)), pltpu.SemaphoreType.DMA((3,))],
        compiler_params=pltpu.CompilerParams(collective_id=0, has_side_effects=True),
        name="gather",
    )(h, dy, w)


def mm(a, b, ca, cb):
    return lax.dot_general(a, b, (((ca,), (cb,)), ((), ())), preferred_element_type=jnp.float32)


def span(q, n):
    return pl.ds(pl.multiple_of(q * n, n), n)


def exchange(flow, place, src, dst, far, step, done=None):
    size = nbytes(src, 1)

    def onward(way, half):
        def then():
            flow.send("y", way, lambda: far.at[half], lambda: dst.at[place.get("y", -way), half], size // 2, done)

        return then

    if step == 2:
        flow.send("y", 1, lambda: src.at[place.get("y", 2), 0], lambda: far.at[0], size // 2, onward(1, 0))
        flow.send("y", -1, lambda: src.at[place.get("y", 2), 1], lambda: far.at[1], size // 2, onward(-1, 1))
    else:
        flow.send("y", step, lambda: src.at[place.get("y", step)], lambda: dst.at[place.get("y")], size, done)


ORDER = (2, 1, -1, 0)


def heads_kernel(nz, h_all, dy_all, w_all, z_got, h_v, dy_v, w_v, z_in, far, load_sem, own_sem, send_sem, recv_sem):
    bf16 = jnp.bfloat16
    place = Place(nz)
    y = place.get("y")
    last = y == NY - 1
    pair = z_in.shape[-1]
    head = pair // 2
    seq = h_v.shape[1]
    part = seq // 2
    lo = (w_all.shape[2] - pair) * 2 // 3
    w_load = pltpu.make_async_copy(w_all.at[0, :, lo : lo + pair], w_v, load_sem.at[0])
    w_load.start()
    loads = []
    for n, step in enumerate(ORDER):
        at = span(place.get("y", step), seq)
        loads.append([pltpu.make_async_copy(a.at[at], b.at[n], load_sem.at[1 + 2 * n + m]) for m, (a, b) in enumerate(((h_all, h_v), (dy_all, dy_v)))])
        for copy in loads[n]:
            copy.start()
    place.meet([("y", 1), ("y", -1)])
    flow = Flow(place, send_sem, recv_sem)
    w_load.wait()
    for n, step in enumerate(ORDER):
        for copy in loads[n]:
            copy.wait()
        q = place.get("y", step)

        @pl.loop(0, 2)
        def _(p):
            at = span(p, part)
            from_h = mm(h_v[n, at, :], w_v[...], 1, 0)
            from_dy = mm(dy_v[n, at, :], w_v[:, head:], 1, 0)
            z_in[q, p, :, :head] = from_h[:, :head].astype(bf16)
            z_in[q, p, :, head:] = jnp.where(last, from_h[:, head:], from_dy).astype(bf16)

        flow.spend(2.3)
        if step:
            exchange(flow, place, z_in, z_got, far, step)
    own = pltpu.make_async_copy(z_in.at[y], z_got.at[y], own_sem)
    own.start()
    flow.run()
    flow.close()
    own.wait()


def head_rows(nz, pair, seq, h_all, dy_all, w_all):
    tokens, width = h_all.shape
    bf16 = h_all.dtype
    dma = pltpu.SemaphoreType.DMA
    halves = (NY, 2, seq // 2, pair)
    return pl.pallas_call(
        functools.partial(heads_kernel, nz),
        out_shape=jax.ShapeDtypeStruct(halves, bf16),
        in_specs=any_specs(3),
        out_specs=pl.BlockSpec(memory_space=pl.ANY),
        scratch_shapes=[
            pltpu.VMEM((NY, seq, width), bf16),
            pltpu.VMEM((NY, seq, width), bf16),
            pltpu.VMEM((width, pair), bf16),
            pltpu.VMEM(halves, bf16),
            pltpu.VMEM(halves[1:], bf16),
            dma((1 + 2 * NY,)),
            dma,
            dma((6,)),
            dma((6,)),
        ],
        compiler_params=pltpu.CompilerParams(collective_id=1, has_side_effects=True, vmem_limit_bytes=VMEM_LIMIT),
        name="heads",
    )(h_all, dy_all, w_all)


SETS = (2, 1, -1, 0)


def attention(z_got, z_back, keys, vals, dk, dv, cos_ref, sin_ref):
    bf16 = jnp.bfloat16
    seq, head = keys.shape
    part = seq // 2
    count = z_got.shape[0] - 1
    scale = head**-0.5
    spread = z_back.shape[2:5] + (head,)
    halves = [pl.ds(p * part, part) for p in range(2)]

    def turn(values, at, sign):
        wide = values.astype(jnp.float32)
        swapped = pltpu.roll(wide, head // 2, 1)
        return (wide * cos_ref[at, :] + sign * (swapped * sin_ref[at, :])).astype(bf16)

    for p in range(2):
        keys[halves[p], :] = turn(z_got[count, p, :, :head], halves[p], 1.0)
        vals[halves[p], :] = z_got[count, p, :, head:]
    dk[...] = jnp.zeros_like(dk)
    dv[...] = jnp.zeros_like(dv)

    @pl.loop(0, count)
    def _(i):
        for p in range(2):
            n = (p + 1) * part
            query = turn(z_got[i, p, :, :head], halves[p], 1.0)
            d_out = z_got[i, p, :, head:]
            scores = mm(query, keys[:n, :], 1, 1) * scale
            causal = lax.broadcasted_iota(jnp.int32, scores.shape, 0) + p * part >= lax.broadcasted_iota(jnp.int32, scores.shape, 1)
            scores = jnp.where(causal, scores, -1e30)
            grown = jnp.exp(scores - jnp.max(scores, axis=1, keepdims=True))
            probs = grown / jnp.sum(grown, axis=1, keepdims=True)
            probs_low = probs.astype(bf16)
            z_back[i, p, :, :, :, head:] = mm(probs_low, vals[:n, :], 1, 0).astype(bf16).reshape(spread)
            d_probs = mm(d_out, vals[:n, :], 1, 1).astype(bf16).astype(jnp.float32)
            d_scores = (probs * (d_probs - jnp.sum(probs * d_probs, axis=1, keepdims=True)) * scale).astype(bf16)
            z_back[i, p, :, :, :, :head] = turn(mm(d_scores, keys[:n, :], 1, 0).astype(bf16), halves[p], -1.0).reshape(spread)
            dk[:n, :] += mm(d_scores, query, 0, 0)
            dv[:n, :] += mm(probs_low, d_out, 0, 0)

    for p in range(2):
        z_back[count, p, :, :, :, :head] = turn(dk[halves[p], :].astype(bf16), halves[p], -1.0).reshape(spread)
        z_back[count, p, :, :, :, head:] = dv[halves[p], :].astype(bf16).reshape(spread)


def gated(place, flow, h_all, dy_all, w_all, acts, row_sem, share, h_rows, dy_rows, w_v):
    bf16 = jnp.bfloat16
    ff = acts.shape[-1] // 3
    lo = 2 * ff
    part = h_rows.shape[1]
    shape = acts.shape[2:5] + (ff,)
    w_loads = [
        pltpu.make_async_copy(w_all.at[0, :, :lo], w_v.at[:, :lo], row_sem.at[2, 0]),
        pltpu.make_async_copy(w_all.at[0, :, w_all.shape[2] - ff :], w_v.at[:, lo:], row_sem.at[2, 1]),
    ]

    def loads(n, slot):
        return [pltpu.make_async_copy(a.at[span(n, part)], b.at[slot], row_sem.at[slot, m]) for m, (a, b) in enumerate(((h_all, h_rows), (dy_all, dy_rows)))]

    def begin():
        for copy in w_loads + loads(0, 0) + loads(1, 1):
            copy.start()

    def go():
        for copy in w_loads:
            copy.wait()
        for q in range(NY):

            @pl.loop(0, 2)
            def _(p):
                n = 2 * q + p
                for copy in loads(n, p):
                    copy.wait()
                gate = mm(h_rows[p], w_v[:, :ff], 1, 0).astype(bf16).astype(jnp.float32)
                up = mm(h_rows[p], w_v[:, ff:lo], 1, 0).astype(bf16).astype(jnp.float32)
                d_act = mm(dy_rows[p], w_v[:, lo:], 1, 0).astype(bf16).astype(jnp.float32)
                if q < NY - 1:
                    for copy in loads(n + 2, p):
                        copy.start()
                sig = jax.nn.sigmoid(gate)
                silu = gate * sig
                acts[q, p, :, :, :, :ff] = (d_act * up * (sig + silu * (1.0 - sig))).astype(bf16).reshape(shape)
                acts[q, p, :, :, :, ff:lo] = (d_act * silu).astype(bf16).reshape(shape)
                acts[q, p, :, :, :, lo:] = (silu * up).astype(bf16).reshape(shape)

            share(q)
            flow.spend(3.0)

    return begin, go


class Plane:
    def __init__(self, place, flow, tiles, land, first, finish, free):
        self.place, self.flow, self.tiles, self.land, self.first = place, flow, tiles, land, first
        self.second = "y" if first == "x" else "x"
        self.piece = nbytes(tiles, 3)
        self.sums, self.waiting, self.finished = {}, {}, [0] * len(SETS)
        self.free = free
        self.rings = []
        for s, other in enumerate(SETS):

            def raw(step, half, s=s):
                return lambda: tiles.at[s % 2, place.get(first, step), half]

            self.rings.append(self.ring(first, raw, lambda step, half, then: then(), s, self.first_done(s, other)))
        self.onward, _ = self.ring(self.second, lambda step, half: self.sums[step, half], self.need, len(SETS), finish)

    def need(self, step, half, then):
        if (step, half) in self.sums:
            then()
        else:
            self.waiting.setdefault((step, half), []).append(then)

    def first_done(self, s, step):
        def done(half, ref):
            self.sums[step, half] = ref
            for then in self.waiting.pop((step, half), []):
                then()
            self.onward(step, half)
            self.finished[s] += 1
            if self.finished[s] == 2:
                self.free(s)

        return done

    def add(self, mine, other):
        a, b = mine(), other()
        a[...] = a[...] + b[...]
        self.flow.now += ADD

    def ring(self, axis, raw, need, s, done):
        flow, add, sent = self.flow, self.add, []

        def slot(i):
            return lambda: self.land.at[s, i]

        def turn(i, goal, half, step):
            def then():
                add(slot(i), raw(goal, half))
                flow.send(axis, step, slot(i), slot(i + 4), self.piece, final[half])

            return lambda: need(goal, half, then)

        def ending(half):
            def then():
                mine, other = (slot(5), slot(2)) if half == 0 else (slot(4), slot(3))
                add(mine, other)
                add(mine, raw(0, half))
                done(half, mine)

            return lambda: need(0, half, then)

        final = [after(2, ending(0)), after(2, ending(1))]
        moves = {
            (2, 1): (1, 0, turn(0, 1, 1, 1)),
            (2, 0): (-1, 1, turn(1, -1, 0, -1)),
            (1, 0): (1, 2, final[0]),
            (-1, 1): (-1, 3, final[1]),
        }

        def start(goal, half):
            if (goal, half) in moves:
                step, i, then = moves[goal, half]
                sent.append(flow.send(axis, step, raw(goal, half), slot(i), self.piece, then))

        return start, sent

    def start(self, s):
        for goal, half in ((2, 1), (2, 0), (1, 0), (-1, 1)):
            self.rings[s][0](goal, half)

    def clear(self, s):
        for k in self.rings[s][1]:
            self.flow.wait_sent(k)


class Grads:
    def __init__(self, nz, place, flow, h_all, dy_all, acts, z_out, z_land, g_sum, far, h_plus, h_minus, dy_minus, tiles, stage, load_sem, stage_sem, own_sem):
        self.__dict__.update({k: v for k, v in locals().items() if k != "self"})
        self.ff = acts.shape[-1] // 3
        self.pair = z_out.shape[-1]
        lo = 2 * self.ff
        self.cols = [(0, self.ff), (self.ff, lo), (lo + self.pair, lo + self.pair + self.ff), (lo, lo + self.pair)]
        self.way = (1, 1, -1, -1)
        self.far_way = (1, -1, 1, -1)
        self.block = tiles.shape[2]
        self.size = nbytes(tiles, 2)
        self.ready, self.waiting, self.used = set(), {}, 0
        self.users = [[] for _ in range(stage.shape[0])]
        self.own = []
        self.idle, self.first = {}, {}

    def load(self, ref, src, index, step, n):
        b = self.place.get("z", -step * (n + 1))
        at = pl.ds(pl.multiple_of(b * self.block, self.block), self.block)
        return pltpu.make_async_copy(src.at[:, at], ref, self.load_sem.at[index])

    def loads_plus(self, n):
        return [self.load(self.h_plus, self.h_all, 0, 1, n)]

    def loads_minus(self, n):
        return [self.load(self.h_minus, self.h_all, 1, -1, n), self.load(self.dy_minus, self.dy_all, 2, -1, n)]

    def begin(self):
        for copy in self.loads_plus(0) + self.loads_minus(0):
            copy.start()

    def set_ready(self, lane, n):
        self.ready.add((lane, n))
        for then in self.waiting.pop((lane, n), []):
            then()
        if n == 0:
            k = self.flow.send("z", self.way[lane], lambda: self.tiles.at[0, lane], lambda: self.z_land.at[0, lane], self.size, self.hop(lane, 0))
            self.first[lane] = k

    def clear(self, lane, n):
        if n == 2:
            self.flow.wait_sent(self.first[lane])

    def tokens(self, ref):
        value = ref[...]
        return value.reshape(-1, value.shape[-1])

    def plus(self, n):
        def do():
            for lane in (0, 1):
                self.clear(lane, n)
            for copy in self.loads_plus(n):
                copy.wait()
            lo = 2 * self.ff
            act = self.acts[:, :, :, :, :, :lo].reshape(-1, lo)
            both = mm(self.h_plus[...], act, 0, 0)
            self.tiles[n % 2, 0] = both[:, : self.ff]
            self.tiles[n % 2, 1] = both[:, self.ff :]
            if n + 1 < self.nz:
                for copy in self.loads_plus(n + 1):
                    copy.start()
            self.set_ready(0, n)
            self.set_ready(1, n)

        self.flow.task(1.4, do)

    def minus(self, n):
        def do():
            for lane in (2, 3):
                self.clear(lane, n)
            for copy in self.loads_minus(n):
                copy.wait()
            last = self.place.get("y") == NY - 1
            head = self.pair // 2
            act = self.acts[:, :, :, :, :, 2 * self.ff :].reshape(-1, self.ff)
            self.tiles[n % 2, 2] = mm(self.dy_minus[...], act, 0, 0)
            out = self.tokens(self.z_out)
            tile = self.tiles.at[n % 2, 3]

            @pl.when(last)
            def _():
                tile[...] = mm(self.h_minus[...], out, 0, 0)

            @pl.when(jnp.logical_not(last))
            def _():
                tile[:, :head] = mm(self.h_minus[...], out[:, :head], 0, 0)
                tile[:, head:] = mm(self.dy_minus[...], out[:, head:], 0, 0)

            if n + 1 < self.nz:
                for copy in self.loads_minus(n + 1):
                    copy.start()
            self.set_ready(2, n)
            self.set_ready(3, n)

        self.flow.task(2.1, do)

    def need(self, lane, n, then):
        if (lane, n) in self.ready:
            then()
        else:
            self.waiting.setdefault((lane, n), []).append(then)

    def next(self, lane, n):
        if n + 2 >= self.nz:
            return
        key = (lane // 2, n)
        self.idle[key] = self.idle.get(key, 0) + 1
        if self.idle[key] == 2:
            (self.plus, self.minus)[lane // 2](n + 2)

    def hop(self, lane, s):
        flow, place = self.flow, self.place

        def come():
            slot = self.used % len(self.users)
            self.used += 1
            for wait in self.users[slot]:
                wait()
            self.users[slot] = []
            here = lambda: self.stage.at[slot]

            def staged():
                self.need(lane, s + 1, use)

            def use():
                ref = here()
                ref[...] = ref[...] + self.tiles[(s + 1) % 2, lane]
                flow.now += ADD
                if s == 0:
                    self.next(lane, 0)
                self.next(lane, s + 1)
                if s + 1 < self.nz - 1:
                    k = flow.send("z", self.way[lane], here, lambda: self.z_land.at[s + 1, lane], self.size, self.hop(lane, s + 1))
                    self.users[slot].append(lambda: flow.wait_sent(k))
                else:
                    self.home(lane, slot)

            flow.local(pltpu.make_async_copy(self.z_land.at[s, lane], here(), self.stage_sem.at[slot]), self.size, staged)

        return come

    def home(self, lane, slot):
        flow, place = self.flow, self.place
        slab = self.block // NY
        first, end = self.cols[lane]

        def rows(step):
            return lambda: self.stage.at[slot, pl.ds(pl.multiple_of(place.get("y", step) * slab, slab), slab)]

        def mine(step=0):
            return lambda: self.g_sum.at[place.get("y", step), :, first:end]

        size = self.size // NY
        way = self.far_way[lane]

        def onward():
            flow.send("y", way, lambda: self.far.at[lane], mine(-way), size)

        sent = [flow.send("y", way, rows(2), lambda: self.far.at[lane], size, onward)]
        sent += [flow.send("y", step, rows(step), mine(), size) for step in (1, -1)]
        copy = pltpu.make_async_copy(rows(0)(), mine()(), self.own_sem.at[lane])
        copy.start()
        self.users[slot] += [functools.partial(flow.wait_sent, k) for k in sent] + [copy.wait]

    def close(self):
        for users in self.users:
            for wait in users:
                wait()


def back_kernel(
    nz,
    z_in,
    h_all,
    dy_all,
    w_all,
    cos_ref,
    sin_ref,
    p_sum,
    q_sum,
    g_sum,
    z_land,
    z_got,
    z_back,
    z_out,
    far_back,
    acts,
    pair_acts,
    far,
    p_land,
    q_land,
    keys,
    vals,
    dk,
    dv,
    load_sem,
    row_sem,
    w_sem,
    g_load_sem,
    stage_sem,
    own_sem,
    send_sem,
    recv_sem,
):
    bf16, f32 = jnp.bfloat16, jnp.float32
    place = Place(nz)
    y, c = place.get("y"), place.get("c")
    other = place.get("c", 1)
    last = y == NY - 1
    seq, head = keys.shape
    pair = 2 * head
    rows, cols = pair_acts.shape[3:]
    ff = (cols - pair) // 3
    lo, hi = 2 * ff, 2 * ff + pair
    tokens, width = h_all.shape
    block = width // nz
    part = seq // 2

    z_load = pltpu.make_async_copy(z_in, z_got, load_sem)
    z_load.start()
    early = Flow(place, send_sem, recv_sem)
    peers = [("x", 1), ("x", -1), ("y", 1), ("y", -1), ("z", 1), ("z", -1), ("c", 1)]

    def share(q):
        early.send("c", 1, lambda: acts.at[q, :, :, other, :, :lo], lambda: pair_acts.at[q, :, :, :, :lo], nbytes(pair_acts, 1) * lo // cols)
        early.send("c", 1, lambda: acts.at[q, :, :, other, :, lo:], lambda: pair_acts.at[q, :, :, :, hi:], nbytes(pair_acts, 1) * ff // cols)

    def all_out():
        early.send("c", 1, lambda: z_out.at[:, :, :, other], lambda: pair_acts.at[:, :, :, :, lo:hi], nbytes(z_out, 0) // NC)

    def first(h_rows, dy_rows, w_v):
        begin, go = gated(place, early, h_all, dy_all, w_all, acts, row_sem, share, h_rows, dy_rows, w_v)
        begin()
        z_load.wait()
        attention(z_got, z_back, keys, vals, dk, dv, cos_ref, sin_ref)
        place.meet(peers)
        out_done = after(4, all_out)
        for step in ORDER[:3]:
            exchange(early, place, z_back, z_out, far_back, step, out_done)
        z_out[y] = z_back[y]
        go()
        early.run()
        early.close()

    pl.run_scoped(
        first,
        pltpu.VMEM((2, part, width), bf16),
        pltpu.VMEM((2, part, width), bf16),
        pltpu.VMEM((width, 3 * ff), bf16),
    )

    def second(p_tile, q_tile, w_v, h_plus, h_minus, dy_minus, tiles, stage):
        flow = Flow(place, send_sem, recv_sem, len(early.copies), early.now)
        grads = Grads(nz, place, flow, h_all, dy_all, acts, z_out, z_land, g_sum, far, h_plus, h_minus, dy_minus, tiles, stage, g_load_sem, stage_sem, own_sem)
        grads.begin()
        lane = lax.broadcasted_iota(jnp.int32, (rows, pair), 1)
        for_d = jnp.logical_or(lane < head, last)

        def chunk(k, i, p, xx):
            if k == 0:
                own = acts[i, p, xx, c]
                return own[:, :lo], z_out[i, p, xx, c], own[:, lo:]
            theirs = pair_acts[i, p, xx]
            return theirs[:, :lo], theirs[:, lo:hi], theirs[:, hi:]

        def for_out(k, i, p, xx):
            _, mixed, act = chunk(k, i, p, xx)
            return jnp.concatenate([jnp.where(for_d, jnp.zeros_like(mixed), mixed), act], axis=1)

        def for_in(k, i, p, xx):
            grad, mixed, _ = chunk(k, i, p, xx)
            return jnp.concatenate([grad, jnp.where(for_d, mixed, jnp.zeros_like(mixed))], axis=1)

        def over(first, count, a, b, body):
            def copy(d, slot):
                at = pl.ds(pl.multiple_of(d * block, block), block)
                return pltpu.make_async_copy(w_all.at[:, at, a:b], w_v.at[slot, :, :, a:b], w_sem.at[slot])

            for n in range(min(2, count)):
                copy(first + n, n).start()

            @pl.loop(0, count)
            def _(n):
                slot = lax.rem(n, 2)
                copy(first + n, slot).wait()
                body(first + n, w_v.at[slot])

                @pl.when(n + 2 < count)
                def _():
                    copy(first + n + 2, slot).start()

        def product(parts, w, a, b):
            total = None
            for k in range(NC):
                left = jnp.concatenate([one(k) for one in parts], axis=0)
                one = mm(left, w[k, :, a:b], 1, 1)
                total = one if total is None else total + one
            return total

        shape = (NX, 2, rows // 2, block)

        def p_rows(s):
            x = place.get("x", SETS[s])
            p, xx = lax.div(x, NX // 2), lax.rem(x, NX // 2)
            return [lambda k, i=i: for_out(k, i, p, xx) for i in range(NY)]

        def q_rows(s, make):
            i = place.get("y", SETS[s])
            return [lambda k, p=p, xx=xx: make(k, i, p, xx) for p in range(2) for xx in range(NX // 2)]

        def p_task(s):
            def do():
                if s >= 2:
                    planes[0].clear(s - 2)

                def body(d, w):
                    p_tile[s % 2, :, :, :, pl.ds(pl.multiple_of(d * block, block), block)] = product(p_rows(s), w, lo, cols).reshape(shape)

                over(0, nz - 1, lo, cols, body)
                planes[0].start(s)

            flow.task(2.8, do)

        def q_task(s):
            def do():
                if s >= 2:
                    planes[1].clear(s - 2)

                def edge(d, w):
                    q_tile[s % 2, :, :, :, width:] = product(q_rows(s, for_out), w, lo, cols).reshape(shape)

                def body(d, w):
                    q_tile[s % 2, :, :, :, pl.ds(pl.multiple_of(d * block, block), block)] = product(q_rows(s, for_in), w, 0, hi).reshape(shape)

                over(nz - 1, 1, lo, cols, edge)
                over(0, nz, 0, hi, body)
                planes[1].start(s)

            flow.task(5.5, do)

        def finish(out):
            def done(half, ref):
                out[half] = ref()[...]

            return done

        def free(task):
            return lambda s: task(s + 2) if s + 2 < len(SETS) else None

        planes = [
            Plane(place, flow, p_tile, p_land, "y", finish(p_sum), free(p_task)),
            Plane(place, flow, q_tile, q_land, "x", finish(q_sum), free(q_task)),
        ]

        grads.plus(0)
        grads.minus(0)
        p_task(0)
        q_task(0)
        grads.plus(1)
        grads.minus(1)
        p_task(1)
        q_task(1)
        flow.run()
        flow.close()
        grads.close()

    g_piece = (block, ff)
    pl.run_scoped(
        second,
        pltpu.VMEM((2, NY, 2, rows // 2, width - block), f32),
        pltpu.VMEM((2, NX, 2, rows // 2, width + block), f32),
        pltpu.VMEM((2, NC, block, cols), bf16),
        pltpu.VMEM((tokens, block), bf16),
        pltpu.VMEM((tokens, block), bf16),
        pltpu.VMEM((tokens, block), bf16),
        pltpu.VMEM((2, 4) + g_piece, f32),
        pltpu.VMEM((STAGES,) + g_piece, f32),
    )


STAGES = 6


def back(nz, z_in, h_all, dy_all, w_all, cos, sin):
    tokens, width = h_all.shape
    seq, head = cos.shape
    pair = 2 * head
    cols = w_all.shape[2]
    ff = (cols - pair) // 3
    rows = seq // (NX * NC)
    block = width // nz
    bf16, f32 = h_all.dtype, jnp.float32
    vmem = pl.BlockSpec(memory_space=pltpu.VMEM)
    dma = pltpu.SemaphoreType.DMA
    blocks = (NY, 2, NX // 2, NC, rows, pair)
    p_piece = (rows // 2, width - block)
    q_piece = (rows // 2, width + block)
    count = 6 + 2 * NY + 1 + 4 * (nz - 1) + 4 * 4 + 2 * 5 * 6
    return pl.pallas_call(
        functools.partial(back_kernel, nz),
        out_shape=(
            jax.ShapeDtypeStruct((2,) + p_piece, f32),
            jax.ShapeDtypeStruct((2,) + q_piece, f32),
            jax.ShapeDtypeStruct((NY, block // NY, cols), f32),
            jax.ShapeDtypeStruct((nz - 1, 4, block, ff), f32),
        ),
        in_specs=any_specs(4) + [vmem, vmem],
        out_specs=(vmem, vmem) + tuple(any_specs(2)),
        scratch_shapes=[
            pltpu.VMEM(z_in.shape, bf16),
            pltpu.VMEM(blocks, bf16),
            pltpu.VMEM(blocks, bf16),
            pltpu.VMEM(blocks[1:], bf16),
            pltpu.VMEM(blocks[:-1] + (3 * ff,), bf16),
            pltpu.VMEM(blocks[:3] + (rows, cols), bf16),
            pltpu.VMEM((4, block // NY, ff), f32),
            pltpu.VMEM((5, 6) + p_piece, f32),
            pltpu.VMEM((5, 6) + q_piece, f32),
            pltpu.VMEM((seq, head), bf16),
            pltpu.VMEM((seq, head), bf16),
            pltpu.VMEM((seq, head), f32),
            pltpu.VMEM((seq, head), f32),
            dma,
            dma((3, 2)),
            dma((2,)),
            dma((3,)),
            dma((STAGES,)),
            dma((4,)),
            dma((count,)),
            dma((count,)),
        ],
        compiler_params=pltpu.CompilerParams(collective_id=2, has_side_effects=True, vmem_limit_bytes=VMEM_LIMIT),
        name="back",
    )(z_in, h_all, dy_all, w_all, cos, sin)[:3]


def norm_fwd(row_vals, norm_gain):
    return row_vals * lax.rsqrt(jnp.mean(row_vals * row_vals, axis=-1, keepdims=True) + NORM_EPS) * norm_gain


def solution(mesh):
    act_spec = P("fsdp", "model", None)
    col_spec = P("fsdp", "model")
    row_spec = P("model", "fsdp")
    nz = mesh.shape["fsdp"] // NY

    def layer_body(x_in, dy_in, norm_gain, w_qkv, w_out, w_gate, w_up, w_down, rope_cos, rope_sin):
        bf16 = jnp.bfloat16
        _, rows, width = x_in.shape
        slab = w_qkv.shape[0]
        head = 2 * rope_cos.shape[1]
        group = w_out.shape[0] // head
        seq = rows * NX * NC
        ff = w_gate.shape[1] // NY

        x_rows = x_in[0].astype(jnp.float32)
        normed, norm_pull = jax.vjp(lambda row_vals: norm_fwd(row_vals, norm_gain), x_rows)
        h_loc = normed.astype(bf16).reshape(2, rows // 2, width)
        dy_loc = dy_in.reshape(2, rows // 2, width)
        q, k, v = w_qkv[:, : group * head], w_qkv[:, group * head : -head], w_qkv[:, -head:]
        out_t, down_t = w_out.T, w_down.T
        parts = []
        for i in range(NY):
            at = slice(i * head, (i + 1) * head)
            ffs = slice(i * ff, (i + 1) * ff)
            heads = [q[:, at], out_t[:, at]] if i < NY - 1 else [k, v]
            parts.append(jnp.concatenate([w_gate[:, ffs], w_up[:, ffs]] + heads + [down_t[:, ffs]], axis=1))
        w_loc = jnp.stack(parts)
        cos = jnp.concatenate([rope_cos, rope_cos], axis=1)
        sin = jnp.concatenate([-rope_sin, rope_sin], axis=1)

        h_all, dy_all, w_all = gather(nz, h_loc, dy_loc, w_loc)
        tokens = NY * seq
        cols = w_loc.shape[2]
        h_all = h_all.reshape(tokens, width)
        dy_all = dy_all.reshape(tokens, width)
        w_all = w_all.reshape(NC, width, cols)
        z_got = head_rows(nz, 2 * head, seq, h_all, dy_all, w_all)
        p_sum, q_sum, g_sum = back(nz, z_got, h_all, dy_all, w_all, cos, sin)
        p_sum = p_sum.reshape(rows, -1)
        q_sum = q_sum.reshape(rows, -1)

        y_sum = jnp.concatenate([p_sum, q_sum[:, width:]], axis=1)
        y_out = (x_rows + y_sum).astype(bf16)
        d_h = q_sum[:, :width].astype(bf16)
        dx_out = (dy_in[0].astype(jnp.float32) + norm_pull(d_h.astype(jnp.float32))[0]).astype(bf16)
        lo = 2 * ff
        mid = lo + head
        hi = mid + head

        def take(first, end, n=NY):
            return jnp.concatenate([g_sum[i, :, first:end] for i in range(n)], axis=1)

        return (
            y_out[None],
            dx_out[None],
            jnp.concatenate([take(lo, mid), g_sum[NY - 1, :, mid:hi]], axis=1),
            take(mid, hi, group).T,
            take(0, ff),
            take(ff, lo),
            take(hi, cols).T,
        )

    return jax.shard_map(
        layer_body,
        mesh=mesh,
        in_specs=(act_spec, act_spec, P(), col_spec, row_spec, col_spec, col_spec, row_spec, P(), P()),
        out_specs=(act_spec, act_spec, col_spec, row_spec, col_spec, col_spec, row_spec),
        check_vma=False,
    )
```

```python
import functools
import heapq

import jax
import jax.numpy as jnp
from jax import lax
from jax.experimental import pallas as pl
from jax.experimental.pallas import tpu as pltpu
from jax.sharding import PartitionSpec as P

NORM_EPS = 1e-5
NY, NX, NC = 4, 4, 2
MESH = pl.DeviceIdType.MESH
LINK = 46.6e3
PAIR = 330e3
LOCAL = 1500e3
HOP = 3.5
ADD = 0.4
VMEM_LIMIT = 67043328


class Place:
    def __init__(self, nz):
        i, j = lax.axis_index("fsdp"), lax.axis_index("model")
        self.size = {"z": nz, "y": NY, "x": NX, "c": NC}
        self.at = {"z": lax.div(i, NY), "y": lax.rem(i, NY), "x": lax.div(j, NC), "c": lax.rem(j, NC)}

    def get(self, axis, step=0):
        n = self.size[axis]
        return lax.rem(self.at[axis] + (step + 2 * n) % n, n)

    def device(self, axis, step):
        at = dict(self.at)
        at[axis] = self.get(axis, step)
        return {"fsdp": at["z"] * NY + at["y"], "model": at["x"] * NC + at["c"]}

    def meet(self, peers):
        barrier = pltpu.get_barrier_semaphore()
        for axis, step in peers:
            pl.semaphore_signal(barrier, inc=1, device_id=self.device(axis, step), device_id_type=MESH)
        pl.semaphore_wait(barrier, len(peers))


class Flow:
    def __init__(self, place, send_sem, recv_sem, base=0, now=0.0):
        self.place, self.send_sem, self.recv_sem, self.base = place, send_sem, recv_sem, base
        self.now, self.free, self.events, self.copies, self.tasks, self.order = now, {}, [], [], [], 0
        self.sent = set()

    def event(self, when, wait, then):
        heapq.heappush(self.events, (when, self.order, wait, then))
        self.order += 1

    def send(self, axis, step, src, dst, size, then=None, link=None):
        k = len(self.copies)
        link = link or (axis, step)
        begin = max(self.now, self.free.get(link, 0.0))
        rate, lag = (PAIR, 1.5) if axis == "c" else (LINK, HOP)
        self.free[link] = begin + size / rate
        copy = pltpu.make_async_remote_copy(
            src_ref=src(),
            dst_ref=dst(),
            send_sem=self.send_sem.at[self.base + k],
            recv_sem=self.recv_sem.at[self.base + k],
            device_id=self.place.device(axis, step),
            device_id_type=MESH,
        )
        copy.start()
        self.copies.append(copy)
        self.event(self.free[link] + lag, copy.wait_recv, then)
        return k

    def local(self, copy, size, then):
        copy.start()
        self.event(self.now + size / LOCAL + 1.0, copy.wait, then)

    def task(self, cost, do):
        self.tasks.append((cost, do))

    def take(self):
        when, _, wait, then = heapq.heappop(self.events)
        self.now = max(self.now, when)
        wait()
        if then is not None:
            then()

    def spend(self, cost):
        self.now += cost
        while self.events and self.events[0][0] <= self.now:
            self.take()

    def wait_sent(self, k):
        if k not in self.sent:
            self.copies[k].wait_send()
        self.sent.add(k)

    def run(self):
        while self.events or self.tasks:
            if self.tasks and (not self.events or self.events[0][0] > self.now):
                cost, do = self.tasks.pop(0)
                self.now += cost
                do()
            else:
                self.take()

    def close(self):
        for k in range(len(self.copies)):
            self.wait_sent(k)


def after(count, then):
    left = [count]

    def one():
        left[0] -= 1
        if left[0] == 0:
            then()

    return one


def nbytes(ref, lead):
    n = 1
    for d in ref.shape[lead:]:
        n *= d
    return n * jnp.dtype(ref.dtype).itemsize


def gather_kernel(nz, h_ref, dy_ref, w_ref, h_all, dy_all, w_all, send_sem, recv_sem, own_sem):
    place = Place(nz)
    y, x, c, z = place.get("y"), place.get("x"), place.get("c"), place.get("z")
    place.meet([("x", 1), ("x", -1), ("y", 1), ("y", -1), ("y", 2), ("z", 1), ("z", -1), ("c", 1)])
    flow = Flow(place, send_sem, recv_sem)
    own = [
        pltpu.make_async_copy(h_ref, h_all.at[y, x, c], own_sem.at[0]),
        pltpu.make_async_copy(dy_ref, dy_all.at[y, x, c], own_sem.at[1]),
        pltpu.make_async_copy(w_ref.at[y], w_all.at[0, z, y], own_sem.at[2]),
    ]
    for copy in own:
        copy.start()
    piece = nbytes(h_ref, 1)

    def spot(ref, dy, dx, half):
        return lambda: ref.at[place.get("y", dy), place.get("x", dx), c, half]

    def spread(axis, half, offset, src, got):
        def come(step, onward):
            def then():
                if onward:
                    flow.send(axis, -step, got.spot(axis, step, offset, half), got.spot(axis, step, offset, half), piece, lambda: got(axis, 2, offset, half))
                got(axis, step, offset, half)

            return then

        flow.send(axis, 1, src, got.spot(axis, 0, offset, half), piece, come(-1, half == 0))
        flow.send(axis, -1, src, got.spot(axis, 0, offset, half), piece, come(1, half == 1))

    class Got:
        def __init__(self, ref, first):
            self.ref, self.first, self.second = ref, first, "y" if first == "x" else "x"

        def spot(self, axis, step, offset, half):
            d = {axis: step, ("y" if axis == "x" else "x"): offset}
            return spot(self.ref, d["y"], d["x"], half)

        def __call__(self, axis, step, offset, half):
            here = self.spot(axis, step, offset, half)
            if axis == self.first:
                spread(self.second, half, step, here, self)
            flow.send("c", 1, here, here, piece)

    size = nbytes(w_ref, 1)

    def w_spot(who, dz, dy):
        return lambda: w_all.at[who, place.get("z", dz), place.get("y", dy)]

    def ring(step, dy, src=None):
        def hop(n):
            def then():
                here = src if src and n == 0 else w_spot(0, -step * n, dy)
                if n < nz - 1:
                    flow.send("z", step, here, w_spot(0, -step * n, dy), size, hop(n + 1))
                flow.send("c", 1, here, w_spot(1, -step * n, dy), size)

            return then

        return hop(0)

    def w_at(dy):
        return lambda: w_ref.at[place.get("y", dy)]

    flow.send("y", -1, w_at(-1), w_spot(0, 0, 0), size, ring(1, 1))
    flow.send("y", 1, w_at(1), w_spot(0, 0, 0), size, ring(-1, -1))
    flow.send("y", 2, w_at(2), w_spot(0, 0, 0), size, ring(-1, 2), link=("y", 1))
    ring(1, 0, w_at(0))()
    arrays = [(h_ref, Got(h_all, "x")), (dy_ref, Got(dy_all, "y"))]
    for ref, got in arrays:
        for half in (0, 1):
            spread(got.first, half, 0, lambda ref=ref, half=half: ref.at[half], got)
    for ref, got in arrays:
        for half in (0, 1):
            src = lambda ref=ref, half=half: ref.at[half]
            spread(got.second, half, 0, src, got)
            flow.send("c", 1, src, got.spot(got.second, 0, 0, half), piece)
    flow.run()
    flow.close()
    for copy in own:
        copy.wait()


def any_specs(n):
    return [pl.BlockSpec(memory_space=pl.ANY)] * n


def gather(nz, h, dy, w):
    half, rows, width = h.shape
    everywhere = (NY, NX, NC) + h.shape
    count = 60 + 64 + 3 + 4 * (nz - 1) + 4 * nz
    vmem = pl.BlockSpec(memory_space=pltpu.VMEM)
    return pl.pallas_call(
        functools.partial(gather_kernel, nz),
        out_shape=(
            jax.ShapeDtypeStruct(everywhere, h.dtype),
            jax.ShapeDtypeStruct(everywhere, dy.dtype),
            jax.ShapeDtypeStruct((NC, nz) + w.shape, w.dtype),
        ),
        in_specs=[vmem] * 3,
        out_specs=tuple(any_specs(3)),
        scratch_shapes=[pltpu.SemaphoreType.DMA((count,)), pltpu.SemaphoreType.DMA((count,)), pltpu.SemaphoreType.DMA((3,))],
        compiler_params=pltpu.CompilerParams(collective_id=0, has_side_effects=True),
        name="gather",
    )(h, dy, w)


def mm(a, b, ca, cb):
    return lax.dot_general(a, b, (((ca,), (cb,)), ((), ())), preferred_element_type=jnp.float32)


def span(q, n):
    return pl.ds(pl.multiple_of(q * n, n), n)


def exchange(flow, place, src, dst, far, step, done=None):
    size = nbytes(src, 1)

    def onward(way, half):
        def then():
            flow.send("y", way, lambda: far.at[half], lambda: dst.at[place.get("y", -way), half], size // 2, done)

        return then

    if step == 2:
        flow.send("y", 1, lambda: src.at[place.get("y", 2), 0], lambda: far.at[0], size // 2, onward(1, 0))
        flow.send("y", -1, lambda: src.at[place.get("y", 2), 1], lambda: far.at[1], size // 2, onward(-1, 1))
    else:
        flow.send("y", step, lambda: src.at[place.get("y", step)], lambda: dst.at[place.get("y")], size, done)


ORDER = (2, 1, -1, 0)


def heads_kernel(nz, h_all, dy_all, w_all, z_got, h_v, dy_v, w_v, z_in, far, load_sem, own_sem, send_sem, recv_sem):
    bf16 = jnp.bfloat16
    place = Place(nz)
    y = place.get("y")
    last = y == NY - 1
    pair = z_in.shape[-1]
    head = pair // 2
    seq = h_v.shape[1]
    part = seq // 2
    lo = (w_all.shape[2] - pair) * 2 // 3
    w_load = pltpu.make_async_copy(w_all.at[0, :, lo : lo + pair], w_v, load_sem.at[0])
    w_load.start()
    loads = []
    for n, step in enumerate(ORDER):
        at = span(place.get("y", step), seq)
        loads.append([pltpu.make_async_copy(a.at[at], b.at[n], load_sem.at[1 + 2 * n + m]) for m, (a, b) in enumerate(((h_all, h_v), (dy_all, dy_v)))])
        for copy in loads[n]:
            copy.start()
    place.meet([("y", 1), ("y", -1)])
    flow = Flow(place, send_sem, recv_sem)
    w_load.wait()
    for n, step in enumerate(ORDER):
        for copy in loads[n]:
            copy.wait()
        q = place.get("y", step)

        @pl.loop(0, 2)
        def _(p):
            at = span(p, part)
            from_h = mm(h_v[n, at, :], w_v[...], 1, 0)
            from_dy = mm(dy_v[n, at, :], w_v[:, head:], 1, 0)
            z_in[q, p, :, :head] = from_h[:, :head].astype(bf16)
            z_in[q, p, :, head:] = jnp.where(last, from_h[:, head:], from_dy).astype(bf16)

        flow.spend(2.3)
        if step:
            exchange(flow, place, z_in, z_got, far, step)
    own = pltpu.make_async_copy(z_in.at[y], z_got.at[y], own_sem)
    own.start()
    flow.run()
    flow.close()
    own.wait()


def head_rows(nz, pair, seq, h_all, dy_all, w_all):
    tokens, width = h_all.shape
    bf16 = h_all.dtype
    dma = pltpu.SemaphoreType.DMA
    halves = (NY, 2, seq // 2, pair)
    return pl.pallas_call(
        functools.partial(heads_kernel, nz),
        out_shape=jax.ShapeDtypeStruct(halves, bf16),
        in_specs=any_specs(3),
        out_specs=pl.BlockSpec(memory_space=pl.ANY),
        scratch_shapes=[
            pltpu.VMEM((NY, seq, width), bf16),
            pltpu.VMEM((NY, seq, width), bf16),
            pltpu.VMEM((width, pair), bf16),
            pltpu.VMEM(halves, bf16),
            pltpu.VMEM(halves[1:], bf16),
            dma((1 + 2 * NY,)),
            dma,
            dma((6,)),
            dma((6,)),
        ],
        compiler_params=pltpu.CompilerParams(collective_id=1, has_side_effects=True, vmem_limit_bytes=VMEM_LIMIT),
        name="heads",
    )(h_all, dy_all, w_all)


SETS = (2, 1, -1, 0)


def attention(z_got, z_back, keys, vals, dk, dv, cos_ref, sin_ref):
    bf16 = jnp.bfloat16
    seq, head = keys.shape
    part = seq // 2
    count = z_got.shape[0] - 1
    scale = head**-0.5
    spread = z_back.shape[2:5] + (head,)
    halves = [pl.ds(p * part, part) for p in range(2)]

    def turn(values, at, sign):
        wide = values.astype(jnp.float32)
        swapped = pltpu.roll(wide, head // 2, 1)
        return (wide * cos_ref[at, :] + sign * (swapped * sin_ref[at, :])).astype(bf16)

    for p in range(2):
        keys[halves[p], :] = turn(z_got[count, p, :, :head], halves[p], 1.0)
        vals[halves[p], :] = z_got[count, p, :, head:]
    dk[...] = jnp.zeros_like(dk)
    dv[...] = jnp.zeros_like(dv)

    @pl.loop(0, count)
    def _(i):
        for p in range(2):
            n = (p + 1) * part
            query = turn(z_got[i, p, :, :head], halves[p], 1.0)
            d_out = z_got[i, p, :, head:]
            scores = mm(query, keys[:n, :], 1, 1) * scale
            causal = lax.broadcasted_iota(jnp.int32, scores.shape, 0) + p * part >= lax.broadcasted_iota(jnp.int32, scores.shape, 1)
            scores = jnp.where(causal, scores, -1e30)
            grown = jnp.exp(scores - jnp.max(scores, axis=1, keepdims=True))
            probs = grown / jnp.sum(grown, axis=1, keepdims=True)
            probs_low = probs.astype(bf16)
            z_back[i, p, :, :, :, head:] = mm(probs_low, vals[:n, :], 1, 0).astype(bf16).reshape(spread)
            d_probs = mm(d_out, vals[:n, :], 1, 1).astype(bf16).astype(jnp.float32)
            d_scores = (probs * (d_probs - jnp.sum(probs * d_probs, axis=1, keepdims=True)) * scale).astype(bf16)
            z_back[i, p, :, :, :, :head] = turn(mm(d_scores, keys[:n, :], 1, 0).astype(bf16), halves[p], -1.0).reshape(spread)
            dk[:n, :] += mm(d_scores, query, 0, 0)
            dv[:n, :] += mm(probs_low, d_out, 0, 0)

    for p in range(2):
        z_back[count, p, :, :, :, :head] = turn(dk[halves[p], :].astype(bf16), halves[p], -1.0).reshape(spread)
        z_back[count, p, :, :, :, head:] = dv[halves[p], :].astype(bf16).reshape(spread)


def gated(place, flow, h_all, dy_all, w_all, acts, row_sem, share, h_rows, dy_rows, w_v):
    bf16 = jnp.bfloat16
    ff = acts.shape[-1] // 3
    lo = 2 * ff
    part = h_rows.shape[1]
    shape = acts.shape[2:5] + (ff,)
    w_loads = [
        pltpu.make_async_copy(w_all.at[0, :, :lo], w_v.at[:, :lo], row_sem.at[2, 0]),
        pltpu.make_async_copy(w_all.at[0, :, w_all.shape[2] - ff :], w_v.at[:, lo:], row_sem.at[2, 1]),
    ]

    def loads(n, slot):
        return [pltpu.make_async_copy(a.at[span(n, part)], b.at[slot], row_sem.at[slot, m]) for m, (a, b) in enumerate(((h_all, h_rows), (dy_all, dy_rows)))]

    def begin():
        for copy in w_loads + loads(0, 0) + loads(1, 1):
            copy.start()

    def go():
        for copy in w_loads:
            copy.wait()
        for q in range(NY):

            @pl.loop(0, 2)
            def _(p):
                n = 2 * q + p
                for copy in loads(n, p):
                    copy.wait()
                gate = mm(h_rows[p], w_v[:, :ff], 1, 0).astype(bf16).astype(jnp.float32)
                up = mm(h_rows[p], w_v[:, ff:lo], 1, 0).astype(bf16).astype(jnp.float32)
                d_act = mm(dy_rows[p], w_v[:, lo:], 1, 0).astype(bf16).astype(jnp.float32)
                if q < NY - 1:
                    for copy in loads(n + 2, p):
                        copy.start()
                sig = jax.nn.sigmoid(gate)
                silu = gate * sig
                acts[q, p, :, :, :, :ff] = (d_act * up * (sig + silu * (1.0 - sig))).astype(bf16).reshape(shape)
                acts[q, p, :, :, :, ff:lo] = (d_act * silu).astype(bf16).reshape(shape)
                acts[q, p, :, :, :, lo:] = (silu * up).astype(bf16).reshape(shape)

            share(q)
            flow.spend(3.0)

    return begin, go


class Plane:
    def __init__(self, place, flow, tiles, land, first, finish, free):
        self.place, self.flow, self.tiles, self.land, self.first = place, flow, tiles, land, first
        self.second = "y" if first == "x" else "x"
        self.piece = nbytes(tiles, 3)
        self.sums, self.waiting, self.finished = {}, {}, [0] * len(SETS)
        self.free = free
        self.rings = []
        for s, other in enumerate(SETS):

            def raw(step, half, s=s):
                return lambda: tiles.at[s % 2, place.get(first, step), half]

            self.rings.append(self.ring(first, raw, lambda step, half, then: then(), s, self.first_done(s, other)))
        self.onward, _ = self.ring(self.second, lambda step, half: self.sums[step, half], self.need, len(SETS), finish)

    def need(self, step, half, then):
        if (step, half) in self.sums:
            then()
        else:
            self.waiting.setdefault((step, half), []).append(then)

    def first_done(self, s, step):
        def done(half, ref):
            self.sums[step, half] = ref
            for then in self.waiting.pop((step, half), []):
                then()
            self.onward(step, half)
            self.finished[s] += 1
            if self.finished[s] == 2:
                self.free(s)

        return done

    def add(self, mine, other):
        a, b = mine(), other()
        a[...] = a[...] + b[...]
        self.flow.now += ADD

    def ring(self, axis, raw, need, s, done):
        flow, add, sent = self.flow, self.add, []

        def slot(i):
            return lambda: self.land.at[s, i]

        def turn(i, goal, half, step):
            def then():
                add(slot(i), raw(goal, half))
                flow.send(axis, step, slot(i), slot(i + 4), self.piece, final[half])

            return lambda: need(goal, half, then)

        def ending(half):
            def then():
                mine, other = (slot(5), slot(2)) if half == 0 else (slot(4), slot(3))
                add(mine, other)
                add(mine, raw(0, half))
                done(half, mine)

            return lambda: need(0, half, then)

        final = [after(2, ending(0)), after(2, ending(1))]
        moves = {
            (2, 1): (1, 0, turn(0, 1, 1, 1)),
            (2, 0): (-1, 1, turn(1, -1, 0, -1)),
            (1, 0): (1, 2, final[0]),
            (-1, 1): (-1, 3, final[1]),
        }

        def start(goal, half):
            if (goal, half) in moves:
                step, i, then = moves[goal, half]
                sent.append(flow.send(axis, step, raw(goal, half), slot(i), self.piece, then))

        return start, sent

    def start(self, s):
        for goal, half in ((2, 1), (2, 0), (1, 0), (-1, 1)):
            self.rings[s][0](goal, half)

    def clear(self, s):
        for k in self.rings[s][1]:
            self.flow.wait_sent(k)


class Grads:
    flow = None


    def __init__(self, nz, place, h_all, dy_all, acts, z_out, z_land, g_sum, far, h_plus, h_minus, dy_minus, tiles, stage, load_sem, stage_sem, own_sem):
        self.__dict__.update({k: v for k, v in locals().items() if k != "self"})
        self.ff = acts.shape[-1] // 3
        self.pair = z_out.shape[-1]
        lo = 2 * self.ff
        self.cols = [(0, self.ff), (self.ff, lo), (lo + self.pair, lo + self.pair + self.ff), (lo, lo + self.pair)]
        self.way = (1, 1, -1, -1)
        self.far_way = (1, -1, 1, -1)
        self.block = tiles.shape[2]
        self.size = nbytes(tiles, 2)
        self.ready, self.waiting, self.used = set(), {}, 0
        self.users = [[] for _ in range(stage.shape[0])]
        self.own = []
        self.idle, self.first = {}, {}

    def load(self, ref, src, index, step, n):
        b = self.place.get("z", -step * (n + 1))
        at = pl.ds(pl.multiple_of(b * self.block, self.block), self.block)
        return pltpu.make_async_copy(src.at[:, at], ref, self.load_sem.at[index])

    def loads_plus(self, n):
        return [self.load(self.h_plus, self.h_all, 0, 1, n)]

    def loads_minus(self, n):
        return [self.load(self.h_minus, self.h_all, 1, -1, n), self.load(self.dy_minus, self.dy_all, 2, -1, n)]

    def begin(self):
        for copy in self.loads_plus(0) + self.loads_minus(0):
            copy.start()

    def gather_up(self, tiles, some):
        seq = self.h_plus.shape[0] // NY
        for tile, value in zip(tiles, some(0, pl.ds(0, seq))):
            tile[...] = value

        @pl.loop(1, NY)
        def _(q):
            for tile, value in zip(tiles, some(q, span(q, seq))):
                tile[...] += value

    def set_ready(self, lane, n):
        self.ready.add((lane, n))
        for then in self.waiting.pop((lane, n), []):
            then()
        if n == 0:
            k = self.flow.send("z", self.way[lane], lambda: self.tiles.at[0, lane], lambda: self.z_land.at[0, lane], self.size, self.hop(lane, 0))
            self.first[lane] = k

    def clear(self, lane, n):
        if n == 2:
            self.flow.wait_sent(self.first[lane])

    def tokens(self, ref):
        value = ref[...]
        return value.reshape(-1, value.shape[-1])

    def make_plus(self, n):
        for copy in self.loads_plus(n):
            copy.wait()
        lo = 2 * self.ff

        def some(q, rows):
            both = mm(self.h_plus[rows, :], self.acts[q, :, :, :, :, :lo].reshape(-1, lo), 0, 0)
            return both[:, : self.ff], both[:, self.ff :]

        self.gather_up([self.tiles.at[n % 2, 0], self.tiles.at[n % 2, 1]], some)
        if n + 1 < self.nz:
            for copy in self.loads_plus(n + 1):
                copy.start()

    def for_down(self, q, rows):
        return [mm(self.dy_minus[rows, :], self.acts[q, :, :, :, :, 2 * self.ff :].reshape(-1, self.ff), 0, 0)]

    def for_heads(self, q, rows):
        last = self.place.get("y") == NY - 1
        head = self.pair // 2
        out = self.z_out[q].reshape(-1, self.pair)
        both = mm(self.h_minus[rows, :], out, 0, 0)
        right = jnp.where(last, both[:, head:], mm(self.dy_minus[rows, :], out[:, head:], 0, 0))
        return [jnp.concatenate([both[:, :head], right], axis=1)]

    def make_minus(self, n):
        for copy in self.loads_minus(n):
            copy.wait()
        self.gather_up([self.tiles.at[n % 2, 2], self.tiles.at[n % 2, 3]], lambda q, rows: self.for_down(q, rows) + self.for_heads(q, rows))
        self.load_minus_next(n)

    def load_minus_next(self, n):
        if n + 1 < self.nz:
            for copy in self.loads_minus(n + 1):
                copy.start()

    def make_first(self):
        self.make_plus(0)
        for copy in self.loads_minus(0):
            copy.wait()
        self.gather_up([self.tiles.at[0, 2]], self.for_down)

    def heads_first(self):
        def do():
            self.gather_up([self.tiles.at[0, 3]], self.for_heads)
            self.load_minus_next(0)
            self.set_ready(3, 0)

        self.flow.task(1.3, do)

    def plus(self, n):
        def do():
            for lane in (0, 1):
                self.clear(lane, n)
            self.make_plus(n)
            for lane in (0, 1):
                self.set_ready(lane, n)

        self.flow.task(1.6, do)

    def minus(self, n):
        def do():
            for lane in (2, 3):
                self.clear(lane, n)
            self.make_minus(n)
            for lane in (2, 3):
                self.set_ready(lane, n)

        self.flow.task(2.2, do)

    def need(self, lane, n, then):
        if (lane, n) in self.ready:
            then()
        else:
            self.waiting.setdefault((lane, n), []).append(then)

    def next(self, lane, n):
        if n + 2 >= self.nz:
            return
        key = (lane // 2, n)
        self.idle[key] = self.idle.get(key, 0) + 1
        if self.idle[key] == 2:
            (self.plus, self.minus)[lane // 2](n + 2)

    def hop(self, lane, s):
        flow, place = self.flow, self.place

        def come():
            slot = self.used % len(self.users)
            self.used += 1
            for wait in self.users[slot]:
                wait()
            self.users[slot] = []
            here = lambda: self.stage.at[slot]

            def staged():
                self.need(lane, s + 1, use)

            def use():
                ref = here()
                ref[...] = ref[...] + self.tiles[(s + 1) % 2, lane]
                flow.now += ADD
                if s == 0:
                    self.next(lane, 0)
                self.next(lane, s + 1)
                if s + 1 < self.nz - 1:
                    k = flow.send("z", self.way[lane], here, lambda: self.z_land.at[s + 1, lane], self.size, self.hop(lane, s + 1))
                    self.users[slot].append(lambda: flow.wait_sent(k))
                else:
                    self.home(lane, slot)

            flow.local(pltpu.make_async_copy(self.z_land.at[s, lane], here(), self.stage_sem.at[slot]), self.size, staged)

        return come

    def home(self, lane, slot):
        flow, place = self.flow, self.place
        slab = self.block // NY
        first, end = self.cols[lane]

        def rows(step):
            return lambda: self.stage.at[slot, pl.ds(pl.multiple_of(place.get("y", step) * slab, slab), slab)]

        def mine(step=0):
            return lambda: self.g_sum.at[place.get("y", step), :, first:end]

        size = self.size // NY
        way = self.far_way[lane]

        def onward():
            flow.send("y", way, lambda: self.far.at[lane], mine(-way), size)

        sent = [flow.send("y", way, rows(2), lambda: self.far.at[lane], size, onward)]
        sent += [flow.send("y", step, rows(step), mine(), size) for step in (1, -1)]
        copy = pltpu.make_async_copy(rows(0)(), mine()(), self.own_sem.at[lane])
        copy.start()
        self.users[slot] += [functools.partial(flow.wait_sent, k) for k in sent] + [copy.wait]

    def close(self):
        for users in self.users:
            for wait in users:
                wait()


def back_kernel(
    nz,
    z_in,
    h_all,
    dy_all,
    w_all,
    cos_ref,
    sin_ref,
    p_sum,
    q_sum,
    g_sum,
    z_land,
    z_got,
    z_back,
    z_out,
    far_back,
    acts,
    pair_acts,
    far,
    p_land,
    q_land,
    keys,
    vals,
    dk,
    dv,
    h_plus,
    h_minus,
    dy_minus,
    tiles,
    stage,
    load_sem,
    row_sem,
    w_sem,
    g_load_sem,
    stage_sem,
    own_sem,
    send_sem,
    recv_sem,
):
    bf16, f32 = jnp.bfloat16, jnp.float32
    place = Place(nz)
    y, c = place.get("y"), place.get("c")
    other = place.get("c", 1)
    last = y == NY - 1
    seq, head = keys.shape
    pair = 2 * head
    rows, cols = pair_acts.shape[3:]
    ff = (cols - pair) // 3
    lo, hi = 2 * ff, 2 * ff + pair
    tokens, width = h_all.shape
    block = width // nz
    part = seq // 2

    z_load = pltpu.make_async_copy(z_in, z_got, load_sem)
    z_load.start()
    early = Flow(place, send_sem, recv_sem)
    peers = [("x", 1), ("x", -1), ("y", 1), ("y", -1), ("z", 1), ("z", -1), ("c", 1)]

    def share(q):
        early.send("c", 1, lambda: acts.at[q, :, :, other, :, :lo], lambda: pair_acts.at[q, :, :, :, :lo], nbytes(pair_acts, 1) * lo // cols)
        early.send("c", 1, lambda: acts.at[q, :, :, other, :, lo:], lambda: pair_acts.at[q, :, :, :, hi:], nbytes(pair_acts, 1) * ff // cols)

    def all_out():
        early.send("c", 1, lambda: z_out.at[:, :, :, other], lambda: pair_acts.at[:, :, :, :, lo:hi], nbytes(z_out, 0) // NC)

    grads = Grads(nz, place, h_all, dy_all, acts, z_out, z_land, g_sum, far, h_plus, h_minus, dy_minus, tiles, stage, g_load_sem, stage_sem, own_sem)

    def first(h_rows, dy_rows, w_v):
        begin, go = gated(place, early, h_all, dy_all, w_all, acts, row_sem, share, h_rows, dy_rows, w_v)
        begin()
        grads.begin()
        z_load.wait()
        attention(z_got, z_back, keys, vals, dk, dv, cos_ref, sin_ref)
        place.meet(peers)
        out_done = after(4, all_out)
        for step in ORDER[:3]:
            exchange(early, place, z_back, z_out, far_back, step, out_done)
        z_out[y] = z_back[y]
        go()
        grads.make_first()
        early.now += 2.6
        early.run()
        early.close()

    pl.run_scoped(
        first,
        pltpu.VMEM((2, part, width), bf16),
        pltpu.VMEM((2, part, width), bf16),
        pltpu.VMEM((width, 3 * ff), bf16),
    )

    def second(p_tile, q_tile, w_v):
        flow = Flow(place, send_sem, recv_sem, len(early.copies), early.now)
        grads.flow = flow
        lane = lax.broadcasted_iota(jnp.int32, (rows, pair), 1)
        for_d = jnp.logical_or(lane < head, last)

        def chunk(k, i, p, xx):
            if k == 0:
                own = acts[i, p, xx, c]
                return own[:, :lo], z_out[i, p, xx, c], own[:, lo:]
            theirs = pair_acts[i, p, xx]
            return theirs[:, :lo], theirs[:, lo:hi], theirs[:, hi:]

        def for_out(k, i, p, xx):
            _, mixed, act = chunk(k, i, p, xx)
            return jnp.concatenate([jnp.where(for_d, jnp.zeros_like(mixed), mixed), act], axis=1)

        def for_in(k, i, p, xx):
            grad, mixed, _ = chunk(k, i, p, xx)
            return jnp.concatenate([grad, jnp.where(for_d, mixed, jnp.zeros_like(mixed))], axis=1)

        depth = w_v.shape[0]

        def w_copy(kind, d, slot):
            at = pl.ds(pl.multiple_of(d * block, block), block)
            cut = slice(lo, cols) if kind == 0 else slice(0, cols)
            return pltpu.make_async_copy(w_all.at[:, at, cut], w_v.at[slot, :, :, cut], w_sem.at[slot])

        counts = (nz - 1, nz)
        base, total = [], 0
        for kind, _ in PASSES:
            base.append(total)
            total += counts[kind]
        kind = PASSES[0][0]
        for n in range(depth):
            w_copy(kind, n, n).start() if n < counts[kind] else w_copy(PASSES[1][0], n - counts[kind], n).start()
        turn = [0]

        def blocks(s, kind, first, count, body):
            n = turn[0]
            assert PASSES[n] == (kind, s)
            if first + count == counts[kind]:
                turn[0] += 1

            @pl.loop(first, first + count)
            def _(d):
                slot = lax.rem(base[n] + d, depth)
                w_copy(kind, d, slot).wait()
                body(d, w_v.at[slot])

                @pl.when(d + depth < counts[kind])
                def _():
                    w_copy(kind, d + depth, slot).start()

                if n + 1 < len(PASSES):

                    @pl.when(d + depth >= counts[kind])
                    def _():
                        w_copy(PASSES[n + 1][0], d + depth - counts[kind], slot).start()

        def product(parts, w, a, b):
            total = None
            for k in range(NC):
                left = jnp.concatenate([one(k) for one in parts], axis=0)
                one = mm(left, w[k, :, a:b], 1, 1)
                total = one if total is None else total + one
            return total

        shape = (NX, 2, rows // 2, block)

        def p_rows(s):
            x = place.get("x", SETS[s])
            p, xx = lax.div(x, NX // 2), lax.rem(x, NX // 2)
            return [lambda k, i=i: for_out(k, i, p, xx) for i in range(NY)]

        def q_rows(s, make):
            i = place.get("y", SETS[s])
            return [lambda k, p=p, xx=xx: make(k, i, p, xx) for p in range(2) for xx in range(NX // 2)]

        def place_of(d):
            return pl.ds(pl.multiple_of(d * block, block), block)

        def p_task(s):
            def body(d, w):
                p_tile[s % 2, :, :, :, place_of(d)] = product(p_rows(s), w, lo, cols).reshape(shape)

            def do():
                if s >= 2:
                    planes[0].clear(s - 2)
                blocks(s, 0, 0, nz - 1, body)
                planes[0].start(s)

            flow.task(P_TIME, do)

        def q_task(s):
            def body(d, w):
                q_tile[s % 2, :, :, :, place_of(d)] = product(q_rows(s, for_in), w, 0, hi).reshape(shape)

                @pl.when(d == nz - 1)
                def _():
                    q_tile[s % 2, :, :, :, width:] = product(q_rows(s, for_out), w, lo, cols).reshape(shape)

            def start():
                if s >= 2:
                    planes[1].clear(s - 2)
                blocks(s, 1, 0, nz // 2, body)

            def end():
                blocks(s, 1, nz // 2, nz - nz // 2, body)
                planes[1].start(s)

            flow.task(Q_HALF, start)
            flow.task(Q_HALF, end)

        def finish(out):
            def done(half, ref):
                out[half] = ref()[...]

            return done

        def free(task):
            return lambda s: task(s + 2) if s + 2 < len(SETS) else None

        planes = [
            Plane(place, flow, p_tile, p_land, "y", finish(p_sum), free(p_task)),
            Plane(place, flow, q_tile, q_land, "x", finish(q_sum), free(q_task)),
        ]

        for lane in range(3):
            grads.set_ready(lane, 0)
        q_task(0)
        p_task(0)
        grads.heads_first()
        grads.plus(1)
        grads.minus(1)
        p_task(1)
        q_task(1)
        flow.run()
        flow.close()
        grads.close()

    pl.run_scoped(
        second,
        pltpu.VMEM((2, NY, 2, rows // 2, width - block), f32),
        pltpu.VMEM((2, NX, 2, rows // 2, width + block), f32),
        pltpu.VMEM((3, NC, block, cols), bf16),
    )


STAGES = 6
PASSES = ((1, 0), (0, 0), (0, 1), (1, 1), (1, 2), (0, 2), (0, 3), (1, 3))
P_TIME = 3.0
Q_HALF = 2.6


def back(nz, z_in, h_all, dy_all, w_all, cos, sin):
    tokens, width = h_all.shape
    seq, head = cos.shape
    pair = 2 * head
    cols = w_all.shape[2]
    ff = (cols - pair) // 3
    rows = seq // (NX * NC)
    block = width // nz
    bf16, f32 = h_all.dtype, jnp.float32
    vmem = pl.BlockSpec(memory_space=pltpu.VMEM)
    dma = pltpu.SemaphoreType.DMA
    blocks = (NY, 2, NX // 2, NC, rows, pair)
    p_piece = (rows // 2, width - block)
    q_piece = (rows // 2, width + block)
    count = 6 + 2 * NY + 1 + 4 * (nz - 1) + 4 * 4 + 2 * 5 * 6
    return pl.pallas_call(
        functools.partial(back_kernel, nz),
        out_shape=(
            jax.ShapeDtypeStruct((2,) + p_piece, f32),
            jax.ShapeDtypeStruct((2,) + q_piece, f32),
            jax.ShapeDtypeStruct((NY, block // NY, cols), f32),
            jax.ShapeDtypeStruct((nz - 1, 4, block, ff), f32),
        ),
        in_specs=any_specs(4) + [vmem, vmem],
        out_specs=(vmem, vmem) + tuple(any_specs(2)),
        scratch_shapes=[
            pltpu.VMEM(z_in.shape, bf16),
            pltpu.VMEM(blocks, bf16),
            pltpu.VMEM(blocks, bf16),
            pltpu.VMEM(blocks[1:], bf16),
            pltpu.VMEM(blocks[:-1] + (3 * ff,), bf16),
            pltpu.VMEM(blocks[:3] + (rows, cols), bf16),
            pltpu.VMEM((4, block // NY, ff), f32),
            pltpu.VMEM((5, 6) + p_piece, f32),
            pltpu.VMEM((5, 6) + q_piece, f32),
            pltpu.VMEM((seq, head), bf16),
            pltpu.VMEM((seq, head), bf16),
            pltpu.VMEM((seq, head), f32),
            pltpu.VMEM((seq, head), f32),
            pltpu.VMEM((tokens, block), bf16),
            pltpu.VMEM((tokens, block), bf16),
            pltpu.VMEM((tokens, block), bf16),
            pltpu.VMEM((2, 4, block, ff), f32),
            pltpu.VMEM((STAGES, block, ff), f32),
            dma,
            dma((3, 2)),
            dma((3,)),
            dma((3,)),
            dma((STAGES,)),
            dma((4,)),
            dma((count,)),
            dma((count,)),
        ],
        compiler_params=pltpu.CompilerParams(collective_id=2, has_side_effects=True, vmem_limit_bytes=VMEM_LIMIT),
        name="back",
    )(z_in, h_all, dy_all, w_all, cos, sin)[:3]


def norm_fwd(row_vals, norm_gain):
    return row_vals * lax.rsqrt(jnp.mean(row_vals * row_vals, axis=-1, keepdims=True) + NORM_EPS) * norm_gain


def solution(mesh):
    act_spec = P("fsdp", "model", None)
    col_spec = P("fsdp", "model")
    row_spec = P("model", "fsdp")
    nz = mesh.shape["fsdp"] // NY

    def layer_body(x_in, dy_in, norm_gain, w_qkv, w_out, w_gate, w_up, w_down, rope_cos, rope_sin):
        bf16 = jnp.bfloat16
        _, rows, width = x_in.shape
        slab = w_qkv.shape[0]
        head = 2 * rope_cos.shape[1]
        group = w_out.shape[0] // head
        seq = rows * NX * NC
        ff = w_gate.shape[1] // NY

        x_rows = x_in[0].astype(jnp.float32)
        normed, norm_pull = jax.vjp(lambda row_vals: norm_fwd(row_vals, norm_gain), x_rows)
        h_loc = normed.astype(bf16).reshape(2, rows // 2, width)
        dy_loc = dy_in.reshape(2, rows // 2, width)
        q, k, v = w_qkv[:, : group * head], w_qkv[:, group * head : -head], w_qkv[:, -head:]
        out_t, down_t = w_out.T, w_down.T
        parts = []
        for i in range(NY):
            at = slice(i * head, (i + 1) * head)
            ffs = slice(i * ff, (i + 1) * ff)
            heads = [q[:, at], out_t[:, at]] if i < NY - 1 else [k, v]
            parts.append(jnp.concatenate([w_gate[:, ffs], w_up[:, ffs]] + heads + [down_t[:, ffs]], axis=1))
        w_loc = jnp.stack(parts)
        cos = jnp.concatenate([rope_cos, rope_cos], axis=1)
        sin = jnp.concatenate([-rope_sin, rope_sin], axis=1)

        h_all, dy_all, w_all = gather(nz, h_loc, dy_loc, w_loc)
        tokens = NY * seq
        cols = w_loc.shape[2]
        h_all = h_all.reshape(tokens, width)
        dy_all = dy_all.reshape(tokens, width)
        w_all = w_all.reshape(NC, width, cols)
        z_got = head_rows(nz, 2 * head, seq, h_all, dy_all, w_all)
        p_sum, q_sum, g_sum = back(nz, z_got, h_all, dy_all, w_all, cos, sin)
        p_sum = p_sum.reshape(rows, -1)
        q_sum = q_sum.reshape(rows, -1)

        y_sum = jnp.concatenate([p_sum, q_sum[:, width:]], axis=1)
        y_out = (x_rows + y_sum).astype(bf16)
        d_h = q_sum[:, :width].astype(bf16)
        dx_out = (dy_in[0].astype(jnp.float32) + norm_pull(d_h.astype(jnp.float32))[0]).astype(bf16)
        lo = 2 * ff
        mid = lo + head
        hi = mid + head

        def take(first, end, n=NY):
            return jnp.concatenate([g_sum[i, :, first:end] for i in range(n)], axis=1)

        return (
            y_out[None],
            dx_out[None],
            jnp.concatenate([take(lo, mid), g_sum[NY - 1, :, mid:hi]], axis=1),
            take(mid, hi, group).T,
            take(0, ff),
            take(ff, lo),
            take(hi, cols).T,
        )

    return jax.shard_map(
        layer_body,
        mesh=mesh,
        in_specs=(act_spec, act_spec, P(), col_spec, row_spec, col_spec, col_spec, row_spec, P(), P()),
        out_specs=(act_spec, act_spec, col_spec, row_spec, col_spec, col_spec, row_spec),
        check_vma=False,
    )
```

```python
import functools
import heapq

import jax
import jax.numpy as jnp
from jax import lax
from jax.experimental import pallas as pl
from jax.experimental.pallas import tpu as pltpu
from jax.sharding import PartitionSpec as P

NORM_EPS = 1e-5
NY, NX, NC = 4, 4, 2
MESH = pl.DeviceIdType.MESH
LINK = 46.6e3
PAIR = 330e3
LOCAL = 1500e3
HOP = 3.5
ADD = 0.4
VMEM_LIMIT = 67043328


class Place:
    def __init__(self, nz):
        i, j = lax.axis_index("fsdp"), lax.axis_index("model")
        self.size = {"z": nz, "y": NY, "x": NX, "c": NC}
        self.at = {"z": lax.div(i, NY), "y": lax.rem(i, NY), "x": lax.div(j, NC), "c": lax.rem(j, NC)}

    def get(self, axis, step=0):
        n = self.size[axis]
        return lax.rem(self.at[axis] + (step + 2 * n) % n, n)

    def device(self, axis, step):
        at = dict(self.at)
        at[axis] = self.get(axis, step)
        return {"fsdp": at["z"] * NY + at["y"], "model": at["x"] * NC + at["c"]}

    def meet(self, peers):
        barrier = pltpu.get_barrier_semaphore()
        for axis, step in peers:
            pl.semaphore_signal(barrier, inc=1, device_id=self.device(axis, step), device_id_type=MESH)
        pl.semaphore_wait(barrier, len(peers))


class Flow:
    def __init__(self, place, send_sem, recv_sem, base=0, now=0.0):
        self.place, self.send_sem, self.recv_sem, self.base = place, send_sem, recv_sem, base
        self.now, self.free, self.events, self.copies, self.tasks, self.order = now, {}, [], [], [], 0
        self.sent = set()

    def event(self, when, wait, then):
        heapq.heappush(self.events, (when, self.order, wait, then))
        self.order += 1

    def send(self, axis, step, src, dst, size, then=None, link=None):
        k = len(self.copies)
        link = link or (axis, step)
        begin = max(self.now, self.free.get(link, 0.0))
        rate, lag = (PAIR, 1.5) if axis == "c" else (LINK, HOP)
        self.free[link] = begin + size / rate
        copy = pltpu.make_async_remote_copy(
            src_ref=src(),
            dst_ref=dst(),
            send_sem=self.send_sem.at[self.base + k],
            recv_sem=self.recv_sem.at[self.base + k],
            device_id=self.place.device(axis, step),
            device_id_type=MESH,
        )
        copy.start()
        self.copies.append(copy)
        self.event(self.free[link] + lag, copy.wait_recv, then)
        return k

    def at(self, when, then):
        self.event(when, lambda: None, then)

    def local(self, copy, size, then):
        copy.start()
        self.event(self.now + size / LOCAL + 1.0, copy.wait, then)

    def task(self, cost, do):
        self.tasks.append((cost, do))

    def take(self):
        when, _, wait, then = heapq.heappop(self.events)
        self.now = max(self.now, when)
        wait()
        if then is not None:
            then()

    def spend(self, cost):
        self.now += cost
        while self.events and self.events[0][0] <= self.now:
            self.take()

    def wait_sent(self, k):
        if k not in self.sent:
            self.copies[k].wait_send()
        self.sent.add(k)

    def run(self):
        while self.events or self.tasks:
            if self.tasks and (not self.events or self.events[0][0] > self.now):
                cost, do = self.tasks.pop(0)
                self.now += cost
                do()
            else:
                self.take()

    def close(self):
        for k in range(len(self.copies)):
            self.wait_sent(k)


def after(count, then):
    left = [count]

    def one():
        left[0] -= 1
        if left[0] == 0:
            then()

    return one


def nbytes(ref, lead):
    n = 1
    for d in ref.shape[lead:]:
        n *= d
    return n * jnp.dtype(ref.dtype).itemsize


def any_specs(n):
    return [pl.BlockSpec(memory_space=pl.ANY)] * n


def mm(a, b, ca, cb):
    return lax.dot_general(a, b, (((ca,), (cb,)), ((), ())), preferred_element_type=jnp.float32)


def span(q, n):
    return pl.ds(pl.multiple_of(q * n, n), n)


def exchange(flow, place, src, dst, far, step, done=None):
    size = nbytes(src, 1)

    def onward(way, half):
        def then():
            flow.send("y", way, lambda: far.at[half], lambda: dst.at[place.get("y", -way), half], size // 2, done)

        return then

    if step == 2:
        flow.send("y", 1, lambda: src.at[place.get("y", 2), 0], lambda: far.at[0], size // 2, onward(1, 0))
        flow.send("y", -1, lambda: src.at[place.get("y", 2), 1], lambda: far.at[1], size // 2, onward(-1, 1))
    else:
        flow.send("y", step, lambda: src.at[place.get("y", step)], lambda: dst.at[place.get("y")], size, done)


ORDER = (2, 1, -1, 0)


class Gather:
    def __init__(self, place, flow, own, full, first, cut, arrive):
        self.place, self.flow, self.own, self.full, self.first, self.cut, self.arrive = place, flow, own, full, first, cut, arrive
        self.second = "y" if first == "x" else "x"
        self.size = nbytes(own, 1) * (cut.stop - cut.start) // own.shape[-1]

    def mine(self, half):
        return lambda: self.own.at[half, :, self.cut]

    def spot(self, at, half):
        y, x, c = (self.place.get(axis, at.get(axis, 0)) for axis in "yxc")
        return lambda: self.full.at[y, x, c, half, :, self.cut]

    def spread(self, axis, at, half, src):
        def come(step, onward):
            def then():
                here = dict(at, **{axis: step})
                if onward:
                    far = dict(at, **{axis: 2})
                    self.flow.send(axis, -step, self.spot(here, half), self.spot(here, half), self.size, lambda: self.got(axis, far, half))
                self.got(axis, here, half)

            return then

        self.flow.send(axis, 1, src, self.spot(at, half), self.size, come(-1, half == 0))
        self.flow.send(axis, -1, src, self.spot(at, half), self.size, come(1, half == 1))

    def got(self, axis, at, half):
        if axis == self.first:
            self.spread(self.second, at, half, self.spot(at, half))
        self.pair(at, half, self.spot(at, half))
        self.arrive(at.get("y", 0), at.get("x", 0))

    def pair(self, at, half, src):
        there = lambda: self.arrive(at.get("y", 0), at.get("x", 0))
        self.flow.send("c", 1, src, self.spot(at, half), self.size, there)

    def start_first(self):
        for half in (0, 1):
            self.spread(self.first, {}, half, self.mine(half))

    def start_second(self):
        for half in (0, 1):
            self.spread(self.second, {}, half, self.mine(half))
            self.pair({}, half, self.mine(half))


def front_kernel(nz, h_ref, dy_ref, w_ref, h_all, dy_all, w_all, z_got, w_heads, rows_v, z_in, far, send_sem, recv_sem, own_sem, rows_sem):
    bf16 = jnp.bfloat16
    place = Place(nz)
    y, x, c, z = (place.get(axis) for axis in "yxcz")
    last = y == NY - 1
    pair = z_in.shape[-1]
    head = pair // 2
    width = h_ref.shape[-1]
    cols = w_ref.shape[-1]
    lo = (cols - pair) * 2 // 3
    hi = lo + pair
    rows = z_in.shape[2]
    flow = Flow(place, send_sem, recv_sem)
    w_own = pltpu.make_async_copy(w_ref.at[y], w_all.at[0, z, y], own_sem.at[2])
    w_own.start()
    w_heads[z, y] = w_ref[y, :, lo:hi]
    place.meet([("x", 1), ("x", -1), ("y", 1), ("y", -1), ("y", 2), ("z", 1), ("z", -1), ("c", 1)])

    slots = rows_v.shape[0]
    free, queue, ready = list(range(slots)), [], []
    pieces = {}
    parts_done = {}
    weights = [4 * nz]

    def load():
        while free and queue and weights[0] == 0:
            kind, dy, dx = queue.pop(0)
            slot = free.pop(0)
            src = (h_all, dy_all)[kind].at[place.get("y", dy), place.get("x", dx)]
            copy = pltpu.make_async_copy(src, rows_v.at[slot], rows_sem.at[slot])
            flow.local(copy, nbytes(rows_v, 1), lambda slot=slot, kind=kind, dy=dy, dx=dx: flow.task(CHUNK_TIME, lambda: product(kind, dy, dx, slot)))

    def arrive(kind):
        need = (8, 4)[kind]

        def one(dy, dx):
            key = (kind, dy, dx)
            pieces[key] = pieces.get(key, 0) + 1
            if pieces[key] == need:
                queue.append(key)
                load()

        return one

    def weight_come():
        weights[0] -= 1
        if weights[0] == 0:
            load()

    def product(kind, dy, dx, slot):
        at = place.get("y", dy), place.get("x", dx)
        step = 2 if nz % 2 == 0 else 1
        deep = step * (width // nz)

        def dot(first):
            def some(i, total):
                left = rows_v[slot, :, :, :, span(i, deep)].reshape(rows, deep)
                right = w_heads[pl.ds(i * step, step), :, :, first:].reshape(deep, pair - first)
                return total + mm(left, right, 1, 0)

            return lax.fori_loop(0, nz // step, some, jnp.zeros((rows, pair - first), jnp.float32))

        if kind == 0:
            made = dot(0).astype(bf16)
            z_in[at[0], at[1], :, :head] = made[:, :head]

            @pl.when(last)
            def _():
                z_in[at[0], at[1], :, head:] = made[:, head:]

        else:

            @pl.when(jnp.logical_not(last))
            def _():
                z_in[at[0], at[1], :, head:] = dot(head).astype(bf16)

        free.append(slot)
        load()
        parts_done[dy, dx] = parts_done.get((dy, dx), 0) + 1
        if parts_done[dy, dx] == 2:
            deliver(dy, dx)

    own_copies = []

    def deliver(dy, dx):
        at = lambda: z_in.at[place.get("y", dy), place.get("x", dx)]
        size = nbytes(z_in, 2)

        def there(step=0):
            return lambda: z_got.at[place.get("y", step), place.get("x", dx)]

        if dy == 0:
            copy = pltpu.make_async_copy(at(), there()(), own_sem.at[4 + dx % NX])
            copy.start()
            own_copies.append(copy)
        elif dy == 2:
            way = 1 if dx in (0, 2) else -1

            def onward():
                flow.send("y", way, lambda: far.at[dx % NX], there(-way), size)

            flow.send("y", way, at, lambda: far.at[dx % NX], size, onward)
        else:
            flow.send("y", dy, at, there(), size)

    def w_part(ref, who, dz, dy, cut):
        if ref is None:
            return lambda: w_heads.at[place.get("z", dz), place.get("y", dy)]
        return lambda: w_all.at[who, place.get("z", dz), place.get("y", dy), :, cut]

    cuts = [slice(lo, hi), slice(0, lo), slice(hi, cols)]

    def ring(step, dy, n_cut, src=None, hops=nz - 1, lead=True):
        cut = cuts[n_cut]
        home = None if n_cut == 0 else w_all
        size = nbytes(w_ref, 1) * (cut.stop - cut.start) // cols

        def hop(n):
            def then():
                here = src if src and n == 0 else w_part(home, 0, -step * n, dy, cut)
                if n < hops:
                    flow.send("z", step, here, w_part(home, 0, -step * n, dy, cut), size, hop(n + 1))
                if n or lead:
                    flow.send("c", 1, here, w_part(w_all, 1, -step * n, dy, cut), size)
                    if n_cut == 0:
                        weight_come()

            return then

        return hop(0)

    def rings(dy, n_cut, src=None):
        if n_cut:
            return ring(1 if dy in (0, 1) else -1, dy, n_cut, src)
        both = [ring(1, dy, 0, src, nz // 2), ring(-1, dy, 0, src, (nz - 1) // 2, False)]
        return lambda: [one() for one in both]

    def w_at(dy, cut):
        return lambda: w_ref.at[place.get("y", dy), :, cut]

    tail = width // nz * H_TAIL
    gathers = [
        Gather(place, flow, h_ref, h_all, "x", slice(0, width - tail), arrive(0)),
        Gather(place, flow, dy_ref, dy_all, "y", slice(0, width), arrive(1)),
        Gather(place, flow, h_ref, h_all, "y", slice(width - tail, width), arrive(0)),
    ]
    def w_start(n_cut, dys):
        cut = cuts[n_cut]
        home = None if n_cut == 0 else w_all
        size = nbytes(w_ref, 1) * (cut.stop - cut.start) // cols
        there = w_part(home, 0, 0, 0, cut)
        for dy in dys:
            if dy == 0:
                rings(0, n_cut, w_at(0, cut))()
            elif dy == 2:
                flow.send("y", 2, w_at(2, cut), there, size, rings(2, n_cut), link=("y", 1))
            else:
                flow.send("y", -dy, w_at(-dy, cut), there, size, rings(dy, n_cut))

    w_start(0, (0, 1, -1, 2))
    for one in gathers:
        one.start_first()
    flow.at(W_TIMES[0], lambda: [w_start(1, (0, -1)), w_start(2, (0, -1))])
    flow.at(W_TIMES[1], lambda: [w_start(1, (1, 2)), w_start(2, (1, 2))])
    for one in gathers:
        one.start_second()
    for n, (ref, full) in enumerate(((h_ref, h_all), (dy_ref, dy_all))):
        copy = pltpu.make_async_copy(ref, full.at[y, x, c], own_sem.at[n])
        there = arrive(n)
        flow.local(copy, nbytes(ref, 0), lambda n=n, there=there: [there(0, 0) for _ in range((4, 2)[n])])
    flow.run()
    heads_home = pltpu.make_async_copy(w_heads, w_all.at[0, :, :, :, lo:hi], own_sem.at[3])
    w_own.wait()
    heads_home.start()
    flow.close()
    for copy in own_copies:
        copy.wait()
    heads_home.wait()


CHUNK_TIME = 1.0
W_TIMES = (0.0, 0.0)
H_TAIL = 1


def front(nz, pair, h, dy, w):
    half, rows, width = h.shape
    everywhere = (NY, NX, NC) + h.shape
    cols = w.shape[-1]
    gathers = 3 * (30 + 32)
    count = gathers + 3 * 3 + 3 * 4 * (nz - 1) + 3 * 4 * nz + 2 * NX + 2 * NX
    vmem = pl.BlockSpec(memory_space=pltpu.VMEM)
    dma = pltpu.SemaphoreType.DMA
    chunk = NC * half * rows
    z_shape = (NY, NX, chunk, pair)
    slots = 8
    return pl.pallas_call(
        functools.partial(front_kernel, nz),
        out_shape=(
            jax.ShapeDtypeStruct(everywhere, h.dtype),
            jax.ShapeDtypeStruct(everywhere, dy.dtype),
            jax.ShapeDtypeStruct((NC, nz) + w.shape, w.dtype),
            jax.ShapeDtypeStruct(z_shape, h.dtype),
        ),
        in_specs=[vmem] * 3,
        out_specs=tuple(any_specs(4)),
        scratch_shapes=[
            pltpu.VMEM((nz,) + w.shape[:-1] + (pair,), w.dtype),
            pltpu.VMEM((slots, NC) + h.shape, h.dtype),
            pltpu.VMEM(z_shape, h.dtype),
            pltpu.VMEM((NX, chunk, pair), h.dtype),
            dma((count,)),
            dma((count,)),
            dma((4 + NX,)),
            dma((slots,)),
        ],
        compiler_params=pltpu.CompilerParams(collective_id=0, has_side_effects=True, vmem_limit_bytes=VMEM_LIMIT),
        name="front",
    )(h, dy, w)


SETS = (2, 1, -1, 0)


def attention(z_got, z_back, keys, vals, dk, dv, cos_ref, sin_ref):
    bf16 = jnp.bfloat16
    seq, head = keys.shape
    part = seq // 2
    count = z_got.shape[0] - 1
    scale = head**-0.5
    spread = z_back.shape[2:5] + (head,)
    halves = [pl.ds(p * part, part) for p in range(2)]

    def turn(values, at, sign):
        wide = values.astype(jnp.float32)
        swapped = pltpu.roll(wide, head // 2, 1)
        return (wide * cos_ref[at, :] + sign * (swapped * sin_ref[at, :])).astype(bf16)

    for p in range(2):
        keys[halves[p], :] = turn(z_got[count, p, :, :head], halves[p], 1.0)
        vals[halves[p], :] = z_got[count, p, :, head:]
    dk[...] = jnp.zeros_like(dk)
    dv[...] = jnp.zeros_like(dv)

    @pl.loop(0, count)
    def _(i):
        for p in range(2):
            n = (p + 1) * part
            query = turn(z_got[i, p, :, :head], halves[p], 1.0)
            d_out = z_got[i, p, :, head:]
            scores = mm(query, keys[:n, :], 1, 1) * scale
            causal = lax.broadcasted_iota(jnp.int32, scores.shape, 0) + p * part >= lax.broadcasted_iota(jnp.int32, scores.shape, 1)
            scores = jnp.where(causal, scores, -1e30)
            grown = jnp.exp(scores - jnp.max(scores, axis=1, keepdims=True))
            probs = grown / jnp.sum(grown, axis=1, keepdims=True)
            probs_low = probs.astype(bf16)
            z_back[i, p, :, :, :, head:] = mm(probs_low, vals[:n, :], 1, 0).astype(bf16).reshape(spread)
            d_probs = mm(d_out, vals[:n, :], 1, 1).astype(bf16).astype(jnp.float32)
            d_scores = (probs * (d_probs - jnp.sum(probs * d_probs, axis=1, keepdims=True)) * scale).astype(bf16)
            z_back[i, p, :, :, :, :head] = turn(mm(d_scores, keys[:n, :], 1, 0).astype(bf16), halves[p], -1.0).reshape(spread)
            dk[:n, :] += mm(d_scores, query, 0, 0)
            dv[:n, :] += mm(probs_low, d_out, 0, 0)

    for p in range(2):
        z_back[count, p, :, :, :, :head] = turn(dk[halves[p], :].astype(bf16), halves[p], -1.0).reshape(spread)
        z_back[count, p, :, :, :, head:] = dv[halves[p], :].astype(bf16).reshape(spread)


def gated(place, flow, h_all, dy_all, w_all, acts, row_sem, share, h_rows, dy_rows, w_v):
    bf16 = jnp.bfloat16
    ff = acts.shape[-1] // 3
    lo = 2 * ff
    part = h_rows.shape[1]
    shape = acts.shape[2:5] + (ff,)
    w_loads = [
        pltpu.make_async_copy(w_all.at[0, :, :lo], w_v.at[:, :lo], row_sem.at[2, 0]),
        pltpu.make_async_copy(w_all.at[0, :, w_all.shape[2] - ff :], w_v.at[:, lo:], row_sem.at[2, 1]),
    ]

    def loads(n, slot):
        return [pltpu.make_async_copy(a.at[span(n, part)], b.at[slot], row_sem.at[slot, m]) for m, (a, b) in enumerate(((h_all, h_rows), (dy_all, dy_rows)))]

    def begin():
        for copy in w_loads + loads(0, 0) + loads(1, 1):
            copy.start()

    def go():
        for copy in w_loads:
            copy.wait()
        for q in range(NY):

            @pl.loop(0, 2)
            def _(p):
                n = 2 * q + p
                for copy in loads(n, p):
                    copy.wait()
                gate = mm(h_rows[p], w_v[:, :ff], 1, 0).astype(bf16).astype(jnp.float32)
                up = mm(h_rows[p], w_v[:, ff:lo], 1, 0).astype(bf16).astype(jnp.float32)
                d_act = mm(dy_rows[p], w_v[:, lo:], 1, 0).astype(bf16).astype(jnp.float32)
                if q < NY - 1:
                    for copy in loads(n + 2, p):
                        copy.start()
                sig = jax.nn.sigmoid(gate)
                silu = gate * sig
                acts[q, p, :, :, :, :ff] = (d_act * up * (sig + silu * (1.0 - sig))).astype(bf16).reshape(shape)
                acts[q, p, :, :, :, ff:lo] = (d_act * silu).astype(bf16).reshape(shape)
                acts[q, p, :, :, :, lo:] = (silu * up).astype(bf16).reshape(shape)

            share(q)
            flow.spend(3.0)

    return begin, go


class Plane:
    def __init__(self, place, flow, tiles, land, first, finish, free):
        self.place, self.flow, self.tiles, self.land, self.first = place, flow, tiles, land, first
        self.second = "y" if first == "x" else "x"
        self.piece = nbytes(tiles, 3)
        self.sums, self.waiting, self.finished = {}, {}, [0] * len(SETS)
        self.free = free
        self.rings = []
        for s, other in enumerate(SETS):

            def raw(step, half, s=s):
                return lambda: tiles.at[s % 2, place.get(first, step), half]

            self.rings.append(self.ring(first, raw, lambda step, half, then: then(), s, self.first_done(s, other)))
        self.onward, _ = self.ring(self.second, lambda step, half: self.sums[step, half], self.need, len(SETS), finish)

    def need(self, step, half, then):
        if (step, half) in self.sums:
            then()
        else:
            self.waiting.setdefault((step, half), []).append(then)

    def first_done(self, s, step):
        def done(half, ref):
            self.sums[step, half] = ref
            for then in self.waiting.pop((step, half), []):
                then()
            self.onward(step, half)
            self.finished[s] += 1
            if self.finished[s] == 2:
                self.free(s)

        return done

    def add(self, mine, other):
        a, b = mine(), other()
        a[...] = a[...] + b[...]
        self.flow.now += ADD

    def ring(self, axis, raw, need, s, done):
        flow, add, sent = self.flow, self.add, []

        def slot(i):
            return lambda: self.land.at[s, i]

        def turn(i, goal, half, step):
            def then():
                add(slot(i), raw(goal, half))
                flow.send(axis, step, slot(i), slot(i + 4), self.piece, final[half])

            return lambda: need(goal, half, then)

        def ending(half):
            def then():
                mine, other = (slot(5), slot(2)) if half == 0 else (slot(4), slot(3))
                add(mine, other)
                add(mine, raw(0, half))
                done(half, mine)

            return lambda: need(0, half, then)

        final = [after(2, ending(0)), after(2, ending(1))]
        moves = {
            (2, 1): (1, 0, turn(0, 1, 1, 1)),
            (2, 0): (-1, 1, turn(1, -1, 0, -1)),
            (1, 0): (1, 2, final[0]),
            (-1, 1): (-1, 3, final[1]),
        }

        def start(goal, half):
            if (goal, half) in moves:
                step, i, then = moves[goal, half]
                sent.append(flow.send(axis, step, raw(goal, half), slot(i), self.piece, then))

        return start, sent

    def start(self, s):
        for goal, half in ((2, 1), (2, 0), (1, 0), (-1, 1)):
            self.rings[s][0](goal, half)

    def clear(self, s):
        for k in self.rings[s][1]:
            self.flow.wait_sent(k)


class Grads:
    flow = None


    def __init__(self, nz, place, h_all, dy_all, acts, z_out, z_land, g_sum, far, h_plus, h_minus, dy_minus, tiles, stage, load_sem, stage_sem, own_sem):
        self.__dict__.update({k: v for k, v in locals().items() if k != "self"})
        self.ff = acts.shape[-1] // 3
        self.pair = z_out.shape[-1]
        lo = 2 * self.ff
        self.cols = [(0, self.ff), (self.ff, lo), (lo + self.pair, lo + self.pair + self.ff), (lo, lo + self.pair)]
        self.way = (1, 1, -1, -1)
        self.far_way = (1, -1, 1, -1)
        self.block = tiles.shape[2]
        self.size = nbytes(tiles, 2)
        self.ready, self.waiting, self.used = set(), {}, 0
        self.users = [[] for _ in range(stage.shape[0])]
        self.own = []
        self.idle, self.first = {}, {}

    def load(self, ref, src, index, step, n):
        b = self.place.get("z", -step * (n + 1))
        at = pl.ds(pl.multiple_of(b * self.block, self.block), self.block)
        return pltpu.make_async_copy(src.at[:, at], ref, self.load_sem.at[index])

    def loads_plus(self, n):
        return [self.load(self.h_plus, self.h_all, 0, 1, n)]

    def loads_minus(self, n):
        return [self.load(self.h_minus, self.h_all, 1, -1, n), self.load(self.dy_minus, self.dy_all, 2, -1, n)]

    def begin(self):
        for copy in self.loads_plus(0) + self.loads_minus(0):
            copy.start()

    def gather_up(self, tiles, some):
        seq = self.h_plus.shape[0] // NY
        for tile in tiles:
            tile[...] = jnp.zeros_like(tile)

        @pl.loop(0, NY)
        def _(q):
            for tile, value in zip(tiles, some(q, span(q, seq))):
                tile[...] += value

    def set_ready(self, lane, n):
        self.ready.add((lane, n))
        for then in self.waiting.pop((lane, n), []):
            then()
        if n == 0:
            k = self.flow.send("z", self.way[lane], lambda: self.tiles.at[0, lane], lambda: self.z_land.at[0, lane], self.size, self.hop(lane, 0))
            self.first[lane] = k

    def clear(self, lane, n):
        if n == 2:
            self.flow.wait_sent(self.first[lane])

    def tokens(self, ref):
        value = ref[...]
        return value.reshape(-1, value.shape[-1])

    def make_plus(self, n):
        for copy in self.loads_plus(n):
            copy.wait()
        lo = 2 * self.ff

        def some(q, rows):
            both = mm(self.h_plus[rows, :], self.acts[q, :, :, :, :, :lo].reshape(-1, lo), 0, 0)
            return both[:, : self.ff], both[:, self.ff :]

        self.gather_up([self.tiles.at[n % 2, 0], self.tiles.at[n % 2, 1]], some)
        if n + 1 < self.nz:
            for copy in self.loads_plus(n + 1):
                copy.start()

    def for_down(self, q, rows):
        return [mm(self.dy_minus[rows, :], self.acts[q, :, :, :, :, 2 * self.ff :].reshape(-1, self.ff), 0, 0)]

    def for_heads(self, q, rows):
        last = self.place.get("y") == NY - 1
        head = self.pair // 2
        out = self.z_out[q].reshape(-1, self.pair)
        both = mm(self.h_minus[rows, :], out, 0, 0)
        right = jnp.where(last, both[:, head:], mm(self.dy_minus[rows, :], out[:, head:], 0, 0))
        return [jnp.concatenate([both[:, :head], right], axis=1)]

    def make_minus(self, n):
        for copy in self.loads_minus(n):
            copy.wait()
        self.gather_up([self.tiles.at[n % 2, 2], self.tiles.at[n % 2, 3]], lambda q, rows: self.for_down(q, rows) + self.for_heads(q, rows))
        self.load_minus_next(n)

    def load_minus_next(self, n):
        if n + 1 < self.nz:
            for copy in self.loads_minus(n + 1):
                copy.start()

    def make_first(self):
        self.make_plus(0)
        for copy in self.loads_minus(0):
            copy.wait()
        self.gather_up([self.tiles.at[0, 2]], self.for_down)

    def heads_first(self):
        def do():
            self.gather_up([self.tiles.at[0, 3]], self.for_heads)
            self.load_minus_next(0)
            self.set_ready(3, 0)

        self.flow.task(1.3, do)

    def plus(self, n):
        def do():
            for lane in (0, 1):
                self.clear(lane, n)
            self.make_plus(n)
            for lane in (0, 1):
                self.set_ready(lane, n)

        self.flow.task(1.6, do)

    def minus(self, n):
        def do():
            for lane in (2, 3):
                self.clear(lane, n)
            self.make_minus(n)
            for lane in (2, 3):
                self.set_ready(lane, n)

        self.flow.task(2.2, do)

    def need(self, lane, n, then):
        if (lane, n) in self.ready:
            then()
        else:
            self.waiting.setdefault((lane, n), []).append(then)

    def next(self, lane, n):
        if n + 2 >= self.nz:
            return
        key = (lane // 2, n)
        self.idle[key] = self.idle.get(key, 0) + 1
        if self.idle[key] == 2:
            (self.plus, self.minus)[lane // 2](n + 2)

    def hop(self, lane, s):
        flow, place = self.flow, self.place

        def come():
            slot = self.used % len(self.users)
            self.used += 1
            for wait in self.users[slot]:
                wait()
            self.users[slot] = []
            here = lambda: self.stage.at[slot]

            def staged():
                self.need(lane, s + 1, use)

            def use():
                ref = here()
                ref[...] = ref[...] + self.tiles[(s + 1) % 2, lane]
                flow.now += ADD
                if s == 0:
                    self.next(lane, 0)
                self.next(lane, s + 1)
                if s + 1 < self.nz - 1:
                    k = flow.send("z", self.way[lane], here, lambda: self.z_land.at[s + 1, lane], self.size, self.hop(lane, s + 1))
                    self.users[slot].append(lambda: flow.wait_sent(k))
                else:
                    self.home(lane, slot)

            flow.local(pltpu.make_async_copy(self.z_land.at[s, lane], here(), self.stage_sem.at[slot]), self.size, staged)

        return come

    def home(self, lane, slot):
        flow, place = self.flow, self.place
        slab = self.block // NY
        first, end = self.cols[lane]

        def rows(step):
            return lambda: self.stage.at[slot, pl.ds(pl.multiple_of(place.get("y", step) * slab, slab), slab)]

        def mine(step=0):
            return lambda: self.g_sum.at[place.get("y", step), :, first:end]

        size = self.size // NY
        way = self.far_way[lane]

        def onward():
            flow.send("y", way, lambda: self.far.at[lane], mine(-way), size)

        sent = [flow.send("y", way, rows(2), lambda: self.far.at[lane], size, onward)]
        sent += [flow.send("y", step, rows(step), mine(), size) for step in (1, -1)]
        copy = pltpu.make_async_copy(rows(0)(), mine()(), self.own_sem.at[lane])
        copy.start()
        self.users[slot] += [functools.partial(flow.wait_sent, k) for k in sent] + [copy.wait]

    def close(self):
        for users in self.users:
            for wait in users:
                wait()


def back_kernel(
    nz,
    z_in,
    h_all,
    dy_all,
    w_all,
    cos_ref,
    sin_ref,
    p_sum,
    q_sum,
    g_sum,
    z_land,
    z_got,
    z_back,
    z_out,
    far_back,
    acts,
    pair_acts,
    far,
    p_land,
    q_land,
    keys,
    vals,
    dk,
    dv,
    h_plus,
    h_minus,
    dy_minus,
    tiles,
    stage,
    load_sem,
    row_sem,
    w_sem,
    g_load_sem,
    stage_sem,
    own_sem,
    send_sem,
    recv_sem,
):
    bf16, f32 = jnp.bfloat16, jnp.float32
    place = Place(nz)
    y, c = place.get("y"), place.get("c")
    other = place.get("c", 1)
    last = y == NY - 1
    seq, head = keys.shape
    pair = 2 * head
    rows, cols = pair_acts.shape[3:]
    ff = (cols - pair) // 3
    lo, hi = 2 * ff, 2 * ff + pair
    tokens, width = h_all.shape
    block = width // nz
    part = seq // 2

    z_load = pltpu.make_async_copy(z_in, z_got, load_sem)
    z_load.start()
    early = Flow(place, send_sem, recv_sem)
    peers = [("x", 1), ("x", -1), ("y", 1), ("y", -1), ("z", 1), ("z", -1), ("c", 1)]

    def share(q):
        early.send("c", 1, lambda: acts.at[q, :, :, other, :, :lo], lambda: pair_acts.at[q, :, :, :, :lo], nbytes(pair_acts, 1) * lo // cols)
        early.send("c", 1, lambda: acts.at[q, :, :, other, :, lo:], lambda: pair_acts.at[q, :, :, :, hi:], nbytes(pair_acts, 1) * ff // cols)

    def all_out():
        early.send("c", 1, lambda: z_out.at[:, :, :, other], lambda: pair_acts.at[:, :, :, :, lo:hi], nbytes(z_out, 0) // NC)

    grads = Grads(nz, place, h_all, dy_all, acts, z_out, z_land, g_sum, far, h_plus, h_minus, dy_minus, tiles, stage, g_load_sem, stage_sem, own_sem)

    def first(h_rows, dy_rows, w_v):
        begin, go = gated(place, early, h_all, dy_all, w_all, acts, row_sem, share, h_rows, dy_rows, w_v)
        begin()
        grads.begin()
        z_load.wait()
        attention(z_got, z_back, keys, vals, dk, dv, cos_ref, sin_ref)
        place.meet(peers)
        out_done = after(4, all_out)
        for step in ORDER[:3]:
            exchange(early, place, z_back, z_out, far_back, step, out_done)
        z_out[y] = z_back[y]
        go()
        grads.make_first()
        early.now += 2.6
        early.run()
        early.close()

    pl.run_scoped(
        first,
        pltpu.VMEM((2, part, width), bf16),
        pltpu.VMEM((2, part, width), bf16),
        pltpu.VMEM((width, 3 * ff), bf16),
    )

    def second(p_tile, q_tile, w_v):
        flow = Flow(place, send_sem, recv_sem, len(early.copies), early.now)
        grads.flow = flow
        lane = lax.broadcasted_iota(jnp.int32, (rows, pair), 1)
        for_d = jnp.logical_or(lane < head, last)

        def chunk(k, i, p, xx):
            if k == 0:
                own = acts[i, p, xx, c]
                return own[:, :lo], z_out[i, p, xx, c], own[:, lo:]
            theirs = pair_acts[i, p, xx]
            return theirs[:, :lo], theirs[:, lo:hi], theirs[:, hi:]

        def for_out(k, i, p, xx):
            _, mixed, act = chunk(k, i, p, xx)
            return jnp.concatenate([jnp.where(for_d, jnp.zeros_like(mixed), mixed), act], axis=1)

        def for_in(k, i, p, xx):
            grad, mixed, _ = chunk(k, i, p, xx)
            return jnp.concatenate([grad, jnp.where(for_d, mixed, jnp.zeros_like(mixed))], axis=1)

        depth = w_v.shape[0]

        def w_copy(kind, d, slot):
            at = pl.ds(pl.multiple_of(d * block, block), block)
            cut = slice(lo, cols) if kind == 0 else slice(0, cols)
            return pltpu.make_async_copy(w_all.at[:, at, cut], w_v.at[slot, :, :, cut], w_sem.at[slot])

        counts = (nz - 1, nz)
        base, total = [], 0
        for kind, _ in PASSES:
            base.append(total)
            total += counts[kind]
        kind = PASSES[0][0]
        for n in range(depth):
            w_copy(kind, n, n).start() if n < counts[kind] else w_copy(PASSES[1][0], n - counts[kind], n).start()
        turn = [0]

        def blocks(s, kind, first, count, body):
            n = turn[0]
            assert PASSES[n] == (kind, s)
            if first + count == counts[kind]:
                turn[0] += 1

            @pl.loop(first, first + count)
            def _(d):
                slot = lax.rem(base[n] + d, depth)
                w_copy(kind, d, slot).wait()
                body(d, w_v.at[slot])

                @pl.when(d + depth < counts[kind])
                def _():
                    w_copy(kind, d + depth, slot).start()

                if n + 1 < len(PASSES):

                    @pl.when(d + depth >= counts[kind])
                    def _():
                        w_copy(PASSES[n + 1][0], d + depth - counts[kind], slot).start()

        def product(parts, w, a, b):
            total = None
            for k in range(NC):
                left = jnp.concatenate([one(k) for one in parts], axis=0)
                one = mm(left, w[k, :, a:b], 1, 1)
                total = one if total is None else total + one
            return total

        shape = (NX, 2, rows // 2, block)

        def p_rows(s):
            x = place.get("x", SETS[s])
            p, xx = lax.div(x, NX // 2), lax.rem(x, NX // 2)
            return [lambda k, i=i: for_out(k, i, p, xx) for i in range(NY)]

        def q_rows(s, make):
            i = place.get("y", SETS[s])
            return [lambda k, p=p, xx=xx: make(k, i, p, xx) for p in range(2) for xx in range(NX // 2)]

        def place_of(d):
            return pl.ds(pl.multiple_of(d * block, block), block)

        def p_task(s):
            def body(d, w):
                p_tile[s % 2, :, :, :, place_of(d)] = product(p_rows(s), w, lo, cols).reshape(shape)

            def do():
                if s >= 2:
                    planes[0].clear(s - 2)
                blocks(s, 0, 0, nz - 1, body)
                planes[0].start(s)

            flow.task(P_TIME, do)

        def q_task(s):
            def body(d, w):
                q_tile[s % 2, :, :, :, place_of(d)] = product(q_rows(s, for_in), w, 0, hi).reshape(shape)

                @pl.when(d == nz - 1)
                def _():
                    q_tile[s % 2, :, :, :, width:] = product(q_rows(s, for_out), w, lo, cols).reshape(shape)

            def start():
                if s >= 2:
                    planes[1].clear(s - 2)
                blocks(s, 1, 0, nz // 2, body)

            def end():
                blocks(s, 1, nz // 2, nz - nz // 2, body)
                planes[1].start(s)

            flow.task(Q_HALF, start)
            flow.task(Q_HALF, end)

        def finish(out):
            def done(half, ref):
                out[half] = ref()[...]

            return done

        def free(task):
            return lambda s: task(s + 2) if s + 2 < len(SETS) else None

        planes = [
            Plane(place, flow, p_tile, p_land, "y", finish(p_sum), free(p_task)),
            Plane(place, flow, q_tile, q_land, "x", finish(q_sum), free(q_task)),
        ]

        for lane in range(3):
            grads.set_ready(lane, 0)
        q_task(0)
        p_task(0)
        grads.heads_first()
        grads.plus(1)
        grads.minus(1)
        p_task(1)
        q_task(1)
        flow.run()
        flow.close()
        grads.close()

    pl.run_scoped(
        second,
        pltpu.VMEM((2, NY, 2, rows // 2, width - block), f32),
        pltpu.VMEM((2, NX, 2, rows // 2, width + block), f32),
        pltpu.VMEM((3, NC, block, cols), bf16),
    )


STAGES = 6
PASSES = ((1, 0), (0, 0), (0, 1), (1, 1), (1, 2), (0, 2), (0, 3), (1, 3))
P_TIME = 3.0
Q_HALF = 2.6


def back(nz, z_in, h_all, dy_all, w_all, cos, sin):
    tokens, width = h_all.shape
    seq, head = cos.shape
    pair = 2 * head
    cols = w_all.shape[2]
    ff = (cols - pair) // 3
    rows = seq // (NX * NC)
    block = width // nz
    bf16, f32 = h_all.dtype, jnp.float32
    vmem = pl.BlockSpec(memory_space=pltpu.VMEM)
    dma = pltpu.SemaphoreType.DMA
    blocks = (NY, 2, NX // 2, NC, rows, pair)
    p_piece = (rows // 2, width - block)
    q_piece = (rows // 2, width + block)
    count = 6 + 2 * NY + 1 + 4 * (nz - 1) + 4 * 4 + 2 * 5 * 6
    return pl.pallas_call(
        functools.partial(back_kernel, nz),
        out_shape=(
            jax.ShapeDtypeStruct((2,) + p_piece, f32),
            jax.ShapeDtypeStruct((2,) + q_piece, f32),
            jax.ShapeDtypeStruct((NY, block // NY, cols), f32),
            jax.ShapeDtypeStruct((nz - 1, 4, block, ff), f32),
        ),
        in_specs=any_specs(4) + [vmem, vmem],
        out_specs=(vmem, vmem) + tuple(any_specs(2)),
        scratch_shapes=[
            pltpu.VMEM(z_in.shape, bf16),
            pltpu.VMEM(blocks, bf16),
            pltpu.VMEM(blocks, bf16),
            pltpu.VMEM(blocks[1:], bf16),
            pltpu.VMEM(blocks[:-1] + (3 * ff,), bf16),
            pltpu.VMEM(blocks[:3] + (rows, cols), bf16),
            pltpu.VMEM((4, block // NY, ff), f32),
            pltpu.VMEM((5, 6) + p_piece, f32),
            pltpu.VMEM((5, 6) + q_piece, f32),
            pltpu.VMEM((seq, head), bf16),
            pltpu.VMEM((seq, head), bf16),
            pltpu.VMEM((seq, head), f32),
            pltpu.VMEM((seq, head), f32),
            pltpu.VMEM((tokens, block), bf16),
            pltpu.VMEM((tokens, block), bf16),
            pltpu.VMEM((tokens, block), bf16),
            pltpu.VMEM((2, 4, block, ff), f32),
            pltpu.VMEM((STAGES, block, ff), f32),
            dma,
            dma((3, 2)),
            dma((3,)),
            dma((3,)),
            dma((STAGES,)),
            dma((4,)),
            dma((count,)),
            dma((count,)),
        ],
        compiler_params=pltpu.CompilerParams(collective_id=2, has_side_effects=True, vmem_limit_bytes=VMEM_LIMIT),
        name="back",
    )(z_in, h_all, dy_all, w_all, cos, sin)[:3]


def norm_fwd(row_vals, norm_gain):
    return row_vals * lax.rsqrt(jnp.mean(row_vals * row_vals, axis=-1, keepdims=True) + NORM_EPS) * norm_gain


def solution(mesh):
    act_spec = P("fsdp", "model", None)
    col_spec = P("fsdp", "model")
    row_spec = P("model", "fsdp")
    nz = mesh.shape["fsdp"] // NY

    def layer_body(x_in, dy_in, norm_gain, w_qkv, w_out, w_gate, w_up, w_down, rope_cos, rope_sin):
        bf16 = jnp.bfloat16
        _, rows, width = x_in.shape
        slab = w_qkv.shape[0]
        head = 2 * rope_cos.shape[1]
        group = w_out.shape[0] // head
        seq = rows * NX * NC
        ff = w_gate.shape[1] // NY

        x_rows = x_in[0].astype(jnp.float32)
        normed, norm_pull = jax.vjp(lambda row_vals: norm_fwd(row_vals, norm_gain), x_rows)
        h_loc = normed.astype(bf16).reshape(2, rows // 2, width)
        dy_loc = dy_in.reshape(2, rows // 2, width)
        q, k, v = w_qkv[:, : group * head], w_qkv[:, group * head : -head], w_qkv[:, -head:]
        out_t, down_t = w_out.T, w_down.T
        parts = []
        for i in range(NY):
            at = slice(i * head, (i + 1) * head)
            ffs = slice(i * ff, (i + 1) * ff)
            heads = [q[:, at], out_t[:, at]] if i < NY - 1 else [k, v]
            parts.append(jnp.concatenate([w_gate[:, ffs], w_up[:, ffs]] + heads + [down_t[:, ffs]], axis=1))
        w_loc = jnp.stack(parts)
        cos = jnp.concatenate([rope_cos, rope_cos], axis=1)
        sin = jnp.concatenate([-rope_sin, rope_sin], axis=1)

        h_all, dy_all, w_all, z_got = front(nz, 2 * head, h_loc, dy_loc, w_loc)
        tokens = NY * seq
        cols = w_loc.shape[2]
        h_all = h_all.reshape(tokens, width)
        dy_all = dy_all.reshape(tokens, width)
        w_all = w_all.reshape(NC, width, cols)
        z_got = z_got.reshape(NY, 2, seq // 2, 2 * head)
        p_sum, q_sum, g_sum = back(nz, z_got, h_all, dy_all, w_all, cos, sin)
        p_sum = p_sum.reshape(rows, -1)
        q_sum = q_sum.reshape(rows, -1)

        y_sum = jnp.concatenate([p_sum, q_sum[:, width:]], axis=1)
        y_out = (x_rows + y_sum).astype(bf16)
        d_h = q_sum[:, :width].astype(bf16)
        dx_out = (dy_in[0].astype(jnp.float32) + norm_pull(d_h.astype(jnp.float32))[0]).astype(bf16)
        lo = 2 * ff
        mid = lo + head
        hi = mid + head

        def take(first, end, n=NY):
            return jnp.concatenate([g_sum[i, :, first:end] for i in range(n)], axis=1)

        return (
            y_out[None],
            dx_out[None],
            jnp.concatenate([take(lo, mid), g_sum[NY - 1, :, mid:hi]], axis=1),
            take(mid, hi, group).T,
            take(0, ff),
            take(ff, lo),
            take(hi, cols).T,
        )

    return jax.shard_map(
        layer_body,
        mesh=mesh,
        in_specs=(act_spec, act_spec, P(), col_spec, row_spec, col_spec, col_spec, row_spec, P(), P()),
        out_specs=(act_spec, act_spec, col_spec, row_spec, col_spec, col_spec, row_spec),
        check_vma=False,
    )
```

```python
import functools
import heapq

import jax
import jax.numpy as jnp
from jax import lax
from jax.experimental import pallas as pl
from jax.experimental.pallas import tpu as pltpu
from jax.sharding import PartitionSpec as P

NORM_EPS = 1e-5
NY, NX, NC = 4, 4, 2
MESH = pl.DeviceIdType.MESH
LINK = 46.6e3
PAIR = 330e3
LOCAL = 1500e3
HOP = 3.5
ADD = 0.4
VMEM_LIMIT = 67043328


class Place:
    def __init__(self, nz):
        i, j = lax.axis_index("fsdp"), lax.axis_index("model")
        self.size = {"z": nz, "y": NY, "x": NX, "c": NC}
        self.at = {"z": lax.div(i, NY), "y": lax.rem(i, NY), "x": lax.div(j, NC), "c": lax.rem(j, NC)}

    def get(self, axis, step=0):
        n = self.size[axis]
        return lax.rem(self.at[axis] + (step + 2 * n) % n, n)

    def device(self, axis, step):
        at = dict(self.at)
        at[axis] = self.get(axis, step)
        return {"fsdp": at["z"] * NY + at["y"], "model": at["x"] * NC + at["c"]}

    def meet(self, peers):
        barrier = pltpu.get_barrier_semaphore()
        for axis, step in peers:
            pl.semaphore_signal(barrier, inc=1, device_id=self.device(axis, step), device_id_type=MESH)
        pl.semaphore_wait(barrier, len(peers))


class Flow:
    def __init__(self, place, send_sem, recv_sem, base=0, now=0.0):
        self.place, self.send_sem, self.recv_sem, self.base = place, send_sem, recv_sem, base
        self.now, self.free, self.events, self.copies, self.tasks, self.order = now, {}, [], [], [], 0
        self.sent = set()

    def event(self, when, wait, then):
        heapq.heappush(self.events, (when, self.order, wait, then))
        self.order += 1

    def send(self, axis, step, src, dst, size, then=None, link=None, alt=None):
        k = len(self.copies)
        link = link or (axis, step)
        begin = max(self.now, self.free.get(link, 0.0))
        rate, lag = (PAIR, 1.5) if axis == "c" else (LINK, HOP)
        self.free[link] = begin + size / rate

        def make(dst):
            return pltpu.make_async_remote_copy(
                src_ref=src(),
                dst_ref=dst(),
                send_sem=self.send_sem.at[self.base + k],
                recv_sem=self.recv_sem.at[self.base + k],
                device_id=self.place.device(axis, step),
                device_id_type=MESH,
            )

        copy = make(dst)
        if alt is None:
            copy.start()
        else:
            when, other = alt
            pl.when(jnp.logical_not(when))(copy.start)
            pl.when(when)(make(other).start)
        self.copies.append(copy)
        self.event(self.free[link] + lag, copy.wait_recv, then)
        return k

    def at(self, when, then):
        self.event(when, lambda: None, then)

    def local(self, copy, size, then):
        copy.start()
        self.event(self.now + size / LOCAL + 1.0, copy.wait, then)

    def task(self, cost, do):
        self.tasks.append((cost, do))

    def take(self):
        when, _, wait, then = heapq.heappop(self.events)
        self.now = max(self.now, when)
        wait()
        if then is not None:
            then()

    def spend(self, cost):
        self.now += cost
        while self.events and self.events[0][0] <= self.now:
            self.take()

    def wait_sent(self, k):
        if k not in self.sent:
            self.copies[k].wait_send()
        self.sent.add(k)

    def run(self):
        while self.events or self.tasks:
            if self.tasks and (not self.events or self.events[0][0] > self.now):
                cost, do = self.tasks.pop(0)
                self.now += cost
                do()
            else:
                self.take()

    def close(self):
        for k in range(len(self.copies)):
            self.wait_sent(k)


def after(count, then):
    left = [count]

    def one():
        left[0] -= 1
        if left[0] == 0:
            then()

    return one


def nbytes(ref, lead):
    n = 1
    for d in ref.shape[lead:]:
        n *= d
    return n * jnp.dtype(ref.dtype).itemsize


def any_specs(n):
    return [pl.BlockSpec(memory_space=pl.ANY)] * n


def mm(a, b, ca, cb):
    return lax.dot_general(a, b, (((ca,), (cb,)), ((), ())), preferred_element_type=jnp.float32)


def span(q, n):
    return pl.ds(pl.multiple_of(q * n, n), n)


def exchange(flow, place, src, dst, far, step, done=None):
    size = nbytes(src, 1)

    def onward(way, half):
        def then():
            flow.send("y", way, lambda: far.at[half], lambda: dst.at[place.get("y", -way), half], size // 2, done)

        return then

    if step == 2:
        flow.send("y", 1, lambda: src.at[place.get("y", 2), 0], lambda: far.at[0], size // 2, onward(1, 0))
        flow.send("y", -1, lambda: src.at[place.get("y", 2), 1], lambda: far.at[1], size // 2, onward(-1, 1))
    else:
        flow.send("y", step, lambda: src.at[place.get("y", step)], lambda: dst.at[place.get("y")], size, done)


ORDER = (2, 1, -1, 0)


class Gather:
    def __init__(self, place, flow, own, full, first, cut, arrive):
        self.place, self.flow, self.own, self.full, self.first, self.cut, self.arrive = place, flow, own, full, first, cut, arrive
        self.second = "y" if first == "x" else "x"
        self.size = nbytes(own, 1) * (cut.stop - cut.start) // own.shape[-1]

    def mine(self, half):
        return lambda: self.own.at[half, :, self.cut]

    def spot(self, at, half):
        y, x, c = (self.place.get(axis, at.get(axis, 0)) for axis in "yxc")
        return lambda: self.full.at[y, x, c, half, :, self.cut]

    def spread(self, axis, at, half, src):
        def come(step, onward):
            def then():
                here = dict(at, **{axis: step})
                if onward:
                    far = dict(at, **{axis: 2})
                    self.flow.send(axis, -step, self.spot(here, half), self.spot(here, half), self.size, lambda: self.got(axis, far, half))
                self.got(axis, here, half)

            return then

        self.flow.send(axis, 1, src, self.spot(at, half), self.size, come(-1, half == 0))
        self.flow.send(axis, -1, src, self.spot(at, half), self.size, come(1, half == 1))

    def got(self, axis, at, half):
        if axis == self.first:
            self.spread(self.second, at, half, self.spot(at, half))
        self.pair(at, half, self.spot(at, half))
        self.arrive(at.get("y", 0), at.get("x", 0))

    def pair(self, at, half, src):
        there = lambda: self.arrive(at.get("y", 0), at.get("x", 0))
        self.flow.send("c", 1, src, self.spot(at, half), self.size, there)

    def start_first(self):
        for half in (0, 1):
            self.spread(self.first, {}, half, self.mine(half))

    def start_second(self):
        for half in (0, 1):
            self.spread(self.second, {}, half, self.mine(half))
            self.pair({}, half, self.mine(half))


def front_kernel(
    nz, x_ref, dy_ref, gain, w_qkv, w_out, w_gate, w_up, w_down, h_all, dy_all, w_all, z_got, h_ref, w_ref, w_heads, rows_v, z_in, far, send_sem, recv_sem, own_sem, rows_sem
):
    bf16 = jnp.bfloat16
    place = Place(nz)
    for half in range(2):
        wide = x_ref[half].astype(jnp.float32)
        h_ref[half] = (wide * lax.rsqrt(jnp.mean(wide * wide, axis=-1, keepdims=True) + NORM_EPS) * gain[...]).astype(bf16)
    wide_ff = w_gate.shape[1] // NY
    one = w_out.shape[1] // (NY - 1)
    for q in range(NY):
        ffs = slice(q * wide_ff, (q + 1) * wide_ff)
        w_ref[q, :, :wide_ff] = w_gate[:, ffs]
        w_ref[q, :, wide_ff : 2 * wide_ff] = w_up[:, ffs]
        at = 2 * wide_ff
        w_ref[q, :, at : at + one] = w_qkv[:, q * one : (q + 1) * one]
        w_ref[q, :, at + one : at + 2 * one] = w_out[:, q * one : (q + 1) * one] if q < NY - 1 else w_qkv[:, NY * one :]
        w_ref[q, :, at + 2 * one :] = w_down[:, ffs]
    y, x, c, z = (place.get(axis) for axis in "yxcz")
    last = y == NY - 1
    pair = z_in.shape[-1]
    head = pair // 2
    width = h_ref.shape[-1]
    cols = w_ref.shape[-1]
    lo = (cols - pair) * 2 // 3
    hi = lo + pair
    rows = z_in.shape[2]
    flow = Flow(place, send_sem, recv_sem)
    w_own = pltpu.make_async_copy(w_ref.at[y], w_all.at[0, z, y], own_sem.at[2])
    w_own.start()
    w_heads[z, y] = w_ref[y, :, lo:hi]
    place.meet([("x", 1), ("x", -1), ("y", 1), ("y", -1), ("y", 2), ("z", 1), ("z", -1), ("c", 1)])

    slots = rows_v.shape[0]
    free, queue, ready = list(range(slots)), [], []
    pieces = {}
    parts_done = {}
    weights = [4 * nz]

    def load():
        while free and queue and weights[0] == 0:
            kind, dy, dx = queue.pop(0)
            slot = free.pop(0)
            src = (h_all, dy_all)[kind].at[place.get("y", dy), place.get("x", dx)]
            copy = pltpu.make_async_copy(src, rows_v.at[slot], rows_sem.at[slot])
            flow.local(copy, nbytes(rows_v, 1), lambda slot=slot, kind=kind, dy=dy, dx=dx: flow.task(CHUNK_TIME, lambda: product(kind, dy, dx, slot)))

    def arrive(kind):
        need = (8, 4)[kind]

        def one(dy, dx):
            key = (kind, dy, dx)
            pieces[key] = pieces.get(key, 0) + 1
            if pieces[key] == need:
                queue.append(key)
                load()

        return one

    def weight_come():
        weights[0] -= 1
        if weights[0] == 0:
            load()

    def product(kind, dy, dx, slot):
        at = place.get("y", dy), place.get("x", dx)
        step = 2 if nz % 2 == 0 else 1
        deep = step * (width // nz)

        def dot(first):
            def some(i, total):
                left = rows_v[slot, :, :, :, span(i, deep)].reshape(rows, deep)
                right = w_heads[pl.ds(i * step, step), :, :, first:].reshape(deep, pair - first)
                return total + mm(left, right, 1, 0)

            return lax.fori_loop(0, nz // step, some, jnp.zeros((rows, pair - first), jnp.float32))

        if kind == 0:
            made = dot(0).astype(bf16)
            z_in[at[0], at[1], :, :head] = made[:, :head]

            @pl.when(last)
            def _():
                z_in[at[0], at[1], :, head:] = made[:, head:]

        else:

            @pl.when(jnp.logical_not(last))
            def _():
                z_in[at[0], at[1], :, head:] = dot(head).astype(bf16)

        free.append(slot)
        load()
        parts_done[dy, dx] = parts_done.get((dy, dx), 0) + 1
        if parts_done[dy, dx] == 2:
            deliver(dy, dx)

    own_copies = []

    def deliver(dy, dx):
        at = lambda: z_in.at[place.get("y", dy), place.get("x", dx)]
        size = nbytes(z_in, 2)

        def there(step=0):
            return lambda: z_got.at[place.get("y", step), place.get("x", dx)]

        if dy == 0:
            copy = pltpu.make_async_copy(at(), there()(), own_sem.at[4 + dx % NX])
            copy.start()
            own_copies.append(copy)
        elif dy == 2:
            way = 1 if dx in (0, 2) else -1

            def onward():
                flow.send("y", way, lambda: far.at[dx % NX], there(-way), size)

            flow.send("y", way, at, lambda: far.at[dx % NX], size, onward)
        else:
            flow.send("y", dy, at, there(), size)

    def w_part(ref, who, dz, dy, cut):
        if ref is None:
            return lambda: w_heads.at[place.get("z", dz), place.get("y", dy)]
        return lambda: w_all.at[who, place.get("z", dz), place.get("y", dy), :, cut]

    cuts = [slice(lo, hi), slice(0, lo), slice(hi, cols)]

    def ring(step, dy, n_cut, src=None, hops=nz - 1, lead=True):
        cut = cuts[n_cut]
        home = None if n_cut == 0 else w_all
        size = nbytes(w_ref, 1) * (cut.stop - cut.start) // cols

        def hop(n):
            def then():
                here = src if src and n == 0 else w_part(home, 0, -step * n, dy, cut)
                if n < hops:
                    flow.send("z", step, here, w_part(home, 0, -step * n, dy, cut), size, hop(n + 1))
                if n or lead:
                    flow.send("c", 1, here, w_part(w_all, 1, -step * n, dy, cut), size)
                    if n_cut == 0:
                        weight_come()

            return then

        return hop(0)

    def rings(dy, n_cut, src=None):
        if n_cut:
            return ring(1 if dy in (0, 1) else -1, dy, n_cut, src)
        both = [ring(1, dy, 0, src, nz // 2), ring(-1, dy, 0, src, (nz - 1) // 2, False)]
        return lambda: [one() for one in both]

    def w_at(dy, cut):
        return lambda: w_ref.at[place.get("y", dy), :, cut]

    tail = width // nz * H_TAIL
    gathers = [
        Gather(place, flow, h_ref, h_all, "x", slice(0, width - tail), arrive(0)),
        Gather(place, flow, dy_ref, dy_all, "y", slice(0, width), arrive(1)),
        Gather(place, flow, h_ref, h_all, "y", slice(width - tail, width), arrive(0)),
    ]
    def w_start(n_cut, dys):
        cut = cuts[n_cut]
        home = None if n_cut == 0 else w_all
        size = nbytes(w_ref, 1) * (cut.stop - cut.start) // cols
        there = w_part(home, 0, 0, 0, cut)
        for dy in dys:
            if dy == 0:
                rings(0, n_cut, w_at(0, cut))()
            elif dy == 2:
                flow.send("y", 2, w_at(2, cut), there, size, rings(2, n_cut), link=("y", 1))
            else:
                flow.send("y", -dy, w_at(-dy, cut), there, size, rings(dy, n_cut))

    w_start(0, (0, 1, -1, 2))
    for one in gathers:
        one.start_first()
    flow.at(W_TIMES[0], lambda: [w_start(1, (0, -1)), w_start(2, (0, -1))])
    flow.at(W_TIMES[1], lambda: [w_start(1, (1, 2)), w_start(2, (1, 2))])
    for one in gathers:
        one.start_second()
    for n, (ref, full) in enumerate(((h_ref, h_all), (dy_ref, dy_all))):
        copy = pltpu.make_async_copy(ref, full.at[y, x, c], own_sem.at[n])
        there = arrive(n)
        flow.local(copy, nbytes(ref, 0), lambda n=n, there=there: [there(0, 0) for _ in range((4, 2)[n])])
    flow.run()
    heads_home = pltpu.make_async_copy(w_heads, w_all.at[0, :, :, :, lo:hi], own_sem.at[3])
    w_own.wait()
    heads_home.start()
    flow.close()
    for copy in own_copies:
        copy.wait()
    heads_home.wait()


CHUNK_TIME = 1.0
W_TIMES = (0.0, 0.0)
H_TAIL = 1


def front(nz, x, dy, gain, w_qkv, w_out, w_gate, w_up, w_down):
    half, rows, width = x.shape
    everywhere = (NY, NX, NC) + x.shape
    slab = w_qkv.shape[0]
    pair = 2 * w_out.shape[1] // (NY - 1)
    cols = pair + 3 * w_gate.shape[1] // NY
    w_shape = (NY, slab, cols)
    bf16 = x.dtype
    gathers = 3 * (30 + 32)
    count = gathers + 3 * 3 + 3 * 4 * (nz - 1) + 3 * 4 * nz + 2 * NX + 2 * NX
    vmem = pl.BlockSpec(memory_space=pltpu.VMEM)
    dma = pltpu.SemaphoreType.DMA
    chunk = NC * half * rows
    z_shape = (NY, NX, chunk, pair)
    slots = 8
    return pl.pallas_call(
        functools.partial(front_kernel, nz),
        out_shape=(
            jax.ShapeDtypeStruct(everywhere, bf16),
            jax.ShapeDtypeStruct(everywhere, bf16),
            jax.ShapeDtypeStruct((NC, nz) + w_shape, bf16),
            jax.ShapeDtypeStruct(z_shape, bf16),
        ),
        in_specs=[vmem] * 8,
        out_specs=tuple(any_specs(4)),
        scratch_shapes=[
            pltpu.VMEM(x.shape, bf16),
            pltpu.VMEM(w_shape, bf16),
            pltpu.VMEM((nz,) + w_shape[:-1] + (pair,), bf16),
            pltpu.VMEM((slots, NC) + x.shape, bf16),
            pltpu.VMEM(z_shape, bf16),
            pltpu.VMEM((NX, chunk, pair), bf16),
            dma((count,)),
            dma((count,)),
            dma((4 + NX,)),
            dma((slots,)),
        ],
        compiler_params=pltpu.CompilerParams(collective_id=0, has_side_effects=True, vmem_limit_bytes=VMEM_LIMIT),
        name="front",
    )(x, dy, gain, w_qkv, w_out, w_gate, w_up, w_down)


SETS = (2, 1, -1, 0)


def attention(z_got, z_back, keys, vals, dk, dv, cos_ref, sin_ref):
    bf16 = jnp.bfloat16
    seq, head = keys.shape
    part = seq // 2
    count = z_got.shape[0] - 1
    scale = head**-0.5
    spread = z_back.shape[2:5] + (head,)
    halves = [pl.ds(p * part, part) for p in range(2)]

    def turn(values, at, sign):
        wide = values.astype(jnp.float32)
        swapped = pltpu.roll(wide, head // 2, 1)
        return (wide * cos_ref[at, :] + sign * (swapped * sin_ref[at, :])).astype(bf16)

    for p in range(2):
        keys[halves[p], :] = turn(z_got[count, p, :, :head], halves[p], 1.0)
        vals[halves[p], :] = z_got[count, p, :, head:]
    dk[...] = jnp.zeros_like(dk)
    dv[...] = jnp.zeros_like(dv)

    @pl.loop(0, count)
    def _(i):
        for p in range(2):
            n = (p + 1) * part
            query = turn(z_got[i, p, :, :head], halves[p], 1.0)
            d_out = z_got[i, p, :, head:]
            scores = mm(query, keys[:n, :], 1, 1) * scale
            causal = lax.broadcasted_iota(jnp.int32, scores.shape, 0) + p * part >= lax.broadcasted_iota(jnp.int32, scores.shape, 1)
            scores = jnp.where(causal, scores, -1e30)
            grown = jnp.exp(scores - jnp.max(scores, axis=1, keepdims=True))
            probs = grown / jnp.sum(grown, axis=1, keepdims=True)
            probs_low = probs.astype(bf16)
            z_back[i, p, :, :, :, head:] = mm(probs_low, vals[:n, :], 1, 0).astype(bf16).reshape(spread)
            d_probs = mm(d_out, vals[:n, :], 1, 1).astype(bf16).astype(jnp.float32)
            d_scores = (probs * (d_probs - jnp.sum(probs * d_probs, axis=1, keepdims=True)) * scale).astype(bf16)
            z_back[i, p, :, :, :, :head] = turn(mm(d_scores, keys[:n, :], 1, 0).astype(bf16), halves[p], -1.0).reshape(spread)
            dk[:n, :] += mm(d_scores, query, 0, 0)
            dv[:n, :] += mm(probs_low, d_out, 0, 0)

    for p in range(2):
        z_back[count, p, :, :, :, :head] = turn(dk[halves[p], :].astype(bf16), halves[p], -1.0).reshape(spread)
        z_back[count, p, :, :, :, head:] = dv[halves[p], :].astype(bf16).reshape(spread)


def gated(place, flow, h_all, dy_all, w_all, acts, row_sem, share, h_rows, dy_rows, w_v):
    bf16 = jnp.bfloat16
    ff = acts.shape[-1] // 3
    lo = 2 * ff
    part = h_rows.shape[1]
    shape = acts.shape[2:5] + (ff,)
    w_loads = [
        pltpu.make_async_copy(w_all.at[0, :, :lo], w_v.at[:, :lo], row_sem.at[2, 0]),
        pltpu.make_async_copy(w_all.at[0, :, w_all.shape[2] - ff :], w_v.at[:, lo:], row_sem.at[2, 1]),
    ]

    def loads(n, slot):
        return [pltpu.make_async_copy(a.at[span(n, part)], b.at[slot], row_sem.at[slot, m]) for m, (a, b) in enumerate(((h_all, h_rows), (dy_all, dy_rows)))]

    def begin():
        for copy in w_loads + loads(0, 0) + loads(1, 1):
            copy.start()

    def go():
        for copy in w_loads:
            copy.wait()
        for q in range(NY):

            @pl.loop(0, 2)
            def _(p):
                n = 2 * q + p
                for copy in loads(n, p):
                    copy.wait()
                gate = mm(h_rows[p], w_v[:, :ff], 1, 0).astype(bf16).astype(jnp.float32)
                up = mm(h_rows[p], w_v[:, ff:lo], 1, 0).astype(bf16).astype(jnp.float32)
                d_act = mm(dy_rows[p], w_v[:, lo:], 1, 0).astype(bf16).astype(jnp.float32)
                if q < NY - 1:
                    for copy in loads(n + 2, p):
                        copy.start()
                sig = jax.nn.sigmoid(gate)
                silu = gate * sig
                acts[q, p, :, :, :, :ff] = (d_act * up * (sig + silu * (1.0 - sig))).astype(bf16).reshape(shape)
                acts[q, p, :, :, :, ff:lo] = (d_act * silu).astype(bf16).reshape(shape)
                acts[q, p, :, :, :, lo:] = (silu * up).astype(bf16).reshape(shape)

            share(q)
            flow.spend(3.0)

    return begin, go


class Plane:
    def __init__(self, place, flow, tiles, land, first, finish, free):
        self.place, self.flow, self.tiles, self.land, self.first = place, flow, tiles, land, first
        self.second = "y" if first == "x" else "x"
        self.piece = nbytes(tiles, 3)
        self.sums, self.waiting, self.finished = {}, {}, [0] * len(SETS)
        self.free = free
        self.rings = []
        for s, other in enumerate(SETS):

            def raw(step, half, s=s):
                return lambda: tiles.at[s % 2, place.get(first, step), half]

            self.rings.append(self.ring(first, raw, lambda step, half, then: then(), s, self.first_done(s, other)))
        self.onward, _ = self.ring(self.second, lambda step, half: self.sums[step, half], self.need, len(SETS), finish)

    def need(self, step, half, then):
        if (step, half) in self.sums:
            then()
        else:
            self.waiting.setdefault((step, half), []).append(then)

    def first_done(self, s, step):
        def done(half, ref):
            self.sums[step, half] = ref
            for then in self.waiting.pop((step, half), []):
                then()
            self.onward(step, half)
            self.finished[s] += 1
            if self.finished[s] == 2:
                self.free(s)

        return done

    def add(self, mine, other):
        a, b = mine(), other()
        a[...] = a[...] + b[...]
        self.flow.now += ADD

    def ring(self, axis, raw, need, s, done):
        flow, add, sent = self.flow, self.add, []

        def slot(i):
            return lambda: self.land.at[s, i]

        def turn(i, goal, half, step):
            def then():
                add(slot(i), raw(goal, half))
                flow.send(axis, step, slot(i), slot(i + 4), self.piece, final[half])

            return lambda: need(goal, half, then)

        def ending(half):
            def then():
                mine, other = (slot(5), slot(2)) if half == 0 else (slot(4), slot(3))
                add(mine, other)
                add(mine, raw(0, half))
                done(half, mine)

            return lambda: need(0, half, then)

        final = [after(2, ending(0)), after(2, ending(1))]
        moves = {
            (2, 1): (1, 0, turn(0, 1, 1, 1)),
            (2, 0): (-1, 1, turn(1, -1, 0, -1)),
            (1, 0): (1, 2, final[0]),
            (-1, 1): (-1, 3, final[1]),
        }

        def start(goal, half):
            if (goal, half) in moves:
                step, i, then = moves[goal, half]
                sent.append(flow.send(axis, step, raw(goal, half), slot(i), self.piece, then))

        return start, sent

    def start(self, s):
        for goal, half in ((2, 1), (2, 0), (1, 0), (-1, 1)):
            self.rings[s][0](goal, half)

    def clear(self, s):
        for k in self.rings[s][1]:
            self.flow.wait_sent(k)


class Grads:
    flow = None


    def __init__(self, nz, place, h_all, dy_all, acts, z_out, z_land, outs, far, h_plus, h_minus, dy_minus, tiles, stage, load_sem, stage_sem, own_sem):
        self.__dict__.update({k: v for k, v in locals().items() if k != "self"})
        self.ff = acts.shape[-1] // 3
        self.pair = z_out.shape[-1]
        lo = 2 * self.ff
        self.cols = [(0, self.ff), (self.ff, lo), (lo + self.pair, lo + self.pair + self.ff), (lo, lo + self.pair)]
        self.way = (1, 1, -1, -1)
        self.far_way = (1, -1, 1, -1)
        self.block = tiles.shape[2]
        self.size = nbytes(tiles, 2)
        self.ready, self.waiting, self.used = set(), {}, 0
        self.users = [[] for _ in range(stage.shape[0])]
        self.own = []
        self.idle, self.first = {}, {}

    def load(self, ref, src, index, step, n):
        b = self.place.get("z", -step * (n + 1))
        at = pl.ds(pl.multiple_of(b * self.block, self.block), self.block)
        return pltpu.make_async_copy(src.at[:, at], ref, self.load_sem.at[index])

    def loads_plus(self, n):
        return [self.load(self.h_plus, self.h_all, 0, 1, n)]

    def loads_minus(self, n):
        return [self.load(self.h_minus, self.h_all, 1, -1, n), self.load(self.dy_minus, self.dy_all, 2, -1, n)]

    def begin(self):
        for copy in self.loads_plus(0) + self.loads_minus(0):
            copy.start()

    def gather_up(self, tiles, some):
        seq = self.h_plus.shape[0] // NY
        for tile in tiles:
            tile[...] = jnp.zeros_like(tile)

        @pl.loop(0, NY)
        def _(q):
            for tile, value in zip(tiles, some(q, span(q, seq))):
                tile[...] += value

    def set_ready(self, lane, n):
        self.ready.add((lane, n))
        for then in self.waiting.pop((lane, n), []):
            then()
        if n == 0:
            k = self.flow.send("z", self.way[lane], lambda: self.tiles.at[0, lane], lambda: self.z_land.at[0, lane], self.size, self.hop(lane, 0))
            self.first[lane] = k

    def clear(self, lane, n):
        if n == 2:
            self.flow.wait_sent(self.first[lane])

    def tokens(self, ref):
        value = ref[...]
        return value.reshape(-1, value.shape[-1])

    def make_plus(self, n):
        for copy in self.loads_plus(n):
            copy.wait()
        lo = 2 * self.ff

        def some(q, rows):
            both = mm(self.h_plus[rows, :], self.acts[q, :, :, :, :, :lo].reshape(-1, lo), 0, 0)
            return both[:, : self.ff], both[:, self.ff :]

        self.gather_up([self.tiles.at[n % 2, 0], self.tiles.at[n % 2, 1]], some)
        if n + 1 < self.nz:
            for copy in self.loads_plus(n + 1):
                copy.start()

    def for_down(self, q, rows):
        return [mm(self.dy_minus[rows, :], self.acts[q, :, :, :, :, 2 * self.ff :].reshape(-1, self.ff), 0, 0)]

    def for_heads(self, q, rows):
        last = self.place.get("y") == NY - 1
        head = self.pair // 2
        out = self.z_out[q].reshape(-1, self.pair)
        both = mm(self.h_minus[rows, :], out, 0, 0)
        right = jnp.where(last, both[:, head:], mm(self.dy_minus[rows, :], out[:, head:], 0, 0))
        return [jnp.concatenate([both[:, :head], right], axis=1)]

    def make_minus(self, n):
        for copy in self.loads_minus(n):
            copy.wait()
        self.gather_up([self.tiles.at[n % 2, 2], self.tiles.at[n % 2, 3]], lambda q, rows: self.for_down(q, rows) + self.for_heads(q, rows))
        self.load_minus_next(n)

    def load_minus_next(self, n):
        if n + 1 < self.nz:
            for copy in self.loads_minus(n + 1):
                copy.start()

    def make_first(self):
        self.make_plus(0)
        for copy in self.loads_minus(0):
            copy.wait()
        self.gather_up([self.tiles.at[0, 2]], self.for_down)

    def heads_first(self):
        def do():
            self.gather_up([self.tiles.at[0, 3]], self.for_heads)
            self.load_minus_next(0)
            self.set_ready(3, 0)

        self.flow.task(1.3, do)

    def plus(self, n):
        def do():
            for lane in (0, 1):
                self.clear(lane, n)
            self.make_plus(n)
            for lane in (0, 1):
                self.set_ready(lane, n)

        self.flow.task(1.6, do)

    def minus(self, n):
        def do():
            for lane in (2, 3):
                self.clear(lane, n)
            self.make_minus(n)
            for lane in (2, 3):
                self.set_ready(lane, n)

        self.flow.task(2.2, do)

    def need(self, lane, n, then):
        if (lane, n) in self.ready:
            then()
        else:
            self.waiting.setdefault((lane, n), []).append(then)

    def next(self, lane, n):
        if n + 2 >= self.nz:
            return
        key = (lane // 2, n)
        self.idle[key] = self.idle.get(key, 0) + 1
        if self.idle[key] == 2:
            (self.plus, self.minus)[lane // 2](n + 2)

    def hop(self, lane, s):
        flow, place = self.flow, self.place

        def come():
            slot = self.used % len(self.users)
            self.used += 1
            for wait in self.users[slot]:
                wait()
            self.users[slot] = []
            here = lambda: self.stage.at[slot]

            def staged():
                self.need(lane, s + 1, use)

            def use():
                ref = here()
                ref[...] = ref[...] + self.tiles[(s + 1) % 2, lane]
                flow.now += ADD
                if s == 0:
                    self.next(lane, 0)
                self.next(lane, s + 1)
                if s + 1 < self.nz - 1:
                    k = flow.send("z", self.way[lane], here, lambda: self.z_land.at[s + 1, lane], self.size, self.hop(lane, s + 1))
                    self.users[slot].append(lambda: flow.wait_sent(k))
                else:
                    self.home(lane, slot)

            flow.local(pltpu.make_async_copy(self.z_land.at[s, lane], here(), self.stage_sem.at[slot]), self.size, staged)

        return come

    def home(self, lane, slot):
        flow, place = self.flow, self.place
        slab = self.block // NY
        way = self.far_way[lane]
        size = self.size // NY

        def rows(step, cut=slice(None)):
            return lambda: self.stage.at[slot, pl.ds(pl.multiple_of(place.get("y", step) * slab, slab), slab), cut]

        def columns(out, step, wide):
            at = place.get("y", step) * wide
            return lambda: self.outs[out].at[:, pl.ds(pl.multiple_of(at, wide), wide)]

        def deliver(size, src, far, dst, n, other=None):
            def alt(step):
                return None if other is None else (place.get("y", step) == NY - 1, other(step))

            def onward():
                flow.send("y", way, far, dst(-way), size, alt=alt(-way))

            sent = [flow.send("y", way, src(2), far, size, onward)]
            sent += [flow.send("y", step, src(step), dst(0), size, alt=alt(0)) for step in (1, -1)]
            copies = [(None, pltpu.make_async_copy(src(0)(), dst(0)(), self.own_sem.at[n]))]
            if other is not None:
                last = place.get("y") == NY - 1
                copies = [(jnp.logical_not(last), copies[0][1]), (last, pltpu.make_async_copy(src(0)(), other(0)(), self.own_sem.at[n]))]
            for when, copy in copies:
                if when is None:
                    copy.start()
                else:
                    pl.when(when)(copy.start)
            self.users[slot] += [functools.partial(flow.wait_sent, k) for k in sent] + [copies[0][1].wait]

        if lane < 3:
            deliver(size, rows, lambda: self.far.at[lane], lambda step: columns(lane, step, self.ff), lane)
            return
        head = self.pair // 2
        first, second = slice(0, head), slice(head, self.pair)
        deliver(size // 2, lambda step: rows(step, first), lambda: self.far.at[3, :, first], lambda step: columns(3, step, head), 3)
        value = lambda: self.outs[3].at[:, NY * head :]

        def out_rows(step):
            at = lax.rem(place.get("y", step), NY - 1) * head
            return lambda: self.outs[4].at[:, pl.ds(pl.multiple_of(at, head), head)]

        deliver(size // 2, lambda step: rows(step, second), lambda: self.far.at[3, :, second], out_rows, 4, lambda step: value)

    def close(self):
        for users in self.users:
            for wait in users:
                wait()


def back_kernel(
    nz,
    z_in,
    h_all,
    dy_all,
    w_all,
    cos_in,
    sin_in,
    x_ref,
    dy_ref,
    gain,
    y_out,
    dx_out,
    g_qkv,
    g_out,
    g_gate,
    g_up,
    g_down,
    z_land,
    cos_ref,
    sin_ref,
    z_got,
    z_back,
    z_out,
    far_back,
    acts,
    pair_acts,
    far,
    p_land,
    q_land,
    keys,
    vals,
    dk,
    dv,
    h_plus,
    h_minus,
    dy_minus,
    tiles,
    stage,
    load_sem,
    row_sem,
    w_sem,
    g_load_sem,
    stage_sem,
    own_sem,
    send_sem,
    recv_sem,
):
    bf16, f32 = jnp.bfloat16, jnp.float32
    place = Place(nz)
    y, c = place.get("y"), place.get("c")
    other = place.get("c", 1)
    last = y == NY - 1
    seq, head = keys.shape
    pair = 2 * head
    rows, cols = pair_acts.shape[3:]
    ff = (cols - pair) // 3
    lo, hi = 2 * ff, 2 * ff + pair
    tokens, width = h_all.shape
    block = width // nz
    part = seq // 2

    z_load = pltpu.make_async_copy(z_in, z_got, load_sem)
    z_load.start()
    cos_ref[...] = jnp.concatenate([cos_in[...], cos_in[...]], axis=0).T
    sin_ref[...] = jnp.concatenate([-sin_in[...], sin_in[...]], axis=0).T
    early = Flow(place, send_sem, recv_sem)
    peers = [("x", 1), ("x", -1), ("y", 1), ("y", -1), ("z", 1), ("z", -1), ("c", 1)]

    def share(q):
        early.send("c", 1, lambda: acts.at[q, :, :, other, :, :lo], lambda: pair_acts.at[q, :, :, :, :lo], nbytes(pair_acts, 1) * lo // cols)
        early.send("c", 1, lambda: acts.at[q, :, :, other, :, lo:], lambda: pair_acts.at[q, :, :, :, hi:], nbytes(pair_acts, 1) * ff // cols)

    def all_out():
        early.send("c", 1, lambda: z_out.at[:, :, :, other], lambda: pair_acts.at[:, :, :, :, lo:hi], nbytes(z_out, 0) // NC)

    grads = Grads(nz, place, h_all, dy_all, acts, z_out, z_land, (g_gate, g_up, g_down, g_qkv, g_out), far, h_plus, h_minus, dy_minus, tiles, stage, g_load_sem, stage_sem, own_sem)

    def first(h_rows, dy_rows, w_v):
        begin, go = gated(place, early, h_all, dy_all, w_all, acts, row_sem, share, h_rows, dy_rows, w_v)
        begin()
        grads.begin()
        z_load.wait()
        attention(z_got, z_back, keys, vals, dk, dv, cos_ref, sin_ref)
        place.meet(peers)
        out_done = after(4, all_out)
        for step in ORDER[:3]:
            exchange(early, place, z_back, z_out, far_back, step, out_done)
        z_out[y] = z_back[y]
        go()
        grads.make_first()
        early.now += 2.6
        early.run()
        early.close()

    pl.run_scoped(
        first,
        pltpu.VMEM((2, part, width), bf16),
        pltpu.VMEM((2, part, width), bf16),
        pltpu.VMEM((width, 3 * ff), bf16),
    )

    def second(p_tile, q_tile, w_v):
        flow = Flow(place, send_sem, recv_sem, len(early.copies), early.now)
        grads.flow = flow
        lane = lax.broadcasted_iota(jnp.int32, (rows, pair), 1)
        for_d = jnp.logical_or(lane < head, last)

        def chunk(k, i, p, xx):
            if k == 0:
                own = acts[i, p, xx, c]
                return own[:, :lo], z_out[i, p, xx, c], own[:, lo:]
            theirs = pair_acts[i, p, xx]
            return theirs[:, :lo], theirs[:, lo:hi], theirs[:, hi:]

        def for_out(k, i, p, xx):
            _, mixed, act = chunk(k, i, p, xx)
            return jnp.concatenate([jnp.where(for_d, jnp.zeros_like(mixed), mixed), act], axis=1)

        def for_in(k, i, p, xx):
            grad, mixed, _ = chunk(k, i, p, xx)
            return jnp.concatenate([grad, jnp.where(for_d, mixed, jnp.zeros_like(mixed))], axis=1)

        depth = w_v.shape[0]

        def w_copy(kind, d, slot):
            at = pl.ds(pl.multiple_of(d * block, block), block)
            cut = slice(lo, cols) if kind == 0 else slice(0, cols)
            return pltpu.make_async_copy(w_all.at[:, at, cut], w_v.at[slot, :, :, cut], w_sem.at[slot])

        counts = (nz - 1, nz)
        base, total = [], 0
        for kind, _ in PASSES:
            base.append(total)
            total += counts[kind]
        kind = PASSES[0][0]
        for n in range(depth):
            w_copy(kind, n, n).start() if n < counts[kind] else w_copy(PASSES[1][0], n - counts[kind], n).start()
        turn = [0]

        def blocks(s, kind, first, count, body):
            n = turn[0]
            assert PASSES[n] == (kind, s)
            if first + count == counts[kind]:
                turn[0] += 1

            @pl.loop(first, first + count)
            def _(d):
                slot = lax.rem(base[n] + d, depth)
                w_copy(kind, d, slot).wait()
                body(d, w_v.at[slot])

                @pl.when(d + depth < counts[kind])
                def _():
                    w_copy(kind, d + depth, slot).start()

                if n + 1 < len(PASSES):

                    @pl.when(d + depth >= counts[kind])
                    def _():
                        w_copy(PASSES[n + 1][0], d + depth - counts[kind], slot).start()

        def product(parts, w, a, b):
            total = None
            for k in range(NC):
                left = jnp.concatenate([one(k) for one in parts], axis=0)
                one = mm(left, w[k, :, a:b], 1, 1)
                total = one if total is None else total + one
            return total

        shape = (NX, 2, rows // 2, block)

        def p_rows(s):
            x = place.get("x", SETS[s])
            p, xx = lax.div(x, NX // 2), lax.rem(x, NX // 2)
            return [lambda k, i=i: for_out(k, i, p, xx) for i in range(NY)]

        def q_rows(s, make):
            i = place.get("y", SETS[s])
            return [lambda k, p=p, xx=xx: make(k, i, p, xx) for p in range(2) for xx in range(NX // 2)]

        def place_of(d):
            return pl.ds(pl.multiple_of(d * block, block), block)

        def p_task(s):
            def body(d, w):
                p_tile[s % 2, :, :, :, place_of(d)] = product(p_rows(s), w, lo, cols).reshape(shape)

            def do():
                if s >= 2:
                    planes[0].clear(s - 2)
                blocks(s, 0, 0, nz - 1, body)
                planes[0].start(s)

            flow.task(P_TIME, do)

        def q_task(s):
            def body(d, w):
                q_tile[s % 2, :, :, :, place_of(d)] = product(q_rows(s, for_in), w, 0, hi).reshape(shape)

                @pl.when(d == nz - 1)
                def _():
                    q_tile[s % 2, :, :, :, width:] = product(q_rows(s, for_out), w, lo, cols).reshape(shape)

            def start():
                if s >= 2:
                    planes[1].clear(s - 2)
                blocks(s, 1, 0, nz // 2, body)

            def end():
                blocks(s, 1, nz // 2, nz - nz // 2, body)
                planes[1].start(s)

            flow.task(Q_HALF, start)
            flow.task(Q_HALF, end)

        edge = width - block
        def p_finish(half, ref):
            y_out[half, :, :edge] = (x_ref[half, :, :edge].astype(f32) + ref()[...]).astype(bf16)

        def q_finish(half, ref):
            y_out[half, :, edge:] = (x_ref[half, :, edge:].astype(f32) + ref()[:, width:]).astype(bf16)
            wide = x_ref[half].astype(f32)
            scale = lax.rsqrt(jnp.mean(wide * wide, axis=-1, keepdims=True) + NORM_EPS)
            d_normed = ref()[:, :width].astype(bf16).astype(f32) * gain[...]
            mean = jnp.mean(d_normed * wide, axis=-1, keepdims=True)
            grad = d_normed * scale - wide * (scale * scale * scale * mean)
            dx_out[half] = (dy_ref[half].astype(f32) + grad).astype(bf16)

        def free(task):
            return lambda s: task(s + 2) if s + 2 < len(SETS) else None

        planes = [
            Plane(place, flow, p_tile, p_land, "y", p_finish, free(p_task)),
            Plane(place, flow, q_tile, q_land, "x", q_finish, free(q_task)),
        ]

        for lane in range(3):
            grads.set_ready(lane, 0)
        q_task(0)
        p_task(0)
        grads.heads_first()
        grads.plus(1)
        grads.minus(1)
        p_task(1)
        q_task(1)
        flow.run()
        flow.close()
        grads.close()

    pl.run_scoped(
        second,
        pltpu.VMEM((2, NY, 2, rows // 2, width - block), f32),
        pltpu.VMEM((2, NX, 2, rows // 2, width + block), f32),
        pltpu.VMEM((3, NC, block, cols), bf16),
    )


STAGES = 6
PASSES = ((1, 0), (0, 0), (0, 1), (1, 1), (1, 2), (0, 2), (0, 3), (1, 3))
P_TIME = 3.0
Q_HALF = 2.6


def back(nz, z_in, h_all, dy_all, w_all, cos, sin, x, dy, gain):
    tokens, width = h_all.shape
    seq, head = cos.shape[1], 2 * cos.shape[0]
    pair = 2 * head
    cols = w_all.shape[2]
    ff = (cols - pair) // 3
    rows = seq // (NX * NC)
    block = width // nz
    bf16, f32 = h_all.dtype, jnp.float32
    vmem = pl.BlockSpec(memory_space=pltpu.VMEM)
    dma = pltpu.SemaphoreType.DMA
    blocks = (NY, 2, NX // 2, NC, rows, pair)
    p_piece = (rows // 2, width - block)
    q_piece = (rows // 2, width + block)
    count = 6 + 2 * NY + 1 + 4 * (nz - 1) + 5 * 4 + 2 * 5 * 6
    slab = block // NY
    weight = jax.ShapeDtypeStruct((slab, NY * ff), f32)
    return pl.pallas_call(
        functools.partial(back_kernel, nz),
        out_shape=(
            jax.ShapeDtypeStruct(x.shape, bf16),
            jax.ShapeDtypeStruct(x.shape, bf16),
            jax.ShapeDtypeStruct((slab, (NY + 1) * head), f32),
            jax.ShapeDtypeStruct((slab, (NY - 1) * head), f32),
            weight,
            weight,
            weight,
            jax.ShapeDtypeStruct((nz - 1, 4, block, ff), f32),
        ),
        in_specs=any_specs(4) + [vmem] * 5,
        out_specs=(vmem, vmem) + tuple(any_specs(6)),
        scratch_shapes=[
            pltpu.VMEM((seq, head), f32),
            pltpu.VMEM((seq, head), f32),
            pltpu.VMEM(z_in.shape, bf16),
            pltpu.VMEM(blocks, bf16),
            pltpu.VMEM(blocks, bf16),
            pltpu.VMEM(blocks[1:], bf16),
            pltpu.VMEM(blocks[:-1] + (3 * ff,), bf16),
            pltpu.VMEM(blocks[:3] + (rows, cols), bf16),
            pltpu.VMEM((4, block // NY, ff), f32),
            pltpu.VMEM((5, 6) + p_piece, f32),
            pltpu.VMEM((5, 6) + q_piece, f32),
            pltpu.VMEM((seq, head), bf16),
            pltpu.VMEM((seq, head), bf16),
            pltpu.VMEM((seq, head), f32),
            pltpu.VMEM((seq, head), f32),
            pltpu.VMEM((tokens, block), bf16),
            pltpu.VMEM((tokens, block), bf16),
            pltpu.VMEM((tokens, block), bf16),
            pltpu.VMEM((2, 4, block, ff), f32),
            pltpu.VMEM((STAGES, block, ff), f32),
            dma,
            dma((3, 2)),
            dma((3,)),
            dma((3,)),
            dma((STAGES,)),
            dma((5,)),
            dma((count,)),
            dma((count,)),
        ],
        compiler_params=pltpu.CompilerParams(collective_id=2, has_side_effects=True, vmem_limit_bytes=VMEM_LIMIT),
        name="back",
    )(z_in, h_all, dy_all, w_all, cos, sin, x, dy, gain)[:7]


def solution(mesh):
    act_spec = P("fsdp", "model", None)
    col_spec = P("fsdp", "model")
    row_spec = P("model", "fsdp")
    nz = mesh.shape["fsdp"] // NY

    def layer_body(x_in, dy_in, norm_gain, w_qkv, w_out, w_gate, w_up, w_down, rope_cos, rope_sin):
        _, rows, width = x_in.shape
        head = 2 * rope_cos.shape[1]
        seq = rows * NX * NC
        tokens = NY * seq
        x = x_in.reshape(2, rows // 2, width)
        dy = dy_in.reshape(2, rows // 2, width)
        gain = norm_gain.reshape(1, width)
        h_all, dy_all, w_all, z_got = front(nz, x, dy, gain, w_qkv, w_out.T, w_gate, w_up, w_down.T)
        y_out, dx_out, g_qkv, g_out, g_gate, g_up, g_down = back(
            nz,
            z_got.reshape(NY, 2, seq // 2, 2 * head),
            h_all.reshape(tokens, width),
            dy_all.reshape(tokens, width),
            w_all.reshape(NC, width, -1),
            rope_cos.T,
            rope_sin.T,
            x,
            dy,
            gain,
        )
        return y_out.reshape(x_in.shape), dx_out.reshape(x_in.shape), g_qkv, g_out.T, g_gate, g_up, g_down.T

    return jax.shard_map(
        layer_body,
        mesh=mesh,
        in_specs=(act_spec, act_spec, P(), col_spec, row_spec, col_spec, col_spec, row_spec, P(), P()),
        out_specs=(act_spec, act_spec, col_spec, row_spec, col_spec, col_spec, row_spec),
        check_vma=False,
    )
```

```python
import functools
import heapq

import jax
import jax.numpy as jnp
from jax import lax
from jax.experimental import pallas as pl
from jax.experimental.pallas import tpu as pltpu
from jax.sharding import PartitionSpec as P

NORM_EPS = 1e-5
NY, NX, NC = 4, 4, 2
MESH = pl.DeviceIdType.MESH
LINK = 46.6e3
PAIR = 330e3
LOCAL = 1500e3
HOP = 3.5
ADD = 0.4
VMEM_LIMIT = 67043328


class Place:
    def __init__(self, nz):
        i, j = lax.axis_index("fsdp"), lax.axis_index("model")
        self.size = {"z": nz, "y": NY, "x": NX, "c": NC}
        self.at = {"z": lax.div(i, NY), "y": lax.rem(i, NY), "x": lax.div(j, NC), "c": lax.rem(j, NC)}

    def get(self, axis, step=0):
        n = self.size[axis]
        return lax.rem(self.at[axis] + (step + 2 * n) % n, n)

    def device(self, axis, step):
        at = dict(self.at)
        at[axis] = self.get(axis, step)
        return {"fsdp": at["z"] * NY + at["y"], "model": at["x"] * NC + at["c"]}

    def meet(self, peers):
        barrier = pltpu.get_barrier_semaphore()
        for axis, step in peers:
            pl.semaphore_signal(barrier, inc=1, device_id=self.device(axis, step), device_id_type=MESH)
        pl.semaphore_wait(barrier, len(peers))


class Flow:
    def __init__(self, place, send_sem, recv_sem, base=0, now=0.0):
        self.place, self.send_sem, self.recv_sem, self.base = place, send_sem, recv_sem, base
        self.now, self.free, self.events, self.copies, self.tasks, self.order = now, {}, [], [], [], 0
        self.sent = set()

    def event(self, when, wait, then):
        heapq.heappush(self.events, (when, self.order, wait, then))
        self.order += 1

    def send(self, axis, step, src, dst, size, then=None, link=None, alt=None):
        k = len(self.copies)
        link = link or (axis, step)
        begin = max(self.now, self.free.get(link, 0.0))
        rate, lag = (PAIR, 1.5) if axis == "c" else (LINK, HOP)
        self.free[link] = begin + size / rate

        def make(dst):
            return pltpu.make_async_remote_copy(
                src_ref=src(),
                dst_ref=dst(),
                send_sem=self.send_sem.at[self.base + k],
                recv_sem=self.recv_sem.at[self.base + k],
                device_id=self.place.device(axis, step),
                device_id_type=MESH,
            )

        copy = make(dst)
        if alt is None:
            copy.start()
        else:
            when, other = alt
            pl.when(jnp.logical_not(when))(copy.start)
            pl.when(when)(make(other).start)
        self.copies.append(copy)
        self.event(self.free[link] + lag, copy.wait_recv, then)
        return k

    def at(self, when, then):
        self.event(when, lambda: None, then)

    def local(self, copy, size, then):
        copy.start()
        self.event(self.now + size / LOCAL + 1.0, copy.wait, then)

    def task(self, cost, do):
        self.tasks.append((cost, do))

    def take(self):
        when, _, wait, then = heapq.heappop(self.events)
        self.now = max(self.now, when)
        wait()
        if then is not None:
            then()

    def spend(self, cost):
        self.now += cost
        while self.events and self.events[0][0] <= self.now:
            self.take()

    def wait_sent(self, k):
        if k not in self.sent:
            self.copies[k].wait_send()
        self.sent.add(k)

    def run(self):
        while self.events or self.tasks:
            if self.tasks and (not self.events or self.events[0][0] > self.now):
                cost, do = self.tasks.pop(0)
                self.now += cost
                do()
            else:
                self.take()

    def close(self):
        for k in range(len(self.copies)):
            self.wait_sent(k)


def after(count, then):
    left = [count]

    def one():
        left[0] -= 1
        if left[0] == 0:
            then()

    return one


def nbytes(ref, lead):
    n = 1
    for d in ref.shape[lead:]:
        n *= d
    return n * jnp.dtype(ref.dtype).itemsize


def any_specs(n):
    return [pl.BlockSpec(memory_space=pl.ANY)] * n


def mm(a, b, ca, cb):
    return lax.dot_general(a, b, (((ca,), (cb,)), ((), ())), preferred_element_type=jnp.float32)


def span(q, n):
    return pl.ds(pl.multiple_of(q * n, n), n)


def exchange(flow, place, src, dst, far, step, done):
    size = nbytes(src, 1)

    def onward(way, half):
        def then():
            flow.send("y", way, lambda: far.at[half], lambda: dst.at[place.get("y", -way), half], size // 2, lambda: done(2, half))

        return then

    if step == 2:
        flow.send("y", 1, lambda: src.at[place.get("y", 2), 0], lambda: far.at[0], size // 2, onward(1, 0))
        flow.send("y", -1, lambda: src.at[place.get("y", 2), 1], lambda: far.at[1], size // 2, onward(-1, 1))
    else:
        flow.send("y", step, lambda: src.at[place.get("y", step)], lambda: dst.at[place.get("y")], size, lambda: done(-step, None))


ORDER = (2, 1, -1, 0)


class Gather:
    def __init__(self, place, flow, own, full, first, cut, arrive):
        self.place, self.flow, self.own, self.full, self.first, self.cut, self.arrive = place, flow, own, full, first, cut, arrive
        self.second = "y" if first == "x" else "x"
        self.size = nbytes(own, 1) * (cut.stop - cut.start) // own.shape[-1]

    def mine(self, half):
        return lambda: self.own.at[half, :, self.cut]

    def spot(self, at, half):
        y, x, c = (self.place.get(axis, at.get(axis, 0)) for axis in "yxc")
        return lambda: self.full.at[y, x, c, half, :, self.cut]

    def moves(self, axis, at, half, src):
        def come(step, onward):
            def then():
                here = dict(at, **{axis: step})
                if onward:
                    far = dict(at, **{axis: 2})
                    self.flow.send(axis, -step, self.spot(here, half), self.spot(here, half), self.size, lambda: self.got(axis, far, half))
                self.got(axis, here, half)

            return then

        return {
            1: lambda: self.flow.send(axis, 1, src, self.spot(at, half), self.size, come(-1, half == 0)),
            -1: lambda: self.flow.send(axis, -1, src, self.spot(at, half), self.size, come(1, half == 1)),
        }

    def spread(self, axis, at, half, src):
        for move in self.moves(axis, at, half, src).values():
            move()

    def got(self, axis, at, half):
        if axis == self.first:
            self.spread(self.second, at, half, self.spot(at, half))
        self.pair(at, half, self.spot(at, half))
        self.arrive(at.get("y", 0), at.get("x", 0))

    def pair(self, at, half, src):
        there = lambda: self.arrive(at.get("y", 0), at.get("x", 0))
        self.flow.send("c", 1, src, self.spot(at, half), self.size, there)

    def start_first(self):
        self.spread_own(self.first)

    def start_second(self):
        self.spread_own(self.second)
        for half in (0, 1):
            self.pair({}, half, self.mine(half))

    def spread_own(self, axis):
        sends = {(half, step): move for half in (0, 1) for step, move in self.moves(axis, {}, half, self.mine(half)).items()}
        for key in ((0, 1), (1, -1), (1, 1), (0, -1)):
            sends[key]()


def front_kernel(
    nz, x_ref, dy_ref, gain, w_qkv, w_out, w_gate, w_up, w_down, h_all, dy_all, w_all, z_got, h_ref, w_ref, w_heads, rows_v, z_in, far, send_sem, recv_sem, own_sem, rows_sem
):
    bf16 = jnp.bfloat16
    place = Place(nz)
    for half in range(2):
        wide = x_ref[half].astype(jnp.float32)
        h_ref[half] = (wide * lax.rsqrt(jnp.mean(wide * wide, axis=-1, keepdims=True) + NORM_EPS) * gain[...]).astype(bf16)
    wide_ff = w_gate.shape[1] // NY
    one = w_out.shape[1] // (NY - 1)
    for q in range(NY):
        ffs = slice(q * wide_ff, (q + 1) * wide_ff)
        w_ref[q, :, :wide_ff] = w_gate[:, ffs]
        w_ref[q, :, wide_ff : 2 * wide_ff] = w_up[:, ffs]
        at = 2 * wide_ff
        w_ref[q, :, at : at + one] = w_qkv[:, q * one : (q + 1) * one]
        w_ref[q, :, at + one : at + 2 * one] = w_out[:, q * one : (q + 1) * one] if q < NY - 1 else w_qkv[:, NY * one :]
        w_ref[q, :, at + 2 * one :] = w_down[:, ffs]
    y, x, c, z = (place.get(axis) for axis in "yxcz")
    last = y == NY - 1
    pair = z_in.shape[-1]
    head = pair // 2
    width = h_ref.shape[-1]
    cols = w_ref.shape[-1]
    lo = (cols - pair) * 2 // 3
    hi = lo + pair
    rows = z_in.shape[2]
    flow = Flow(place, send_sem, recv_sem)
    w_own = pltpu.make_async_copy(w_ref.at[y, :, :lo], w_all.at[0, z, y, :, :lo], own_sem.at[2])
    w_own_down = pltpu.make_async_copy(w_ref.at[y, :, hi:], w_all.at[0, z, y, :, hi:], own_sem.at[4 + NX])
    w_own.start()
    w_own_down.start()
    heads_home = pltpu.make_async_copy(w_heads, w_all.at[0, :, :, :, lo:hi], own_sem.at[3])
    w_heads[z, y] = w_ref[y, :, lo:hi]
    place.meet([("x", 1), ("x", -1), ("y", 1), ("y", -1), ("y", 2), ("z", 1), ("z", -1), ("c", 1)])

    slots = rows_v.shape[0]
    free, queue, ready = list(range(slots)), [], []
    pieces = {}
    parts_done = {}
    weights = [4 * nz]

    def load():
        while free and queue and weights[0] == 0:
            kind, dy, dx = queue.pop(0)
            slot = free.pop(0)
            src = (h_all, dy_all)[kind].at[place.get("y", dy), place.get("x", dx)]
            copy = pltpu.make_async_copy(src, rows_v.at[slot], rows_sem.at[slot])
            flow.local(copy, nbytes(rows_v, 1), lambda slot=slot, kind=kind, dy=dy, dx=dx: flow.task(CHUNK_TIME, lambda: product(kind, dy, dx, slot)))

    def arrive(kind):
        need = (8, 4)[kind]

        def one(dy, dx):
            key = (kind, dy, dx)
            pieces[key] = pieces.get(key, 0) + 1
            if pieces[key] == need:
                queue.append(key)
                load()

        return one

    def weight_come():
        weights[0] -= 1
        if weights[0] == 0:
            heads_home.start()
            load()

    def product(kind, dy, dx, slot):
        at = place.get("y", dy), place.get("x", dx)
        step = 2 if nz % 2 == 0 else 1
        deep = step * (width // nz)

        def dot(first):
            def some(i, total):
                left = rows_v[slot, :, :, :, span(i, deep)].reshape(rows, deep)
                right = w_heads[pl.ds(i * step, step), :, :, first:].reshape(deep, pair - first)
                return total + mm(left, right, 1, 0)

            return lax.fori_loop(0, nz // step, some, jnp.zeros((rows, pair - first), jnp.float32))

        if kind == 0:
            made = dot(0).astype(bf16)
            z_in[at[0], at[1], :, :head] = made[:, :head]

            @pl.when(last)
            def _():
                z_in[at[0], at[1], :, head:] = made[:, head:]

        else:

            @pl.when(jnp.logical_not(last))
            def _():
                z_in[at[0], at[1], :, head:] = dot(head).astype(bf16)

        free.append(slot)
        load()
        parts_done[dy, dx] = parts_done.get((dy, dx), 0) + 1
        if parts_done[dy, dx] == 2:
            deliver(dy, dx)

    own_copies = []

    def deliver(dy, dx):
        at = lambda: z_in.at[place.get("y", dy), place.get("x", dx)]
        size = nbytes(z_in, 2)

        def there(step=0):
            return lambda: z_got.at[place.get("y", step), place.get("x", dx)]

        if dy == 0:
            copy = pltpu.make_async_copy(at(), there()(), own_sem.at[4 + dx % NX])
            copy.start()
            own_copies.append(copy)
        elif dy == 2 and dx in DIRECT:
            flow.send("y", 2, at, there(), size, link=("y", 1))
        elif dy == 2:
            way = 1 if dx in (0, 2) else -1

            def onward():
                flow.send("y", way, lambda: far.at[dx % NX], there(-way), size)

            flow.send("y", way, at, lambda: far.at[dx % NX], size, onward)
        else:
            flow.send("y", dy, at, there(), size)

    def w_part(ref, who, dz, dy, cut):
        if ref is None:
            return lambda: w_heads.at[place.get("z", dz), place.get("y", dy)]
        return lambda: w_all.at[who, place.get("z", dz), place.get("y", dy), :, cut]

    cuts = [slice(lo, hi), slice(0, lo), slice(hi, cols)]

    def ring(step, dy, n_cut, src=None, hops=nz - 1, lead=True):
        cut = cuts[n_cut]
        home = None if n_cut == 0 else w_all
        size = nbytes(w_ref, 1) * (cut.stop - cut.start) // cols

        def hop(n):
            def then():
                here = src if src and n == 0 else w_part(home, 0, -step * n, dy, cut)
                if n < hops:
                    flow.send("z", step, here, w_part(home, 0, -step * n, dy, cut), size, hop(n + 1))
                if n or lead:
                    flow.send("c", 1, here, w_part(w_all, 1, -step * n, dy, cut), size)
                    if n_cut == 0:
                        weight_come()

            return then

        return hop(0)

    def rings(dy, n_cut, src=None):
        if n_cut:
            return ring(1 if dy in (0, 1) else -1, dy, n_cut, src)
        both = [ring(1, dy, 0, src, nz // 2), ring(-1, dy, 0, src, (nz - 1) // 2, False)]
        return lambda: [one() for one in both]

    def w_at(dy, cut):
        return lambda: w_ref.at[place.get("y", dy), :, cut]

    tail = width // nz * H_TAIL
    gathers = [
        Gather(place, flow, h_ref, h_all, "x", slice(0, width - tail), arrive(0)),
        Gather(place, flow, dy_ref, dy_all, "y", slice(0, width), arrive(1)),
        Gather(place, flow, h_ref, h_all, "y", slice(width - tail, width), arrive(0)),
    ]
    def w_start(n_cut, dys):
        cut = cuts[n_cut]
        home = None if n_cut == 0 else w_all
        size = nbytes(w_ref, 1) * (cut.stop - cut.start) // cols
        there = w_part(home, 0, 0, 0, cut)
        for dy in dys:
            if dy == 0:
                rings(0, n_cut, w_at(0, cut))()
            elif dy == 2:
                flow.send("y", 2, w_at(2, cut), there, size, rings(2, n_cut), link=("y", 1))
            else:
                flow.send("y", -dy, w_at(-dy, cut), there, size, rings(dy, n_cut))

    w_start(0, (0, 1, -1, 2))
    for one in gathers:
        one.start_first()
    flow.at(W_TIMES[0], lambda: [w_start(1, (0, -1)), w_start(2, (0, -1))])
    flow.at(W_TIMES[1], lambda: [w_start(1, (1, 2)), w_start(2, (1, 2))])
    for one in gathers:
        one.start_second()
    for n, (ref, full) in enumerate(((h_ref, h_all), (dy_ref, dy_all))):
        copy = pltpu.make_async_copy(ref, full.at[y, x, c], own_sem.at[n])
        there = arrive(n)
        flow.local(copy, nbytes(ref, 0), lambda n=n, there=there: [there(0, 0) for _ in range((4, 2)[n])])
    flow.run()
    w_own.wait()
    w_own_down.wait()
    flow.close()
    for copy in own_copies:
        copy.wait()
    heads_home.wait()


CHUNK_TIME = 1.0
W_TIMES = (0.0, 0.0)
DIRECT = (2, 1, -1)
H_TAIL = 1


def front(nz, x, dy, gain, w_qkv, w_out, w_gate, w_up, w_down):
    half, rows, width = x.shape
    everywhere = (NY, NX, NC) + x.shape
    slab = w_qkv.shape[0]
    pair = 2 * w_out.shape[1] // (NY - 1)
    cols = pair + 3 * w_gate.shape[1] // NY
    w_shape = (NY, slab, cols)
    bf16 = x.dtype
    gathers = 3 * (30 + 32)
    count = gathers + 3 * 3 + 3 * 4 * (nz - 1) + 3 * 4 * nz + 2 * NX + 2 * NX
    vmem = pl.BlockSpec(memory_space=pltpu.VMEM)
    dma = pltpu.SemaphoreType.DMA
    chunk = NC * half * rows
    z_shape = (NY, NX, chunk, pair)
    slots = 8
    return pl.pallas_call(
        functools.partial(front_kernel, nz),
        out_shape=(
            jax.ShapeDtypeStruct(everywhere, bf16),
            jax.ShapeDtypeStruct(everywhere, bf16),
            jax.ShapeDtypeStruct((NC, nz) + w_shape, bf16),
            jax.ShapeDtypeStruct(z_shape, bf16),
        ),
        in_specs=[vmem] * 8,
        out_specs=tuple(any_specs(4)),
        scratch_shapes=[
            pltpu.VMEM(x.shape, bf16),
            pltpu.VMEM(w_shape, bf16),
            pltpu.VMEM((nz,) + w_shape[:-1] + (pair,), bf16),
            pltpu.VMEM((slots, NC) + x.shape, bf16),
            pltpu.VMEM(z_shape, bf16),
            pltpu.VMEM((NX, chunk, pair), bf16),
            dma((count,)),
            dma((count,)),
            dma((5 + NX,)),
            dma((slots,)),
        ],
        compiler_params=pltpu.CompilerParams(collective_id=0, has_side_effects=True, vmem_limit_bytes=VMEM_LIMIT),
        name="front",
    )(x, dy, gain, w_qkv, w_out, w_gate, w_up, w_down)


SETS = (2, 1, -1, 0)


def attention(z_got, z_back, keys, vals, dk, dv, cos_ref, sin_ref):
    bf16 = jnp.bfloat16
    seq, head = keys.shape
    part = seq // 2
    count = z_got.shape[0] - 1
    scale = head**-0.5
    spread = z_back.shape[2:5] + (head,)
    halves = [pl.ds(p * part, part) for p in range(2)]

    def turn(values, at, sign):
        wide = values.astype(jnp.float32)
        swapped = pltpu.roll(wide, head // 2, 1)
        return (wide * cos_ref[at, :] + sign * (swapped * sin_ref[at, :])).astype(bf16)

    for p in range(2):
        keys[halves[p], :] = turn(z_got[count, p, :, :head], halves[p], 1.0)
        vals[halves[p], :] = z_got[count, p, :, head:]
    dk[...] = jnp.zeros_like(dk)
    dv[...] = jnp.zeros_like(dv)

    @pl.loop(0, count)
    def _(i):
        for p in range(2):
            n = (p + 1) * part
            query = turn(z_got[i, p, :, :head], halves[p], 1.0)
            d_out = z_got[i, p, :, head:]
            scores = mm(query, keys[:n, :], 1, 1) * scale
            causal = lax.broadcasted_iota(jnp.int32, scores.shape, 0) + p * part >= lax.broadcasted_iota(jnp.int32, scores.shape, 1)
            scores = jnp.where(causal, scores, -1e30)
            grown = jnp.exp(scores - jnp.max(scores, axis=1, keepdims=True))
            probs = grown / jnp.sum(grown, axis=1, keepdims=True)
            probs_low = probs.astype(bf16)
            z_back[i, p, :, :, :, head:] = mm(probs_low, vals[:n, :], 1, 0).astype(bf16).reshape(spread)
            d_probs = mm(d_out, vals[:n, :], 1, 1).astype(bf16).astype(jnp.float32)
            d_scores = (probs * (d_probs - jnp.sum(probs * d_probs, axis=1, keepdims=True)) * scale).astype(bf16)
            z_back[i, p, :, :, :, :head] = turn(mm(d_scores, keys[:n, :], 1, 0).astype(bf16), halves[p], -1.0).reshape(spread)
            dk[:n, :] += mm(d_scores, query, 0, 0)
            dv[:n, :] += mm(probs_low, d_out, 0, 0)

    for p in range(2):
        z_back[count, p, :, :, :, :head] = turn(dk[halves[p], :].astype(bf16), halves[p], -1.0).reshape(spread)
        z_back[count, p, :, :, :, head:] = dv[halves[p], :].astype(bf16).reshape(spread)


def gated(place, flow, h_all, dy_all, w_all, acts, row_sem, share, h_rows, dy_rows, w_v):
    bf16 = jnp.bfloat16
    ff = acts.shape[-1] // 3
    lo = 2 * ff
    part = h_rows.shape[1]
    shape = acts.shape[2:5] + (ff,)
    w_loads = [
        pltpu.make_async_copy(w_all.at[0, :, :lo], w_v.at[:, :lo], row_sem.at[2, 0]),
        pltpu.make_async_copy(w_all.at[0, :, w_all.shape[2] - ff :], w_v.at[:, lo:], row_sem.at[2, 1]),
    ]

    def loads(n, slot):
        return [pltpu.make_async_copy(a.at[span(n, part)], b.at[slot], row_sem.at[slot, m]) for m, (a, b) in enumerate(((h_all, h_rows), (dy_all, dy_rows)))]

    def begin():
        for copy in w_loads + loads(0, 0) + loads(1, 1):
            copy.start()

    def go():
        for copy in w_loads:
            copy.wait()
        for q in range(NY):

            @pl.loop(0, 2)
            def _(p):
                n = 2 * q + p
                for copy in loads(n, p):
                    copy.wait()
                gate = mm(h_rows[p], w_v[:, :ff], 1, 0).astype(bf16).astype(jnp.float32)
                up = mm(h_rows[p], w_v[:, ff:lo], 1, 0).astype(bf16).astype(jnp.float32)
                d_act = mm(dy_rows[p], w_v[:, lo:], 1, 0).astype(bf16).astype(jnp.float32)
                if q < NY - 1:
                    for copy in loads(n + 2, p):
                        copy.start()
                sig = jax.nn.sigmoid(gate)
                silu = gate * sig
                acts[q, p, :, :, :, :ff] = (d_act * up * (sig + silu * (1.0 - sig))).astype(bf16).reshape(shape)
                acts[q, p, :, :, :, ff:lo] = (d_act * silu).astype(bf16).reshape(shape)
                acts[q, p, :, :, :, lo:] = (silu * up).astype(bf16).reshape(shape)

            share(q)
            flow.spend(3.0)

    return begin, go


class Plane:
    def __init__(self, place, flow, tiles, land, first, finish, free):
        self.place, self.flow, self.tiles, self.land, self.first = place, flow, tiles, land, first
        self.second = "y" if first == "x" else "x"
        self.piece = nbytes(tiles, 3)
        self.sums, self.waiting, self.finished = {}, {}, [0] * len(SETS)
        self.free = free
        self.rings = []
        for s, other in enumerate(SETS):

            def raw(step, half, s=s):
                return lambda: tiles.at[s % 2, place.get(first, step), half]

            self.rings.append(self.ring(first, raw, lambda step, half, then: then(), s, self.first_done(s, other)))
        self.onward, _ = self.ring(self.second, lambda step, half: self.sums[step, half], self.need, len(SETS), finish)

    def need(self, step, half, then):
        if (step, half) in self.sums:
            then()
        else:
            self.waiting.setdefault((step, half), []).append(then)

    def first_done(self, s, step):
        def done(half, ref):
            self.sums[step, half] = ref
            for then in self.waiting.pop((step, half), []):
                then()
            self.onward(step, half)
            self.finished[s] += 1
            if self.finished[s] == 2:
                self.free(s)

        return done

    def add(self, mine, other):
        a, b = mine(), other()
        a[...] = a[...] + b[...]
        self.flow.now += ADD

    def ring(self, axis, raw, need, s, done):
        flow, add, sent = self.flow, self.add, []

        def slot(i):
            return lambda: self.land.at[s, i]

        def turn(i, goal, half, step):
            def then():
                add(slot(i), raw(goal, half))
                flow.send(axis, step, slot(i), slot(i + 4), self.piece, final[half])

            return lambda: need(goal, half, then)

        def ending(half):
            def then():
                mine, other = (slot(5), slot(2)) if half == 0 else (slot(4), slot(3))
                add(mine, other)
                add(mine, raw(0, half))
                done(half, mine)

            return lambda: need(0, half, then)

        final = [after(2, ending(0)), after(2, ending(1))]
        moves = {
            (2, 1): (1, 0, turn(0, 1, 1, 1)),
            (2, 0): (-1, 1, turn(1, -1, 0, -1)),
            (1, 0): (1, 2, final[0]),
            (-1, 1): (-1, 3, final[1]),
        }

        def start(goal, half):
            if (goal, half) in moves:
                step, i, then = moves[goal, half]
                sent.append(flow.send(axis, step, raw(goal, half), slot(i), self.piece, then))

        return start, sent

    def start(self, s):
        for goal, half in ((2, 1), (2, 0), (1, 0), (-1, 1)):
            self.rings[s][0](goal, half)

    def clear(self, s):
        for k in self.rings[s][1]:
            self.flow.wait_sent(k)


class Grads:
    flow = None


    def __init__(self, nz, place, h_all, dy_all, acts, z_out, z_land, outs, far, h_plus, h_minus, dy_minus, tiles, stage, load_sem, stage_sem, own_sem):
        self.__dict__.update({k: v for k, v in locals().items() if k != "self"})
        self.ff = acts.shape[-1] // 3
        self.pair = z_out.shape[-1]
        lo = 2 * self.ff
        self.cols = [(0, self.ff), (self.ff, lo), (lo + self.pair, lo + self.pair + self.ff), (lo, lo + self.pair)]
        self.way = (1, 1, -1, -1)
        self.far_way = (1, -1, 1, -1)
        self.block = tiles.shape[2]
        self.size = nbytes(tiles, 2)
        self.ready, self.waiting, self.used = set(), {}, 0
        self.users = [[] for _ in range(stage.shape[0])]
        self.own = []
        self.idle, self.first = {}, {}

    def load(self, ref, src, index, step, n):
        b = self.place.get("z", -step * (n + 1))
        at = pl.ds(pl.multiple_of(b * self.block, self.block), self.block)
        return pltpu.make_async_copy(src.at[:, at], ref, self.load_sem.at[index])

    def loads_plus(self, n):
        return [self.load(self.h_plus, self.h_all, 0, 1, n)]

    def loads_minus(self, n):
        return [self.load(self.h_minus, self.h_all, 1, -1, n), self.load(self.dy_minus, self.dy_all, 2, -1, n)]

    def begin(self):
        for copy in self.loads_plus(0) + self.loads_minus(0):
            copy.start()

    def gather_up(self, tiles, some):
        seq = self.h_plus.shape[0] // NY
        for tile in tiles:
            tile[...] = jnp.zeros_like(tile)

        @pl.loop(0, NY)
        def _(q):
            for tile, value in zip(tiles, some(q, span(q, seq))):
                tile[...] += value

    def set_ready(self, lane, n):
        self.ready.add((lane, n))
        for then in self.waiting.pop((lane, n), []):
            then()
        if n == 0:
            k = self.flow.send("z", self.way[lane], lambda: self.tiles.at[0, lane], lambda: self.z_land.at[0, lane], self.size, self.hop(lane, 0))
            self.first[lane] = k

    def clear(self, lane, n):
        if n == 2:
            self.flow.wait_sent(self.first[lane])

    def tokens(self, ref):
        value = ref[...]
        return value.reshape(-1, value.shape[-1])

    def make_plus(self, n):
        for copy in self.loads_plus(n):
            copy.wait()
        lo = 2 * self.ff

        def some(q, rows):
            both = mm(self.h_plus[rows, :], self.acts[q, :, :, :, :, :lo].reshape(-1, lo), 0, 0)
            return both[:, : self.ff], both[:, self.ff :]

        self.gather_up([self.tiles.at[n % 2, 0], self.tiles.at[n % 2, 1]], some)
        if n + 1 < self.nz:
            for copy in self.loads_plus(n + 1):
                copy.start()

    def for_down(self, q, rows):
        return [mm(self.dy_minus[rows, :], self.acts[q, :, :, :, :, 2 * self.ff :].reshape(-1, self.ff), 0, 0)]

    def for_heads(self, q, rows):
        last = self.place.get("y") == NY - 1
        head = self.pair // 2
        out = self.z_out[q].reshape(-1, self.pair)
        both = mm(self.h_minus[rows, :], out, 0, 0)
        right = jnp.where(last, both[:, head:], mm(self.dy_minus[rows, :], out[:, head:], 0, 0))
        return [jnp.concatenate([both[:, :head], right], axis=1)]

    def make_minus(self, n):
        for copy in self.loads_minus(n):
            copy.wait()
        self.gather_up([self.tiles.at[n % 2, 2], self.tiles.at[n % 2, 3]], lambda q, rows: self.for_down(q, rows) + self.for_heads(q, rows))
        self.load_minus_next(n)

    def load_minus_next(self, n):
        if n + 1 < self.nz:
            for copy in self.loads_minus(n + 1):
                copy.start()

    def make_first(self):
        self.make_plus(0)
        for copy in self.loads_minus(0):
            copy.wait()
        self.gather_up([self.tiles.at[0, 2]], self.for_down)

    def heads_first(self):
        def do():
            self.gather_up([self.tiles.at[0, 3]], self.for_heads)
            self.load_minus_next(0)
            self.set_ready(3, 0)

        self.flow.task(1.3, do)

    def plus(self, n):
        def do():
            for lane in (0, 1):
                self.clear(lane, n)
            self.make_plus(n)
            for lane in (0, 1):
                self.set_ready(lane, n)

        self.flow.task(1.6, do)

    def minus(self, n):
        def do():
            for lane in (2, 3):
                self.clear(lane, n)
            self.make_minus(n)
            for lane in (2, 3):
                self.set_ready(lane, n)

        self.flow.task(2.2, do)

    def need(self, lane, n, then):
        if (lane, n) in self.ready:
            then()
        else:
            self.waiting.setdefault((lane, n), []).append(then)

    def next(self, lane, n):
        if n + 2 >= self.nz:
            return
        key = (lane // 2, n)
        self.idle[key] = self.idle.get(key, 0) + 1
        if self.idle[key] == 2:
            (self.plus, self.minus)[lane // 2](n + 2)

    def hop(self, lane, s):
        flow, place = self.flow, self.place

        def come():
            slot = self.used % len(self.users)
            self.used += 1
            for wait in self.users[slot]:
                wait()
            self.users[slot] = []
            here = lambda: self.stage.at[slot]

            def staged():
                self.need(lane, s + 1, use)

            def use():
                ref = here()
                ref[...] = ref[...] + self.tiles[(s + 1) % 2, lane]
                flow.now += ADD
                if s == 0:
                    self.next(lane, 0)
                self.next(lane, s + 1)
                if s + 1 < self.nz - 1:
                    k = flow.send("z", self.way[lane], here, lambda: self.z_land.at[s + 1, lane], self.size, self.hop(lane, s + 1))
                    self.users[slot].append(lambda: flow.wait_sent(k))
                else:
                    self.home(lane, slot)

            flow.local(pltpu.make_async_copy(self.z_land.at[s, lane], here(), self.stage_sem.at[slot]), self.size, staged)

        return come

    def home(self, lane, slot):
        flow, place = self.flow, self.place
        slab = self.block // NY
        way = self.far_way[lane]
        size = self.size // NY

        def rows(step, cut=slice(None)):
            return lambda: self.stage.at[slot, pl.ds(pl.multiple_of(place.get("y", step) * slab, slab), slab), cut]

        def columns(out, step, wide):
            at = place.get("y", step) * wide
            return lambda: self.outs[out].at[:, pl.ds(pl.multiple_of(at, wide), wide)]

        def deliver(size, src, far, dst, n, other=None):
            def alt(step):
                return None if other is None else (place.get("y", step) == NY - 1, other(step))

            def onward():
                flow.send("y", way, far, dst(-way), size, alt=alt(-way))

            sent = [flow.send("y", way, src(2), far, size, onward)]
            sent += [flow.send("y", step, src(step), dst(0), size, alt=alt(0)) for step in (1, -1)]
            copies = [(None, pltpu.make_async_copy(src(0)(), dst(0)(), self.own_sem.at[n]))]
            if other is not None:
                last = place.get("y") == NY - 1
                copies = [(jnp.logical_not(last), copies[0][1]), (last, pltpu.make_async_copy(src(0)(), other(0)(), self.own_sem.at[n]))]
            for when, copy in copies:
                if when is None:
                    copy.start()
                else:
                    pl.when(when)(copy.start)
            self.users[slot] += [functools.partial(flow.wait_sent, k) for k in sent] + [copies[0][1].wait]

        if lane < 3:
            deliver(size, rows, lambda: self.far.at[lane], lambda step: columns(lane, step, self.ff), lane)
            return
        head = self.pair // 2
        first, second = slice(0, head), slice(head, self.pair)
        deliver(size // 2, lambda step: rows(step, first), lambda: self.far.at[3, :, first], lambda step: columns(3, step, head), 3)
        value = lambda: self.outs[3].at[:, NY * head :]

        def out_rows(step):
            at = lax.rem(place.get("y", step), NY - 1) * head
            return lambda: self.outs[4].at[:, pl.ds(pl.multiple_of(at, head), head)]

        deliver(size // 2, lambda step: rows(step, second), lambda: self.far.at[3, :, second], out_rows, 4, lambda step: value)

    def close(self):
        for users in self.users:
            for wait in users:
                wait()


def back_kernel(
    nz,
    z_in,
    h_all,
    dy_all,
    w_all,
    cos_in,
    sin_in,
    gain,
    x_in,
    dy_in,
    y_out,
    dx_out,
    g_qkv,
    g_out,
    g_gate,
    g_up,
    g_down,
    z_land,
    x_ref,
    dy_ref,
    cos_ref,
    sin_ref,
    z_got,
    z_back,
    z_out,
    far_back,
    acts,
    pair_acts,
    far,
    p_land,
    q_land,
    keys,
    vals,
    dk,
    dv,
    h_plus,
    h_minus,
    dy_minus,
    tiles,
    stage,
    load_sem,
    row_sem,
    w_sem,
    g_load_sem,
    stage_sem,
    own_sem,
    send_sem,
    recv_sem,
):
    bf16, f32 = jnp.bfloat16, jnp.float32
    place = Place(nz)
    y, c = place.get("y"), place.get("c")
    other = place.get("c", 1)
    last = y == NY - 1
    seq, head = keys.shape
    pair = 2 * head
    rows, cols = pair_acts.shape[3:]
    ff = (cols - pair) // 3
    lo, hi = 2 * ff, 2 * ff + pair
    tokens, width = h_all.shape
    block = width // nz
    part = seq // 2

    z_load = pltpu.make_async_copy(z_in, z_got, load_sem)
    z_load.start()
    row_loads = [pltpu.make_async_copy(a, b, own_sem.at[5 + n]) for n, (a, b) in enumerate(((x_in, x_ref), (dy_in, dy_ref)))]
    cos_ref[...] = jnp.concatenate([cos_in[...], cos_in[...]], axis=0).T
    sin_ref[...] = jnp.concatenate([-sin_in[...], sin_in[...]], axis=0).T
    early = Flow(place, send_sem, recv_sem)
    peers = [("x", 1), ("x", -1), ("y", 1), ("y", -1), ("z", 1), ("z", -1), ("c", 1)]

    def share(q):
        early.send("c", 1, lambda: acts.at[q, :, :, other, :, :lo], lambda: pair_acts.at[q, :, :, :, :lo], nbytes(pair_acts, 1) * lo // cols)
        early.send("c", 1, lambda: acts.at[q, :, :, other, :, lo:], lambda: pair_acts.at[q, :, :, :, hi:], nbytes(pair_acts, 1) * ff // cols)

    def out_come(step, half):
        cut = slice(None) if half is None else half
        part = nbytes(z_out, 1) // NC // (1 if half is None else 2)
        src = lambda: z_out.at[place.get("y", step), cut, :, other]
        early.send("c", 1, src, lambda: pair_acts.at[place.get("y", step), cut, :, :, lo:hi], part)

    grads = Grads(nz, place, h_all, dy_all, acts, z_out, z_land, (g_gate, g_up, g_down, g_qkv, g_out), far, h_plus, h_minus, dy_minus, tiles, stage, g_load_sem, stage_sem, own_sem)

    def first(h_rows, dy_rows, w_v):
        begin, go = gated(place, early, h_all, dy_all, w_all, acts, row_sem, share, h_rows, dy_rows, w_v)
        begin()
        grads.begin()
        for copy in row_loads:
            copy.start()
        z_load.wait()
        attention(z_got, z_back, keys, vals, dk, dv, cos_ref, sin_ref)
        place.meet(peers)
        for step in ORDER[:3]:
            exchange(early, place, z_back, z_out, far_back, step, out_come)
        z_out[y] = z_back[y]
        early.send("c", 1, lambda: z_back.at[y, :, :, other], lambda: pair_acts.at[y, :, :, :, lo:hi], nbytes(z_out, 1) // NC)
        go()
        grads.make_first()
        early.now += 2.6
        early.run()
        early.close()
        for copy in row_loads:
            copy.wait()

    pl.run_scoped(
        first,
        pltpu.VMEM((2, part, width), bf16),
        pltpu.VMEM((2, part, width), bf16),
        pltpu.VMEM((width, 3 * ff), bf16),
    )

    def second(p_tile, q_tile, w_v):
        flow = Flow(place, send_sem, recv_sem, len(early.copies), early.now)
        grads.flow = flow
        lane = lax.broadcasted_iota(jnp.int32, (rows, pair), 1)
        for_d = jnp.logical_or(lane < head, last)

        def chunk(k, i, p, xx):
            if k == 0:
                own = acts[i, p, xx, c]
                return own[:, :lo], z_out[i, p, xx, c], own[:, lo:]
            theirs = pair_acts[i, p, xx]
            return theirs[:, :lo], theirs[:, lo:hi], theirs[:, hi:]

        def for_out(k, i, p, xx):
            _, mixed, act = chunk(k, i, p, xx)
            return jnp.concatenate([jnp.where(for_d, jnp.zeros_like(mixed), mixed), act], axis=1)

        def for_in(k, i, p, xx):
            grad, mixed, _ = chunk(k, i, p, xx)
            return jnp.concatenate([grad, jnp.where(for_d, mixed, jnp.zeros_like(mixed))], axis=1)

        depth = w_v.shape[0]

        def w_copy(kind, d, slot):
            at = pl.ds(pl.multiple_of(d * block, block), block)
            cut = slice(lo, cols) if kind == 0 else slice(0, cols)
            return pltpu.make_async_copy(w_all.at[:, at, cut], w_v.at[slot, :, :, cut], w_sem.at[slot])

        counts = (nz - 1, nz)
        base, total = [], 0
        for kind, _ in PASSES:
            base.append(total)
            total += counts[kind]
        kind = PASSES[0][0]
        for n in range(depth):
            w_copy(kind, n, n).start() if n < counts[kind] else w_copy(PASSES[1][0], n - counts[kind], n).start()
        turn = [0]

        def blocks(s, kind, first, count, body):
            n = turn[0]
            assert PASSES[n] == (kind, s)
            if first + count == counts[kind]:
                turn[0] += 1

            @pl.loop(first, first + count)
            def _(d):
                slot = lax.rem(base[n] + d, depth)
                w_copy(kind, d, slot).wait()
                body(d, w_v.at[slot])

                @pl.when(d + depth < counts[kind])
                def _():
                    w_copy(kind, d + depth, slot).start()

                if n + 1 < len(PASSES):

                    @pl.when(d + depth >= counts[kind])
                    def _():
                        w_copy(PASSES[n + 1][0], d + depth - counts[kind], slot).start()

        def product(parts, w, a, b):
            total = None
            for k in range(NC):
                left = jnp.concatenate([one(k) for one in parts], axis=0)
                one = mm(left, w[k, :, a:b], 1, 1)
                total = one if total is None else total + one
            return total

        shape = (NX, 2, rows // 2, block)

        def p_rows(s):
            x = place.get("x", SETS[s])
            p, xx = lax.div(x, NX // 2), lax.rem(x, NX // 2)
            return [lambda k, i=i: for_out(k, i, p, xx) for i in range(NY)]

        def q_rows(s, make):
            i = place.get("y", SETS[s])
            return [lambda k, p=p, xx=xx: make(k, i, p, xx) for p in range(2) for xx in range(NX // 2)]

        def place_of(d):
            return pl.ds(pl.multiple_of(d * block, block), block)

        def p_task(s):
            def body(d, w):
                p_tile[s % 2, :, :, :, place_of(d)] = product(p_rows(s), w, lo, cols).reshape(shape)

            def do():
                if s >= 2:
                    planes[0].clear(s - 2)
                blocks(s, 0, 0, nz - 1, body)
                planes[0].start(s)

            flow.task(P_TIME, do)

        def q_task(s):
            def body(d, w):
                q_tile[s % 2, :, :, :, place_of(d)] = product(q_rows(s, for_in), w, 0, hi).reshape(shape)

                @pl.when(d == nz - 1)
                def _():
                    q_tile[s % 2, :, :, :, width:] = product(q_rows(s, for_out), w, lo, cols).reshape(shape)

            def start():
                if s >= 2:
                    planes[1].clear(s - 2)
                blocks(s, 1, 0, nz // 2, body)

            def end():
                blocks(s, 1, nz // 2, nz - nz // 2, body)
                planes[1].start(s)

            flow.task(Q_HALF, start)
            flow.task(Q_HALF, end)

        edge = width - block
        def p_finish(half, ref):
            y_out[half, :, :edge] = (x_ref[half, :, :edge].astype(f32) + ref()[...]).astype(bf16)

        def q_finish(half, ref):
            y_out[half, :, edge:] = (x_ref[half, :, edge:].astype(f32) + ref()[:, width:]).astype(bf16)
            wide = x_ref[half].astype(f32)
            scale = lax.rsqrt(jnp.mean(wide * wide, axis=-1, keepdims=True) + NORM_EPS)
            d_normed = ref()[:, :width].astype(bf16).astype(f32) * gain[...]
            mean = jnp.mean(d_normed * wide, axis=-1, keepdims=True)
            grad = d_normed * scale - wide * (scale * scale * scale * mean)
            dx_out[half] = (dy_ref[half].astype(f32) + grad).astype(bf16)

        def free(task):
            return lambda s: task(s + 2) if s + 2 < len(SETS) else None

        planes = [
            Plane(place, flow, p_tile, p_land, "y", p_finish, free(p_task)),
            Plane(place, flow, q_tile, q_land, "x", q_finish, free(q_task)),
        ]

        for lane in range(3):
            grads.set_ready(lane, 0)
        q_task(0)
        p_task(0)
        grads.heads_first()
        grads.plus(1)
        grads.minus(1)
        p_task(1)
        q_task(1)
        flow.run()
        flow.close()
        grads.close()

    pl.run_scoped(
        second,
        pltpu.VMEM((2, NY, 2, rows // 2, width - block), f32),
        pltpu.VMEM((2, NX, 2, rows // 2, width + block), f32),
        pltpu.VMEM((3, NC, block, cols), bf16),
    )


STAGES = 5
PASSES = ((1, 0), (0, 0), (0, 1), (1, 1), (1, 2), (0, 2), (0, 3), (1, 3))
P_TIME = 3.0
Q_HALF = 2.6


def back(nz, z_in, h_all, dy_all, w_all, cos, sin, x, dy, gain):
    tokens, width = h_all.shape
    seq, head = cos.shape[1], 2 * cos.shape[0]
    pair = 2 * head
    cols = w_all.shape[2]
    ff = (cols - pair) // 3
    rows = seq // (NX * NC)
    block = width // nz
    bf16, f32 = h_all.dtype, jnp.float32
    vmem = pl.BlockSpec(memory_space=pltpu.VMEM)
    dma = pltpu.SemaphoreType.DMA
    blocks = (NY, 2, NX // 2, NC, rows, pair)
    p_piece = (rows // 2, width - block)
    q_piece = (rows // 2, width + block)
    count = 6 + 2 * NY + 5 + 4 * (nz - 1) + 5 * 4 + 2 * 5 * 6
    slab = block // NY
    weight = jax.ShapeDtypeStruct((slab, NY * ff), f32)
    return pl.pallas_call(
        functools.partial(back_kernel, nz),
        out_shape=(
            jax.ShapeDtypeStruct(x.shape, bf16),
            jax.ShapeDtypeStruct(x.shape, bf16),
            jax.ShapeDtypeStruct((slab, (NY + 1) * head), f32),
            jax.ShapeDtypeStruct((slab, (NY - 1) * head), f32),
            weight,
            weight,
            weight,
            jax.ShapeDtypeStruct((nz - 1, 4, block, ff), f32),
        ),
        in_specs=any_specs(4) + [vmem] * 3 + any_specs(2),
        out_specs=(vmem, vmem) + tuple(any_specs(6)),
        scratch_shapes=[
            pltpu.VMEM(x.shape, bf16),
            pltpu.VMEM(x.shape, bf16),
            pltpu.VMEM((seq, head), f32),
            pltpu.VMEM((seq, head), f32),
            pltpu.VMEM(z_in.shape, bf16),
            pltpu.VMEM(blocks, bf16),
            pltpu.VMEM(blocks, bf16),
            pltpu.VMEM(blocks[1:], bf16),
            pltpu.VMEM(blocks[:-1] + (3 * ff,), bf16),
            pltpu.VMEM(blocks[:3] + (rows, cols), bf16),
            pltpu.VMEM((4, block // NY, ff), f32),
            pltpu.VMEM((5, 6) + p_piece, f32),
            pltpu.VMEM((5, 6) + q_piece, f32),
            pltpu.VMEM((seq, head), bf16),
            pltpu.VMEM((seq, head), bf16),
            pltpu.VMEM((seq, head), f32),
            pltpu.VMEM((seq, head), f32),
            pltpu.VMEM((tokens, block), bf16),
            pltpu.VMEM((tokens, block), bf16),
            pltpu.VMEM((tokens, block), bf16),
            pltpu.VMEM((2, 4, block, ff), f32),
            pltpu.VMEM((STAGES, block, ff), f32),
            dma,
            dma((3, 2)),
            dma((3,)),
            dma((3,)),
            dma((STAGES,)),
            dma((7,)),
            dma((count,)),
            dma((count,)),
        ],
        compiler_params=pltpu.CompilerParams(collective_id=2, has_side_effects=True, vmem_limit_bytes=VMEM_LIMIT),
        name="back",
    )(z_in, h_all, dy_all, w_all, cos, sin, gain, x, dy)[:7]


def settle_kernel(*refs):
    n = len(refs) // 3
    ins, outs, held = refs[:n], refs[n : 2 * n], refs[2 * n : 3 * n]
    in_sem, out_sem = refs[3 * n :]
    come = [pltpu.make_async_copy(a, b, in_sem.at[i]) for i, (a, b) in enumerate(zip(ins, held))]
    go = [pltpu.make_async_copy(a, b, out_sem.at[i]) for i, (a, b) in enumerate(zip(held, outs))]
    for copy in come:
        copy.start()
    for first, second in zip(come, go):
        first.wait()
        second.start()
    for copy in go:
        copy.wait()


def settle(arrays):
    n = len(arrays)
    return pl.pallas_call(
        settle_kernel,
        out_shape=tuple(jax.ShapeDtypeStruct(a.shape, a.dtype) for a in arrays),
        in_specs=any_specs(n),
        out_specs=tuple(any_specs(n)),
        scratch_shapes=[pltpu.VMEM(a.shape, a.dtype) for a in arrays] + [pltpu.SemaphoreType.DMA((n,))] * 2,
        name="settle",
    )(*arrays)


def solution(mesh):
    act_spec = P("fsdp", "model", None)
    col_spec = P("fsdp", "model")
    row_spec = P("model", "fsdp")
    nz = mesh.shape["fsdp"] // NY

    def layer_body(x_in, dy_in, norm_gain, w_qkv, w_out, w_gate, w_up, w_down, rope_cos, rope_sin):
        _, rows, width = x_in.shape
        head = 2 * rope_cos.shape[1]
        seq = rows * NX * NC
        tokens = NY * seq
        x = x_in.reshape(2, rows // 2, width)
        dy = dy_in.reshape(2, rows // 2, width)
        gain = norm_gain.reshape(1, width)
        h_all, dy_all, w_all, z_got = front(nz, x, dy, gain, w_qkv, w_out.T, w_gate, w_up, w_down.T)
        results = back(
            nz,
            z_got.reshape(NY, 2, seq // 2, 2 * head),
            h_all.reshape(tokens, width),
            dy_all.reshape(tokens, width),
            w_all.reshape(NC, width, -1),
            rope_cos.T,
            rope_sin.T,
            x,
            dy,
            gain,
        )
        y_out, dx_out, g_qkv, g_out, g_gate, g_up, g_down = settle(results)
        return y_out.reshape(x_in.shape), dx_out.reshape(x_in.shape), g_qkv, g_out.T, g_gate, g_up, g_down.T

    return jax.shard_map(
        layer_body,
        mesh=mesh,
        in_specs=(act_spec, act_spec, P(), col_spec, row_spec, col_spec, col_spec, row_spec, P(), P()),
        out_specs=(act_spec, act_spec, col_spec, row_spec, col_spec, col_spec, row_spec),
        check_vma=False,
    )
```

```python
import functools
import heapq

import jax
import jax.numpy as jnp
from jax import lax
from jax.experimental import pallas as pl
from jax.experimental.pallas import tpu as pltpu
from jax.sharding import PartitionSpec as P

NORM_EPS = 1e-5
NY, NX, NC = 4, 4, 2
MESH = pl.DeviceIdType.MESH
LINK = 46.6e3
PAIR = 450e3
LOCAL = 1500e3
HOP = 3.1
ADD = 0.4
VMEM_LIMIT = 67043328


class Place:
    def __init__(self, nz):
        i, j = lax.axis_index("fsdp"), lax.axis_index("model")
        self.size = {"z": nz, "y": NY, "x": NX, "c": NC}
        self.at = {"z": lax.div(i, NY), "y": lax.rem(i, NY), "x": lax.div(j, NC), "c": lax.rem(j, NC)}

    def get(self, axis, step=0):
        n = self.size[axis]
        return lax.rem(self.at[axis] + (step + 2 * n) % n, n)

    def device(self, axis, step):
        at = dict(self.at)
        at[axis] = self.get(axis, step)
        return {"fsdp": at["z"] * NY + at["y"], "model": at["x"] * NC + at["c"]}

    def meet(self, peers):
        barrier = pltpu.get_barrier_semaphore()
        for axis, step in peers:
            pl.semaphore_signal(barrier, inc=1, device_id=self.device(axis, step), device_id_type=MESH)
        pl.semaphore_wait(barrier, len(peers))


class Flow:
    def __init__(self, place, send_sem, recv_sem, base=0, now=0.0):
        self.place, self.send_sem, self.recv_sem, self.base = place, send_sem, recv_sem, base
        self.now, self.free, self.events, self.copies, self.tasks, self.order = now, {}, [], [], [], 0
        self.sent = set()

    def event(self, when, wait, then):
        heapq.heappush(self.events, (when, self.order, wait, then))
        self.order += 1

    def send(self, axis, step, src, dst, size, then=None, link=None, alt=None):
        k = len(self.copies)
        link = link or (axis, step)
        begin = max(self.now, self.free.get(link, 0.0))
        rate, lag = (PAIR, 1.5) if axis == "c" else (LINK, HOP)
        self.free[link] = begin + size / rate

        def make(dst):
            return pltpu.make_async_remote_copy(
                src_ref=src(),
                dst_ref=dst(),
                send_sem=self.send_sem.at[self.base + k],
                recv_sem=self.recv_sem.at[self.base + k],
                device_id=self.place.device(axis, step),
                device_id_type=MESH,
            )

        copy = make(dst)
        if alt is None:
            copy.start()
        else:
            when, other = alt
            pl.when(jnp.logical_not(when))(copy.start)
            pl.when(when)(make(other).start)
        self.copies.append(copy)
        self.event(self.free[link] + lag, copy.wait_recv, then)
        return k

    def at(self, when, then):
        self.event(when, lambda: None, then)

    def local(self, copy, size, then):
        copy.start()
        self.event(self.now + size / LOCAL + 1.0, copy.wait, then)

    def task(self, cost, do):
        self.tasks.append((cost, do))

    def take(self):
        when, _, wait, then = heapq.heappop(self.events)
        self.now = max(self.now, when)
        wait()
        if then is not None:
            then()

    def spend(self, cost):
        self.now += cost
        while self.events and self.events[0][0] <= self.now:
            self.take()

    def wait_sent(self, k):
        if k not in self.sent:
            self.copies[k].wait_send()
        self.sent.add(k)

    def run(self):
        while self.events or self.tasks:
            if self.tasks and (not self.events or self.events[0][0] > self.now):
                cost, do = self.tasks.pop(0)
                self.now += cost
                do()
            else:
                self.take()

    def close(self):
        for k in range(len(self.copies)):
            self.wait_sent(k)


def after(count, then):
    left = [count]

    def one():
        left[0] -= 1
        if left[0] == 0:
            then()

    return one


def nbytes(ref, lead):
    n = 1
    for d in ref.shape[lead:]:
        n *= d
    return n * jnp.dtype(ref.dtype).itemsize


def any_specs(n):
    return [pl.BlockSpec(memory_space=pl.ANY)] * n


def mm(a, b, ca, cb):
    return lax.dot_general(a, b, (((ca,), (cb,)), ((), ())), preferred_element_type=jnp.float32)


def span(q, n):
    return pl.ds(pl.multiple_of(q * n, n), n)


def exchange(flow, place, src, dst, far, step, done):
    size = nbytes(src, 1)

    def onward(way, half):
        def then():
            flow.send("y", way, lambda: far.at[half], lambda: dst.at[place.get("y", -way), half], size // 2, lambda: done(2, half))

        return then

    if step == 2:
        flow.send("y", 1, lambda: src.at[place.get("y", 2), 0], lambda: far.at[0], size // 2, onward(1, 0))
        flow.send("y", -1, lambda: src.at[place.get("y", 2), 1], lambda: far.at[1], size // 2, onward(-1, 1))
    else:
        flow.send("y", step, lambda: src.at[place.get("y", step)], lambda: dst.at[place.get("y")], size, lambda: done(-step, None))


ORDER = (2, 1, -1, 0)


class Gather:
    def __init__(self, place, flow, own, full, first, cut, arrive):
        self.place, self.flow, self.own, self.full, self.first, self.cut, self.arrive = place, flow, own, full, first, cut, arrive
        self.second = "y" if first == "x" else "x"
        self.size = nbytes(own, 1) * (cut.stop - cut.start) // own.shape[-1]

    def mine(self, half):
        return lambda: self.own.at[half, :, self.cut]

    def spot(self, at, half):
        y, x, c = (self.place.get(axis, at.get(axis, 0)) for axis in "yxc")
        return lambda: self.full.at[y, x, c, half, :, self.cut]

    def moves(self, axis, at, half, src):
        def come(step, onward):
            def then():
                here = dict(at, **{axis: step})
                if onward:
                    far = dict(at, **{axis: 2})
                    self.flow.send(axis, -step, self.spot(here, half), self.spot(here, half), self.size, lambda: self.got(axis, far, half))
                self.got(axis, here, half)

            return then

        return {
            1: lambda: self.flow.send(axis, 1, src, self.spot(at, half), self.size, come(-1, half == 0)),
            -1: lambda: self.flow.send(axis, -1, src, self.spot(at, half), self.size, come(1, half == 1)),
        }

    def spread(self, axis, at, half, src):
        for move in self.moves(axis, at, half, src).values():
            move()

    def got(self, axis, at, half):
        if axis == self.first:
            self.spread(self.second, at, half, self.spot(at, half))
        self.pair(at, half, self.spot(at, half))
        self.arrive(at.get("y", 0), at.get("x", 0))

    def pair(self, at, half, src):
        there = lambda: self.arrive(at.get("y", 0), at.get("x", 0))
        self.flow.send("c", 1, src, self.spot(at, half), self.size, there)

    def start_first(self):
        self.spread_own(self.first)

    def start_second(self):
        self.spread_own(self.second)
        for half in (0, 1):
            self.pair({}, half, self.mine(half))

    def spread_own(self, axis):
        sends = {(half, step): move for half in (0, 1) for step, move in self.moves(axis, {}, half, self.mine(half)).items()}
        for key in ((0, 1), (1, -1), (1, 1), (0, -1)):
            sends[key]()


def front_kernel(
    nz, x_ref, dy_ref, gain, w_qkv, w_out, w_gate, w_up, w_down, h_all, dy_all, w_all, z_got, h_ref, w_ref, w_heads, h_v, dy_v, z_in, far, send_sem, recv_sem, own_sem, rows_sem
):
    bf16 = jnp.bfloat16
    place = Place(nz)
    for half in range(2):
        wide = x_ref[half].astype(jnp.float32)
        h_ref[half] = (wide * lax.rsqrt(jnp.mean(wide * wide, axis=-1, keepdims=True) + NORM_EPS) * gain[...]).astype(bf16)
    wide_ff = w_gate.shape[1] // NY
    one = w_out.shape[1] // (NY - 1)
    for q in range(NY):
        ffs = slice(q * wide_ff, (q + 1) * wide_ff)
        w_ref[q, :, :wide_ff] = w_gate[:, ffs]
        w_ref[q, :, wide_ff : 2 * wide_ff] = w_up[:, ffs]
        at = 2 * wide_ff
        w_ref[q, :, at : at + one] = w_qkv[:, q * one : (q + 1) * one]
        w_ref[q, :, at + one : at + 2 * one] = w_out[:, q * one : (q + 1) * one] if q < NY - 1 else w_qkv[:, NY * one :]
        w_ref[q, :, at + 2 * one :] = w_down[:, ffs]
    y, x, c, z = (place.get(axis) for axis in "yxcz")
    last = y == NY - 1
    pair = z_in.shape[-1]
    head = pair // 2
    width = h_ref.shape[-1]
    cols = w_ref.shape[-1]
    lo = (cols - pair) * 2 // 3
    hi = lo + pair
    rows = z_in.shape[2]
    flow = Flow(place, send_sem, recv_sem)
    w_own = pltpu.make_async_copy(w_ref.at[y, :, :lo], w_all.at[0, z, y, :, :lo], own_sem.at[2])
    w_own_down = pltpu.make_async_copy(w_ref.at[y, :, hi:], w_all.at[0, z, y, :, hi:], own_sem.at[4 + NX])
    w_own.start()
    w_own_down.start()
    heads_home = pltpu.make_async_copy(w_heads, w_all.at[0, :, :, :, lo:hi], own_sem.at[3])
    w_heads[z, y] = w_ref[y, :, lo:hi]
    place.meet([("x", 1), ("x", -1), ("y", 1), ("y", -1), ("y", 2), ("z", 1), ("z", -1), ("c", 1)])

    queue = []
    pieces = {}
    parts_done = {}
    weights = [4 * nz]
    writes = []

    def load():
        while queue and weights[0] == 0:
            key = queue.pop(0)
            flow.task(CHUNK_TIME, lambda key=key: product(*key))

    def complete(key):
        kind, dy, dx = key
        src, dst = ((h_v, h_all), (dy_v, dy_all))[kind]
        at = place.get("y", dy), place.get("x", dx)
        copy = pltpu.make_async_copy(src.at[at], dst.at[at], rows_sem.at[len(writes)])
        copy.start()
        writes.append(copy)
        queue.append(key)
        load()

    def arrive(kind):
        need = (8, 4)[kind]

        def one(dy, dx):
            key = (kind, dy, dx)
            pieces[key] = pieces.get(key, 0) + 1
            if pieces[key] == need:
                complete(key)

        return one

    def weight_come():
        weights[0] -= 1
        if weights[0] == 0:
            heads_home.start()
            load()

    def product(kind, dy, dx):
        rows_v = (h_v, dy_v)[kind]
        at = place.get("y", dy), place.get("x", dx)
        step = 2 if nz % 2 == 0 else 1
        deep = step * (width // nz)

        def dot(first):
            def some(i, total):
                left = rows_v[at[0], at[1], :, :, :, span(i, deep)].reshape(rows, deep)
                right = w_heads[pl.ds(i * step, step), :, :, first:].reshape(deep, pair - first)
                return total + mm(left, right, 1, 0)

            return lax.fori_loop(0, nz // step, some, jnp.zeros((rows, pair - first), jnp.float32))

        if kind == 0:
            made = dot(0).astype(bf16)
            z_in[at[0], at[1], :, :head] = made[:, :head]

            @pl.when(last)
            def _():
                z_in[at[0], at[1], :, head:] = made[:, head:]

        else:

            @pl.when(jnp.logical_not(last))
            def _():
                z_in[at[0], at[1], :, head:] = dot(head).astype(bf16)

        parts_done[dy, dx] = parts_done.get((dy, dx), 0) + 1
        if parts_done[dy, dx] == 2:
            deliver(dy, dx)

    own_copies = []

    def deliver(dy, dx):
        at = lambda: z_in.at[place.get("y", dy), place.get("x", dx)]
        size = nbytes(z_in, 2)

        def there(step=0):
            return lambda: z_got.at[place.get("y", step), place.get("x", dx)]

        if dy == 0:
            copy = pltpu.make_async_copy(at(), there()(), own_sem.at[4 + dx % NX])
            copy.start()
            own_copies.append(copy)
        elif dy == 2 and dx in DIRECT:
            flow.send("y", 2, at, there(), size, link=("y", 1))
        elif dy == 2:
            way = 1 if dx in (0, 2) else -1

            def onward():
                flow.send("y", way, lambda: far.at[dx % NX], there(-way), size)

            flow.send("y", way, at, lambda: far.at[dx % NX], size, onward)
        else:
            flow.send("y", dy, at, there(), size)

    def w_part(ref, who, dz, dy, cut):
        if ref is None:
            return lambda: w_heads.at[place.get("z", dz), place.get("y", dy)]
        return lambda: w_all.at[who, place.get("z", dz), place.get("y", dy), :, cut]

    cuts = [slice(lo, hi), slice(0, lo), slice(hi, cols)]

    def ring(step, dy, n_cut, src=None, hops=nz - 1, lead=True):
        cut = cuts[n_cut]
        home = None if n_cut == 0 else w_all
        size = nbytes(w_ref, 1) * (cut.stop - cut.start) // cols

        def hop(n):
            def then():
                here = src if src and n == 0 else w_part(home, 0, -step * n, dy, cut)
                if n < hops:
                    flow.send("z", step, here, w_part(home, 0, -step * n, dy, cut), size, hop(n + 1))
                if n or lead:
                    flow.send("c", 1, here, w_part(w_all, 1, -step * n, dy, cut), size)
                    if n_cut == 0:
                        weight_come()

            return then

        return hop(0)

    def rings(dy, n_cut, src=None):
        if n_cut:
            return ring(1 if dy in (0, 1) else -1, dy, n_cut, src)
        both = [ring(1, dy, 0, src, nz // 2), ring(-1, dy, 0, src, (nz - 1) // 2, False)]
        return lambda: [one() for one in both]

    def w_at(dy, cut):
        return lambda: w_ref.at[place.get("y", dy), :, cut]

    tail = width // nz * H_TAIL
    gathers = [
        Gather(place, flow, h_ref, h_v, "x", slice(0, width - tail), arrive(0)),
        Gather(place, flow, dy_ref, dy_v, "y", slice(0, width), arrive(1)),
        Gather(place, flow, h_ref, h_v, "y", slice(width - tail, width), arrive(0)),
    ]
    def w_start(n_cut, dys):
        cut = cuts[n_cut]
        home = None if n_cut == 0 else w_all
        size = nbytes(w_ref, 1) * (cut.stop - cut.start) // cols
        there = w_part(home, 0, 0, 0, cut)
        for dy in dys:
            if dy == 0:
                rings(0, n_cut, w_at(0, cut))()
            elif dy == 2:
                flow.send("y", 2, w_at(2, cut), there, size, rings(2, n_cut), link=("y", 1))
            else:
                flow.send("y", -dy, w_at(-dy, cut), there, size, rings(dy, n_cut))

    w_start(0, (0, 1, -1, 2))
    for one in gathers:
        one.start_first()
    flow.at(W_TIMES[0], lambda: [w_start(1, (0, -1)), w_start(2, (0, -1))])
    flow.at(W_TIMES[1], lambda: [w_start(1, (1, 2)), w_start(2, (1, 2))])
    for one in gathers:
        one.start_second()
    for n, (ref, full) in enumerate(((h_ref, h_v), (dy_ref, dy_v))):
        full[y, x, c] = ref[...]
        for _ in range((4, 2)[n]):
            arrive(n)(0, 0)
    flow.run()
    w_own.wait()
    w_own_down.wait()
    flow.close()
    for copy in own_copies + writes:
        copy.wait()
    heads_home.wait()


CHUNK_TIME = 1.0
W_TIMES = (0.0, 0.0)
DIRECT = (2,)
H_TAIL = 1


def front(nz, x, dy, gain, w_qkv, w_out, w_gate, w_up, w_down):
    half, rows, width = x.shape
    everywhere = (NY, NX, NC) + x.shape
    slab = w_qkv.shape[0]
    pair = 2 * w_out.shape[1] // (NY - 1)
    cols = pair + 3 * w_gate.shape[1] // NY
    w_shape = (NY, slab, cols)
    bf16 = x.dtype
    gathers = 3 * (30 + 32)
    count = gathers + 3 * 3 + 3 * 4 * (nz - 1) + 3 * 4 * nz + 2 * NX + 2 * NX
    vmem = pl.BlockSpec(memory_space=pltpu.VMEM)
    dma = pltpu.SemaphoreType.DMA
    chunk = NC * half * rows
    z_shape = (NY, NX, chunk, pair)
    return pl.pallas_call(
        functools.partial(front_kernel, nz),
        out_shape=(
            jax.ShapeDtypeStruct(everywhere, bf16),
            jax.ShapeDtypeStruct(everywhere, bf16),
            jax.ShapeDtypeStruct((NC, nz) + w_shape, bf16),
            jax.ShapeDtypeStruct(z_shape, bf16),
        ),
        in_specs=[vmem] * 8,
        out_specs=tuple(any_specs(4)),
        scratch_shapes=[
            pltpu.VMEM(x.shape, bf16),
            pltpu.VMEM(w_shape, bf16),
            pltpu.VMEM((nz,) + w_shape[:-1] + (pair,), bf16),
            pltpu.VMEM(everywhere, bf16),
            pltpu.VMEM(everywhere, bf16),
            pltpu.VMEM(z_shape, bf16),
            pltpu.VMEM((NX, chunk, pair), bf16),
            dma((count,)),
            dma((count,)),
            dma((5 + NX,)),
            dma((2 * NY * NX,)),
        ],
        compiler_params=pltpu.CompilerParams(collective_id=0, has_side_effects=True, vmem_limit_bytes=VMEM_LIMIT),
        name="front",
    )(x, dy, gain, w_qkv, w_out, w_gate, w_up, w_down)


SETS = (2, 1, -1, 0)


def attention(z_got, z_back, keys, vals, dk, dv, cos_ref, sin_ref):
    bf16 = jnp.bfloat16
    seq, head = keys.shape
    part = seq // 2
    count = z_got.shape[0] - 1
    scale = head**-0.5
    spread = z_back.shape[2:5] + (head,)
    halves = [pl.ds(p * part, part) for p in range(2)]

    def turn(values, at, sign):
        wide = values.astype(jnp.float32)
        swapped = pltpu.roll(wide, head // 2, 1)
        return (wide * cos_ref[at, :] + sign * (swapped * sin_ref[at, :])).astype(bf16)

    for p in range(2):
        keys[halves[p], :] = turn(z_got[count, p, :, :head], halves[p], 1.0)
        vals[halves[p], :] = z_got[count, p, :, head:]
    dk[...] = jnp.zeros_like(dk)
    dv[...] = jnp.zeros_like(dv)

    @pl.loop(0, count)
    def _(i):
        for p in range(2):
            n = (p + 1) * part
            query = turn(z_got[i, p, :, :head], halves[p], 1.0)
            d_out = z_got[i, p, :, head:]
            scores = mm(query, keys[:n, :], 1, 1) * scale
            causal = lax.broadcasted_iota(jnp.int32, scores.shape, 0) + p * part >= lax.broadcasted_iota(jnp.int32, scores.shape, 1)
            scores = jnp.where(causal, scores, -1e30)
            grown = jnp.exp(scores - jnp.max(scores, axis=1, keepdims=True))
            probs = grown / jnp.sum(grown, axis=1, keepdims=True)
            probs_low = probs.astype(bf16)
            z_back[i, p, :, :, :, head:] = mm(probs_low, vals[:n, :], 1, 0).astype(bf16).reshape(spread)
            d_probs = mm(d_out, vals[:n, :], 1, 1).astype(bf16).astype(jnp.float32)
            d_scores = (probs * (d_probs - jnp.sum(probs * d_probs, axis=1, keepdims=True)) * scale).astype(bf16)
            z_back[i, p, :, :, :, :head] = turn(mm(d_scores, keys[:n, :], 1, 0).astype(bf16), halves[p], -1.0).reshape(spread)
            dk[:n, :] += mm(d_scores, query, 0, 0)
            dv[:n, :] += mm(probs_low, d_out, 0, 0)

    for p in range(2):
        z_back[count, p, :, :, :, :head] = turn(dk[halves[p], :].astype(bf16), halves[p], -1.0).reshape(spread)
        z_back[count, p, :, :, :, head:] = dv[halves[p], :].astype(bf16).reshape(spread)


def gated(place, flow, h_all, dy_all, w_all, acts, row_sem, share, h_rows, dy_rows, w_v):
    bf16 = jnp.bfloat16
    ff = acts.shape[-1] // 3
    lo = 2 * ff
    part = h_rows.shape[1]
    shape = acts.shape[2:5] + (ff,)
    w_loads = [
        pltpu.make_async_copy(w_all.at[0, :, :lo], w_v.at[:, :lo], row_sem.at[2, 0]),
        pltpu.make_async_copy(w_all.at[0, :, w_all.shape[2] - ff :], w_v.at[:, lo:], row_sem.at[2, 1]),
    ]

    def loads(n, slot):
        return [pltpu.make_async_copy(a.at[span(n, part)], b.at[slot], row_sem.at[slot, m]) for m, (a, b) in enumerate(((h_all, h_rows), (dy_all, dy_rows)))]

    def begin():
        for copy in w_loads + loads(0, 0) + loads(1, 1):
            copy.start()

    def go():
        for copy in w_loads:
            copy.wait()
        for q in range(NY):

            @pl.loop(0, 2)
            def _(p):
                n = 2 * q + p
                for copy in loads(n, p):
                    copy.wait()
                gate = mm(h_rows[p], w_v[:, :ff], 1, 0).astype(bf16).astype(jnp.float32)
                up = mm(h_rows[p], w_v[:, ff:lo], 1, 0).astype(bf16).astype(jnp.float32)
                d_act = mm(dy_rows[p], w_v[:, lo:], 1, 0).astype(bf16).astype(jnp.float32)
                if q < NY - 1:
                    for copy in loads(n + 2, p):
                        copy.start()
                sig = jax.nn.sigmoid(gate)
                silu = gate * sig
                acts[q, p, :, :, :, :ff] = (d_act * up * (sig + silu * (1.0 - sig))).astype(bf16).reshape(shape)
                acts[q, p, :, :, :, ff:lo] = (d_act * silu).astype(bf16).reshape(shape)
                acts[q, p, :, :, :, lo:] = (silu * up).astype(bf16).reshape(shape)

            share(q)
            flow.spend(3.0)

    return begin, go


class Plane:
    def __init__(self, place, flow, tiles, land, first, finish, free):
        self.place, self.flow, self.tiles, self.land, self.first = place, flow, tiles, land, first
        self.second = "y" if first == "x" else "x"
        self.piece = nbytes(tiles, 3)
        self.sums, self.waiting, self.finished = {}, {}, [0] * len(SETS)
        self.free = free
        self.rings = []
        for s, other in enumerate(SETS):

            def raw(step, half, s=s):
                return lambda: tiles.at[s % 2, place.get(first, step), half]

            self.rings.append(self.ring(first, raw, lambda step, half, then: then(), s, self.first_done(s, other)))
        self.onward, _ = self.ring(self.second, lambda step, half: self.sums[step, half], self.need, len(SETS), finish)

    def need(self, step, half, then):
        if (step, half) in self.sums:
            then()
        else:
            self.waiting.setdefault((step, half), []).append(then)

    def first_done(self, s, step):
        def done(half, ref):
            self.sums[step, half] = ref
            for then in self.waiting.pop((step, half), []):
                then()
            self.onward(step, half)
            self.finished[s] += 1
            if self.finished[s] == 2:
                self.free(s)

        return done

    def add(self, mine, other):
        a, b = mine(), other()
        a[...] = a[...] + b[...]
        self.flow.now += ADD

    def ring(self, axis, raw, need, s, done):
        flow, add, sent = self.flow, self.add, []

        def slot(i):
            return lambda: self.land.at[s, i]

        def turn(i, goal, half, step):
            def then():
                add(slot(i), raw(goal, half))
                flow.send(axis, step, slot(i), slot(i + 4), self.piece, final[half])

            return lambda: need(goal, half, then)

        def ending(half):
            def then():
                mine, other = (slot(5), slot(2)) if half == 0 else (slot(4), slot(3))
                add(mine, other)
                add(mine, raw(0, half))
                done(half, mine)

            return lambda: need(0, half, then)

        final = [after(2, ending(0)), after(2, ending(1))]
        moves = {
            (2, 1): (1, 0, turn(0, 1, 1, 1)),
            (2, 0): (-1, 1, turn(1, -1, 0, -1)),
            (1, 0): (1, 2, final[0]),
            (-1, 1): (-1, 3, final[1]),
        }

        def start(goal, half):
            if (goal, half) in moves:
                step, i, then = moves[goal, half]
                sent.append(flow.send(axis, step, raw(goal, half), slot(i), self.piece, then))

        return start, sent

    def start(self, s):
        for goal, half in ((2, 1), (2, 0), (1, 0), (-1, 1)):
            self.rings[s][0](goal, half)

    def clear(self, s):
        for k in self.rings[s][1]:
            self.flow.wait_sent(k)


class Grads:
    flow = None


    def __init__(self, nz, place, h_all, dy_all, acts, z_out, z_land, outs, far, h_plus, h_minus, dy_minus, tiles, stage, load_sem, stage_sem, own_sem):
        self.__dict__.update({k: v for k, v in locals().items() if k != "self"})
        self.ff = acts.shape[-1] // 3
        self.pair = z_out.shape[-1]
        lo = 2 * self.ff
        self.cols = [(0, self.ff), (self.ff, lo), (lo + self.pair, lo + self.pair + self.ff), (lo, lo + self.pair)]
        self.way = (1, 1, -1, -1)
        self.far_way = (1, -1, 1, -1)
        self.block = tiles.shape[2]
        self.size = nbytes(tiles, 2)
        self.ready, self.waiting, self.used = set(), {}, 0
        self.users = [[] for _ in range(stage.shape[0])]
        self.own = []
        self.idle, self.first = {}, {}

    def load(self, ref, src, index, step, n):
        b = self.place.get("z", -step * (n + 1))
        at = pl.ds(pl.multiple_of(b * self.block, self.block), self.block)
        return pltpu.make_async_copy(src.at[:, at], ref, self.load_sem.at[index])

    def loads_plus(self, n):
        return [self.load(self.h_plus, self.h_all, 0, 1, n)]

    def loads_minus(self, n):
        return [self.load(self.h_minus, self.h_all, 1, -1, n), self.load(self.dy_minus, self.dy_all, 2, -1, n)]

    def begin(self):
        for copy in self.loads_plus(0) + self.loads_minus(0):
            copy.start()

    def gather_up(self, tiles, some):
        seq = self.h_plus.shape[0] // NY
        for tile in tiles:
            tile[...] = jnp.zeros_like(tile)

        @pl.loop(0, NY)
        def _(q):
            for tile, value in zip(tiles, some(q, span(q, seq))):
                tile[...] += value

    def set_ready(self, lane, n):
        self.ready.add((lane, n))
        for then in self.waiting.pop((lane, n), []):
            then()
        if n == 0:
            k = self.flow.send("z", self.way[lane], lambda: self.tiles.at[0, lane], lambda: self.z_land.at[0, lane], self.size, self.hop(lane, 0))
            self.first[lane] = k

    def clear(self, lane, n):
        if n == 2:
            self.flow.wait_sent(self.first[lane])

    def tokens(self, ref):
        value = ref[...]
        return value.reshape(-1, value.shape[-1])

    def make_plus(self, n):
        for copy in self.loads_plus(n):
            copy.wait()
        lo = 2 * self.ff

        def some(q, rows):
            both = mm(self.h_plus[rows, :], self.acts[q, :, :, :, :, :lo].reshape(-1, lo), 0, 0)
            return both[:, : self.ff], both[:, self.ff :]

        self.gather_up([self.tiles.at[n % 2, 0], self.tiles.at[n % 2, 1]], some)
        if n + 1 < self.nz:
            for copy in self.loads_plus(n + 1):
                copy.start()

    def for_down(self, q, rows):
        return [mm(self.dy_minus[rows, :], self.acts[q, :, :, :, :, 2 * self.ff :].reshape(-1, self.ff), 0, 0)]

    def for_heads(self, q, rows):
        last = self.place.get("y") == NY - 1
        head = self.pair // 2
        out = self.z_out[q].reshape(-1, self.pair)
        both = mm(self.h_minus[rows, :], out, 0, 0)
        right = jnp.where(last, both[:, head:], mm(self.dy_minus[rows, :], out[:, head:], 0, 0))
        return [jnp.concatenate([both[:, :head], right], axis=1)]

    def make_minus(self, n):
        for copy in self.loads_minus(n):
            copy.wait()
        self.gather_up([self.tiles.at[n % 2, 2], self.tiles.at[n % 2, 3]], lambda q, rows: self.for_down(q, rows) + self.for_heads(q, rows))
        self.load_minus_next(n)

    def load_minus_next(self, n):
        if n + 1 < self.nz:
            for copy in self.loads_minus(n + 1):
                copy.start()

    def make_first(self):
        self.make_plus(0)
        for copy in self.loads_minus(0):
            copy.wait()
        self.gather_up([self.tiles.at[0, 2]], self.for_down)

    def heads_first(self):
        def do():
            self.gather_up([self.tiles.at[0, 3]], self.for_heads)
            self.load_minus_next(0)
            self.set_ready(3, 0)

        self.flow.task(1.3, do)

    def plus(self, n):
        def do():
            for lane in (0, 1):
                self.clear(lane, n)
            self.make_plus(n)
            for lane in (0, 1):
                self.set_ready(lane, n)

        self.flow.task(1.6, do)

    def minus(self, n):
        def do():
            for lane in (2, 3):
                self.clear(lane, n)
            self.make_minus(n)
            for lane in (2, 3):
                self.set_ready(lane, n)

        self.flow.task(2.2, do)

    def need(self, lane, n, then):
        if (lane, n) in self.ready:
            then()
        else:
            self.waiting.setdefault((lane, n), []).append(then)

    def next(self, lane, n):
        if n + 2 >= self.nz:
            return
        key = (lane // 2, n)
        self.idle[key] = self.idle.get(key, 0) + 1
        if self.idle[key] == 2:
            (self.plus, self.minus)[lane // 2](n + 2)

    def hop(self, lane, s):
        flow, place = self.flow, self.place

        def come():
            slot = self.used % len(self.users)
            self.used += 1
            for wait in self.users[slot]:
                wait()
            self.users[slot] = []
            here = lambda: self.stage.at[slot]

            def staged():
                self.need(lane, s + 1, use)

            def use():
                ref = here()
                ref[...] = ref[...] + self.tiles[(s + 1) % 2, lane]
                flow.now += ADD
                if s == 0:
                    self.next(lane, 0)
                self.next(lane, s + 1)
                if s + 1 < self.nz - 1:
                    k = flow.send("z", self.way[lane], here, lambda: self.z_land.at[s + 1, lane], self.size, self.hop(lane, s + 1))
                    self.users[slot].append(lambda: flow.wait_sent(k))
                else:
                    self.home(lane, slot)

            flow.local(pltpu.make_async_copy(self.z_land.at[s, lane], here(), self.stage_sem.at[slot]), self.size, staged)

        return come

    def home(self, lane, slot):
        flow, place = self.flow, self.place
        slab = self.block // NY
        way = self.far_way[lane]
        size = self.size // NY

        def rows(step, cut=slice(None)):
            return lambda: self.stage.at[slot, pl.ds(pl.multiple_of(place.get("y", step) * slab, slab), slab), cut]

        def columns(out, step, wide):
            at = place.get("y", step) * wide
            return lambda: self.outs[out].at[:, pl.ds(pl.multiple_of(at, wide), wide)]

        def deliver(size, src, far, dst, n, other=None):
            def alt(step):
                return None if other is None else (place.get("y", step) == NY - 1, other(step))

            def onward():
                flow.send("y", way, far, dst(-way), size, alt=alt(-way))

            sent = [flow.send("y", way, src(2), far, size, onward)]
            sent += [flow.send("y", step, src(step), dst(0), size, alt=alt(0)) for step in (1, -1)]
            copies = [(None, pltpu.make_async_copy(src(0)(), dst(0)(), self.own_sem.at[n]))]
            if other is not None:
                last = place.get("y") == NY - 1
                copies = [(jnp.logical_not(last), copies[0][1]), (last, pltpu.make_async_copy(src(0)(), other(0)(), self.own_sem.at[n]))]
            for when, copy in copies:
                if when is None:
                    copy.start()
                else:
                    pl.when(when)(copy.start)
            self.users[slot] += [functools.partial(flow.wait_sent, k) for k in sent] + [copies[0][1].wait]

        if lane < 3:
            deliver(size, rows, lambda: self.far.at[lane], lambda step: columns(lane, step, self.ff), lane)
            return
        head = self.pair // 2
        first, second = slice(0, head), slice(head, self.pair)
        deliver(size // 2, lambda step: rows(step, first), lambda: self.far.at[3, :, first], lambda step: columns(3, step, head), 3)
        value = lambda: self.outs[3].at[:, NY * head :]

        def out_rows(step):
            at = lax.rem(place.get("y", step), NY - 1) * head
            return lambda: self.outs[4].at[:, pl.ds(pl.multiple_of(at, head), head)]

        deliver(size // 2, lambda step: rows(step, second), lambda: self.far.at[3, :, second], out_rows, 4, lambda step: value)

    def close(self):
        for users in self.users:
            for wait in users:
                wait()


def back_kernel(
    nz,
    z_in,
    h_all,
    dy_all,
    w_all,
    cos_in,
    sin_in,
    gain,
    x_in,
    dy_in,
    y_out,
    dx_out,
    g_qkv,
    g_out,
    g_gate,
    g_up,
    g_down,
    z_land,
    x_ref,
    dy_ref,
    cos_ref,
    sin_ref,
    z_got,
    z_back,
    z_out,
    far_back,
    acts,
    pair_acts,
    far,
    p_land,
    q_land,
    keys,
    vals,
    dk,
    dv,
    h_plus,
    h_minus,
    dy_minus,
    tiles,
    stage,
    load_sem,
    row_sem,
    w_sem,
    g_load_sem,
    stage_sem,
    own_sem,
    send_sem,
    recv_sem,
):
    bf16, f32 = jnp.bfloat16, jnp.float32
    place = Place(nz)
    y, c = place.get("y"), place.get("c")
    other = place.get("c", 1)
    last = y == NY - 1
    seq, head = keys.shape
    pair = 2 * head
    rows, cols = pair_acts.shape[3:]
    ff = (cols - pair) // 3
    lo, hi = 2 * ff, 2 * ff + pair
    tokens, width = h_all.shape
    block = width // nz
    part = seq // 2

    z_load = pltpu.make_async_copy(z_in, z_got, load_sem)
    z_load.start()
    row_loads = [pltpu.make_async_copy(a, b, own_sem.at[5 + n]) for n, (a, b) in enumerate(((x_in, x_ref), (dy_in, dy_ref)))]
    cos_ref[...] = jnp.concatenate([cos_in[...], cos_in[...]], axis=0).T
    sin_ref[...] = jnp.concatenate([-sin_in[...], sin_in[...]], axis=0).T
    early = Flow(place, send_sem, recv_sem)
    peers = [("x", 1), ("x", -1), ("y", 1), ("y", -1), ("z", 1), ("z", -1), ("c", 1)]

    def share(q):
        early.send("c", 1, lambda: acts.at[q, :, :, other, :, :lo], lambda: pair_acts.at[q, :, :, :, :lo], nbytes(pair_acts, 1) * lo // cols)
        early.send("c", 1, lambda: acts.at[q, :, :, other, :, lo:], lambda: pair_acts.at[q, :, :, :, hi:], nbytes(pair_acts, 1) * ff // cols)

    def out_come(step, half):
        cut = slice(None) if half is None else half
        part = nbytes(z_out, 1) // NC // (1 if half is None else 2)
        src = lambda: z_out.at[place.get("y", step), cut, :, other]
        early.send("c", 1, src, lambda: pair_acts.at[place.get("y", step), cut, :, :, lo:hi], part)

    grads = Grads(nz, place, h_all, dy_all, acts, z_out, z_land, (g_gate, g_up, g_down, g_qkv, g_out), far, h_plus, h_minus, dy_minus, tiles, stage, g_load_sem, stage_sem, own_sem)

    def first(h_rows, dy_rows, w_v):
        begin, go = gated(place, early, h_all, dy_all, w_all, acts, row_sem, share, h_rows, dy_rows, w_v)
        begin()
        grads.begin()
        for copy in row_loads:
            copy.start()
        z_load.wait()
        attention(z_got, z_back, keys, vals, dk, dv, cos_ref, sin_ref)
        place.meet(peers)
        for step in ORDER[:3]:
            exchange(early, place, z_back, z_out, far_back, step, out_come)
        z_out[y] = z_back[y]
        early.send("c", 1, lambda: z_back.at[y, :, :, other], lambda: pair_acts.at[y, :, :, :, lo:hi], nbytes(z_out, 1) // NC)
        go()
        grads.make_first()
        early.now += 2.6
        early.run()
        early.close()
        for copy in row_loads:
            copy.wait()

    pl.run_scoped(
        first,
        pltpu.VMEM((2, part, width), bf16),
        pltpu.VMEM((2, part, width), bf16),
        pltpu.VMEM((width, 3 * ff), bf16),
    )

    def second(p_tile, q_tile, w_v):
        flow = Flow(place, send_sem, recv_sem, len(early.copies), early.now)
        grads.flow = flow
        lane = lax.broadcasted_iota(jnp.int32, (rows, pair), 1)
        for_d = jnp.logical_or(lane < head, last)

        def chunk(k, i, p, xx):
            if k == 0:
                own = acts[i, p, xx, c]
                return own[:, :lo], z_out[i, p, xx, c], own[:, lo:]
            theirs = pair_acts[i, p, xx]
            return theirs[:, :lo], theirs[:, lo:hi], theirs[:, hi:]

        def for_out(k, i, p, xx):
            _, mixed, act = chunk(k, i, p, xx)
            return jnp.concatenate([jnp.where(for_d, jnp.zeros_like(mixed), mixed), act], axis=1)

        def for_in(k, i, p, xx):
            grad, mixed, _ = chunk(k, i, p, xx)
            return jnp.concatenate([grad, jnp.where(for_d, mixed, jnp.zeros_like(mixed))], axis=1)

        depth = w_v.shape[0]

        def w_copy(kind, d, slot):
            at = pl.ds(pl.multiple_of(d * block, block), block)
            cut = slice(lo, cols) if kind == 0 else slice(0, cols)
            return pltpu.make_async_copy(w_all.at[:, at, cut], w_v.at[slot, :, :, cut], w_sem.at[slot])

        counts = (nz - 1, nz)
        base, total = [], 0
        for kind, _ in PASSES:
            base.append(total)
            total += counts[kind]
        kind = PASSES[0][0]
        for n in range(depth):
            w_copy(kind, n, n).start() if n < counts[kind] else w_copy(PASSES[1][0], n - counts[kind], n).start()
        turn = [0]

        def blocks(s, kind, first, count, body):
            n = turn[0]
            assert PASSES[n] == (kind, s)
            if first + count == counts[kind]:
                turn[0] += 1

            @pl.loop(first, first + count)
            def _(d):
                slot = lax.rem(base[n] + d, depth)
                w_copy(kind, d, slot).wait()
                body(d, w_v.at[slot])

                @pl.when(d + depth < counts[kind])
                def _():
                    w_copy(kind, d + depth, slot).start()

                if n + 1 < len(PASSES):

                    @pl.when(d + depth >= counts[kind])
                    def _():
                        w_copy(PASSES[n + 1][0], d + depth - counts[kind], slot).start()

        def product(parts, w, a, b):
            total = None
            for k in range(NC):
                left = jnp.concatenate([one(k) for one in parts], axis=0)
                one = mm(left, w[k, :, a:b], 1, 1)
                total = one if total is None else total + one
            return total

        shape = (NX, 2, rows // 2, block)

        def p_rows(s):
            x = place.get("x", SETS[s])
            p, xx = lax.div(x, NX // 2), lax.rem(x, NX // 2)
            return [lambda k, i=i: for_out(k, i, p, xx) for i in range(NY)]

        def q_rows(s, make):
            i = place.get("y", SETS[s])
            return [lambda k, p=p, xx=xx: make(k, i, p, xx) for p in range(2) for xx in range(NX // 2)]

        def place_of(d):
            return pl.ds(pl.multiple_of(d * block, block), block)

        def p_task(s):
            def body(d, w):
                p_tile[s % 2, :, :, :, place_of(d)] = product(p_rows(s), w, lo, cols).reshape(shape)

            def do():
                if s >= 2:
                    planes[0].clear(s - 2)
                blocks(s, 0, 0, nz - 1, body)
                planes[0].start(s)

            flow.task(P_TIME, do)

        def q_task(s):
            def body(d, w):
                q_tile[s % 2, :, :, :, place_of(d)] = product(q_rows(s, for_in), w, 0, hi).reshape(shape)

                @pl.when(d == nz - 1)
                def _():
                    q_tile[s % 2, :, :, :, width:] = product(q_rows(s, for_out), w, lo, cols).reshape(shape)

            def start():
                if s >= 2:
                    planes[1].clear(s - 2)
                blocks(s, 1, 0, nz // 2, body)

            def end():
                blocks(s, 1, nz // 2, nz - nz // 2, body)
                planes[1].start(s)

            flow.task(Q_HALF, start)
            flow.task(Q_HALF, end)

        edge = width - block
        def p_finish(half, ref):
            y_out[half, :, :edge] = (x_ref[half, :, :edge].astype(f32) + ref()[...]).astype(bf16)

        def q_finish(half, ref):
            y_out[half, :, edge:] = (x_ref[half, :, edge:].astype(f32) + ref()[:, width:]).astype(bf16)
            wide = x_ref[half].astype(f32)
            scale = lax.rsqrt(jnp.mean(wide * wide, axis=-1, keepdims=True) + NORM_EPS)
            d_normed = ref()[:, :width].astype(bf16).astype(f32) * gain[...]
            mean = jnp.mean(d_normed * wide, axis=-1, keepdims=True)
            grad = d_normed * scale - wide * (scale * scale * scale * mean)
            dx_out[half] = (dy_ref[half].astype(f32) + grad).astype(bf16)

        def free(task):
            return lambda s: task(s + 2) if s + 2 < len(SETS) else None

        planes = [
            Plane(place, flow, p_tile, p_land, "y", p_finish, free(p_task)),
            Plane(place, flow, q_tile, q_land, "x", q_finish, free(q_task)),
        ]

        for lane in range(3):
            grads.set_ready(lane, 0)
        q_task(0)
        p_task(0)
        grads.heads_first()
        grads.plus(1)
        grads.minus(1)
        p_task(1)
        q_task(1)
        flow.run()
        flow.close()
        grads.close()

    pl.run_scoped(
        second,
        pltpu.VMEM((2, NY, 2, rows // 2, width - block), f32),
        pltpu.VMEM((2, NX, 2, rows // 2, width + block), f32),
        pltpu.VMEM((3, NC, block, cols), bf16),
    )


STAGES = 5
PASSES = ((1, 0), (0, 0), (0, 1), (1, 1), (1, 2), (0, 2), (0, 3), (1, 3))
P_TIME = 3.0
Q_HALF = 2.6


def back(nz, z_in, h_all, dy_all, w_all, cos, sin, x, dy, gain):
    tokens, width = h_all.shape
    seq, head = cos.shape[1], 2 * cos.shape[0]
    pair = 2 * head
    cols = w_all.shape[2]
    ff = (cols - pair) // 3
    rows = seq // (NX * NC)
    block = width // nz
    bf16, f32 = h_all.dtype, jnp.float32
    vmem = pl.BlockSpec(memory_space=pltpu.VMEM)
    dma = pltpu.SemaphoreType.DMA
    blocks = (NY, 2, NX // 2, NC, rows, pair)
    p_piece = (rows // 2, width - block)
    q_piece = (rows // 2, width + block)
    count = 6 + 2 * NY + 5 + 4 * (nz - 1) + 5 * 4 + 2 * 5 * 6
    slab = block // NY
    weight = jax.ShapeDtypeStruct((slab, NY * ff), f32)
    return pl.pallas_call(
        functools.partial(back_kernel, nz),
        out_shape=(
            jax.ShapeDtypeStruct(x.shape, bf16),
            jax.ShapeDtypeStruct(x.shape, bf16),
            jax.ShapeDtypeStruct((slab, (NY + 1) * head), f32),
            jax.ShapeDtypeStruct((slab, (NY - 1) * head), f32),
            weight,
            weight,
            weight,
            jax.ShapeDtypeStruct((nz - 1, 4, block, ff), f32),
        ),
        in_specs=any_specs(4) + [vmem] * 3 + any_specs(2),
        out_specs=(vmem, vmem) + tuple(any_specs(6)),
        scratch_shapes=[
            pltpu.VMEM(x.shape, bf16),
            pltpu.VMEM(x.shape, bf16),
            pltpu.VMEM((seq, head), f32),
            pltpu.VMEM((seq, head), f32),
            pltpu.VMEM(z_in.shape, bf16),
            pltpu.VMEM(blocks, bf16),
            pltpu.VMEM(blocks, bf16),
            pltpu.VMEM(blocks[1:], bf16),
            pltpu.VMEM(blocks[:-1] + (3 * ff,), bf16),
            pltpu.VMEM(blocks[:3] + (rows, cols), bf16),
            pltpu.VMEM((4, block // NY, ff), f32),
            pltpu.VMEM((5, 6) + p_piece, f32),
            pltpu.VMEM((5, 6) + q_piece, f32),
            pltpu.VMEM((seq, head), bf16),
            pltpu.VMEM((seq, head), bf16),
            pltpu.VMEM((seq, head), f32),
            pltpu.VMEM((seq, head), f32),
            pltpu.VMEM((tokens, block), bf16),
            pltpu.VMEM((tokens, block), bf16),
            pltpu.VMEM((tokens, block), bf16),
            pltpu.VMEM((2, 4, block, ff), f32),
            pltpu.VMEM((STAGES, block, ff), f32),
            dma,
            dma((3, 2)),
            dma((3,)),
            dma((3,)),
            dma((STAGES,)),
            dma((7,)),
            dma((count,)),
            dma((count,)),
        ],
        compiler_params=pltpu.CompilerParams(collective_id=2, has_side_effects=True, vmem_limit_bytes=VMEM_LIMIT),
        name="back",
    )(z_in, h_all, dy_all, w_all, cos, sin, gain, x, dy)[:7]


def settle_kernel(*refs):
    n = len(refs) // 3
    ins, outs, held = refs[:n], refs[n : 2 * n], refs[2 * n : 3 * n]
    in_sem, out_sem = refs[3 * n :]
    come = [pltpu.make_async_copy(a, b, in_sem.at[i]) for i, (a, b) in enumerate(zip(ins, held))]
    go = [pltpu.make_async_copy(a, b, out_sem.at[i]) for i, (a, b) in enumerate(zip(held, outs))]
    for copy in come:
        copy.start()
    for first, second in zip(come, go):
        first.wait()
        second.start()
    for copy in go:
        copy.wait()


def settle(arrays):
    n = len(arrays)
    return pl.pallas_call(
        settle_kernel,
        out_shape=tuple(jax.ShapeDtypeStruct(a.shape, a.dtype) for a in arrays),
        in_specs=any_specs(n),
        out_specs=tuple(any_specs(n)),
        scratch_shapes=[pltpu.VMEM(a.shape, a.dtype) for a in arrays] + [pltpu.SemaphoreType.DMA((n,))] * 2,
        name="settle",
    )(*arrays)


def solution(mesh):
    act_spec = P("fsdp", "model", None)
    col_spec = P("fsdp", "model")
    row_spec = P("model", "fsdp")
    nz = mesh.shape["fsdp"] // NY

    def layer_body(x_in, dy_in, norm_gain, w_qkv, w_out, w_gate, w_up, w_down, rope_cos, rope_sin):
        _, rows, width = x_in.shape
        head = 2 * rope_cos.shape[1]
        seq = rows * NX * NC
        tokens = NY * seq
        x = x_in.reshape(2, rows // 2, width)
        dy = dy_in.reshape(2, rows // 2, width)
        gain = norm_gain.reshape(1, width)
        h_all, dy_all, w_all, z_got = front(nz, x, dy, gain, w_qkv, w_out.T, w_gate, w_up, w_down.T)
        results = back(
            nz,
            z_got.reshape(NY, 2, seq // 2, 2 * head),
            h_all.reshape(tokens, width),
            dy_all.reshape(tokens, width),
            w_all.reshape(NC, width, -1),
            rope_cos.T,
            rope_sin.T,
            x,
            dy,
            gain,
        )
        y_out, dx_out, g_qkv, g_out, g_gate, g_up, g_down = settle(results)
        return y_out.reshape(x_in.shape), dx_out.reshape(x_in.shape), g_qkv, g_out.T, g_gate, g_up, g_down.T

    return jax.shard_map(
        layer_body,
        mesh=mesh,
        in_specs=(act_spec, act_spec, P(), col_spec, row_spec, col_spec, col_spec, row_spec, P(), P()),
        out_specs=(act_spec, act_spec, col_spec, row_spec, col_spec, col_spec, row_spec),
        check_vma=False,
    )
```

```python
import functools
import heapq

import jax
import jax.numpy as jnp
from jax import lax
from jax.experimental import pallas as pl
from jax.experimental.pallas import tpu as pltpu
from jax.sharding import PartitionSpec as P

NORM_EPS = 1e-5
NY, NX, NC = 4, 4, 2
MESH = pl.DeviceIdType.MESH
LINK = 46.6e3
PAIR = 450e3
LOCAL = 1500e3
LEFT = 2.0
HOP = 3.1
ADD = 0.4
VMEM_LIMIT = 67043328


class Place:
    def __init__(self, nz):
        i, j = lax.axis_index("fsdp"), lax.axis_index("model")
        self.size = {"z": nz, "y": NY, "x": NX, "c": NC}
        self.at = {"z": lax.div(i, NY), "y": lax.rem(i, NY), "x": lax.div(j, NC), "c": lax.rem(j, NC)}

    def get(self, axis, step=0):
        n = self.size[axis]
        return lax.rem(self.at[axis] + (step + 2 * n) % n, n)

    def device(self, axis, step):
        at = dict(self.at)
        at[axis] = self.get(axis, step)
        return {"fsdp": at["z"] * NY + at["y"], "model": at["x"] * NC + at["c"]}

    def greet(self, peers):
        barrier = pltpu.get_barrier_semaphore()
        for axis, step in peers:
            pl.semaphore_signal(barrier, inc=1, device_id=self.device(axis, step), device_id_type=MESH)
        self.met = len(peers)

    def meet(self):
        pl.semaphore_wait(pltpu.get_barrier_semaphore(), self.met)


class Flow:
    def __init__(self, place, send_sem, recv_sem, base=0, now=0.0):
        self.place, self.send_sem, self.recv_sem, self.base = place, send_sem, recv_sem, base
        self.now, self.free, self.events, self.copies, self.tasks, self.order = now, {}, [], [], [], 0
        self.sent, self.leaving = set(), []

    def event(self, when, wait, then):
        heapq.heappush(self.events, (when, self.order, wait, then))
        self.order += 1

    def send(self, axis, step, src, dst, size, then=None, link=None, alt=None):
        k = len(self.copies)
        link = link or (axis, step)
        begin = max(self.now, self.free.get(link, 0.0))
        rate, lag = (PAIR, 1.5) if axis == "c" else (LINK, HOP)
        self.free[link] = begin + size / rate

        def make(dst):
            return pltpu.make_async_remote_copy(
                src_ref=src(),
                dst_ref=dst(),
                send_sem=self.send_sem.at[self.base + k],
                recv_sem=self.recv_sem.at[self.base + k],
                device_id=self.place.device(axis, step),
                device_id_type=MESH,
            )

        copy = make(dst)
        if alt is None:
            copy.start()
        else:
            when, other = alt
            pl.when(jnp.logical_not(when))(copy.start)
            pl.when(when)(make(other).start)
        self.copies.append(copy)
        heapq.heappush(self.leaving, (self.free[link] + LEFT, k))
        self.event(self.free[link] + lag, copy.wait_recv, then)
        return k

    def at(self, when, then):
        self.event(when, lambda: None, then)

    def local(self, copy, size, then):
        copy.start()
        self.event(self.now + size / LOCAL + 1.0, copy.wait, then)

    def task(self, cost, do):
        self.tasks.append((cost, do))

    def take(self):
        when, _, wait, then = heapq.heappop(self.events)
        if when > self.now:
            while self.leaving and self.leaving[0][0] <= self.now:
                self.wait_sent(heapq.heappop(self.leaving)[1])
        self.now = max(self.now, when)
        wait()
        if then is not None:
            then()

    def spend(self, cost):
        self.now += cost
        while self.events and self.events[0][0] <= self.now:
            self.take()

    def wait_sent(self, k):
        if k not in self.sent:
            self.copies[k].wait_send()
        self.sent.add(k)

    def run(self):
        while self.events or self.tasks:
            if self.tasks and (not self.events or self.events[0][0] > self.now):
                cost, do = self.tasks.pop(0)
                self.now += cost
                do()
            else:
                self.take()

    def close(self):
        for k in range(len(self.copies)):
            self.wait_sent(k)


def after(count, then):
    left = [count]

    def one():
        left[0] -= 1
        if left[0] == 0:
            then()

    return one


def nbytes(ref, lead):
    n = 1
    for d in ref.shape[lead:]:
        n *= d
    return n * jnp.dtype(ref.dtype).itemsize


def any_specs(n):
    return [pl.BlockSpec(memory_space=pl.ANY)] * n


def mm(a, b, ca, cb):
    return lax.dot_general(a, b, (((ca,), (cb,)), ((), ())), preferred_element_type=jnp.float32)


def span(q, n):
    return pl.ds(pl.multiple_of(q * n, n), n)


def exchange(flow, place, src, dst, far, step, done):
    size = nbytes(src, 1)

    def onward(way, half):
        def then():
            flow.send("y", way, lambda: far.at[half], lambda: dst.at[place.get("y", -way), half], size // 2, lambda: done(2, half))

        return then

    if step == 2:
        flow.send("y", 1, lambda: src.at[place.get("y", 2), 0], lambda: far.at[0], size // 2, onward(1, 0))
        flow.send("y", -1, lambda: src.at[place.get("y", 2), 1], lambda: far.at[1], size // 2, onward(-1, 1))
    else:
        flow.send("y", step, lambda: src.at[place.get("y", step)], lambda: dst.at[place.get("y")], size, lambda: done(-step, None))


ORDER = (2, 1, -1, 0)


class Gather:
    def __init__(self, place, flow, own, full, first, cut, arrive):
        self.place, self.flow, self.own, self.full, self.first, self.cut, self.arrive = place, flow, own, full, first, cut, arrive
        self.second = "y" if first == "x" else "x"
        self.size = nbytes(own, 1) * (cut.stop - cut.start) // own.shape[-1]

    def mine(self, half):
        return lambda: self.own.at[half, :, self.cut]

    def spot(self, at, half):
        y, x, c = (self.place.get(axis, at.get(axis, 0)) for axis in "yxc")
        return lambda: self.full.at[y, x, c, half, :, self.cut]

    def moves(self, axis, at, half, src):
        def come(step, onward):
            def then():
                here = dict(at, **{axis: step})
                if onward:
                    far = dict(at, **{axis: 2})
                    self.flow.send(axis, -step, self.spot(here, half), self.spot(here, half), self.size, lambda: self.got(axis, far, half))
                self.got(axis, here, half)

            return then

        return {
            1: lambda: self.flow.send(axis, 1, src, self.spot(at, half), self.size, come(-1, half == 0)),
            -1: lambda: self.flow.send(axis, -1, src, self.spot(at, half), self.size, come(1, half == 1)),
        }

    def spread(self, axis, at, half, src):
        for move in self.moves(axis, at, half, src).values():
            move()

    def got(self, axis, at, half):
        if axis == self.first:
            self.spread(self.second, at, half, self.spot(at, half))
        self.pair(at, half, self.spot(at, half))
        self.arrive(at.get("y", 0), at.get("x", 0))

    def pair(self, at, half, src):
        there = lambda: self.arrive(at.get("y", 0), at.get("x", 0))
        self.flow.send("c", 1, src, self.spot(at, half), self.size, there)

    def start_first(self):
        self.spread_own(self.first)

    def start_second(self):
        self.spread_own(self.second)
        for half in (0, 1):
            self.pair({}, half, self.mine(half))

    def spread_own(self, axis):
        sends = {(half, step): move for half in (0, 1) for step, move in self.moves(axis, {}, half, self.mine(half)).items()}
        for key in ((0, 1), (1, -1), (1, 1), (0, -1)):
            sends[key]()


def front_kernel(
    nz, x_ref, dy_ref, gain, w_qkv, w_out, w_gate, w_up, w_down, h_all, dy_all, w_all, z_got, h_ref, w_ref, w_heads, h_v, dy_v, z_in, far, send_sem, recv_sem, own_sem, rows_sem
):
    bf16 = jnp.bfloat16
    place = Place(nz)
    place.greet([("x", 1), ("x", -1), ("y", 1), ("y", -1), ("y", 2), ("z", 1), ("z", -1), ("c", 1)])
    for half in range(2):
        wide = x_ref[half].astype(jnp.float32)
        h_ref[half] = (wide * lax.rsqrt(jnp.mean(wide * wide, axis=-1, keepdims=True) + NORM_EPS) * gain[...]).astype(bf16)
    wide_ff = w_gate.shape[1] // NY
    one = w_out.shape[1] // (NY - 1)
    for q in range(NY):
        ffs = slice(q * wide_ff, (q + 1) * wide_ff)
        w_ref[q, :, :wide_ff] = w_gate[:, ffs]
        w_ref[q, :, wide_ff : 2 * wide_ff] = w_up[:, ffs]
        at = 2 * wide_ff
        w_ref[q, :, at : at + one] = w_qkv[:, q * one : (q + 1) * one]
        w_ref[q, :, at + one : at + 2 * one] = w_out[:, q * one : (q + 1) * one] if q < NY - 1 else w_qkv[:, NY * one :]
        w_ref[q, :, at + 2 * one :] = w_down[:, ffs]
    y, x, c, z = (place.get(axis) for axis in "yxcz")
    last = y == NY - 1
    pair = z_in.shape[-1]
    head = pair // 2
    width = h_ref.shape[-1]
    cols = w_ref.shape[-1]
    lo = (cols - pair) * 2 // 3
    hi = lo + pair
    rows = z_in.shape[2]
    flow = Flow(place, send_sem, recv_sem)
    w_own = pltpu.make_async_copy(w_ref.at[y, :, :lo], w_all.at[0, z, y, :, :lo], own_sem.at[2])
    w_own_down = pltpu.make_async_copy(w_ref.at[y, :, hi:], w_all.at[0, z, y, :, hi:], own_sem.at[4 + NX])
    w_own.start()
    w_own_down.start()
    heads_home = pltpu.make_async_copy(w_heads, w_all.at[0, :, :, :, lo:hi], own_sem.at[3])
    w_heads[z, y] = w_ref[y, :, lo:hi]
    for full, ref in ((h_v, h_ref), (dy_v, dy_ref)):
        full[y, x, c] = ref[...]
    place.meet()

    queue = []
    pieces = {}
    parts_done = {}
    weights = [4 * nz]
    writes = []

    def load():
        while queue and weights[0] == 0:
            key = queue.pop(0)
            flow.task(CHUNK_TIME, lambda key=key: product(*key))

    def complete(key):
        kind, dy, dx = key
        src, dst = ((h_v, h_all), (dy_v, dy_all))[kind]
        at = place.get("y", dy), place.get("x", dx)
        copy = pltpu.make_async_copy(src.at[at], dst.at[at], rows_sem.at[len(writes)])
        copy.start()
        writes.append(copy)
        queue.append(key)
        load()

    def arrive(kind):
        need = (8, 4)[kind]

        def one(dy, dx):
            key = (kind, dy, dx)
            pieces[key] = pieces.get(key, 0) + 1
            if pieces[key] == need:
                complete(key)

        return one

    def weight_come():
        weights[0] -= 1
        if weights[0] == 0:
            heads_home.start()
            load()

    def product(kind, dy, dx):
        rows_v = (h_v, dy_v)[kind]
        at = place.get("y", dy), place.get("x", dx)
        step = 2 if nz % 2 == 0 else 1
        deep = step * (width // nz)

        def dot(first):
            def some(i, total):
                left = rows_v[at[0], at[1], :, :, :, span(i, deep)].reshape(rows, deep)
                right = w_heads[pl.ds(i * step, step), :, :, first:].reshape(deep, pair - first)
                return total + mm(left, right, 1, 0)

            return lax.fori_loop(0, nz // step, some, jnp.zeros((rows, pair - first), jnp.float32))

        if kind == 0:
            made = dot(0).astype(bf16)
            z_in[at[0], at[1], :, :head] = made[:, :head]

            @pl.when(last)
            def _():
                z_in[at[0], at[1], :, head:] = made[:, head:]

        else:

            @pl.when(jnp.logical_not(last))
            def _():
                z_in[at[0], at[1], :, head:] = dot(head).astype(bf16)

        parts_done[dy, dx] = parts_done.get((dy, dx), 0) + 1
        if parts_done[dy, dx] == 2:
            deliver(dy, dx)

    own_copies = []

    def deliver(dy, dx):
        at = lambda: z_in.at[place.get("y", dy), place.get("x", dx)]
        size = nbytes(z_in, 2)

        def there(step=0):
            return lambda: z_got.at[place.get("y", step), place.get("x", dx)]

        if dy == 0:
            copy = pltpu.make_async_copy(at(), there()(), own_sem.at[4 + dx % NX])
            copy.start()
            own_copies.append(copy)
        elif dy == 2 and dx in DIRECT:
            flow.send("y", 2, at, there(), size, link=("y", 1))
        elif dy == 2:
            way = 1 if dx in (0, 2) else -1

            def onward():
                flow.send("y", way, lambda: far.at[dx % NX], there(-way), size)

            flow.send("y", way, at, lambda: far.at[dx % NX], size, onward)
        else:
            flow.send("y", dy, at, there(), size)

    def w_part(ref, who, dz, dy, cut):
        if ref is None:
            return lambda: w_heads.at[place.get("z", dz), place.get("y", dy)]
        return lambda: w_all.at[who, place.get("z", dz), place.get("y", dy), :, cut]

    cuts = [slice(lo, hi), slice(0, lo), slice(hi, cols)]

    def ring(step, dy, n_cut, src=None, hops=nz - 1, lead=True):
        cut = cuts[n_cut]
        home = None if n_cut == 0 else w_all
        size = nbytes(w_ref, 1) * (cut.stop - cut.start) // cols

        def hop(n):
            def then():
                here = src if src and n == 0 else w_part(home, 0, -step * n, dy, cut)
                if n < hops:
                    flow.send("z", step, here, w_part(home, 0, -step * n, dy, cut), size, hop(n + 1))
                if n or lead:
                    flow.send("c", 1, here, w_part(w_all, 1, -step * n, dy, cut), size)
                    if n_cut == 0:
                        weight_come()

            return then

        return hop(0)

    def rings(dy, n_cut, src=None):
        if n_cut:
            return ring(1 if dy in (0, 1) else -1, dy, n_cut, src)
        both = [ring(1, dy, 0, src, nz // 2), ring(-1, dy, 0, src, (nz - 1) // 2, False)]
        return lambda: [one() for one in both]

    def w_at(dy, cut):
        return lambda: w_ref.at[place.get("y", dy), :, cut]

    tail = width // nz * H_TAIL
    gathers = [
        Gather(place, flow, h_ref, h_v, "x", slice(0, width - tail), arrive(0)),
        Gather(place, flow, dy_ref, dy_v, "y", slice(0, width), arrive(1)),
        Gather(place, flow, h_ref, h_v, "y", slice(width - tail, width), arrive(0)),
    ]
    def w_start(n_cut, dys):
        cut = cuts[n_cut]
        home = None if n_cut == 0 else w_all
        size = nbytes(w_ref, 1) * (cut.stop - cut.start) // cols
        there = w_part(home, 0, 0, 0, cut)
        for dy in dys:
            if dy == 0:
                rings(0, n_cut, w_at(0, cut))()
            elif dy == 2:
                flow.send("y", 2, w_at(2, cut), there, size, rings(2, n_cut), link=("y", 1))
            else:
                flow.send("y", -dy, w_at(-dy, cut), there, size, rings(dy, n_cut))

    w_start(0, (0, 1, -1, 2))
    for one in gathers:
        one.start_first()
    flow.at(W_TIMES[0], lambda: [w_start(1, (0, -1)), w_start(2, (0, -1))])
    flow.at(W_TIMES[1], lambda: [w_start(1, (1, 2)), w_start(2, (1, 2))])
    for one in gathers:
        one.start_second()
    for n in range(2):
        for _ in range((4, 2)[n]):
            arrive(n)(0, 0)
    flow.run()
    w_own.wait()
    w_own_down.wait()
    flow.close()
    for copy in own_copies + writes:
        copy.wait()
    heads_home.wait()


CHUNK_TIME = 1.0
W_TIMES = (0.0, 0.0)
DIRECT = (2,)
H_TAIL = 1


def front(nz, x, dy, gain, w_qkv, w_out, w_gate, w_up, w_down):
    half, rows, width = x.shape
    everywhere = (NY, NX, NC) + x.shape
    slab = w_qkv.shape[0]
    pair = 2 * w_out.shape[1] // (NY - 1)
    cols = pair + 3 * w_gate.shape[1] // NY
    w_shape = (NY, slab, cols)
    bf16 = x.dtype
    gathers = 3 * (30 + 32)
    count = gathers + 3 * 3 + 3 * 4 * (nz - 1) + 3 * 4 * nz + 2 * NX + 2 * NX
    vmem = pl.BlockSpec(memory_space=pltpu.VMEM)
    dma = pltpu.SemaphoreType.DMA
    chunk = NC * half * rows
    z_shape = (NY, NX, chunk, pair)
    return pl.pallas_call(
        functools.partial(front_kernel, nz),
        out_shape=(
            jax.ShapeDtypeStruct(everywhere, bf16),
            jax.ShapeDtypeStruct(everywhere, bf16),
            jax.ShapeDtypeStruct((NC, nz) + w_shape, bf16),
            jax.ShapeDtypeStruct(z_shape, bf16),
        ),
        in_specs=[vmem] * 8,
        out_specs=tuple(any_specs(4)),
        scratch_shapes=[
            pltpu.VMEM(x.shape, bf16),
            pltpu.VMEM(w_shape, bf16),
            pltpu.VMEM((nz,) + w_shape[:-1] + (pair,), bf16),
            pltpu.VMEM(everywhere, bf16),
            pltpu.VMEM(everywhere, bf16),
            pltpu.VMEM(z_shape, bf16),
            pltpu.VMEM((NX, chunk, pair), bf16),
            dma((count,)),
            dma((count,)),
            dma((5 + NX,)),
            dma((2 * NY * NX,)),
        ],
        compiler_params=pltpu.CompilerParams(collective_id=0, has_side_effects=True, vmem_limit_bytes=VMEM_LIMIT),
        name="front",
    )(x, dy, gain, w_qkv, w_out, w_gate, w_up, w_down)


SETS = (2, 1, -1, 0)


def attention(z_got, z_back, keys, vals, dk, dv, cos_ref, sin_ref):
    bf16 = jnp.bfloat16
    seq, head = keys.shape
    part = seq // 2
    count = z_got.shape[0] - 1
    scale = head**-0.5
    spread = z_back.shape[2:5] + (head,)
    halves = [pl.ds(p * part, part) for p in range(2)]

    def turn(values, at, sign):
        wide = values.astype(jnp.float32)
        swapped = pltpu.roll(wide, head // 2, 1)
        return (wide * cos_ref[at, :] + sign * (swapped * sin_ref[at, :])).astype(bf16)

    for p in range(2):
        keys[halves[p], :] = turn(z_got[count, p, :, :head], halves[p], 1.0)
        vals[halves[p], :] = z_got[count, p, :, head:]
    dk[...] = jnp.zeros_like(dk)
    dv[...] = jnp.zeros_like(dv)

    @pl.loop(0, count)
    def _(i):
        for p in range(2):
            n = (p + 1) * part
            query = turn(z_got[i, p, :, :head], halves[p], 1.0)
            d_out = z_got[i, p, :, head:]
            scores = mm(query, keys[:n, :], 1, 1) * scale
            causal = lax.broadcasted_iota(jnp.int32, scores.shape, 0) + p * part >= lax.broadcasted_iota(jnp.int32, scores.shape, 1)
            scores = jnp.where(causal, scores, -1e30)
            grown = jnp.exp(scores - jnp.max(scores, axis=1, keepdims=True))
            probs = grown / jnp.sum(grown, axis=1, keepdims=True)
            probs_low = probs.astype(bf16)
            z_back[i, p, :, :, :, head:] = mm(probs_low, vals[:n, :], 1, 0).astype(bf16).reshape(spread)
            d_probs = mm(d_out, vals[:n, :], 1, 1).astype(bf16).astype(jnp.float32)
            d_scores = (probs * (d_probs - jnp.sum(probs * d_probs, axis=1, keepdims=True)) * scale).astype(bf16)
            z_back[i, p, :, :, :, :head] = turn(mm(d_scores, keys[:n, :], 1, 0).astype(bf16), halves[p], -1.0).reshape(spread)
            dk[:n, :] += mm(d_scores, query, 0, 0)
            dv[:n, :] += mm(probs_low, d_out, 0, 0)

    for p in range(2):
        z_back[count, p, :, :, :, :head] = turn(dk[halves[p], :].astype(bf16), halves[p], -1.0).reshape(spread)
        z_back[count, p, :, :, :, head:] = dv[halves[p], :].astype(bf16).reshape(spread)


def gated(place, flow, h_all, dy_all, w_all, acts, row_sem, share, h_rows, dy_rows, w_v):
    bf16 = jnp.bfloat16
    ff = acts.shape[-1] // 3
    lo = 2 * ff
    part = h_rows.shape[1]
    shape = acts.shape[2:5] + (ff,)
    w_loads = [
        pltpu.make_async_copy(w_all.at[0, :, :lo], w_v.at[:, :lo], row_sem.at[2, 0]),
        pltpu.make_async_copy(w_all.at[0, :, w_all.shape[2] - ff :], w_v.at[:, lo:], row_sem.at[2, 1]),
    ]

    def loads(n, slot):
        return [pltpu.make_async_copy(a.at[span(n, part)], b.at[slot], row_sem.at[slot, m]) for m, (a, b) in enumerate(((h_all, h_rows), (dy_all, dy_rows)))]

    def begin():
        for copy in w_loads + loads(0, 0) + loads(1, 1):
            copy.start()

    def go():
        for copy in w_loads:
            copy.wait()
        for q in range(NY):

            @pl.loop(0, 2)
            def _(p):
                n = 2 * q + p
                for copy in loads(n, p):
                    copy.wait()
                gate = mm(h_rows[p], w_v[:, :ff], 1, 0).astype(bf16).astype(jnp.float32)
                up = mm(h_rows[p], w_v[:, ff:lo], 1, 0).astype(bf16).astype(jnp.float32)
                d_act = mm(dy_rows[p], w_v[:, lo:], 1, 0).astype(bf16).astype(jnp.float32)
                if q < NY - 1:
                    for copy in loads(n + 2, p):
                        copy.start()
                sig = jax.nn.sigmoid(gate)
                silu = gate * sig
                acts[q, p, :, :, :, :ff] = (d_act * up * (sig + silu * (1.0 - sig))).astype(bf16).reshape(shape)
                acts[q, p, :, :, :, ff:lo] = (d_act * silu).astype(bf16).reshape(shape)
                acts[q, p, :, :, :, lo:] = (silu * up).astype(bf16).reshape(shape)

            share(q)
            flow.spend(3.0)

    return begin, go


class Plane:
    def __init__(self, place, flow, tiles, land, first, finish, free):
        self.place, self.flow, self.tiles, self.land, self.first = place, flow, tiles, land, first
        self.second = "y" if first == "x" else "x"
        self.piece = nbytes(tiles, 3)
        self.sums, self.waiting, self.finished = {}, {}, [0] * len(SETS)
        self.free = free
        self.rings = []
        for s, other in enumerate(SETS):

            def raw(step, half, s=s):
                return lambda: tiles.at[s % 2, place.get(first, step), half]

            self.rings.append(self.ring(first, raw, lambda step, half, then: then(), s, self.first_done(s, other)))
        self.onward, _ = self.ring(self.second, lambda step, half: self.sums[step, half], self.need, len(SETS), finish)

    def need(self, step, half, then):
        if (step, half) in self.sums:
            then()
        else:
            self.waiting.setdefault((step, half), []).append(then)

    def first_done(self, s, step):
        def done(half, ref):
            self.sums[step, half] = ref
            for then in self.waiting.pop((step, half), []):
                then()
            self.onward(step, half)
            self.finished[s] += 1
            if self.finished[s] == 2:
                self.free(s)

        return done

    def add(self, mine, other):
        a, b = mine(), other()
        a[...] = a[...] + b[...]
        self.flow.now += ADD

    def ring(self, axis, raw, need, s, done):
        flow, add, sent = self.flow, self.add, []

        def slot(i):
            return lambda: self.land.at[s, i]

        def turn(i, goal, half, step):
            def then():
                add(slot(i), raw(goal, half))
                flow.send(axis, step, slot(i), slot(i + 4), self.piece, final[half])

            return lambda: need(goal, half, then)

        def ending(half):
            def then():
                mine, other = (slot(5), slot(2)) if half == 0 else (slot(4), slot(3))
                add(mine, other)
                add(mine, raw(0, half))
                done(half, mine)

            return lambda: need(0, half, then)

        final = [after(2, ending(0)), after(2, ending(1))]
        moves = {
            (2, 1): (1, 0, turn(0, 1, 1, 1)),
            (2, 0): (-1, 1, turn(1, -1, 0, -1)),
            (1, 0): (1, 2, final[0]),
            (-1, 1): (-1, 3, final[1]),
        }

        def start(goal, half):
            if (goal, half) in moves:
                step, i, then = moves[goal, half]
                sent.append(flow.send(axis, step, raw(goal, half), slot(i), self.piece, then))

        return start, sent

    def start(self, s):
        for goal, half in ((2, 1), (2, 0), (1, 0), (-1, 1)):
            self.rings[s][0](goal, half)

    def clear(self, s):
        for k in self.rings[s][1]:
            self.flow.wait_sent(k)


class Grads:
    flow = None


    def __init__(self, nz, place, h_all, dy_all, acts, z_out, z_land, outs, far, h_plus, h_minus, dy_minus, tiles, stage, load_sem, stage_sem, own_sem):
        self.__dict__.update({k: v for k, v in locals().items() if k != "self"})
        self.ff = acts.shape[-1] // 3
        self.pair = z_out.shape[-1]
        lo = 2 * self.ff
        self.cols = [(0, self.ff), (self.ff, lo), (lo + self.pair, lo + self.pair + self.ff), (lo, lo + self.pair)]
        self.way = (1, 1, -1, -1)
        self.far_way = (1, -1, 1, -1)
        self.block = tiles.shape[2]
        self.size = nbytes(tiles, 2)
        self.ready, self.waiting, self.used = set(), {}, 0
        self.users = [[] for _ in range(stage.shape[0])]
        self.own = []
        self.idle, self.first = {}, {}

    def load(self, ref, src, index, step, n):
        b = self.place.get("z", -step * (n + 1))
        at = pl.ds(pl.multiple_of(b * self.block, self.block), self.block)
        return pltpu.make_async_copy(src.at[:, at], ref, self.load_sem.at[index])

    def loads_plus(self, n):
        return [self.load(self.h_plus, self.h_all, 0, 1, n)]

    def loads_minus(self, n):
        return [self.load(self.h_minus, self.h_all, 1, -1, n), self.load(self.dy_minus, self.dy_all, 2, -1, n)]

    def begin(self):
        for copy in self.loads_plus(0) + self.loads_minus(0):
            copy.start()

    def gather_up(self, tiles, some):
        seq = self.h_plus.shape[0] // NY
        for tile in tiles:
            tile[...] = jnp.zeros_like(tile)

        @pl.loop(0, NY)
        def _(q):
            for tile, value in zip(tiles, some(q, span(q, seq))):
                tile[...] += value

    def set_ready(self, lane, n):
        self.ready.add((lane, n))
        for then in self.waiting.pop((lane, n), []):
            then()
        if n == 0:
            k = self.flow.send("z", self.way[lane], lambda: self.tiles.at[0, lane], lambda: self.z_land.at[0, lane], self.size, self.hop(lane, 0))
            self.first[lane] = k

    def clear(self, lane, n):
        if n == 2:
            self.flow.wait_sent(self.first[lane])

    def tokens(self, ref):
        value = ref[...]
        return value.reshape(-1, value.shape[-1])

    def make_plus(self, n):
        for copy in self.loads_plus(n):
            copy.wait()
        lo = 2 * self.ff

        def some(q, rows):
            both = mm(self.h_plus[rows, :], self.acts[q, :, :, :, :, :lo].reshape(-1, lo), 0, 0)
            return both[:, : self.ff], both[:, self.ff :]

        self.gather_up([self.tiles.at[n % 2, 0], self.tiles.at[n % 2, 1]], some)
        if n + 1 < self.nz:
            for copy in self.loads_plus(n + 1):
                copy.start()

    def for_down(self, q, rows):
        return [mm(self.dy_minus[rows, :], self.acts[q, :, :, :, :, 2 * self.ff :].reshape(-1, self.ff), 0, 0)]

    def for_heads(self, q, rows):
        last = self.place.get("y") == NY - 1
        head = self.pair // 2
        out = self.z_out[q].reshape(-1, self.pair)
        both = mm(self.h_minus[rows, :], out, 0, 0)
        right = jnp.where(last, both[:, head:], mm(self.dy_minus[rows, :], out[:, head:], 0, 0))
        return [jnp.concatenate([both[:, :head], right], axis=1)]

    def make_minus(self, n):
        for copy in self.loads_minus(n):
            copy.wait()
        self.gather_up([self.tiles.at[n % 2, 2], self.tiles.at[n % 2, 3]], lambda q, rows: self.for_down(q, rows) + self.for_heads(q, rows))
        self.load_minus_next(n)

    def load_minus_next(self, n):
        if n + 1 < self.nz:
            for copy in self.loads_minus(n + 1):
                copy.start()

    def make_first(self):
        self.make_plus(0)
        for copy in self.loads_minus(0):
            copy.wait()
        self.gather_up([self.tiles.at[0, 2]], self.for_down)

    def heads_first(self):
        def do():
            self.gather_up([self.tiles.at[0, 3]], self.for_heads)
            self.load_minus_next(0)
            self.set_ready(3, 0)

        self.flow.task(1.3, do)

    def plus(self, n):
        def do():
            for lane in (0, 1):
                self.clear(lane, n)
            self.make_plus(n)
            for lane in (0, 1):
                self.set_ready(lane, n)

        self.flow.task(1.6, do)

    def minus(self, n):
        def do():
            for lane in (2, 3):
                self.clear(lane, n)
            self.make_minus(n)
            for lane in (2, 3):
                self.set_ready(lane, n)

        self.flow.task(2.2, do)

    def need(self, lane, n, then):
        if (lane, n) in self.ready:
            then()
        else:
            self.waiting.setdefault((lane, n), []).append(then)

    def next(self, lane, n):
        if n + 2 >= self.nz:
            return
        key = (lane // 2, n)
        self.idle[key] = self.idle.get(key, 0) + 1
        if self.idle[key] == 2:
            (self.plus, self.minus)[lane // 2](n + 2)

    def hop(self, lane, s):
        flow, place = self.flow, self.place

        def come():
            slot = self.used % len(self.users)
            self.used += 1
            for wait in self.users[slot]:
                wait()
            self.users[slot] = []
            here = lambda: self.stage.at[slot]

            def staged():
                self.need(lane, s + 1, use)

            def use():
                ref = here()
                ref[...] = ref[...] + self.tiles[(s + 1) % 2, lane]
                flow.now += ADD
                if s == 0:
                    self.next(lane, 0)
                self.next(lane, s + 1)
                if s + 1 < self.nz - 1:
                    k = flow.send("z", self.way[lane], here, lambda: self.z_land.at[s + 1, lane], self.size, self.hop(lane, s + 1))
                    self.users[slot].append(lambda: flow.wait_sent(k))
                else:
                    self.home(lane, slot)

            flow.local(pltpu.make_async_copy(self.z_land.at[s, lane], here(), self.stage_sem.at[slot]), self.size, staged)

        return come

    def home(self, lane, slot):
        flow, place = self.flow, self.place
        slab = self.block // NY
        way = self.far_way[lane]
        size = self.size // NY

        def rows(step, cut=slice(None)):
            return lambda: self.stage.at[slot, pl.ds(pl.multiple_of(place.get("y", step) * slab, slab), slab), cut]

        def columns(out, step, wide):
            at = place.get("y", step) * wide
            return lambda: self.outs[out].at[:, pl.ds(pl.multiple_of(at, wide), wide)]

        def deliver(size, src, far, dst, n, other=None):
            def alt(step):
                return None if other is None else (place.get("y", step) == NY - 1, other(step))

            def onward():
                flow.send("y", way, far, dst(-way), size, alt=alt(-way))

            sent = [flow.send("y", way, src(2), far, size, onward)]
            sent += [flow.send("y", step, src(step), dst(0), size, alt=alt(0)) for step in (1, -1)]
            copies = [(None, pltpu.make_async_copy(src(0)(), dst(0)(), self.own_sem.at[n]))]
            if other is not None:
                last = place.get("y") == NY - 1
                copies = [(jnp.logical_not(last), copies[0][1]), (last, pltpu.make_async_copy(src(0)(), other(0)(), self.own_sem.at[n]))]
            for when, copy in copies:
                if when is None:
                    copy.start()
                else:
                    pl.when(when)(copy.start)
            self.users[slot] += [functools.partial(flow.wait_sent, k) for k in sent] + [copies[0][1].wait]

        if lane < 3:
            deliver(size, rows, lambda: self.far.at[lane], lambda step: columns(lane, step, self.ff), lane)
            return
        head = self.pair // 2
        first, second = slice(0, head), slice(head, self.pair)
        deliver(size // 2, lambda step: rows(step, first), lambda: self.far.at[3, :, first], lambda step: columns(3, step, head), 3)
        value = lambda: self.outs[3].at[:, NY * head :]

        def out_rows(step):
            at = lax.rem(place.get("y", step), NY - 1) * head
            return lambda: self.outs[4].at[:, pl.ds(pl.multiple_of(at, head), head)]

        deliver(size // 2, lambda step: rows(step, second), lambda: self.far.at[3, :, second], out_rows, 4, lambda step: value)

    def close(self):
        for users in self.users:
            for wait in users:
                wait()


def back_kernel(
    nz,
    z_in,
    h_all,
    dy_all,
    w_all,
    cos_in,
    sin_in,
    gain,
    x_in,
    dy_in,
    y_out,
    dx_out,
    g_qkv,
    g_out,
    g_gate,
    g_up,
    g_down,
    z_land,
    x_ref,
    dy_ref,
    cos_ref,
    sin_ref,
    z_got,
    z_back,
    z_out,
    far_back,
    acts,
    pair_acts,
    far,
    p_land,
    q_land,
    keys,
    vals,
    dk,
    dv,
    h_plus,
    h_minus,
    dy_minus,
    tiles,
    stage,
    load_sem,
    row_sem,
    w_sem,
    g_load_sem,
    stage_sem,
    own_sem,
    send_sem,
    recv_sem,
):
    bf16, f32 = jnp.bfloat16, jnp.float32
    place = Place(nz)
    y, c = place.get("y"), place.get("c")
    other = place.get("c", 1)
    last = y == NY - 1
    seq, head = keys.shape
    pair = 2 * head
    rows, cols = pair_acts.shape[3:]
    ff = (cols - pair) // 3
    lo, hi = 2 * ff, 2 * ff + pair
    tokens, width = h_all.shape
    block = width // nz
    part = seq // 2

    place.greet([("x", 1), ("x", -1), ("y", 1), ("y", -1), ("z", 1), ("z", -1), ("c", 1)])
    z_load = pltpu.make_async_copy(z_in, z_got, load_sem)
    z_load.start()
    row_loads = [pltpu.make_async_copy(a, b, own_sem.at[5 + n]) for n, (a, b) in enumerate(((x_in, x_ref), (dy_in, dy_ref)))]
    cos_ref[...] = jnp.concatenate([cos_in[...], cos_in[...]], axis=0).T
    sin_ref[...] = jnp.concatenate([-sin_in[...], sin_in[...]], axis=0).T
    early = Flow(place, send_sem, recv_sem)

    def share(q):
        early.send("c", 1, lambda: acts.at[q, :, :, other, :, :lo], lambda: pair_acts.at[q, :, :, :, :lo], nbytes(pair_acts, 1) * lo // cols)
        early.send("c", 1, lambda: acts.at[q, :, :, other, :, lo:], lambda: pair_acts.at[q, :, :, :, hi:], nbytes(pair_acts, 1) * ff // cols)

    def out_come(step, half):
        cut = slice(None) if half is None else half
        part = nbytes(z_out, 1) // NC // (1 if half is None else 2)
        src = lambda: z_out.at[place.get("y", step), cut, :, other]
        early.send("c", 1, src, lambda: pair_acts.at[place.get("y", step), cut, :, :, lo:hi], part)

    grads = Grads(nz, place, h_all, dy_all, acts, z_out, z_land, (g_gate, g_up, g_down, g_qkv, g_out), far, h_plus, h_minus, dy_minus, tiles, stage, g_load_sem, stage_sem, own_sem)

    def first(h_rows, dy_rows, w_v):
        begin, go = gated(place, early, h_all, dy_all, w_all, acts, row_sem, share, h_rows, dy_rows, w_v)
        begin()
        grads.begin()
        for copy in row_loads:
            copy.start()
        z_load.wait()
        attention(z_got, z_back, keys, vals, dk, dv, cos_ref, sin_ref)
        place.meet()
        for step in ORDER[:3]:
            exchange(early, place, z_back, z_out, far_back, step, out_come)
        z_out[y] = z_back[y]
        early.send("c", 1, lambda: z_back.at[y, :, :, other], lambda: pair_acts.at[y, :, :, :, lo:hi], nbytes(z_out, 1) // NC)
        go()
        grads.make_first()
        early.now += 2.6
        early.run()
        early.close()
        for copy in row_loads:
            copy.wait()

    pl.run_scoped(
        first,
        pltpu.VMEM((2, part, width), bf16),
        pltpu.VMEM((2, part, width), bf16),
        pltpu.VMEM((width, 3 * ff), bf16),
    )

    def second(p_tile, q_tile, w_v):
        flow = Flow(place, send_sem, recv_sem, len(early.copies), early.now)
        grads.flow = flow
        lane = lax.broadcasted_iota(jnp.int32, (rows, pair), 1)
        for_d = jnp.logical_or(lane < head, last)

        def chunk(k, i, p, xx):
            if k == 0:
                own = acts[i, p, xx, c]
                return own[:, :lo], z_out[i, p, xx, c], own[:, lo:]
            theirs = pair_acts[i, p, xx]
            return theirs[:, :lo], theirs[:, lo:hi], theirs[:, hi:]

        def for_out(k, i, p, xx):
            _, mixed, act = chunk(k, i, p, xx)
            return jnp.concatenate([jnp.where(for_d, jnp.zeros_like(mixed), mixed), act], axis=1)

        def for_in(k, i, p, xx):
            grad, mixed, _ = chunk(k, i, p, xx)
            return jnp.concatenate([grad, jnp.where(for_d, mixed, jnp.zeros_like(mixed))], axis=1)

        depth = w_v.shape[0]

        def w_copy(kind, d, slot):
            at = pl.ds(pl.multiple_of(d * block, block), block)
            cut = slice(lo, cols) if kind == 0 else slice(0, cols)
            return pltpu.make_async_copy(w_all.at[:, at, cut], w_v.at[slot, :, :, cut], w_sem.at[slot])

        counts = (nz - 1, nz)
        base, total = [], 0
        for kind, _ in PASSES:
            base.append(total)
            total += counts[kind]
        kind = PASSES[0][0]
        for n in range(depth):
            w_copy(kind, n, n).start() if n < counts[kind] else w_copy(PASSES[1][0], n - counts[kind], n).start()
        turn = [0]

        def blocks(s, kind, first, count, body):
            n = turn[0]
            assert PASSES[n] == (kind, s)
            if first + count == counts[kind]:
                turn[0] += 1

            @pl.loop(first, first + count)
            def _(d):
                slot = lax.rem(base[n] + d, depth)
                w_copy(kind, d, slot).wait()
                body(d, w_v.at[slot])

                @pl.when(d + depth < counts[kind])
                def _():
                    w_copy(kind, d + depth, slot).start()

                if n + 1 < len(PASSES):

                    @pl.when(d + depth >= counts[kind])
                    def _():
                        w_copy(PASSES[n + 1][0], d + depth - counts[kind], slot).start()

        def product(parts, w, a, b):
            total = None
            for k in range(NC):
                left = jnp.concatenate([one(k) for one in parts], axis=0)
                one = mm(left, w[k, :, a:b], 1, 1)
                total = one if total is None else total + one
            return total

        shape = (NX, 2, rows // 2, block)

        def p_rows(s):
            x = place.get("x", SETS[s])
            p, xx = lax.div(x, NX // 2), lax.rem(x, NX // 2)
            return [lambda k, i=i: for_out(k, i, p, xx) for i in range(NY)]

        def q_rows(s, make):
            i = place.get("y", SETS[s])
            return [lambda k, p=p, xx=xx: make(k, i, p, xx) for p in range(2) for xx in range(NX // 2)]

        def place_of(d):
            return pl.ds(pl.multiple_of(d * block, block), block)

        def p_task(s):
            def body(d, w):
                p_tile[s % 2, :, :, :, place_of(d)] = product(p_rows(s), w, lo, cols).reshape(shape)

            def do():
                if s >= 2:
                    planes[0].clear(s - 2)
                blocks(s, 0, 0, nz - 1, body)
                planes[0].start(s)

            flow.task(P_TIME, do)

        def q_task(s):
            def body(d, w):
                q_tile[s % 2, :, :, :, place_of(d)] = product(q_rows(s, for_in), w, 0, hi).reshape(shape)

                @pl.when(d == nz - 1)
                def _():
                    q_tile[s % 2, :, :, :, width:] = product(q_rows(s, for_out), w, lo, cols).reshape(shape)

            def start():
                if s >= 2:
                    planes[1].clear(s - 2)
                blocks(s, 1, 0, nz // 2, body)

            def end():
                blocks(s, 1, nz // 2, nz - nz // 2, body)
                planes[1].start(s)

            flow.task(Q_HALF, start)
            flow.task(Q_HALF, end)

        edge = width - block
        def p_finish(half, ref):
            y_out[half, :, :edge] = (x_ref[half, :, :edge].astype(f32) + ref()[...]).astype(bf16)

        def q_finish(half, ref):
            y_out[half, :, edge:] = (x_ref[half, :, edge:].astype(f32) + ref()[:, width:]).astype(bf16)
            wide = x_ref[half].astype(f32)
            scale = lax.rsqrt(jnp.mean(wide * wide, axis=-1, keepdims=True) + NORM_EPS)
            d_normed = ref()[:, :width].astype(bf16).astype(f32) * gain[...]
            mean = jnp.mean(d_normed * wide, axis=-1, keepdims=True)
            grad = d_normed * scale - wide * (scale * scale * scale * mean)
            dx_out[half] = (dy_ref[half].astype(f32) + grad).astype(bf16)

        def free(task):
            return lambda s: task(s + 2) if s + 2 < len(SETS) else None

        planes = [
            Plane(place, flow, p_tile, p_land, "y", p_finish, free(p_task)),
            Plane(place, flow, q_tile, q_land, "x", q_finish, free(q_task)),
        ]

        for lane in range(3):
            grads.set_ready(lane, 0)
        q_task(0)
        p_task(0)
        grads.heads_first()
        grads.plus(1)
        grads.minus(1)
        p_task(1)
        q_task(1)
        flow.run()
        flow.close()
        grads.close()

    pl.run_scoped(
        second,
        pltpu.VMEM((2, NY, 2, rows // 2, width - block), f32),
        pltpu.VMEM((2, NX, 2, rows // 2, width + block), f32),
        pltpu.VMEM((3, NC, block, cols), bf16),
    )


STAGES = 5
PASSES = ((1, 0), (0, 0), (0, 1), (1, 1), (1, 2), (0, 2), (0, 3), (1, 3))
P_TIME = 3.0
Q_HALF = 2.6


def back(nz, z_in, h_all, dy_all, w_all, cos, sin, x, dy, gain):
    tokens, width = h_all.shape
    seq, head = cos.shape[1], 2 * cos.shape[0]
    pair = 2 * head
    cols = w_all.shape[2]
    ff = (cols - pair) // 3
    rows = seq // (NX * NC)
    block = width // nz
    bf16, f32 = h_all.dtype, jnp.float32
    vmem = pl.BlockSpec(memory_space=pltpu.VMEM)
    dma = pltpu.SemaphoreType.DMA
    blocks = (NY, 2, NX // 2, NC, rows, pair)
    p_piece = (rows // 2, width - block)
    q_piece = (rows // 2, width + block)
    count = 6 + 2 * NY + 5 + 4 * (nz - 1) + 5 * 4 + 2 * 5 * 6
    slab = block // NY
    weight = jax.ShapeDtypeStruct((slab, NY * ff), f32)
    return pl.pallas_call(
        functools.partial(back_kernel, nz),
        out_shape=(
            jax.ShapeDtypeStruct(x.shape, bf16),
            jax.ShapeDtypeStruct(x.shape, bf16),
            jax.ShapeDtypeStruct((slab, (NY + 1) * head), f32),
            jax.ShapeDtypeStruct((slab, (NY - 1) * head), f32),
            weight,
            weight,
            weight,
            jax.ShapeDtypeStruct((nz - 1, 4, block, ff), f32),
        ),
        in_specs=any_specs(4) + [vmem] * 3 + any_specs(2),
        out_specs=(vmem, vmem) + tuple(any_specs(6)),
        scratch_shapes=[
            pltpu.VMEM(x.shape, bf16),
            pltpu.VMEM(x.shape, bf16),
            pltpu.VMEM((seq, head), f32),
            pltpu.VMEM((seq, head), f32),
            pltpu.VMEM(z_in.shape, bf16),
            pltpu.VMEM(blocks, bf16),
            pltpu.VMEM(blocks, bf16),
            pltpu.VMEM(blocks[1:], bf16),
            pltpu.VMEM(blocks[:-1] + (3 * ff,), bf16),
            pltpu.VMEM(blocks[:3] + (rows, cols), bf16),
            pltpu.VMEM((4, block // NY, ff), f32),
            pltpu.VMEM((5, 6) + p_piece, f32),
            pltpu.VMEM((5, 6) + q_piece, f32),
            pltpu.VMEM((seq, head), bf16),
            pltpu.VMEM((seq, head), bf16),
            pltpu.VMEM((seq, head), f32),
            pltpu.VMEM((seq, head), f32),
            pltpu.VMEM((tokens, block), bf16),
            pltpu.VMEM((tokens, block), bf16),
            pltpu.VMEM((tokens, block), bf16),
            pltpu.VMEM((2, 4, block, ff), f32),
            pltpu.VMEM((STAGES, block, ff), f32),
            dma,
            dma((3, 2)),
            dma((3,)),
            dma((3,)),
            dma((STAGES,)),
            dma((7,)),
            dma((count,)),
            dma((count,)),
        ],
        compiler_params=pltpu.CompilerParams(collective_id=2, has_side_effects=True, vmem_limit_bytes=VMEM_LIMIT),
        name="back",
    )(z_in, h_all, dy_all, w_all, cos, sin, gain, x, dy)[:7]


def settle_kernel(*refs):
    n = len(refs) // 3
    ins, outs, held = refs[:n], refs[n : 2 * n], refs[2 * n : 3 * n]
    in_sem, out_sem = refs[3 * n :]
    come = [pltpu.make_async_copy(a, b, in_sem.at[i]) for i, (a, b) in enumerate(zip(ins, held))]
    go = [pltpu.make_async_copy(a, b, out_sem.at[i]) for i, (a, b) in enumerate(zip(held, outs))]
    for copy in come:
        copy.start()
    for first, second in zip(come, go):
        first.wait()
        second.start()
    for copy in go:
        copy.wait()


def settle(arrays):
    n = len(arrays)
    return pl.pallas_call(
        settle_kernel,
        out_shape=tuple(jax.ShapeDtypeStruct(a.shape, a.dtype) for a in arrays),
        in_specs=any_specs(n),
        out_specs=tuple(any_specs(n)),
        scratch_shapes=[pltpu.VMEM(a.shape, a.dtype) for a in arrays] + [pltpu.SemaphoreType.DMA((n,))] * 2,
        name="settle",
    )(*arrays)


def solution(mesh):
    act_spec = P("fsdp", "model", None)
    col_spec = P("fsdp", "model")
    row_spec = P("model", "fsdp")
    nz = mesh.shape["fsdp"] // NY

    def layer_body(x_in, dy_in, norm_gain, w_qkv, w_out, w_gate, w_up, w_down, rope_cos, rope_sin):
        _, rows, width = x_in.shape
        head = 2 * rope_cos.shape[1]
        seq = rows * NX * NC
        tokens = NY * seq
        x = x_in.reshape(2, rows // 2, width)
        dy = dy_in.reshape(2, rows // 2, width)
        gain = norm_gain.reshape(1, width)
        h_all, dy_all, w_all, z_got = front(nz, x, dy, gain, w_qkv, w_out.T, w_gate, w_up, w_down.T)
        results = back(
            nz,
            z_got.reshape(NY, 2, seq // 2, 2 * head),
            h_all.reshape(tokens, width),
            dy_all.reshape(tokens, width),
            w_all.reshape(NC, width, -1),
            rope_cos.T,
            rope_sin.T,
            x,
            dy,
            gain,
        )
        y_out, dx_out, g_qkv, g_out, g_gate, g_up, g_down = settle(results)
        return y_out.reshape(x_in.shape), dx_out.reshape(x_in.shape), g_qkv, g_out.T, g_gate, g_up, g_down.T

    return jax.shard_map(
        layer_body,
        mesh=mesh,
        in_specs=(act_spec, act_spec, P(), col_spec, row_spec, col_spec, col_spec, row_spec, P(), P()),
        out_specs=(act_spec, act_spec, col_spec, row_spec, col_spec, col_spec, row_spec),
        check_vma=False,
    )
```

```python
import functools
import heapq

import jax
import jax.numpy as jnp
from jax import lax
from jax.experimental import pallas as pl
from jax.experimental.pallas import tpu as pltpu
from jax.sharding import PartitionSpec as P

NORM_EPS = 1e-5
NY, NX, NC = 4, 4, 2
MESH = pl.DeviceIdType.MESH
LINK = 46.6e3
PAIR = 450e3
LOCAL = 1500e3
LEFT = 2.0
HOP = 3.1
ADD = 0.4
VMEM_LIMIT = 67043328


class Place:
    def __init__(self, nz):
        i, j = lax.axis_index("fsdp"), lax.axis_index("model")
        self.size = {"z": nz, "y": NY, "x": NX, "c": NC}
        self.at = {"z": lax.div(i, NY), "y": lax.rem(i, NY), "x": lax.div(j, NC), "c": lax.rem(j, NC)}

    def get(self, axis, step=0):
        n = self.size[axis]
        return lax.rem(self.at[axis] + (step + 2 * n) % n, n)

    def device(self, axis, step):
        at = dict(self.at)
        at[axis] = self.get(axis, step)
        return {"fsdp": at["z"] * NY + at["y"], "model": at["x"] * NC + at["c"]}

    def greet(self, peers):
        barrier = pltpu.get_barrier_semaphore()
        for axis, step in peers:
            pl.semaphore_signal(barrier, inc=1, device_id=self.device(axis, step), device_id_type=MESH)
        self.met = len(peers)

    def meet(self):
        pl.semaphore_wait(pltpu.get_barrier_semaphore(), self.met)


class Flow:
    def __init__(self, place, send_sem, recv_sem, base=0, now=0.0):
        self.place, self.send_sem, self.recv_sem, self.base = place, send_sem, recv_sem, base
        self.now, self.free, self.events, self.copies, self.tasks, self.order = now, {}, [], [], [], 0
        self.sent, self.leaving = set(), []

    def event(self, when, wait, then):
        heapq.heappush(self.events, (when, self.order, wait, then))
        self.order += 1

    def send(self, axis, step, src, dst, size, then=None, link=None, alt=None):
        k = len(self.copies)
        link = link or (axis, step)
        begin = max(self.now, self.free.get(link, 0.0))
        rate, lag = (PAIR, 1.5) if axis == "c" else (LINK, HOP)
        self.free[link] = begin + size / rate

        def make(dst):
            return pltpu.make_async_remote_copy(
                src_ref=src(),
                dst_ref=dst(),
                send_sem=self.send_sem.at[self.base + k],
                recv_sem=self.recv_sem.at[self.base + k],
                device_id=self.place.device(axis, step),
                device_id_type=MESH,
            )

        copy = make(dst)
        if alt is None:
            copy.start()
        else:
            when, other = alt
            pl.when(jnp.logical_not(when))(copy.start)
            pl.when(when)(make(other).start)
        self.copies.append(copy)
        heapq.heappush(self.leaving, (self.free[link] + LEFT, k))
        self.event(self.free[link] + lag, copy.wait_recv, then)
        return k

    def at(self, when, then):
        self.event(when, lambda: None, then)

    def local(self, copy, size, then):
        copy.start()
        self.event(self.now + size / LOCAL + 1.0, copy.wait, then)

    def task(self, cost, do):
        self.tasks.append((cost, do))

    def take(self):
        when, _, wait, then = heapq.heappop(self.events)
        if when > self.now:
            while self.leaving and self.leaving[0][0] <= self.now:
                self.wait_sent(heapq.heappop(self.leaving)[1])
        self.now = max(self.now, when)
        wait()
        if then is not None:
            then()

    def spend(self, cost):
        self.now += cost
        while self.events and self.events[0][0] <= self.now:
            self.take()

    def wait_sent(self, k):
        if k not in self.sent:
            self.copies[k].wait_send()
        self.sent.add(k)

    def run(self):
        while self.events or self.tasks:
            if self.tasks and (not self.events or self.events[0][0] > self.now):
                cost, do = self.tasks.pop(0)
                self.now += cost
                do()
            else:
                self.take()

    def close(self):
        for k in range(len(self.copies)):
            self.wait_sent(k)


def after(count, then):
    left = [count]

    def one():
        left[0] -= 1
        if left[0] == 0:
            then()

    return one


def nbytes(ref, lead):
    n = 1
    for d in ref.shape[lead:]:
        n *= d
    return n * jnp.dtype(ref.dtype).itemsize


def any_specs(n):
    return [pl.BlockSpec(memory_space=pl.ANY)] * n


def mm(a, b, ca, cb):
    return lax.dot_general(a, b, (((ca,), (cb,)), ((), ())), preferred_element_type=jnp.float32)


def span(q, n):
    return pl.ds(pl.multiple_of(q * n, n), n)


def exchange(flow, place, src, dst, far, step, done):
    size = nbytes(src, 1)

    def onward(way, half):
        def then():
            flow.send("y", way, lambda: far.at[half], lambda: dst.at[place.get("y", -way), half], size // 2, lambda: done(2, half))

        return then

    if step == 2:
        flow.send("y", 1, lambda: src.at[place.get("y", 2), 0], lambda: far.at[0], size // 2, onward(1, 0))
        flow.send("y", -1, lambda: src.at[place.get("y", 2), 1], lambda: far.at[1], size // 2, onward(-1, 1))
    else:
        flow.send("y", step, lambda: src.at[place.get("y", step)], lambda: dst.at[place.get("y")], size, lambda: done(-step, None))


ORDER = (2, 1, -1, 0)


class Gather:
    def __init__(self, place, flow, own, full, first, cut, arrive):
        self.place, self.flow, self.own, self.full, self.first, self.cut, self.arrive = place, flow, own, full, first, cut, arrive
        self.second = "y" if first == "x" else "x"
        self.size = nbytes(own, 1) * (cut.stop - cut.start) // own.shape[-1]

    def mine(self, half):
        return lambda: self.own.at[half, :, self.cut]

    def spot(self, at, half):
        y, x, c = (self.place.get(axis, at.get(axis, 0)) for axis in "yxc")
        return lambda: self.full.at[y, x, c, half, :, self.cut]

    def moves(self, axis, at, half, src):
        def come(step, onward):
            def then():
                here = dict(at, **{axis: step})
                if onward:
                    far = dict(at, **{axis: 2})
                    self.flow.send(axis, -step, self.spot(here, half), self.spot(here, half), self.size, lambda: self.got(axis, far, half))
                self.got(axis, here, half)

            return then

        return {
            1: lambda: self.flow.send(axis, 1, src, self.spot(at, half), self.size, come(-1, half == 0)),
            -1: lambda: self.flow.send(axis, -1, src, self.spot(at, half), self.size, come(1, half == 1)),
        }

    def spread(self, axis, at, half, src):
        for move in self.moves(axis, at, half, src).values():
            move()

    def got(self, axis, at, half):
        if axis == self.first:
            self.spread(self.second, at, half, self.spot(at, half))
        self.pair(at, half, self.spot(at, half))
        self.arrive(at.get("y", 0), at.get("x", 0))

    def pair(self, at, half, src):
        there = lambda: self.arrive(at.get("y", 0), at.get("x", 0))
        self.flow.send("c", 1, src, self.spot(at, half), self.size, there)

    def start_first(self):
        self.spread_own(self.first)

    def start_second(self):
        self.spread_own(self.second)
        for half in (0, 1):
            self.pair({}, half, self.mine(half))

    def spread_own(self, axis):
        sends = {(half, step): move for half in (0, 1) for step, move in self.moves(axis, {}, half, self.mine(half)).items()}
        for key in ((0, 1), (1, -1), (1, 1), (0, -1)):
            sends[key]()


def front_kernel(
    nz, x_in, dy_in, gain, *refs
):
    args, refs = refs[:5], refs[5:]
    held, refs = refs[-8:-1], refs[:-8] + refs[-1:]
    front_body(nz, (x_in, dy_in) + args, held, gain, *refs)


def front_body(
    nz, ins, held, gain, h_all, dy_all, w_all, z_got, h_ref, w_ref, w_heads, h_v, dy_v, z_in, far, send_sem, recv_sem, own_sem, rows_sem, in_sem
):
    x_ref, dy_ref, w_qkv, w_out, w_gate, w_up, w_down = held
    in_copies = [pltpu.make_async_copy(a, b, in_sem.at[n]) for n, (a, b) in enumerate(zip(ins, held))]
    for copy in in_copies:
        copy.start()
    bf16 = jnp.bfloat16
    place = Place(nz)
    place.greet([("x", 1), ("x", -1), ("y", 1), ("y", -1), ("y", 2), ("z", 1), ("z", -1), ("c", 1)])
    in_copies[0].wait()
    for half in range(2):
        wide = x_ref[half].astype(jnp.float32)
        h_ref[half] = (wide * lax.rsqrt(jnp.mean(wide * wide, axis=-1, keepdims=True) + NORM_EPS) * gain[...]).astype(bf16)
    for copy in in_copies[1:]:
        copy.wait()
    wide_ff = w_gate.shape[1] // NY
    one = w_out.shape[1] // (NY - 1)
    for q in range(NY):
        ffs = slice(q * wide_ff, (q + 1) * wide_ff)
        w_ref[q, :, :wide_ff] = w_gate[:, ffs]
        w_ref[q, :, wide_ff : 2 * wide_ff] = w_up[:, ffs]
        at = 2 * wide_ff
        w_ref[q, :, at : at + one] = w_qkv[:, q * one : (q + 1) * one]
        w_ref[q, :, at + one : at + 2 * one] = w_out[:, q * one : (q + 1) * one] if q < NY - 1 else w_qkv[:, NY * one :]
        w_ref[q, :, at + 2 * one :] = w_down[:, ffs]
    y, x, c, z = (place.get(axis) for axis in "yxcz")
    last = y == NY - 1
    pair = z_in.shape[-1]
    head = pair // 2
    width = h_ref.shape[-1]
    cols = w_ref.shape[-1]
    lo = (cols - pair) * 2 // 3
    hi = lo + pair
    rows = z_in.shape[2]
    flow = Flow(place, send_sem, recv_sem)
    w_own = pltpu.make_async_copy(w_ref.at[y, :, :lo], w_all.at[0, z, y, :, :lo], own_sem.at[2])
    w_own_down = pltpu.make_async_copy(w_ref.at[y, :, hi:], w_all.at[0, z, y, :, hi:], own_sem.at[4 + NX])
    w_own.start()
    w_own_down.start()
    heads_home = pltpu.make_async_copy(w_heads, w_all.at[0, :, :, :, lo:hi], own_sem.at[3])
    w_heads[z, y] = w_ref[y, :, lo:hi]
    for full, ref in ((h_v, h_ref), (dy_v, dy_ref)):
        full[y, x, c] = ref[...]
    place.meet()

    queue = []
    pieces = {}
    parts_done = {}
    weights = [4 * nz]
    writes = []

    def load():
        while queue and weights[0] == 0:
            key = queue.pop(0)
            flow.task(CHUNK_TIME, lambda key=key: product(*key))

    def complete(key):
        kind, dy, dx = key
        src, dst = ((h_v, h_all), (dy_v, dy_all))[kind]
        at = place.get("y", dy), place.get("x", dx)
        copy = pltpu.make_async_copy(src.at[at], dst.at[at], rows_sem.at[len(writes)])
        copy.start()
        writes.append(copy)
        queue.append(key)
        load()

    def arrive(kind):
        need = (8, 4)[kind]

        def one(dy, dx):
            key = (kind, dy, dx)
            pieces[key] = pieces.get(key, 0) + 1
            if pieces[key] == need:
                complete(key)

        return one

    def weight_come():
        weights[0] -= 1
        if weights[0] == 0:
            heads_home.start()
            load()

    def product(kind, dy, dx):
        rows_v = (h_v, dy_v)[kind]
        at = place.get("y", dy), place.get("x", dx)
        step = 2 if nz % 2 == 0 else 1
        deep = step * (width // nz)

        def dot(first):
            def some(i, total):
                left = rows_v[at[0], at[1], :, :, :, span(i, deep)].reshape(rows, deep)
                right = w_heads[pl.ds(i * step, step), :, :, first:].reshape(deep, pair - first)
                return total + mm(left, right, 1, 0)

            return lax.fori_loop(0, nz // step, some, jnp.zeros((rows, pair - first), jnp.float32))

        if kind == 0:
            made = dot(0).astype(bf16)
            z_in[at[0], at[1], :, :head] = made[:, :head]

            @pl.when(last)
            def _():
                z_in[at[0], at[1], :, head:] = made[:, head:]

        else:

            @pl.when(jnp.logical_not(last))
            def _():
                z_in[at[0], at[1], :, head:] = dot(head).astype(bf16)

        parts_done[dy, dx] = parts_done.get((dy, dx), 0) + 1
        if parts_done[dy, dx] == 2:
            deliver(dy, dx)

    own_copies = []

    def deliver(dy, dx):
        at = lambda: z_in.at[place.get("y", dy), place.get("x", dx)]
        size = nbytes(z_in, 2)

        def there(step=0):
            return lambda: z_got.at[place.get("y", step), place.get("x", dx)]

        if dy == 0:
            copy = pltpu.make_async_copy(at(), there()(), own_sem.at[4 + dx % NX])
            copy.start()
            own_copies.append(copy)
        elif dy == 2 and dx in DIRECT:
            flow.send("y", 2, at, there(), size, link=("y", 1))
        elif dy == 2:
            way = 1 if dx in (0, 2) else -1

            def onward():
                flow.send("y", way, lambda: far.at[dx % NX], there(-way), size)

            flow.send("y", way, at, lambda: far.at[dx % NX], size, onward)
        else:
            flow.send("y", dy, at, there(), size)

    def w_part(ref, who, dz, dy, cut):
        if ref is None:
            return lambda: w_heads.at[place.get("z", dz), place.get("y", dy)]
        return lambda: w_all.at[who, place.get("z", dz), place.get("y", dy), :, cut]

    cuts = [slice(lo, hi), slice(0, lo), slice(hi, cols)]

    def ring(step, dy, n_cut, src=None, hops=nz - 1, lead=True):
        cut = cuts[n_cut]
        home = None if n_cut == 0 else w_all
        size = nbytes(w_ref, 1) * (cut.stop - cut.start) // cols

        def hop(n):
            def then():
                here = src if src and n == 0 else w_part(home, 0, -step * n, dy, cut)
                if n < hops:
                    flow.send("z", step, here, w_part(home, 0, -step * n, dy, cut), size, hop(n + 1))
                if n or lead:
                    flow.send("c", 1, here, w_part(w_all, 1, -step * n, dy, cut), size)
                    if n_cut == 0:
                        weight_come()

            return then

        return hop(0)

    def rings(dy, n_cut, src=None):
        if n_cut:
            return ring(1 if dy in (0, 1) else -1, dy, n_cut, src)
        both = [ring(1, dy, 0, src, nz // 2), ring(-1, dy, 0, src, (nz - 1) // 2, False)]
        return lambda: [one() for one in both]

    def w_at(dy, cut):
        return lambda: w_ref.at[place.get("y", dy), :, cut]

    tail = width // nz * H_TAIL
    gathers = [
        Gather(place, flow, h_ref, h_v, "x", slice(0, width - tail), arrive(0)),
        Gather(place, flow, dy_ref, dy_v, "y", slice(0, width), arrive(1)),
        Gather(place, flow, h_ref, h_v, "y", slice(width - tail, width), arrive(0)),
    ]
    def w_start(n_cut, dys):
        cut = cuts[n_cut]
        home = None if n_cut == 0 else w_all
        size = nbytes(w_ref, 1) * (cut.stop - cut.start) // cols
        there = w_part(home, 0, 0, 0, cut)
        for dy in dys:
            if dy == 0:
                rings(0, n_cut, w_at(0, cut))()
            elif dy == 2:
                flow.send("y", 2, w_at(2, cut), there, size, rings(2, n_cut), link=("y", 1))
            else:
                flow.send("y", -dy, w_at(-dy, cut), there, size, rings(dy, n_cut))

    w_start(0, (0, 1, -1, 2))
    for one in gathers:
        one.start_first()
    flow.at(W_TIMES[0], lambda: [w_start(1, (0, -1)), w_start(2, (0, -1))])
    flow.at(W_TIMES[1], lambda: [w_start(1, (1, 2)), w_start(2, (1, 2))])
    for one in gathers:
        one.start_second()
    for n in range(2):
        for _ in range((4, 2)[n]):
            arrive(n)(0, 0)
    flow.run()
    w_own.wait()
    w_own_down.wait()
    flow.close()
    for copy in own_copies + writes:
        copy.wait()
    heads_home.wait()


CHUNK_TIME = 1.0
W_TIMES = (0.0, 0.0)
DIRECT = (2,)
H_TAIL = 1


def front(nz, x, dy, gain, w_qkv, w_out, w_gate, w_up, w_down):
    half, rows, width = x.shape
    everywhere = (NY, NX, NC) + x.shape
    slab = w_qkv.shape[0]
    pair = 2 * w_out.shape[1] // (NY - 1)
    cols = pair + 3 * w_gate.shape[1] // NY
    w_shape = (NY, slab, cols)
    bf16 = x.dtype
    gathers = 3 * (30 + 32)
    count = gathers + 3 * 3 + 3 * 4 * (nz - 1) + 3 * 4 * nz + 2 * NX + 2 * NX
    vmem = pl.BlockSpec(memory_space=pltpu.VMEM)
    dma = pltpu.SemaphoreType.DMA
    chunk = NC * half * rows
    z_shape = (NY, NX, chunk, pair)
    return pl.pallas_call(
        functools.partial(front_kernel, nz),
        out_shape=(
            jax.ShapeDtypeStruct(everywhere, bf16),
            jax.ShapeDtypeStruct(everywhere, bf16),
            jax.ShapeDtypeStruct((NC, nz) + w_shape, bf16),
            jax.ShapeDtypeStruct(z_shape, bf16),
        ),
        in_specs=any_specs(2) + [vmem] + any_specs(5),
        out_specs=tuple(any_specs(4)),
        scratch_shapes=[
            pltpu.VMEM(x.shape, bf16),
            pltpu.VMEM(w_shape, bf16),
            pltpu.VMEM((nz,) + w_shape[:-1] + (pair,), bf16),
            pltpu.VMEM(everywhere, bf16),
            pltpu.VMEM(everywhere, bf16),
            pltpu.VMEM(z_shape, bf16),
            pltpu.VMEM((NX, chunk, pair), bf16),
            dma((count,)),
            dma((count,)),
            dma((5 + NX,)),
            dma((2 * NY * NX,)),
        ]
        + [pltpu.VMEM(a.shape, bf16) for a in (x, dy, w_qkv, w_out, w_gate, w_up, w_down)]
        + [
            dma((7,)),
        ],
        compiler_params=pltpu.CompilerParams(collective_id=0, has_side_effects=True, vmem_limit_bytes=VMEM_LIMIT),
        name="front",
    )(x, dy, gain, w_qkv, w_out, w_gate, w_up, w_down)


SETS = (2, 1, -1, 0)


def attention(z_got, z_back, keys, vals, dk, dv, cos_ref, sin_ref):
    bf16 = jnp.bfloat16
    seq, head = keys.shape
    part = seq // 2
    count = z_got.shape[0] - 1
    scale = head**-0.5
    spread = z_back.shape[2:5] + (head,)
    halves = [pl.ds(p * part, part) for p in range(2)]

    def turn(values, at, sign):
        wide = values.astype(jnp.float32)
        swapped = pltpu.roll(wide, head // 2, 1)
        return (wide * cos_ref[at, :] + sign * (swapped * sin_ref[at, :])).astype(bf16)

    for p in range(2):
        keys[halves[p], :] = turn(z_got[count, p, :, :head], halves[p], 1.0)
        vals[halves[p], :] = z_got[count, p, :, head:]
    dk[...] = jnp.zeros_like(dk)
    dv[...] = jnp.zeros_like(dv)

    @pl.loop(0, count)
    def _(i):
        for p in range(2):
            n = (p + 1) * part
            query = turn(z_got[i, p, :, :head], halves[p], 1.0)
            d_out = z_got[i, p, :, head:]
            scores = mm(query, keys[:n, :], 1, 1) * scale
            causal = lax.broadcasted_iota(jnp.int32, scores.shape, 0) + p * part >= lax.broadcasted_iota(jnp.int32, scores.shape, 1)
            scores = jnp.where(causal, scores, -1e30)
            grown = jnp.exp(scores - jnp.max(scores, axis=1, keepdims=True))
            probs = grown / jnp.sum(grown, axis=1, keepdims=True)
            probs_low = probs.astype(bf16)
            z_back[i, p, :, :, :, head:] = mm(probs_low, vals[:n, :], 1, 0).astype(bf16).reshape(spread)
            d_probs = mm(d_out, vals[:n, :], 1, 1).astype(bf16).astype(jnp.float32)
            d_scores = (probs * (d_probs - jnp.sum(probs * d_probs, axis=1, keepdims=True)) * scale).astype(bf16)
            z_back[i, p, :, :, :, :head] = turn(mm(d_scores, keys[:n, :], 1, 0).astype(bf16), halves[p], -1.0).reshape(spread)
            dk[:n, :] += mm(d_scores, query, 0, 0)
            dv[:n, :] += mm(probs_low, d_out, 0, 0)

    for p in range(2):
        z_back[count, p, :, :, :, :head] = turn(dk[halves[p], :].astype(bf16), halves[p], -1.0).reshape(spread)
        z_back[count, p, :, :, :, head:] = dv[halves[p], :].astype(bf16).reshape(spread)


def gated(place, flow, h_all, dy_all, w_all, acts, row_sem, share, h_rows, dy_rows, w_v):
    bf16 = jnp.bfloat16
    ff = acts.shape[-1] // 3
    lo = 2 * ff
    part = h_rows.shape[1]
    shape = acts.shape[2:5] + (ff,)
    w_loads = [
        pltpu.make_async_copy(w_all.at[0, :, :lo], w_v.at[:, :lo], row_sem.at[2, 0]),
        pltpu.make_async_copy(w_all.at[0, :, w_all.shape[2] - ff :], w_v.at[:, lo:], row_sem.at[2, 1]),
    ]

    def loads(n, slot):
        return [pltpu.make_async_copy(a.at[span(n, part)], b.at[slot], row_sem.at[slot, m]) for m, (a, b) in enumerate(((h_all, h_rows), (dy_all, dy_rows)))]

    def begin():
        for copy in w_loads + loads(0, 0) + loads(1, 1):
            copy.start()

    def go():
        for copy in w_loads:
            copy.wait()
        for q in range(NY):

            @pl.loop(0, 2)
            def _(p):
                n = 2 * q + p
                for copy in loads(n, p):
                    copy.wait()
                gate = mm(h_rows[p], w_v[:, :ff], 1, 0).astype(bf16).astype(jnp.float32)
                up = mm(h_rows[p], w_v[:, ff:lo], 1, 0).astype(bf16).astype(jnp.float32)
                d_act = mm(dy_rows[p], w_v[:, lo:], 1, 0).astype(bf16).astype(jnp.float32)
                if q < NY - 1:
                    for copy in loads(n + 2, p):
                        copy.start()
                sig = jax.nn.sigmoid(gate)
                silu = gate * sig
                acts[q, p, :, :, :, :ff] = (d_act * up * (sig + silu * (1.0 - sig))).astype(bf16).reshape(shape)
                acts[q, p, :, :, :, ff:lo] = (d_act * silu).astype(bf16).reshape(shape)
                acts[q, p, :, :, :, lo:] = (silu * up).astype(bf16).reshape(shape)

            share(q)
            flow.spend(3.0)

    return begin, go


class Plane:
    def __init__(self, place, flow, tiles, land, first, finish, free):
        self.place, self.flow, self.tiles, self.land, self.first = place, flow, tiles, land, first
        self.second = "y" if first == "x" else "x"
        self.piece = nbytes(tiles, 3)
        self.sums, self.waiting, self.finished = {}, {}, [0] * len(SETS)
        self.free = free
        self.rings = []
        for s, other in enumerate(SETS):

            def raw(step, half, s=s):
                return lambda: tiles.at[s % 2, place.get(first, step), half]

            self.rings.append(self.ring(first, raw, lambda step, half, then: then(), s, self.first_done(s, other)))
        self.onward, _ = self.ring(self.second, lambda step, half: self.sums[step, half], self.need, len(SETS), finish)

    def need(self, step, half, then):
        if (step, half) in self.sums:
            then()
        else:
            self.waiting.setdefault((step, half), []).append(then)

    def first_done(self, s, step):
        def done(half, ref):
            self.sums[step, half] = ref
            for then in self.waiting.pop((step, half), []):
                then()
            self.onward(step, half)
            self.finished[s] += 1
            if self.finished[s] == 2:
                self.free(s)

        return done

    def add(self, mine, other):
        a, b = mine(), other()
        a[...] = a[...] + b[...]
        self.flow.now += ADD

    def ring(self, axis, raw, need, s, done):
        flow, add, sent = self.flow, self.add, []

        def slot(i):
            return lambda: self.land.at[s, i]

        def turn(i, goal, half, step):
            def then():
                add(slot(i), raw(goal, half))
                flow.send(axis, step, slot(i), slot(i + 4), self.piece, final[half])

            return lambda: need(goal, half, then)

        def ending(half):
            def then():
                mine, other = (slot(5), slot(2)) if half == 0 else (slot(4), slot(3))
                add(mine, other)
                add(mine, raw(0, half))
                done(half, mine)

            return lambda: need(0, half, then)

        final = [after(2, ending(0)), after(2, ending(1))]
        moves = {
            (2, 1): (1, 0, turn(0, 1, 1, 1)),
            (2, 0): (-1, 1, turn(1, -1, 0, -1)),
            (1, 0): (1, 2, final[0]),
            (-1, 1): (-1, 3, final[1]),
        }

        def start(goal, half):
            if (goal, half) in moves:
                step, i, then = moves[goal, half]
                sent.append(flow.send(axis, step, raw(goal, half), slot(i), self.piece, then))

        return start, sent

    def start(self, s):
        for goal, half in ((2, 1), (2, 0), (1, 0), (-1, 1)):
            self.rings[s][0](goal, half)

    def clear(self, s):
        for k in self.rings[s][1]:
            self.flow.wait_sent(k)


class Grads:
    flow = None


    def __init__(self, nz, place, h_all, dy_all, acts, z_out, z_land, outs, far, h_plus, h_minus, dy_minus, tiles, stage, load_sem, stage_sem, own_sem):
        self.__dict__.update({k: v for k, v in locals().items() if k != "self"})
        self.ff = acts.shape[-1] // 3
        self.pair = z_out.shape[-1]
        lo = 2 * self.ff
        self.cols = [(0, self.ff), (self.ff, lo), (lo + self.pair, lo + self.pair + self.ff), (lo, lo + self.pair)]
        self.way = (1, 1, -1, -1)
        self.far_way = (1, -1, 1, -1)
        self.block = tiles.shape[2]
        self.size = nbytes(tiles, 2)
        self.ready, self.waiting, self.used = set(), {}, 0
        self.users = [[] for _ in range(stage.shape[0])]
        self.own = []
        self.idle, self.first = {}, {}

    def load(self, ref, src, index, step, n):
        b = self.place.get("z", -step * (n + 1))
        at = pl.ds(pl.multiple_of(b * self.block, self.block), self.block)
        return pltpu.make_async_copy(src.at[:, at], ref, self.load_sem.at[index])

    def loads_plus(self, n):
        return [self.load(self.h_plus, self.h_all, 0, 1, n)]

    def loads_minus(self, n):
        return [self.load(self.h_minus, self.h_all, 1, -1, n), self.load(self.dy_minus, self.dy_all, 2, -1, n)]

    def begin(self):
        for copy in self.loads_plus(0) + self.loads_minus(0):
            copy.start()

    def gather_up(self, tiles, some):
        seq = self.h_plus.shape[0] // NY
        for tile in tiles:
            tile[...] = jnp.zeros_like(tile)

        @pl.loop(0, NY)
        def _(q):
            for tile, value in zip(tiles, some(q, span(q, seq))):
                tile[...] += value

    def set_ready(self, lane, n):
        self.ready.add((lane, n))
        for then in self.waiting.pop((lane, n), []):
            then()
        if n == 0:
            k = self.flow.send("z", self.way[lane], lambda: self.tiles.at[0, lane], lambda: self.z_land.at[0, lane], self.size, self.hop(lane, 0))
            self.first[lane] = k

    def clear(self, lane, n):
        if n == 2:
            self.flow.wait_sent(self.first[lane])

    def tokens(self, ref):
        value = ref[...]
        return value.reshape(-1, value.shape[-1])

    def make_plus(self, n):
        for copy in self.loads_plus(n):
            copy.wait()
        lo = 2 * self.ff

        def some(q, rows):
            both = mm(self.h_plus[rows, :], self.acts[q, :, :, :, :, :lo].reshape(-1, lo), 0, 0)
            return both[:, : self.ff], both[:, self.ff :]

        self.gather_up([self.tiles.at[n % 2, 0], self.tiles.at[n % 2, 1]], some)
        if n + 1 < self.nz:
            for copy in self.loads_plus(n + 1):
                copy.start()

    def for_down(self, q, rows):
        return [mm(self.dy_minus[rows, :], self.acts[q, :, :, :, :, 2 * self.ff :].reshape(-1, self.ff), 0, 0)]

    def for_heads(self, q, rows):
        last = self.place.get("y") == NY - 1
        head = self.pair // 2
        out = self.z_out[q].reshape(-1, self.pair)
        both = mm(self.h_minus[rows, :], out, 0, 0)
        right = jnp.where(last, both[:, head:], mm(self.dy_minus[rows, :], out[:, head:], 0, 0))
        return [jnp.concatenate([both[:, :head], right], axis=1)]

    def make_minus(self, n):
        for copy in self.loads_minus(n):
            copy.wait()
        self.gather_up([self.tiles.at[n % 2, 2], self.tiles.at[n % 2, 3]], lambda q, rows: self.for_down(q, rows) + self.for_heads(q, rows))
        self.load_minus_next(n)

    def load_minus_next(self, n):
        if n + 1 < self.nz:
            for copy in self.loads_minus(n + 1):
                copy.start()

    def make_first(self):
        self.make_plus(0)
        for copy in self.loads_minus(0):
            copy.wait()
        self.gather_up([self.tiles.at[0, 2]], self.for_down)

    def heads_first(self):
        def do():
            self.gather_up([self.tiles.at[0, 3]], self.for_heads)
            self.load_minus_next(0)
            self.set_ready(3, 0)

        self.flow.task(1.3, do)

    def plus(self, n):
        def do():
            for lane in (0, 1):
                self.clear(lane, n)
            self.make_plus(n)
            for lane in (0, 1):
                self.set_ready(lane, n)

        self.flow.task(1.6, do)

    def minus(self, n):
        def do():
            for lane in (2, 3):
                self.clear(lane, n)
            self.make_minus(n)
            for lane in (2, 3):
                self.set_ready(lane, n)

        self.flow.task(2.2, do)

    def need(self, lane, n, then):
        if (lane, n) in self.ready:
            then()
        else:
            self.waiting.setdefault((lane, n), []).append(then)

    def next(self, lane, n):
        if n + 2 >= self.nz:
            return
        key = (lane // 2, n)
        self.idle[key] = self.idle.get(key, 0) + 1
        if self.idle[key] == 2:
            (self.plus, self.minus)[lane // 2](n + 2)

    def hop(self, lane, s):
        flow, place = self.flow, self.place

        def come():
            slot = self.used % len(self.users)
            self.used += 1
            for wait in self.users[slot]:
                wait()
            self.users[slot] = []
            here = lambda: self.stage.at[slot]

            def staged():
                self.need(lane, s + 1, use)

            def use():
                ref = here()
                ref[...] = ref[...] + self.tiles[(s + 1) % 2, lane]
                flow.now += ADD
                if s == 0:
                    self.next(lane, 0)
                self.next(lane, s + 1)
                if s + 1 < self.nz - 1:
                    k = flow.send("z", self.way[lane], here, lambda: self.z_land.at[s + 1, lane], self.size, self.hop(lane, s + 1))
                    self.users[slot].append(lambda: flow.wait_sent(k))
                else:
                    self.home(lane, slot)

            flow.local(pltpu.make_async_copy(self.z_land.at[s, lane], here(), self.stage_sem.at[slot]), self.size, staged)

        return come

    def home(self, lane, slot):
        flow, place = self.flow, self.place
        slab = self.block // NY
        way = self.far_way[lane]
        size = self.size // NY

        def rows(step, cut=slice(None)):
            return lambda: self.stage.at[slot, pl.ds(pl.multiple_of(place.get("y", step) * slab, slab), slab), cut]

        def columns(out, step, wide):
            at = place.get("y", step) * wide
            return lambda: self.outs[out].at[:, pl.ds(pl.multiple_of(at, wide), wide)]

        def deliver(size, src, far, dst, n, other=None):
            def alt(step):
                return None if other is None else (place.get("y", step) == NY - 1, other(step))

            def onward():
                flow.send("y", way, far, dst(-way), size, alt=alt(-way))

            sent = [flow.send("y", way, src(2), far, size, onward)]
            sent += [flow.send("y", step, src(step), dst(0), size, alt=alt(0)) for step in (1, -1)]
            copies = [(None, pltpu.make_async_copy(src(0)(), dst(0)(), self.own_sem.at[n]))]
            if other is not None:
                last = place.get("y") == NY - 1
                copies = [(jnp.logical_not(last), copies[0][1]), (last, pltpu.make_async_copy(src(0)(), other(0)(), self.own_sem.at[n]))]
            for when, copy in copies:
                if when is None:
                    copy.start()
                else:
                    pl.when(when)(copy.start)
            self.users[slot] += [functools.partial(flow.wait_sent, k) for k in sent] + [copies[0][1].wait]

        if lane < 3:
            deliver(size, rows, lambda: self.far.at[lane], lambda step: columns(lane, step, self.ff), lane)
            return
        head = self.pair // 2
        first, second = slice(0, head), slice(head, self.pair)
        deliver(size // 2, lambda step: rows(step, first), lambda: self.far.at[3, :, first], lambda step: columns(3, step, head), 3)
        value = lambda: self.outs[3].at[:, NY * head :]

        def out_rows(step):
            at = lax.rem(place.get("y", step), NY - 1) * head
            return lambda: self.outs[4].at[:, pl.ds(pl.multiple_of(at, head), head)]

        deliver(size // 2, lambda step: rows(step, second), lambda: self.far.at[3, :, second], out_rows, 4, lambda step: value)

    def close(self):
        for users in self.users:
            for wait in users:
                wait()


def back_kernel(
    nz,
    z_in,
    h_all,
    dy_all,
    w_all,
    cos_in,
    sin_in,
    gain,
    x_in,
    dy_in,
    y_out,
    dx_out,
    g_qkv,
    g_out,
    g_gate,
    g_up,
    g_down,
    z_land,
    x_ref,
    dy_ref,
    cos_ref,
    sin_ref,
    z_got,
    z_back,
    z_out,
    far_back,
    acts,
    pair_acts,
    far,
    p_land,
    q_land,
    keys,
    vals,
    dk,
    dv,
    h_plus,
    h_minus,
    dy_minus,
    tiles,
    stage,
    w_v,
    y_v,
    dx_v,
    load_sem,
    row_sem,
    w_sem,
    g_load_sem,
    stage_sem,
    own_sem,
    out_sem,
    send_sem,
    recv_sem,
):
    bf16, f32 = jnp.bfloat16, jnp.float32
    place = Place(nz)
    y, c = place.get("y"), place.get("c")
    other = place.get("c", 1)
    last = y == NY - 1
    seq, head = keys.shape
    pair = 2 * head
    rows, cols = pair_acts.shape[3:]
    ff = (cols - pair) // 3
    lo, hi = 2 * ff, 2 * ff + pair
    tokens, width = h_all.shape
    block = width // nz
    part = seq // 2

    place.greet([("x", 1), ("x", -1), ("y", 1), ("y", -1), ("z", 1), ("z", -1), ("c", 1)])
    z_load = pltpu.make_async_copy(z_in, z_got, load_sem)
    z_load.start()
    row_loads = [pltpu.make_async_copy(a, b, own_sem.at[5 + n]) for n, (a, b) in enumerate(((x_in, x_ref), (dy_in, dy_ref)))]
    cos_ref[...] = jnp.concatenate([cos_in[...], cos_in[...]], axis=0).T
    sin_ref[...] = jnp.concatenate([-sin_in[...], sin_in[...]], axis=0).T
    early = Flow(place, send_sem, recv_sem)

    depth = w_v.shape[0]

    def w_copy(kind, d, slot):
        at = pl.ds(pl.multiple_of(d * block, block), block)
        cut = slice(lo, cols) if kind == 0 else slice(0, cols)
        return pltpu.make_async_copy(w_all.at[:, at, cut], w_v.at[slot, :, :, cut], w_sem.at[slot])

    counts = (nz - 1, nz)
    base, total = [], 0
    for kind, _ in PASSES:
        base.append(total)
        total += counts[kind]
    kind = PASSES[0][0]
    for n in range(depth):
        w_copy(kind, n, n).start() if n < counts[kind] else w_copy(PASSES[1][0], n - counts[kind], n).start()
    def share(q):
        early.send("c", 1, lambda: acts.at[q, :, :, other, :, :lo], lambda: pair_acts.at[q, :, :, :, :lo], nbytes(pair_acts, 1) * lo // cols)
        early.send("c", 1, lambda: acts.at[q, :, :, other, :, lo:], lambda: pair_acts.at[q, :, :, :, hi:], nbytes(pair_acts, 1) * ff // cols)

    def out_come(step, half):
        cut = slice(None) if half is None else half
        part = nbytes(z_out, 1) // NC // (1 if half is None else 2)
        src = lambda: z_out.at[place.get("y", step), cut, :, other]
        early.send("c", 1, src, lambda: pair_acts.at[place.get("y", step), cut, :, :, lo:hi], part)

    grads = Grads(nz, place, h_all, dy_all, acts, z_out, z_land, (g_gate, g_up, g_down, g_qkv, g_out), far, h_plus, h_minus, dy_minus, tiles, stage, g_load_sem, stage_sem, own_sem)

    def first(h_rows, dy_rows, w_v):
        begin, go = gated(place, early, h_all, dy_all, w_all, acts, row_sem, share, h_rows, dy_rows, w_v)
        begin()
        grads.begin()
        for copy in row_loads:
            copy.start()
        z_load.wait()
        attention(z_got, z_back, keys, vals, dk, dv, cos_ref, sin_ref)
        place.meet()
        for step in ORDER[:3]:
            exchange(early, place, z_back, z_out, far_back, step, out_come)
        z_out[y] = z_back[y]
        early.send("c", 1, lambda: z_back.at[y, :, :, other], lambda: pair_acts.at[y, :, :, :, lo:hi], nbytes(z_out, 1) // NC)
        go()
        grads.make_first()
        early.now += 2.6
        early.run()
        early.close()
        for copy in row_loads:
            copy.wait()

    pl.run_scoped(
        first,
        pltpu.VMEM((2, part, width), bf16),
        pltpu.VMEM((2, part, width), bf16),
        pltpu.VMEM((width, 3 * ff), bf16),
    )

    def second(p_tile, q_tile):
        flow = Flow(place, send_sem, recv_sem, len(early.copies), early.now)
        grads.flow = flow
        lane = lax.broadcasted_iota(jnp.int32, (rows, pair), 1)
        for_d = jnp.logical_or(lane < head, last)

        def chunk(k, i, p, xx):
            if k == 0:
                own = acts[i, p, xx, c]
                return own[:, :lo], z_out[i, p, xx, c], own[:, lo:]
            theirs = pair_acts[i, p, xx]
            return theirs[:, :lo], theirs[:, lo:hi], theirs[:, hi:]

        def for_out(k, i, p, xx):
            _, mixed, act = chunk(k, i, p, xx)
            return jnp.concatenate([jnp.where(for_d, jnp.zeros_like(mixed), mixed), act], axis=1)

        def for_in(k, i, p, xx):
            grad, mixed, _ = chunk(k, i, p, xx)
            return jnp.concatenate([grad, jnp.where(for_d, mixed, jnp.zeros_like(mixed))], axis=1)

        turn = [0]

        def blocks(s, kind, first, count, body):
            n = turn[0]
            assert PASSES[n] == (kind, s)
            if first + count == counts[kind]:
                turn[0] += 1

            @pl.loop(first, first + count)
            def _(d):
                slot = lax.rem(base[n] + d, depth)
                w_copy(kind, d, slot).wait()
                body(d, w_v.at[slot])

                @pl.when(d + depth < counts[kind])
                def _():
                    w_copy(kind, d + depth, slot).start()

                if n + 1 < len(PASSES):

                    @pl.when(d + depth >= counts[kind])
                    def _():
                        w_copy(PASSES[n + 1][0], d + depth - counts[kind], slot).start()

        def product(parts, w, a, b):
            total = None
            for k in range(NC):
                left = jnp.concatenate([one(k) for one in parts], axis=0)
                one = mm(left, w[k, :, a:b], 1, 1)
                total = one if total is None else total + one
            return total

        shape = (NX, 2, rows // 2, block)

        def p_rows(s):
            x = place.get("x", SETS[s])
            p, xx = lax.div(x, NX // 2), lax.rem(x, NX // 2)
            return [lambda k, i=i: for_out(k, i, p, xx) for i in range(NY)]

        def q_rows(s, make):
            i = place.get("y", SETS[s])
            return [lambda k, p=p, xx=xx: make(k, i, p, xx) for p in range(2) for xx in range(NX // 2)]

        def place_of(d):
            return pl.ds(pl.multiple_of(d * block, block), block)

        def p_task(s):
            def body(d, w):
                p_tile[s % 2, :, :, :, place_of(d)] = product(p_rows(s), w, lo, cols).reshape(shape)

            def do():
                if s >= 2:
                    planes[0].clear(s - 2)
                blocks(s, 0, 0, nz - 1, body)
                planes[0].start(s)

            flow.task(P_TIME, do)

        def q_task(s):
            def body(d, w):
                q_tile[s % 2, :, :, :, place_of(d)] = product(q_rows(s, for_in), w, 0, hi).reshape(shape)

                @pl.when(d == nz - 1)
                def _():
                    q_tile[s % 2, :, :, :, width:] = product(q_rows(s, for_out), w, lo, cols).reshape(shape)

            def start():
                if s >= 2:
                    planes[1].clear(s - 2)
                blocks(s, 1, 0, nz // 2, body)

            def end():
                blocks(s, 1, nz // 2, nz - nz // 2, body)
                planes[1].start(s)

            flow.task(Q_HALF, start)
            flow.task(Q_HALF, end)

        edge = width - block
        result_copies = []

        def leave(n, half):
            copy = pltpu.make_async_copy((y_v, dx_v)[n].at[half], (y_out, dx_out)[n].at[half], out_sem.at[n, half])
            copy.start()
            result_copies.append(copy)

        y_done = [after(2, functools.partial(leave, 0, half)) for half in range(2)]

        def p_finish(half, ref):
            y_v[half, :, :edge] = (x_ref[half, :, :edge].astype(f32) + ref()[...]).astype(bf16)
            y_done[half]()

        def q_finish(half, ref):
            y_v[half, :, edge:] = (x_ref[half, :, edge:].astype(f32) + ref()[:, width:]).astype(bf16)
            y_done[half]()
            wide = x_ref[half].astype(f32)
            scale = lax.rsqrt(jnp.mean(wide * wide, axis=-1, keepdims=True) + NORM_EPS)
            d_normed = ref()[:, :width].astype(bf16).astype(f32) * gain[...]
            mean = jnp.mean(d_normed * wide, axis=-1, keepdims=True)
            grad = d_normed * scale - wide * (scale * scale * scale * mean)
            dx_v[half] = (dy_ref[half].astype(f32) + grad).astype(bf16)
            leave(1, half)

        def free(task):
            return lambda s: task(s + 2) if s + 2 < len(SETS) else None

        planes = [
            Plane(place, flow, p_tile, p_land, "y", p_finish, free(p_task)),
            Plane(place, flow, q_tile, q_land, "x", q_finish, free(q_task)),
        ]

        for lane in range(3):
            grads.set_ready(lane, 0)
        q_task(0)
        p_task(0)
        grads.heads_first()
        grads.plus(1)
        grads.minus(1)
        p_task(1)
        q_task(1)
        flow.run()
        flow.close()
        grads.close()
        for copy in result_copies:
            copy.wait()

    pl.run_scoped(
        second,
        pltpu.VMEM((2, NY, 2, rows // 2, width - block), f32),
        pltpu.VMEM((2, NX, 2, rows // 2, width + block), f32),
    )


STAGES = 5
PASSES = ((1, 0), (0, 0), (0, 1), (1, 1), (1, 2), (0, 2), (0, 3), (1, 3))
P_TIME = 3.0
Q_HALF = 2.6


def back(nz, z_in, h_all, dy_all, w_all, cos, sin, x, dy, gain):
    tokens, width = h_all.shape
    seq, head = cos.shape[1], 2 * cos.shape[0]
    pair = 2 * head
    cols = w_all.shape[2]
    ff = (cols - pair) // 3
    rows = seq // (NX * NC)
    block = width // nz
    bf16, f32 = h_all.dtype, jnp.float32
    vmem = pl.BlockSpec(memory_space=pltpu.VMEM)
    dma = pltpu.SemaphoreType.DMA
    blocks = (NY, 2, NX // 2, NC, rows, pair)
    p_piece = (rows // 2, width - block)
    q_piece = (rows // 2, width + block)
    count = 6 + 2 * NY + 5 + 4 * (nz - 1) + 5 * 4 + 2 * 5 * 6
    slab = block // NY
    weight = jax.ShapeDtypeStruct((slab, NY * ff), f32)
    return pl.pallas_call(
        functools.partial(back_kernel, nz),
        out_shape=(
            jax.ShapeDtypeStruct(x.shape, bf16),
            jax.ShapeDtypeStruct(x.shape, bf16),
            jax.ShapeDtypeStruct((slab, (NY + 1) * head), f32),
            jax.ShapeDtypeStruct((slab, (NY - 1) * head), f32),
            weight,
            weight,
            weight,
            jax.ShapeDtypeStruct((nz - 1, 4, block, ff), f32),
        ),
        in_specs=any_specs(4) + [vmem] * 3 + any_specs(2),
        out_specs=tuple(any_specs(8)),
        scratch_shapes=[
            pltpu.VMEM(x.shape, bf16),
            pltpu.VMEM(x.shape, bf16),
            pltpu.VMEM((seq, head), f32),
            pltpu.VMEM((seq, head), f32),
            pltpu.VMEM(z_in.shape, bf16),
            pltpu.VMEM(blocks, bf16),
            pltpu.VMEM(blocks, bf16),
            pltpu.VMEM(blocks[1:], bf16),
            pltpu.VMEM(blocks[:-1] + (3 * ff,), bf16),
            pltpu.VMEM(blocks[:3] + (rows, cols), bf16),
            pltpu.VMEM((4, block // NY, ff), f32),
            pltpu.VMEM((5, 6) + p_piece, f32),
            pltpu.VMEM((5, 6) + q_piece, f32),
            pltpu.VMEM((seq, head), bf16),
            pltpu.VMEM((seq, head), bf16),
            pltpu.VMEM((seq, head), f32),
            pltpu.VMEM((seq, head), f32),
            pltpu.VMEM((tokens, block), bf16),
            pltpu.VMEM((tokens, block), bf16),
            pltpu.VMEM((tokens, block), bf16),
            pltpu.VMEM((2, 4, block, ff), f32),
            pltpu.VMEM((STAGES, block, ff), f32),
            pltpu.VMEM((3, NC, block, cols), bf16),
            pltpu.VMEM(x.shape, bf16),
            pltpu.VMEM(x.shape, bf16),
            dma,
            dma((3, 2)),
            dma((3,)),
            dma((3,)),
            dma((STAGES,)),
            dma((7,)),
            dma((2, 2)),
            dma((count,)),
            dma((count,)),
        ],
        compiler_params=pltpu.CompilerParams(collective_id=2, has_side_effects=True, vmem_limit_bytes=VMEM_LIMIT),
        name="back",
    )(z_in, h_all, dy_all, w_all, cos, sin, gain, x, dy)[:7]


def settle_kernel(*refs):
    n = len(refs) // 3
    ins, outs, held = refs[:n], refs[n : 2 * n], refs[2 * n : 3 * n]
    in_sem, out_sem = refs[3 * n :]
    come = [pltpu.make_async_copy(a, b, in_sem.at[i]) for i, (a, b) in enumerate(zip(ins, held))]
    go = [pltpu.make_async_copy(a, b, out_sem.at[i]) for i, (a, b) in enumerate(zip(held, outs))]
    for copy in come:
        copy.start()
    for first, second in zip(come, go):
        first.wait()
        second.start()
    for copy in go:
        copy.wait()


def settle(arrays):
    n = len(arrays)
    return pl.pallas_call(
        settle_kernel,
        out_shape=tuple(jax.ShapeDtypeStruct(a.shape, a.dtype) for a in arrays),
        in_specs=any_specs(n),
        out_specs=tuple(any_specs(n)),
        scratch_shapes=[pltpu.VMEM(a.shape, a.dtype) for a in arrays] + [pltpu.SemaphoreType.DMA((n,))] * 2,
        name="settle",
    )(*arrays)


def solution(mesh):
    act_spec = P("fsdp", "model", None)
    col_spec = P("fsdp", "model")
    row_spec = P("model", "fsdp")
    nz = mesh.shape["fsdp"] // NY

    def layer_body(x_in, dy_in, norm_gain, w_qkv, w_out, w_gate, w_up, w_down, rope_cos, rope_sin):
        _, rows, width = x_in.shape
        head = 2 * rope_cos.shape[1]
        seq = rows * NX * NC
        tokens = NY * seq
        x = x_in.reshape(2, rows // 2, width)
        dy = dy_in.reshape(2, rows // 2, width)
        gain = norm_gain.reshape(1, width)
        h_all, dy_all, w_all, z_got = front(nz, x, dy, gain, w_qkv, w_out.T, w_gate, w_up, w_down.T)
        results = back(
            nz,
            z_got.reshape(NY, 2, seq // 2, 2 * head),
            h_all.reshape(tokens, width),
            dy_all.reshape(tokens, width),
            w_all.reshape(NC, width, -1),
            rope_cos.T,
            rope_sin.T,
            x,
            dy,
            gain,
        )
        y_out, dx_out, g_qkv, g_out, g_gate, g_up, g_down = settle(results)
        return y_out.reshape(x_in.shape), dx_out.reshape(x_in.shape), g_qkv, g_out.T, g_gate, g_up, g_down.T

    return jax.shard_map(
        layer_body,
        mesh=mesh,
        in_specs=(act_spec, act_spec, P(), col_spec, row_spec, col_spec, col_spec, row_spec, P(), P()),
        out_specs=(act_spec, act_spec, col_spec, row_spec, col_spec, col_spec, row_spec),
        check_vma=False,
    )
```

```python
import functools
import heapq

import jax
import jax.numpy as jnp
from jax import lax
from jax.experimental import pallas as pl
from jax.experimental.pallas import tpu as pltpu
from jax.sharding import PartitionSpec as P

NORM_EPS = 1e-5
NY, NX, NC = 4, 4, 2
MESH = pl.DeviceIdType.MESH
LINK = 46.6e3
PAIR = 450e3
LOCAL = 1500e3
LEFT = 2.0
HOP = 3.1
ADD = 0.4
VMEM_LIMIT = 67043328


class Place:
    def __init__(self, nz):
        i, j = lax.axis_index("fsdp"), lax.axis_index("model")
        self.size = {"z": nz, "y": NY, "x": NX, "c": NC}
        self.at = {"z": lax.div(i, NY), "y": lax.rem(i, NY), "x": lax.div(j, NC), "c": lax.rem(j, NC)}

    def get(self, axis, step=0):
        n = self.size[axis]
        return lax.rem(self.at[axis] + (step + 2 * n) % n, n)

    def device(self, axis, step):
        at = dict(self.at)
        at[axis] = self.get(axis, step)
        return {"fsdp": at["z"] * NY + at["y"], "model": at["x"] * NC + at["c"]}

    def greet(self, peers):
        barrier = pltpu.get_barrier_semaphore()
        for axis, step in peers:
            pl.semaphore_signal(barrier, inc=1, device_id=self.device(axis, step), device_id_type=MESH)
        self.met = len(peers)

    def meet(self):
        pl.semaphore_wait(pltpu.get_barrier_semaphore(), self.met)


class Flow:
    def __init__(self, place, send_sem, recv_sem, base=0, now=0.0):
        self.place, self.send_sem, self.recv_sem, self.base = place, send_sem, recv_sem, base
        self.now, self.free, self.events, self.copies, self.tasks, self.order = now, {}, [], [], [], 0
        self.sent, self.leaving = set(), []

    def event(self, when, wait, then):
        heapq.heappush(self.events, (when, self.order, wait, then))
        self.order += 1

    def send(self, axis, step, src, dst, size, then=None, link=None, alt=None):
        k = len(self.copies)
        link = link or (axis, step)
        begin = max(self.now, self.free.get(link, 0.0))
        rate, lag = (PAIR, 1.5) if axis == "c" else (LINK, HOP)
        self.free[link] = begin + size / rate

        def make(dst):
            return pltpu.make_async_remote_copy(
                src_ref=src(),
                dst_ref=dst(),
                send_sem=self.send_sem.at[self.base + k],
                recv_sem=self.recv_sem.at[self.base + k],
                device_id=self.place.device(axis, step),
                device_id_type=MESH,
            )

        copy = make(dst)
        if alt is None:
            copy.start()
        else:
            when, other = alt
            pl.when(jnp.logical_not(when))(copy.start)
            pl.when(when)(make(other).start)
        self.copies.append(copy)
        heapq.heappush(self.leaving, (self.free[link] + LEFT, k))
        self.event(self.free[link] + lag, copy.wait_recv, then)
        return k

    def at(self, when, then):
        self.event(when, lambda: None, then)

    def local(self, copy, size, then):
        copy.start()
        self.event(self.now + size / LOCAL + 1.0, copy.wait, then)

    def task(self, cost, do):
        self.tasks.append((cost, do))

    def take(self):
        when, _, wait, then = heapq.heappop(self.events)
        if when > self.now:
            while self.leaving and self.leaving[0][0] <= self.now:
                self.wait_sent(heapq.heappop(self.leaving)[1])
        self.now = max(self.now, when)
        wait()
        if then is not None:
            then()

    def spend(self, cost):
        self.now += cost
        while self.events and self.events[0][0] <= self.now:
            self.take()

    def wait_sent(self, k):
        if k not in self.sent:
            self.copies[k].wait_send()
        self.sent.add(k)

    def run(self):
        while self.events or self.tasks:
            if self.tasks and (not self.events or self.events[0][0] > self.now):
                cost, do = self.tasks.pop(0)
                self.now += cost
                do()
            else:
                self.take()

    def close(self):
        for k in range(len(self.copies)):
            self.wait_sent(k)


def after(count, then):
    left = [count]

    def one():
        left[0] -= 1
        if left[0] == 0:
            then()

    return one


def nbytes(ref, lead):
    n = 1
    for d in ref.shape[lead:]:
        n *= d
    return n * jnp.dtype(ref.dtype).itemsize


def any_specs(n):
    return [pl.BlockSpec(memory_space=pl.ANY)] * n


def mm(a, b, ca, cb):
    return lax.dot_general(a, b, (((ca,), (cb,)), ((), ())), preferred_element_type=jnp.float32)


def span(q, n):
    return pl.ds(pl.multiple_of(q * n, n), n)


def exchange(flow, place, src, dst, far, half, done):
    size = nbytes(src, 2)
    way = (1, -1)[half]

    def onward():
        flow.send("y", way, lambda: far.at[half], lambda: dst.at[place.get("y", -way), half], size, lambda: done(2, half))

    flow.send("y", way, lambda: src.at[place.get("y", 2), half], lambda: far.at[half], size, onward)
    for step in (-way, way):
        flow.send("y", step, lambda step=step: src.at[place.get("y", step), half], lambda: dst.at[place.get("y"), half], size, lambda step=step: done(-step, half))


class Gather:
    def __init__(self, place, flow, own, full, first, cut, arrive):
        self.place, self.flow, self.own, self.full, self.first, self.cut, self.arrive = place, flow, own, full, first, cut, arrive
        self.second = "y" if first == "x" else "x"
        self.size = nbytes(own, 1) * (cut.stop - cut.start) // own.shape[-1]

    def mine(self, half):
        return lambda: self.own.at[half, :, self.cut]

    def spot(self, at, half):
        y, x, c = (self.place.get(axis, at.get(axis, 0)) for axis in "yxc")
        return lambda: self.full.at[y, x, c, half, :, self.cut]

    def moves(self, axis, at, half, src):
        def come(step, onward):
            def then():
                here = dict(at, **{axis: step})
                if onward:
                    far = dict(at, **{axis: 2})
                    self.flow.send(axis, -step, self.spot(here, half), self.spot(here, half), self.size, lambda: self.got(axis, far, half))
                self.got(axis, here, half)

            return then

        return {
            1: lambda: self.flow.send(axis, 1, src, self.spot(at, half), self.size, come(-1, half == 0)),
            -1: lambda: self.flow.send(axis, -1, src, self.spot(at, half), self.size, come(1, half == 1)),
        }

    def spread(self, axis, at, half, src):
        for move in self.moves(axis, at, half, src).values():
            move()

    def got(self, axis, at, half):
        if axis == self.first:
            self.spread(self.second, at, half, self.spot(at, half))
        self.pair(at, half, self.spot(at, half))
        self.arrive(at.get("y", 0), at.get("x", 0))

    def pair(self, at, half, src):
        there = lambda: self.arrive(at.get("y", 0), at.get("x", 0))
        self.flow.send("c", 1, src, self.spot(at, half), self.size, there)

    def start_first(self):
        self.spread_own(self.first)

    def start_second(self):
        self.spread_own(self.second)
        for half in (0, 1):
            self.pair({}, half, self.mine(half))

    def spread_own(self, axis):
        sends = {(half, step): move for half in (0, 1) for step, move in self.moves(axis, {}, half, self.mine(half)).items()}
        for key in ((0, 1), (1, -1), (1, 1), (0, -1)):
            sends[key]()


def front_kernel(
    nz, x_in, dy_in, gain, *refs
):
    args, refs = refs[:5], refs[5:]
    held, refs = refs[-8:-1], refs[:-8] + refs[-1:]
    front_body(nz, (x_in, dy_in) + args, held, gain, *refs)


def front_body(
    nz, ins, held, gain, h_all, dy_all, w_all, z_got, h_ref, w_ref, w_heads, h_v, dy_v, z_in, far, send_sem, recv_sem, own_sem, rows_sem, in_sem
):
    x_ref, dy_ref, w_qkv, w_out, w_gate, w_up, w_down = held
    in_copies = [pltpu.make_async_copy(a, b, in_sem.at[n]) for n, (a, b) in enumerate(zip(ins, held))]
    for copy in in_copies:
        copy.start()
    bf16 = jnp.bfloat16
    place = Place(nz)
    place.greet([("x", 1), ("x", -1), ("y", 1), ("y", -1), ("y", 2), ("z", 1), ("z", -1), ("c", 1)])
    in_copies[0].wait()
    for half in range(2):
        wide = x_ref[half].astype(jnp.float32)
        h_ref[half] = (wide * lax.rsqrt(jnp.mean(wide * wide, axis=-1, keepdims=True) + NORM_EPS) * gain[...]).astype(bf16)
    for copy in in_copies[1:]:
        copy.wait()
    wide_ff = w_gate.shape[1] // NY
    one = w_out.shape[1] // (NY - 1)
    for q in range(NY):
        ffs = slice(q * wide_ff, (q + 1) * wide_ff)
        w_ref[q, :, :wide_ff] = w_gate[:, ffs]
        w_ref[q, :, wide_ff : 2 * wide_ff] = w_up[:, ffs]
        at = 2 * wide_ff
        w_ref[q, :, at : at + one] = w_qkv[:, q * one : (q + 1) * one]
        w_ref[q, :, at + one : at + 2 * one] = w_out[:, q * one : (q + 1) * one] if q < NY - 1 else w_qkv[:, NY * one :]
        w_ref[q, :, at + 2 * one :] = w_down[:, ffs]
    y, x, c, z = (place.get(axis) for axis in "yxcz")
    last = y == NY - 1
    pair = z_in.shape[-1]
    head = pair // 2
    width = h_ref.shape[-1]
    cols = w_ref.shape[-1]
    lo = (cols - pair) * 2 // 3
    hi = lo + pair
    rows = z_in.shape[2]
    flow = Flow(place, send_sem, recv_sem)
    w_own = pltpu.make_async_copy(w_ref.at[y, :, :lo], w_all.at[0, z, y, :, :lo], own_sem.at[2])
    w_own_down = pltpu.make_async_copy(w_ref.at[y, :, hi:], w_all.at[0, z, y, :, hi:], own_sem.at[4 + NX])
    w_own.start()
    w_own_down.start()
    heads_home = pltpu.make_async_copy(w_heads, w_all.at[0, :, :, :, lo:hi], own_sem.at[3])
    w_heads[z, y] = w_ref[y, :, lo:hi]
    for full, ref in ((h_v, h_ref), (dy_v, dy_ref)):
        full[y, x, c] = ref[...]
    place.meet()

    queue = []
    pieces = {}
    parts_done = {}
    weights = [4 * nz]
    writes = []

    def load():
        while queue and weights[0] == 0:
            key = queue.pop(0)
            flow.task(CHUNK_TIME, lambda key=key: product(*key))

    def complete(key):
        kind, dy, dx = key
        src, dst = ((h_v, h_all), (dy_v, dy_all))[kind]
        at = place.get("y", dy), place.get("x", dx)
        copy = pltpu.make_async_copy(src.at[at], dst.at[at], rows_sem.at[len(writes)])
        copy.start()
        writes.append(copy)
        queue.append(key)
        load()

    def arrive(kind):
        need = (8, 4)[kind]

        def one(dy, dx):
            key = (kind, dy, dx)
            pieces[key] = pieces.get(key, 0) + 1
            if pieces[key] == need:
                complete(key)

        return one

    def weight_come():
        weights[0] -= 1
        if weights[0] == 0:
            heads_home.start()
            load()

    def product(kind, dy, dx):
        rows_v = (h_v, dy_v)[kind]
        at = place.get("y", dy), place.get("x", dx)
        step = 2 if nz % 2 == 0 else 1
        deep = step * (width // nz)

        def dot(first):
            def some(i, total):
                left = rows_v[at[0], at[1], :, :, :, span(i, deep)].reshape(rows, deep)
                right = w_heads[pl.ds(i * step, step), :, :, first:].reshape(deep, pair - first)
                return total + mm(left, right, 1, 0)

            return lax.fori_loop(0, nz // step, some, jnp.zeros((rows, pair - first), jnp.float32))

        if kind == 0:
            made = dot(0).astype(bf16)
            z_in[at[0], at[1], :, :head] = made[:, :head]

            @pl.when(last)
            def _():
                z_in[at[0], at[1], :, head:] = made[:, head:]

        else:

            @pl.when(jnp.logical_not(last))
            def _():
                z_in[at[0], at[1], :, head:] = dot(head).astype(bf16)

        parts_done[dy, dx] = parts_done.get((dy, dx), 0) + 1
        if parts_done[dy, dx] == 2:
            deliver(dy, dx)

    own_copies = []

    def deliver(dy, dx):
        at = lambda: z_in.at[place.get("y", dy), place.get("x", dx)]
        size = nbytes(z_in, 2)

        def there(step=0):
            return lambda: z_got.at[place.get("y", step), place.get("x", dx)]

        if dy == 0:
            copy = pltpu.make_async_copy(at(), there()(), own_sem.at[4 + dx % NX])
            copy.start()
            own_copies.append(copy)
        elif dy == 2 and dx in DIRECT:
            flow.send("y", 2, at, there(), size, link=("y", 1))
        elif dy == 2:
            way = 1 if dx in (0, 2) else -1

            def onward():
                flow.send("y", way, lambda: far.at[dx % NX], there(-way), size)

            flow.send("y", way, at, lambda: far.at[dx % NX], size, onward)
        else:
            flow.send("y", dy, at, there(), size)

    def w_part(ref, who, dz, dy, cut):
        if ref is None:
            return lambda: w_heads.at[place.get("z", dz), place.get("y", dy)]
        return lambda: w_all.at[who, place.get("z", dz), place.get("y", dy), :, cut]

    cuts = [slice(lo, hi), slice(0, lo), slice(hi, cols)]

    def ring(step, dy, n_cut, src=None, hops=nz - 1, lead=True):
        cut = cuts[n_cut]
        home = None if n_cut == 0 else w_all
        size = nbytes(w_ref, 1) * (cut.stop - cut.start) // cols

        def hop(n):
            def then():
                here = src if src and n == 0 else w_part(home, 0, -step * n, dy, cut)
                if n < hops:
                    flow.send("z", step, here, w_part(home, 0, -step * n, dy, cut), size, hop(n + 1))
                if n or lead:
                    flow.send("c", 1, here, w_part(w_all, 1, -step * n, dy, cut), size)
                    if n_cut == 0:
                        weight_come()

            return then

        return hop(0)

    def rings(dy, n_cut, src=None):
        if n_cut:
            return ring(1 if dy in (0, 1) else -1, dy, n_cut, src)
        both = [ring(1, dy, 0, src, nz // 2), ring(-1, dy, 0, src, (nz - 1) // 2, False)]
        return lambda: [one() for one in both]

    def w_at(dy, cut):
        return lambda: w_ref.at[place.get("y", dy), :, cut]

    tail = width // nz * H_TAIL
    gathers = [
        Gather(place, flow, h_ref, h_v, "x", slice(0, width - tail), arrive(0)),
        Gather(place, flow, dy_ref, dy_v, "y", slice(0, width), arrive(1)),
        Gather(place, flow, h_ref, h_v, "y", slice(width - tail, width), arrive(0)),
    ]
    def w_start(n_cut, dys):
        cut = cuts[n_cut]
        home = None if n_cut == 0 else w_all
        size = nbytes(w_ref, 1) * (cut.stop - cut.start) // cols
        there = w_part(home, 0, 0, 0, cut)
        for dy in dys:
            if dy == 0:
                rings(0, n_cut, w_at(0, cut))()
            elif dy == 2:
                flow.send("y", 2, w_at(2, cut), there, size, rings(2, n_cut), link=("y", 1))
            else:
                flow.send("y", -dy, w_at(-dy, cut), there, size, rings(dy, n_cut))

    w_start(0, (0, 1, -1, 2))
    for one in gathers:
        one.start_first()
    flow.at(W_TIMES[0], lambda: [w_start(1, (0, -1)), w_start(2, (0, -1))])
    flow.at(W_TIMES[1], lambda: [w_start(1, (1, 2)), w_start(2, (1, 2))])
    for one in gathers:
        one.start_second()
    for n in range(2):
        for _ in range((4, 2)[n]):
            arrive(n)(0, 0)
    flow.run()
    w_own.wait()
    w_own_down.wait()
    flow.close()
    for copy in own_copies + writes:
        copy.wait()
    heads_home.wait()


CHUNK_TIME = 1.0
W_TIMES = (0.0, 0.0)
DIRECT = (2,)
H_TAIL = 1


def front(nz, x, dy, gain, w_qkv, w_out, w_gate, w_up, w_down):
    half, rows, width = x.shape
    everywhere = (NY, NX, NC) + x.shape
    slab = w_qkv.shape[0]
    pair = 2 * w_out.shape[1] // (NY - 1)
    cols = pair + 3 * w_gate.shape[1] // NY
    w_shape = (NY, slab, cols)
    bf16 = x.dtype
    gathers = 3 * (30 + 32)
    count = gathers + 3 * 3 + 3 * 4 * (nz - 1) + 3 * 4 * nz + 2 * NX + 2 * NX
    vmem = pl.BlockSpec(memory_space=pltpu.VMEM)
    dma = pltpu.SemaphoreType.DMA
    chunk = NC * half * rows
    z_shape = (NY, NX, chunk, pair)
    return pl.pallas_call(
        functools.partial(front_kernel, nz),
        out_shape=(
            jax.ShapeDtypeStruct(everywhere, bf16),
            jax.ShapeDtypeStruct(everywhere, bf16),
            jax.ShapeDtypeStruct((NC, nz) + w_shape, bf16),
            jax.ShapeDtypeStruct(z_shape, bf16),
        ),
        in_specs=any_specs(2) + [vmem] + any_specs(5),
        out_specs=tuple(any_specs(4)),
        scratch_shapes=[
            pltpu.VMEM(x.shape, bf16),
            pltpu.VMEM(w_shape, bf16),
            pltpu.VMEM((nz,) + w_shape[:-1] + (pair,), bf16),
            pltpu.VMEM(everywhere, bf16),
            pltpu.VMEM(everywhere, bf16),
            pltpu.VMEM(z_shape, bf16),
            pltpu.VMEM((NX, chunk, pair), bf16),
            dma((count,)),
            dma((count,)),
            dma((5 + NX,)),
            dma((2 * NY * NX,)),
        ]
        + [pltpu.VMEM(a.shape, bf16) for a in (x, dy, w_qkv, w_out, w_gate, w_up, w_down)]
        + [
            dma((7,)),
        ],
        compiler_params=pltpu.CompilerParams(collective_id=0, has_side_effects=True, vmem_limit_bytes=VMEM_LIMIT),
        name="front",
    )(x, dy, gain, w_qkv, w_out, w_gate, w_up, w_down)


SETS = (2, 1, -1, 0)


def attention(z_got, z_back, keys, vals, dk, dv, cos_ref, sin_ref, leave):
    bf16 = jnp.bfloat16
    seq, head = keys.shape
    part = seq // 2
    count = z_got.shape[0] - 1
    scale = head**-0.5
    spread = z_back.shape[2:5] + (head,)
    halves = [pl.ds(p * part, part) for p in range(2)]

    def turn(values, at, sign):
        wide = values.astype(jnp.float32)
        swapped = pltpu.roll(wide, head // 2, 1)
        return (wide * cos_ref[at, :] + sign * (swapped * sin_ref[at, :])).astype(bf16)

    for p in range(2):
        keys[halves[p], :] = turn(z_got[count, p, :, :head], halves[p], 1.0)
        vals[halves[p], :] = z_got[count, p, :, head:]
    dk[...] = jnp.zeros_like(dk)
    dv[...] = jnp.zeros_like(dv)

    for p in (1, 0):
        n = (p + 1) * part

        @pl.loop(0, count)
        def _(i):
            query = turn(z_got[i, p, :, :head], halves[p], 1.0)
            d_out = z_got[i, p, :, head:]
            scores = mm(query, keys[:n, :], 1, 1) * scale
            causal = lax.broadcasted_iota(jnp.int32, scores.shape, 0) + p * part >= lax.broadcasted_iota(jnp.int32, scores.shape, 1)
            scores = jnp.where(causal, scores, -1e30)
            grown = jnp.exp(scores - jnp.max(scores, axis=1, keepdims=True))
            probs = grown / jnp.sum(grown, axis=1, keepdims=True)
            probs_low = probs.astype(bf16)
            z_back[i, p, :, :, :, head:] = mm(probs_low, vals[:n, :], 1, 0).astype(bf16).reshape(spread)
            d_probs = mm(d_out, vals[:n, :], 1, 1).astype(bf16).astype(jnp.float32)
            d_scores = (probs * (d_probs - jnp.sum(probs * d_probs, axis=1, keepdims=True)) * scale).astype(bf16)
            z_back[i, p, :, :, :, :head] = turn(mm(d_scores, keys[:n, :], 1, 0).astype(bf16), halves[p], -1.0).reshape(spread)
            dk[:n, :] += mm(d_scores, query, 0, 0)
            dv[:n, :] += mm(probs_low, d_out, 0, 0)

        z_back[count, p, :, :, :, :head] = turn(dk[halves[p], :].astype(bf16), halves[p], -1.0).reshape(spread)
        z_back[count, p, :, :, :, head:] = dv[halves[p], :].astype(bf16).reshape(spread)
        leave(p)


def gated(place, flow, h_all, dy_all, w_all, acts, row_sem, share, h_rows, dy_rows, w_v):
    bf16 = jnp.bfloat16
    ff = acts.shape[-1] // 3
    lo = 2 * ff
    part = h_rows.shape[1]
    shape = acts.shape[2:5] + (ff,)
    w_loads = [
        pltpu.make_async_copy(w_all.at[0, :, :lo], w_v.at[:, :lo], row_sem.at[2, 0]),
        pltpu.make_async_copy(w_all.at[0, :, w_all.shape[2] - ff :], w_v.at[:, lo:], row_sem.at[2, 1]),
    ]

    def loads(n, slot):
        return [pltpu.make_async_copy(a.at[span(n, part)], b.at[slot], row_sem.at[slot, m]) for m, (a, b) in enumerate(((h_all, h_rows), (dy_all, dy_rows)))]

    def begin():
        for copy in w_loads + loads(0, 0) + loads(1, 1):
            copy.start()

    def go():
        for copy in w_loads:
            copy.wait()
        for q in range(NY):

            @pl.loop(0, 2)
            def _(p):
                n = 2 * q + p
                for copy in loads(n, p):
                    copy.wait()
                gate = mm(h_rows[p], w_v[:, :ff], 1, 0).astype(bf16).astype(jnp.float32)
                up = mm(h_rows[p], w_v[:, ff:lo], 1, 0).astype(bf16).astype(jnp.float32)
                d_act = mm(dy_rows[p], w_v[:, lo:], 1, 0).astype(bf16).astype(jnp.float32)
                if q < NY - 1:
                    for copy in loads(n + 2, p):
                        copy.start()
                sig = jax.nn.sigmoid(gate)
                silu = gate * sig
                acts[q, p, :, :, :, :ff] = (d_act * up * (sig + silu * (1.0 - sig))).astype(bf16).reshape(shape)
                acts[q, p, :, :, :, ff:lo] = (d_act * silu).astype(bf16).reshape(shape)
                acts[q, p, :, :, :, lo:] = (silu * up).astype(bf16).reshape(shape)

            share(q)
            flow.spend(3.0)

    return begin, go


class Plane:
    def __init__(self, place, flow, tiles, land, first, finish, free):
        self.place, self.flow, self.tiles, self.land, self.first = place, flow, tiles, land, first
        self.second = "y" if first == "x" else "x"
        self.piece = nbytes(tiles, 3)
        self.sums, self.waiting, self.finished = {}, {}, [0] * len(SETS)
        self.free = free
        self.rings = []
        for s, other in enumerate(SETS):

            def raw(step, half, s=s):
                return lambda: tiles.at[s % 2, place.get(first, step), half]

            self.rings.append(self.ring(first, raw, lambda step, half, then: then(), s, self.first_done(s, other)))
        self.onward, _ = self.ring(self.second, lambda step, half: self.sums[step, half], self.need, len(SETS), finish)

    def need(self, step, half, then):
        if (step, half) in self.sums:
            then()
        else:
            self.waiting.setdefault((step, half), []).append(then)

    def first_done(self, s, step):
        def done(half, ref):
            self.sums[step, half] = ref
            for then in self.waiting.pop((step, half), []):
                then()
            self.onward(step, half)
            self.finished[s] += 1
            if self.finished[s] == 2:
                self.free(s)

        return done

    def add(self, mine, other):
        a, b = mine(), other()
        a[...] = a[...] + b[...]
        self.flow.now += ADD

    def ring(self, axis, raw, need, s, done):
        flow, add, sent = self.flow, self.add, []

        def slot(i):
            return lambda: self.land.at[s, i]

        def turn(i, goal, half, step):
            def then():
                add(slot(i), raw(goal, half))
                flow.send(axis, step, slot(i), slot(i + 4), self.piece, final[half])

            return lambda: need(goal, half, then)

        def ending(half):
            def then():
                mine, other = (slot(5), slot(2)) if half == 0 else (slot(4), slot(3))
                add(mine, other)
                add(mine, raw(0, half))
                done(half, mine)

            return lambda: need(0, half, then)

        final = [after(2, ending(0)), after(2, ending(1))]
        moves = {
            (2, 1): (1, 0, turn(0, 1, 1, 1)),
            (2, 0): (-1, 1, turn(1, -1, 0, -1)),
            (1, 0): (1, 2, final[0]),
            (-1, 1): (-1, 3, final[1]),
        }

        def start(goal, half):
            if (goal, half) in moves:
                step, i, then = moves[goal, half]
                sent.append(flow.send(axis, step, raw(goal, half), slot(i), self.piece, then))

        return start, sent

    def start(self, s):
        for goal, half in ((2, 1), (2, 0), (1, 0), (-1, 1)):
            self.rings[s][0](goal, half)

    def clear(self, s):
        for k in self.rings[s][1]:
            self.flow.wait_sent(k)


class Grads:
    flow = None


    def __init__(self, nz, place, h_all, dy_all, acts, z_out, z_land, outs, far, h_plus, h_minus, dy_minus, tiles, stage, load_sem, stage_sem, own_sem):
        self.__dict__.update({k: v for k, v in locals().items() if k != "self"})
        self.ff = acts.shape[-1] // 3
        self.pair = z_out.shape[-1]
        lo = 2 * self.ff
        self.cols = [(0, self.ff), (self.ff, lo), (lo + self.pair, lo + self.pair + self.ff), (lo, lo + self.pair)]
        self.way = (1, 1, -1, -1)
        self.far_way = (1, -1, 1, -1)
        self.block = tiles.shape[2]
        self.size = nbytes(tiles, 2)
        self.ready, self.waiting, self.used = set(), {}, 0
        self.users = [[] for _ in range(stage.shape[0])]
        self.own = []
        self.idle, self.first = {}, {}

    def load(self, ref, src, index, step, n):
        b = self.place.get("z", -step * (n + 1))
        at = pl.ds(pl.multiple_of(b * self.block, self.block), self.block)
        return pltpu.make_async_copy(src.at[:, at], ref, self.load_sem.at[index])

    def loads_plus(self, n):
        return [self.load(self.h_plus, self.h_all, 0, 1, n)]

    def loads_minus(self, n):
        return [self.load(self.h_minus, self.h_all, 1, -1, n), self.load(self.dy_minus, self.dy_all, 2, -1, n)]

    def begin(self):
        for copy in self.loads_plus(0) + self.loads_minus(0):
            copy.start()

    def gather_up(self, tiles, some):
        seq = self.h_plus.shape[0] // NY
        for tile in tiles:
            tile[...] = jnp.zeros_like(tile)

        @pl.loop(0, NY)
        def _(q):
            for tile, value in zip(tiles, some(q, span(q, seq))):
                tile[...] += value

    def set_ready(self, lane, n):
        self.ready.add((lane, n))
        for then in self.waiting.pop((lane, n), []):
            then()
        if n == 0:
            k = self.flow.send("z", self.way[lane], lambda: self.tiles.at[0, lane], lambda: self.z_land.at[0, lane], self.size, self.hop(lane, 0))
            self.first[lane] = k

    def clear(self, lane, n):
        if n == 2:
            self.flow.wait_sent(self.first[lane])

    def tokens(self, ref):
        value = ref[...]
        return value.reshape(-1, value.shape[-1])

    def make_plus(self, n):
        for copy in self.loads_plus(n):
            copy.wait()
        lo = 2 * self.ff

        def some(q, rows):
            both = mm(self.h_plus[rows, :], self.acts[q, :, :, :, :, :lo].reshape(-1, lo), 0, 0)
            return both[:, : self.ff], both[:, self.ff :]

        self.gather_up([self.tiles.at[n % 2, 0], self.tiles.at[n % 2, 1]], some)
        if n + 1 < self.nz:
            for copy in self.loads_plus(n + 1):
                copy.start()

    def for_down(self, q, rows):
        return [mm(self.dy_minus[rows, :], self.acts[q, :, :, :, :, 2 * self.ff :].reshape(-1, self.ff), 0, 0)]

    def for_heads(self, q, rows):
        last = self.place.get("y") == NY - 1
        head = self.pair // 2
        out = self.z_out[q].reshape(-1, self.pair)
        both = mm(self.h_minus[rows, :], out, 0, 0)
        right = jnp.where(last, both[:, head:], mm(self.dy_minus[rows, :], out[:, head:], 0, 0))
        return [jnp.concatenate([both[:, :head], right], axis=1)]

    def make_minus(self, n):
        for copy in self.loads_minus(n):
            copy.wait()
        self.gather_up([self.tiles.at[n % 2, 2], self.tiles.at[n % 2, 3]], lambda q, rows: self.for_down(q, rows) + self.for_heads(q, rows))
        self.load_minus_next(n)

    def load_minus_next(self, n):
        if n + 1 < self.nz:
            for copy in self.loads_minus(n + 1):
                copy.start()

    def make_first(self):
        self.make_plus(0)
        for copy in self.loads_minus(0):
            copy.wait()
        self.gather_up([self.tiles.at[0, 2]], self.for_down)

    def heads_first(self):
        def do():
            self.gather_up([self.tiles.at[0, 3]], self.for_heads)
            self.load_minus_next(0)
            self.set_ready(3, 0)

        self.flow.task(1.3, do)

    def plus(self, n):
        def do():
            for lane in (0, 1):
                self.clear(lane, n)
            self.make_plus(n)
            for lane in (0, 1):
                self.set_ready(lane, n)

        self.flow.task(1.6, do)

    def minus(self, n):
        def do():
            for lane in (2, 3):
                self.clear(lane, n)
            self.make_minus(n)
            for lane in (2, 3):
                self.set_ready(lane, n)

        self.flow.task(2.2, do)

    def need(self, lane, n, then):
        if (lane, n) in self.ready:
            then()
        else:
            self.waiting.setdefault((lane, n), []).append(then)

    def next(self, lane, n):
        if n + 2 >= self.nz:
            return
        key = (lane // 2, n)
        self.idle[key] = self.idle.get(key, 0) + 1
        if self.idle[key] == 2:
            (self.plus, self.minus)[lane // 2](n + 2)

    def hop(self, lane, s):
        flow, place = self.flow, self.place

        def come():
            slot = self.used % len(self.users)
            self.used += 1
            for wait in self.users[slot]:
                wait()
            self.users[slot] = []
            here = lambda: self.stage.at[slot]

            def staged():
                self.need(lane, s + 1, use)

            def use():
                ref = here()
                ref[...] = ref[...] + self.tiles[(s + 1) % 2, lane]
                flow.now += ADD
                if s == 0:
                    self.next(lane, 0)
                self.next(lane, s + 1)
                if s + 1 < self.nz - 1:
                    k = flow.send("z", self.way[lane], here, lambda: self.z_land.at[s + 1, lane], self.size, self.hop(lane, s + 1))
                    self.users[slot].append(lambda: flow.wait_sent(k))
                else:
                    self.home(lane, slot)

            flow.local(pltpu.make_async_copy(self.z_land.at[s, lane], here(), self.stage_sem.at[slot]), self.size, staged)

        return come

    def home(self, lane, slot):
        flow, place = self.flow, self.place
        slab = self.block // NY
        way = self.far_way[lane]
        size = self.size // NY

        def rows(step, cut=slice(None)):
            return lambda: self.stage.at[slot, pl.ds(pl.multiple_of(place.get("y", step) * slab, slab), slab), cut]

        def columns(out, step, wide):
            at = place.get("y", step) * wide
            return lambda: self.outs[out].at[:, pl.ds(pl.multiple_of(at, wide), wide)]

        def deliver(size, src, far, dst, n, other=None):
            def alt(step):
                return None if other is None else (place.get("y", step) == NY - 1, other(step))

            def onward():
                flow.send("y", way, far, dst(-way), size, alt=alt(-way))

            sent = [flow.send("y", way, src(2), far, size, onward)]
            sent += [flow.send("y", step, src(step), dst(0), size, alt=alt(0)) for step in (1, -1)]
            copies = [(None, pltpu.make_async_copy(src(0)(), dst(0)(), self.own_sem.at[n]))]
            if other is not None:
                last = place.get("y") == NY - 1
                copies = [(jnp.logical_not(last), copies[0][1]), (last, pltpu.make_async_copy(src(0)(), other(0)(), self.own_sem.at[n]))]
            for when, copy in copies:
                if when is None:
                    copy.start()
                else:
                    pl.when(when)(copy.start)
            self.users[slot] += [functools.partial(flow.wait_sent, k) for k in sent] + [copies[0][1].wait]

        if lane < 3:
            deliver(size, rows, lambda: self.far.at[lane], lambda step: columns(lane, step, self.ff), lane)
            return
        head = self.pair // 2
        first, second = slice(0, head), slice(head, self.pair)
        deliver(size // 2, lambda step: rows(step, first), lambda: self.far.at[3, :, first], lambda step: columns(3, step, head), 3)
        value = lambda: self.outs[3].at[:, NY * head :]

        def out_rows(step):
            at = lax.rem(place.get("y", step), NY - 1) * head
            return lambda: self.outs[4].at[:, pl.ds(pl.multiple_of(at, head), head)]

        deliver(size // 2, lambda step: rows(step, second), lambda: self.far.at[3, :, second], out_rows, 4, lambda step: value)

    def close(self):
        for users in self.users:
            for wait in users:
                wait()


def back_kernel(
    nz,
    z_in,
    h_all,
    dy_all,
    w_all,
    cos_in,
    sin_in,
    gain,
    x_in,
    dy_in,
    y_out,
    dx_out,
    g_qkv,
    g_out,
    g_gate,
    g_up,
    g_down,
    z_land,
    x_ref,
    dy_ref,
    cos_ref,
    sin_ref,
    z_got,
    z_back,
    z_out,
    far_back,
    acts,
    pair_acts,
    far,
    p_land,
    q_land,
    keys,
    vals,
    dk,
    dv,
    h_plus,
    h_minus,
    dy_minus,
    tiles,
    stage,
    w_v,
    y_v,
    load_sem,
    row_sem,
    w_sem,
    g_load_sem,
    stage_sem,
    own_sem,
    out_sem,
    send_sem,
    recv_sem,
):
    bf16, f32 = jnp.bfloat16, jnp.float32
    place = Place(nz)
    y, c = place.get("y"), place.get("c")
    other = place.get("c", 1)
    last = y == NY - 1
    seq, head = keys.shape
    pair = 2 * head
    rows, cols = pair_acts.shape[3:]
    ff = (cols - pair) // 3
    lo, hi = 2 * ff, 2 * ff + pair
    tokens, width = h_all.shape
    block = width // nz
    part = seq // 2

    place.greet([("x", 1), ("x", -1), ("y", 1), ("y", -1), ("z", 1), ("z", -1), ("c", 1)])
    z_load = pltpu.make_async_copy(z_in, z_got, load_sem)
    z_load.start()
    row_loads = [pltpu.make_async_copy(a, b, own_sem.at[5 + n]) for n, (a, b) in enumerate(((x_in, x_ref), (dy_in, dy_ref)))]
    cos_ref[...] = jnp.concatenate([cos_in[...], cos_in[...]], axis=0).T
    sin_ref[...] = jnp.concatenate([-sin_in[...], sin_in[...]], axis=0).T
    early = Flow(place, send_sem, recv_sem)

    depth = w_v.shape[0]

    def w_copy(kind, d, slot):
        at = pl.ds(pl.multiple_of(d * block, block), block)
        cut = slice(lo, cols) if kind == 0 else slice(0, cols)
        return pltpu.make_async_copy(w_all.at[:, at, cut], w_v.at[slot, :, :, cut], w_sem.at[slot])

    counts = (nz - 1, nz)
    base, total = [], 0
    for kind, _ in PASSES:
        base.append(total)
        total += counts[kind]
    kind = PASSES[0][0]
    for n in range(depth):
        w_copy(kind, n, n).start() if n < counts[kind] else w_copy(PASSES[1][0], n - counts[kind], n).start()
    def share(q):
        early.send("c", 1, lambda: acts.at[q, :, :, other, :, :lo], lambda: pair_acts.at[q, :, :, :, :lo], nbytes(pair_acts, 1) * lo // cols)
        early.send("c", 1, lambda: acts.at[q, :, :, other, :, lo:], lambda: pair_acts.at[q, :, :, :, hi:], nbytes(pair_acts, 1) * ff // cols)

    def out_come(step, half):
        src = lambda: z_out.at[place.get("y", step), half, :, other]
        early.send("c", 1, src, lambda: pair_acts.at[place.get("y", step), half, :, :, lo:hi], nbytes(z_out, 2) // NC)

    grads = Grads(nz, place, h_all, dy_all, acts, z_out, z_land, (g_gate, g_up, g_down, g_qkv, g_out), far, h_plus, h_minus, dy_minus, tiles, stage, g_load_sem, stage_sem, own_sem)

    def first(h_rows, dy_rows, w_v):
        begin, go = gated(place, early, h_all, dy_all, w_all, acts, row_sem, share, h_rows, dy_rows, w_v)
        begin()
        grads.begin()
        for copy in row_loads:
            copy.start()
        z_load.wait()

        def leave(p):
            if p:
                place.meet()
            else:
                early.spend(1.5)
            exchange(early, place, z_back, z_out, far_back, p, out_come)

        attention(z_got, z_back, keys, vals, dk, dv, cos_ref, sin_ref, leave)
        z_out[y] = z_back[y]
        early.send("c", 1, lambda: z_back.at[y, :, :, other], lambda: pair_acts.at[y, :, :, :, lo:hi], nbytes(z_out, 1) // NC)
        go()
        grads.make_first()
        early.now += 2.6
        early.run()
        early.close()
        for copy in row_loads:
            copy.wait()

    pl.run_scoped(
        first,
        pltpu.VMEM((2, part, width), bf16),
        pltpu.VMEM((2, part, width), bf16),
        pltpu.VMEM((width, 3 * ff), bf16),
    )

    def second(p_tile, q_tile):
        flow = Flow(place, send_sem, recv_sem, len(early.copies), early.now)
        grads.flow = flow
        lane = lax.broadcasted_iota(jnp.int32, (rows, pair), 1)
        for_d = jnp.logical_or(lane < head, last)

        def chunk(k, i, p, xx):
            if k == 0:
                own = acts[i, p, xx, c]
                return own[:, :lo], z_out[i, p, xx, c], own[:, lo:]
            theirs = pair_acts[i, p, xx]
            return theirs[:, :lo], theirs[:, lo:hi], theirs[:, hi:]

        def for_out(k, i, p, xx):
            _, mixed, act = chunk(k, i, p, xx)
            return jnp.concatenate([jnp.where(for_d, jnp.zeros_like(mixed), mixed), act], axis=1)

        def for_in(k, i, p, xx):
            grad, mixed, _ = chunk(k, i, p, xx)
            return jnp.concatenate([grad, jnp.where(for_d, mixed, jnp.zeros_like(mixed))], axis=1)

        turn = [0]

        def blocks(s, kind, first, count, body):
            n = turn[0]
            assert PASSES[n] == (kind, s)
            if first + count == counts[kind]:
                turn[0] += 1

            @pl.loop(first, first + count)
            def _(d):
                slot = lax.rem(base[n] + d, depth)
                w_copy(kind, d, slot).wait()
                body(d, w_v.at[slot])

                @pl.when(d + depth < counts[kind])
                def _():
                    w_copy(kind, d + depth, slot).start()

                if n + 1 < len(PASSES):

                    @pl.when(d + depth >= counts[kind])
                    def _():
                        w_copy(PASSES[n + 1][0], d + depth - counts[kind], slot).start()

        def product(parts, w, a, b):
            total = None
            for k in range(NC):
                left = jnp.concatenate([one(k) for one in parts], axis=0)
                one = mm(left, w[k, :, a:b], 1, 1)
                total = one if total is None else total + one
            return total

        shape = (NX, 2, rows // 2, block)

        def p_rows(s):
            x = place.get("x", SETS[s])
            p, xx = lax.div(x, NX // 2), lax.rem(x, NX // 2)
            return [lambda k, i=i: for_out(k, i, p, xx) for i in range(NY)]

        def q_rows(s, make):
            i = place.get("y", SETS[s])
            return [lambda k, p=p, xx=xx: make(k, i, p, xx) for p in range(2) for xx in range(NX // 2)]

        def place_of(d):
            return pl.ds(pl.multiple_of(d * block, block), block)

        def p_task(s):
            def body(d, w):
                p_tile[s % 2, :, :, :, place_of(d)] = product(p_rows(s), w, lo, cols).reshape(shape)

            def do():
                if s >= 2:
                    planes[0].clear(s - 2)
                blocks(s, 0, 0, nz - 1, body)
                planes[0].start(s)

            flow.task(P_TIME, do)

        def q_task(s):
            def body(d, w):
                q_tile[s % 2, :, :, :, place_of(d)] = product(q_rows(s, for_in), w, 0, hi).reshape(shape)

                @pl.when(d == nz - 1)
                def _():
                    q_tile[s % 2, :, :, :, width:] = product(q_rows(s, for_out), w, lo, cols).reshape(shape)

            def start():
                if s >= 2:
                    planes[1].clear(s - 2)
                blocks(s, 1, 0, nz // 2, body)

            def end():
                blocks(s, 1, nz // 2, nz - nz // 2, body)
                planes[1].start(s)

            flow.task(Q_HALF, start)
            flow.task(Q_HALF, end)

        edge = width - block
        result_copies = []

        def leave(n, half):
            copy = pltpu.make_async_copy((y_v, dy_ref)[n].at[half], (y_out, dx_out)[n].at[half], out_sem.at[n, half])
            copy.start()
            result_copies.append(copy)

        y_done = [after(2, functools.partial(leave, 0, half)) for half in range(2)]

        def p_finish(half, ref):
            y_v[half, :, :edge] = (x_ref[half, :, :edge].astype(f32) + ref()[...]).astype(bf16)
            y_done[half]()

        def q_finish(half, ref):
            y_v[half, :, edge:] = (x_ref[half, :, edge:].astype(f32) + ref()[:, width:]).astype(bf16)
            y_done[half]()
            wide = x_ref[half].astype(f32)
            scale = lax.rsqrt(jnp.mean(wide * wide, axis=-1, keepdims=True) + NORM_EPS)
            d_normed = ref()[:, :width].astype(bf16).astype(f32) * gain[...]
            mean = jnp.mean(d_normed * wide, axis=-1, keepdims=True)
            grad = d_normed * scale - wide * (scale * scale * scale * mean)
            dy_ref[half] = (dy_ref[half].astype(f32) + grad).astype(bf16)
            leave(1, half)

        def free(task):
            return lambda s: task(s + 2) if s + 2 < len(SETS) else None

        planes = [
            Plane(place, flow, p_tile, p_land, "y", p_finish, free(p_task)),
            Plane(place, flow, q_tile, q_land, "x", q_finish, free(q_task)),
        ]

        for lane in range(3):
            grads.set_ready(lane, 0)
        q_task(0)
        p_task(0)
        grads.heads_first()
        grads.plus(1)
        grads.minus(1)
        p_task(1)
        q_task(1)
        flow.run()
        flow.close()
        grads.close()
        for copy in result_copies:
            copy.wait()

    pl.run_scoped(
        second,
        pltpu.VMEM((2, NY, 2, rows // 2, width - block), f32),
        pltpu.VMEM((2, NX, 2, rows // 2, width + block), f32),
    )


STAGES = 6
PASSES = ((1, 0), (0, 0), (0, 1), (1, 1), (1, 2), (0, 2), (0, 3), (1, 3))
P_TIME = 3.0
Q_HALF = 2.6


def back(nz, z_in, h_all, dy_all, w_all, cos, sin, x, dy, gain):
    tokens, width = h_all.shape
    seq, head = cos.shape[1], 2 * cos.shape[0]
    pair = 2 * head
    cols = w_all.shape[2]
    ff = (cols - pair) // 3
    rows = seq // (NX * NC)
    block = width // nz
    bf16, f32 = h_all.dtype, jnp.float32
    vmem = pl.BlockSpec(memory_space=pltpu.VMEM)
    dma = pltpu.SemaphoreType.DMA
    blocks = (NY, 2, NX // 2, NC, rows, pair)
    p_piece = (rows // 2, width - block)
    q_piece = (rows // 2, width + block)
    count = 8 + 2 * NY + 7 + 4 * (nz - 1) + 5 * 4 + 2 * 5 * 6
    slab = block // NY
    weight = jax.ShapeDtypeStruct((slab, NY * ff), f32)
    return pl.pallas_call(
        functools.partial(back_kernel, nz),
        out_shape=(
            jax.ShapeDtypeStruct(x.shape, bf16),
            jax.ShapeDtypeStruct(x.shape, bf16),
            jax.ShapeDtypeStruct((slab, (NY + 1) * head), f32),
            jax.ShapeDtypeStruct((slab, (NY - 1) * head), f32),
            weight,
            weight,
            weight,
            jax.ShapeDtypeStruct((nz - 1, 4, block, ff), f32),
        ),
        in_specs=any_specs(4) + [vmem] * 3 + any_specs(2),
        out_specs=tuple(any_specs(8)),
        scratch_shapes=[
            pltpu.VMEM(x.shape, bf16),
            pltpu.VMEM(x.shape, bf16),
            pltpu.VMEM((seq, head), f32),
            pltpu.VMEM((seq, head), f32),
            pltpu.VMEM(z_in.shape, bf16),
            pltpu.VMEM(blocks, bf16),
            pltpu.VMEM(blocks, bf16),
            pltpu.VMEM(blocks[1:], bf16),
            pltpu.VMEM(blocks[:-1] + (3 * ff,), bf16),
            pltpu.VMEM(blocks[:3] + (rows, cols), bf16),
            pltpu.VMEM((4, block // NY, ff), f32),
            pltpu.VMEM((5, 6) + p_piece, f32),
            pltpu.VMEM((5, 6) + q_piece, f32),
            pltpu.VMEM((seq, head), bf16),
            pltpu.VMEM((seq, head), bf16),
            pltpu.VMEM((seq, head), f32),
            pltpu.VMEM((seq, head), f32),
            pltpu.VMEM((tokens, block), bf16),
            pltpu.VMEM((tokens, block), bf16),
            pltpu.VMEM((tokens, block), bf16),
            pltpu.VMEM((2, 4, block, ff), f32),
            pltpu.VMEM((STAGES, block, ff), f32),
            pltpu.VMEM((3, NC, block, cols), bf16),
            pltpu.VMEM(x.shape, bf16),
            dma,
            dma((3, 2)),
            dma((3,)),
            dma((3,)),
            dma((STAGES,)),
            dma((7,)),
            dma((2, 2)),
            dma((count,)),
            dma((count,)),
        ],
        compiler_params=pltpu.CompilerParams(collective_id=2, has_side_effects=True, vmem_limit_bytes=VMEM_LIMIT),
        name="back",
    )(z_in, h_all, dy_all, w_all, cos, sin, gain, x, dy)[:7]


def settle_kernel(*refs):
    n = len(refs) // 3
    ins, outs, held = refs[:n], refs[n : 2 * n], refs[2 * n : 3 * n]
    in_sem, out_sem = refs[3 * n :]
    come = [pltpu.make_async_copy(a, b, in_sem.at[i]) for i, (a, b) in enumerate(zip(ins, held))]
    go = [pltpu.make_async_copy(a, b, out_sem.at[i]) for i, (a, b) in enumerate(zip(held, outs))]
    for copy in come:
        copy.start()
    for first, second in zip(come, go):
        first.wait()
        second.start()
    for copy in go:
        copy.wait()


def settle(arrays):
    n = len(arrays)
    return pl.pallas_call(
        settle_kernel,
        out_shape=tuple(jax.ShapeDtypeStruct(a.shape, a.dtype) for a in arrays),
        in_specs=any_specs(n),
        out_specs=tuple(any_specs(n)),
        scratch_shapes=[pltpu.VMEM(a.shape, a.dtype) for a in arrays] + [pltpu.SemaphoreType.DMA((n,))] * 2,
        name="settle",
    )(*arrays)


def solution(mesh):
    act_spec = P("fsdp", "model", None)
    col_spec = P("fsdp", "model")
    row_spec = P("model", "fsdp")
    nz = mesh.shape["fsdp"] // NY

    def layer_body(x_in, dy_in, norm_gain, w_qkv, w_out, w_gate, w_up, w_down, rope_cos, rope_sin):
        _, rows, width = x_in.shape
        head = 2 * rope_cos.shape[1]
        seq = rows * NX * NC
        tokens = NY * seq
        x = x_in.reshape(2, rows // 2, width)
        dy = dy_in.reshape(2, rows // 2, width)
        gain = norm_gain.reshape(1, width)
        h_all, dy_all, w_all, z_got = front(nz, x, dy, gain, w_qkv, w_out.T, w_gate, w_up, w_down.T)
        results = back(
            nz,
            z_got.reshape(NY, 2, seq // 2, 2 * head),
            h_all.reshape(tokens, width),
            dy_all.reshape(tokens, width),
            w_all.reshape(NC, width, -1),
            rope_cos.T,
            rope_sin.T,
            x,
            dy,
            gain,
        )
        y_out, dx_out, g_qkv, g_out, g_gate, g_up, g_down = settle(results)
        return y_out.reshape(x_in.shape), dx_out.reshape(x_in.shape), g_qkv, g_out.T, g_gate, g_up, g_down.T

    return jax.shard_map(
        layer_body,
        mesh=mesh,
        in_specs=(act_spec, act_spec, P(), col_spec, row_spec, col_spec, col_spec, row_spec, P(), P()),
        out_specs=(act_spec, act_spec, col_spec, row_spec, col_spec, col_spec, row_spec),
        check_vma=False,
    )
```
